32 devices in a mesh: seq: 8 (over y, x, core), fsdp: 4 (over z).
Axes of the slice: x: 2, y: 2, z: 4, core: 2. Of those that a mesh axis runs over, the one named last changes fastest.
Arguments:
- inputs: bfloat16 [4, 1024, 2048], P('fsdp', 'seq'), may hold values from -6 to 6
- cotangent: bfloat16 [4, 1024, 2048], P('fsdp', 'seq'), may hold values from -6 to 6
- attention_gain: float32 [2048], replicated, may hold values from 0.5 to 1.5
- query_weight: bfloat16 [2048, 2048], P('fsdp'), may hold values from -0.125 to 0.125
- key_weight: bfloat16 [2048, 512], P('fsdp'), may hold values from -0.125 to 0.125
- value_weight: bfloat16 [2048, 512], P('fsdp'), may hold values from -0.125 to 0.125
- output_weight: bfloat16 [2048, 2048], P('fsdp'), may hold values from -1 to 1
- query_gain: float32 [64], replicated, may hold values from 0.5 to 1.5
- key_gain: float32 [64], replicated, may hold values from 0.5 to 1.5
- feedforward_gain: float32 [2048], replicated, may hold values from 0.5 to 1.5
- gate_weight: bfloat16 [2048, 8192], P(None, 'fsdp'), may hold values from -0.125 to 0.125
- up_weight: bfloat16 [2048, 8192], P(None, 'fsdp'), may hold values from -0.125 to 0.125
- down_weight: bfloat16 [2048, 8192], P(None, 'fsdp'), may hold values from -0.0625 to 0.0625
Outputs:
- block_out: bfloat16 [4, 1024, 2048], P('fsdp', 'seq')
- input_grad: bfloat16 [4, 1024, 2048], P('fsdp', 'seq')
- attention_slope: float32 [2048], replicated
- grad_query: float32 [2048, 2048], P('fsdp')
- grad_key: float32 [2048, 512], P('fsdp')
- grad_value: float32 [2048, 512], P('fsdp')
- grad_output: float32 [2048, 2048], P('fsdp')
- query_slope: float32 [64], replicated
- key_slope: float32 [64], replicated
- feedforward_slope: float32 [2048], replicated
- grad_gate: float32 [2048, 8192], P(None, 'fsdp')
- grad_up: float32 [2048, 8192], P(None, 'fsdp')
- grad_down: float32 [2048, 8192], P(None, 'fsdp')
The draws below stay inside these ranges and needn't reach their ends.
All inputs are finite; a program needn't handle non-finite values.
Results may differ from the reference program's by a relative error of at most 0.022.
Values may be sent and summed in bfloat16 or wider, within the bound.
A program may use at most 320 MiB of HBM per device.

```python
import jax
import jax.numpy as jnp
from jax import lax

D = 2048
KVH = 8
HD = 64
FF = 8192
LENGTH = 1024
SEQS = 4


def steps_of(own_key, extent, cuts, smallest, top_value):
    loudness, own = 1.0, jax.random.fold_in(own_key, 6)
    for position, shards_of in cuts:
        draws = jnp.exp(jax.random.uniform(jax.random.fold_in(own, position), (shards_of,), jnp.float32, smallest / len(cuts), top_value / len(cuts)))
        loudness = loudness * jnp.repeat(draws, extent[position] // shards_of).reshape([-1 if axis == position else 1 for axis in range(len(extent))])
    return loudness


def scatter_about(key, extent, scale, reach, cuts=(), held_as=jnp.bfloat16):
    entries = scale * jax.random.normal(key, extent, jnp.float32)
    if cuts:
        entries = entries * steps_of(key, extent, cuts, -0.22, 0.18)
    return jnp.clip(entries, -reach, reach).astype(held_as)


def setup_inputs(seed: int = 0) -> dict:
    splits = jax.random.split(jax.random.key(seed), 14)
    inputs = scatter_about(splits[0], (SEQS, LENGTH, D), 1.0, 6.0, ((0, 4), (1, 8)))
    cotangent = scatter_about(splits[1], (SEQS, LENGTH, D), 1.0, 6.0, ((0, 4), (1, 8)))
    attention_gain = jnp.clip(1.0 + 0.1 * jax.random.normal(splits[2], (D,), jnp.float32), 0.5, 1.5)
    query_weight = scatter_about(splits[3], (D, D), D ** -0.5, 0.125, ((0, 4),))
    key_weight = scatter_about(splits[4], (D, KVH * HD), D ** -0.5, 0.125, ((0, 4),))
    value_weight = scatter_about(splits[5], (D, KVH * HD), D ** -0.5, 0.125, ((0, 4),))
    output_weight = scatter_about(splits[6], (D, D), (max(1, 16 * D // LENGTH)) ** -0.5, 1.0, ((0, 4),))
    query_gain = jnp.clip(1.0 + 0.1 * jax.random.normal(splits[7], (HD,), jnp.float32), 0.5, 1.5)
    key_gain = jnp.clip(1.0 + 0.1 * jax.random.normal(splits[8], (HD,), jnp.float32), 0.5, 1.5)
    feedforward_gain = jnp.clip(1.0 + 0.1 * jax.random.normal(splits[9], (D,), jnp.float32), 0.5, 1.5)
    gate_weight = scatter_about(splits[10], (D, FF), D ** -0.5, 0.125, ((1, 4),))
    up_weight = scatter_about(splits[11], (D, FF), D ** -0.5, 0.125, ((1, 4),))
    down_weight = scatter_about(splits[12], (D, FF), FF ** -0.5, 0.0625, ((1, 4),))
    return dict(inputs=inputs, cotangent=cotangent, attention_gain=attention_gain, query_weight=query_weight, key_weight=key_weight, value_weight=value_weight, output_weight=output_weight, query_gain=query_gain, key_gain=key_gain, feedforward_gain=feedforward_gain, gate_weight=gate_weight, up_weight=up_weight, down_weight=down_weight)


EPS = 1e-05
THETA = 1000000.0

def rotate_half(values):
    half = values.shape[-1] // 2
    return jnp.concatenate([-values[..., half:], values[..., :half]], axis=-1)

def rope_tables(positions, width):
    exponents = jnp.arange(width // 2).astype(jnp.float32) * 2.0 / width
    rates = jnp.power(jnp.float32(THETA), -exponents)
    angle = positions.astype(jnp.float32)[:, None] * rates[None, :]
    angle = jnp.concatenate([angle, angle], axis=-1)
    return (jnp.cos(angle), jnp.sin(angle))

def prepare(proj, gain, cosine, sine):
    rows = proj.shape[0]
    width = gain.shape[0]
    split = proj.reshape(rows, -1, width)
    factor = lax.rsqrt(lax.optimization_barrier(jnp.mean(split * split, axis=-1, keepdims=True)) + EPS)
    normed = split * factor * gain
    turned = normed * cosine[:, None, :] + rotate_half(normed) * sine[:, None, :]
    return turned.reshape(rows, -1)

def matmul(left, right):
    return jnp.dot(left, right, preferred_element_type=jnp.float32)

def rms_factor(values):
    return lax.rsqrt(lax.optimization_barrier(jnp.mean(values * values, axis=-1, keepdims=True)) + EPS)

def norm_back(grad, values, factor, gain):
    scaled = grad * gain
    return factor * (scaled - values * factor * factor * lax.optimization_barrier(jnp.mean(scaled * values, axis=-1, keepdims=True)))

def head_split(matrix, count, width):
    return matrix.reshape(matrix.shape[0], count, width).transpose(1, 0, 2)

def attention(queries, keys, values, width):
    length = queries.shape[0]
    heads = queries.shape[1] // width
    key_heads = keys.shape[1] // width
    groups = heads // key_heads
    query_split = head_split(queries, heads, width)
    key_split = jnp.repeat(head_split(keys, key_heads, width), groups, axis=0)
    value_split = jnp.repeat(head_split(values, key_heads, width), groups, axis=0)
    positions = jnp.arange(length)
    allowed = positions[:, None] >= positions[None, :]
    scale = width ** (-0.5)

    def one_head(pieces):
        query_head, key_head, value_head = pieces
        scores = matmul(query_head, key_head.T) * scale
        weights = jnp.where(allowed, jnp.exp(scores), 0.0)
        total = lax.optimization_barrier(jnp.sum(weights, axis=-1))
        summed = matmul(weights.astype(jnp.bfloat16), value_head)
        return ((summed / total[:, None]).astype(jnp.bfloat16), jnp.log(total))
    outs, log_total = lax.map(one_head, (query_split, key_split, value_split))
    return (outs.transpose(1, 0, 2).reshape(length, heads * width), log_total)

def attention_back(queries, keys, values, outs, log_total, grads, width):
    length = queries.shape[0]
    heads = queries.shape[1] // width
    key_heads = keys.shape[1] // width
    groups = heads // key_heads
    query_split = head_split(queries, heads, width)
    key_split = jnp.repeat(head_split(keys, key_heads, width), groups, axis=0)
    value_split = jnp.repeat(head_split(values, key_heads, width), groups, axis=0)
    out_split = head_split(outs, heads, width)
    grad_split = head_split(grads, heads, width)
    positions = jnp.arange(length)
    allowed = positions[:, None] >= positions[None, :]
    scale = width ** (-0.5)

    def one_head(pieces):
        query_head, key_head, value_head, out_head, log_head, grad_head = pieces
        scores = matmul(query_head, key_head.T) * scale
        weights = jnp.where(allowed, jnp.exp(scores - log_head[:, None]), 0.0)
        value_part = matmul(weights.astype(jnp.bfloat16).T, grad_head)
        prob_grad = matmul(grad_head, value_head.T)
        correction = lax.optimization_barrier(jnp.sum(grad_head.astype(jnp.float32) * out_head.astype(jnp.float32), axis=-1))
        score_grad = (weights * (prob_grad - correction[:, None]) * scale).astype(jnp.bfloat16)
        return (matmul(score_grad, key_head), matmul(score_grad.T, query_head), value_part)
    query_back, key_back, value_back = lax.map(one_head, (query_split, key_split, value_split, out_split, log_total, grad_split))
    key_back = key_back.reshape(key_heads, groups, length, width).sum(axis=1)
    value_back = value_back.reshape(key_heads, groups, length, width).sum(axis=1)
    query_back = query_back.transpose(1, 0, 2).reshape(length, heads * width)
    key_back = key_back.transpose(1, 0, 2).reshape(length, key_heads * width)
    value_back = value_back.transpose(1, 0, 2).reshape(length, key_heads * width)
    return (query_back, key_back, value_back)

def one_sequence(inputs, cotangent, attention_gain, query_weight, key_weight, value_weight, output_weight, query_gain, key_gain, feedforward_gain, gate_weight, up_weight, down_weight):
    width = query_gain.shape[0]
    length = inputs.shape[0]
    cosine, sine = rope_tables(jnp.arange(length), width)
    source = inputs.astype(jnp.float32)
    first = rms_factor(source)
    normed_in = (source * first * attention_gain).astype(jnp.bfloat16)
    query_proj = matmul(normed_in, query_weight)
    key_proj = matmul(normed_in, key_weight)
    values = matmul(normed_in, value_weight).astype(jnp.bfloat16)
    queries = prepare(query_proj, query_gain, cosine, sine).astype(jnp.bfloat16)
    keys = prepare(key_proj, key_gain, cosine, sine).astype(jnp.bfloat16)
    attended, log_total = attention(queries, keys, values, width)
    middle = source + matmul(attended, output_weight)
    second = rms_factor(middle)
    normed_mid = (middle * second * feedforward_gain).astype(jnp.bfloat16)
    gate = matmul(normed_mid, gate_weight)
    lifted = matmul(normed_mid, up_weight)
    sigma = jax.nn.sigmoid(gate)
    hidden = (gate * sigma * lifted).astype(jnp.bfloat16)
    block_out = (middle + matmul(hidden, down_weight.T)).astype(jnp.bfloat16)
    hidden_grad = matmul(cotangent, down_weight)
    gate_grad = (hidden_grad * lifted * sigma * (1.0 + gate * (1.0 - sigma))).astype(jnp.bfloat16)
    lifted_grad = (hidden_grad * gate * sigma).astype(jnp.bfloat16)
    grad_gate = matmul(normed_mid.T, gate_grad)
    grad_up = matmul(normed_mid.T, lifted_grad)
    grad_down = matmul(cotangent.T, hidden)
    mid_grad = matmul(gate_grad, gate_weight.T) + matmul(lifted_grad, up_weight.T)
    feedforward_slope = lax.optimization_barrier(jnp.sum(mid_grad * middle * second, axis=0))
    middle_grad = cotangent.astype(jnp.float32) + norm_back(mid_grad, middle, second, feedforward_gain)
    middle_half = middle_grad.astype(jnp.bfloat16)
    grad_output = matmul(attended.T, middle_half)
    attended_grad = matmul(middle_half, output_weight.T).astype(jnp.bfloat16)
    query_back, key_back, value_back = attention_back(queries, keys, values, attended, log_total, attended_grad, width)
    _, query_pull = jax.vjp(lambda proj_in, gain_in: prepare(proj_in, gain_in, cosine, sine), query_proj, query_gain)
    query_proj_grad, query_slope = query_pull(query_back)
    _, key_pull = jax.vjp(lambda proj_in, gain_in: prepare(proj_in, gain_in, cosine, sine), key_proj, key_gain)
    key_proj_grad, key_slope = key_pull(key_back)
    query_half = query_proj_grad.astype(jnp.bfloat16)
    key_half = key_proj_grad.astype(jnp.bfloat16)
    value_half = value_back.astype(jnp.bfloat16)
    grad_query = matmul(normed_in.T, query_half)
    grad_key = matmul(normed_in.T, key_half)
    grad_value = matmul(normed_in.T, value_half)
    in_grad = matmul(query_half, query_weight.T) + matmul(key_half, key_weight.T) + matmul(value_half, value_weight.T)
    attention_slope = lax.optimization_barrier(jnp.sum(in_grad * source * first, axis=0))
    input_grad = (middle_grad + norm_back(in_grad, source, first, attention_gain)).astype(jnp.bfloat16)
    grads = (attention_slope, grad_query, grad_key, grad_value, grad_output, query_slope, key_slope, feedforward_slope, grad_gate, grad_up, grad_down)
    return (block_out, input_grad, grads)

def reference(inputs, cotangent, attention_gain, query_weight, key_weight, value_weight, output_weight, query_gain, key_gain, feedforward_gain, gate_weight, up_weight, down_weight):
    shapes = (attention_gain, query_weight, key_weight, value_weight, output_weight, query_gain, key_gain, feedforward_gain, gate_weight, up_weight, down_weight)
    initial = tuple((jnp.zeros(item.shape, jnp.float32) for item in shapes))

    def sequence_step(carry, pair):
        block_out, input_grad, grads = one_sequence(pair[0], pair[1], attention_gain, query_weight, key_weight, value_weight, output_weight, query_gain, key_gain, feedforward_gain, gate_weight, up_weight, down_weight)
        return (jax.tree.map(jnp.add, carry, grads), (block_out, input_grad))
    totals, (outs, backs) = lax.scan(sequence_step, initial, (inputs, cotangent))
    return (outs, backs, totals[0], totals[1], totals[2], totals[3], totals[4], totals[5], totals[6], totals[7], totals[8], totals[9], totals[10])
```

```python
import jax
import jax.numpy as jnp
from jax import lax
from jax.sharding import PartitionSpec as P

EPS = 1e-05
THETA = 1000000.0


def rotate_half(values):
    half = values.shape[-1] // 2
    return jnp.concatenate([-values[..., half:], values[..., :half]], axis=-1)


def rope_tables(positions, width):
    exponents = jnp.arange(width // 2).astype(jnp.float32) * 2.0 / width
    rates = jnp.power(jnp.float32(THETA), -exponents)
    angle = positions.astype(jnp.float32)[:, None] * rates[None, :]
    angle = jnp.concatenate([angle, angle], axis=-1)
    return (jnp.cos(angle), jnp.sin(angle))


def prepare(proj, gain, cosine, sine):
    rows = proj.shape[0]
    width = gain.shape[0]
    split = proj.reshape(rows, -1, width)
    factor = lax.rsqrt(jnp.mean(split * split, axis=-1, keepdims=True) + EPS)
    normed = split * factor * gain
    turned = normed * cosine[:, None, :] + rotate_half(normed) * sine[:, None, :]
    return turned.reshape(rows, -1)


def matmul(left, right):
    return jnp.dot(left, right, preferred_element_type=jnp.float32)


def inner_rows(left, right):
    return lax.dot_general(
        left, right, (((0,), (0,)), ((), ())), preferred_element_type=jnp.float32
    )


def inner_cols(left, right):
    return lax.dot_general(
        left, right, (((1,), (1,)), ((), ())), preferred_element_type=jnp.float32
    )


def rms_factor(values):
    return lax.rsqrt(jnp.mean(values * values, axis=-1, keepdims=True) + EPS)


def norm_back(grad, values, factor, gain):
    scaled = grad * gain
    return factor * (
        scaled - values * factor * factor * jnp.mean(scaled * values, axis=-1, keepdims=True)
    )


def gate_back(hidden_grad, gate, lifted):
    sigma = jax.nn.sigmoid(gate)
    gate_grad = (hidden_grad * lifted * sigma * (1.0 + gate * (1.0 - sigma))).astype(jnp.bfloat16)
    lifted_grad = (hidden_grad * gate * sigma).astype(jnp.bfloat16)
    return (gate_grad, lifted_grad)


def activate(gate, lifted):
    return (gate * jax.nn.sigmoid(gate) * lifted).astype(jnp.bfloat16)


def split_heads(query_rows, pair_rows, groups, width):
    length = query_rows.shape[0]
    key_heads = pair_rows.shape[1] // (2 * width)
    queries = query_rows.reshape(length, key_heads, groups, width)
    keys = pair_rows[:, : key_heads * width].reshape(length, key_heads, width)
    values = pair_rows[:, key_heads * width :].reshape(length, key_heads, width)
    return (queries, keys, values, key_heads)


def attend_heads(query_rows, pair_rows, groups, width):
    length = query_rows.shape[0]
    queries, keys, values, key_heads = split_heads(query_rows, pair_rows, groups, width)
    block = min(512, length)
    scale = width ** (-0.5)
    offsets = jnp.arange(block)

    def query_step(index, state):
        out_rows, log_rows = state
        query_block = lax.dynamic_slice_in_dim(queries, index * block, block, 0)

        def key_step(inner, carry):
            summed, total = carry
            key_block = lax.dynamic_slice_in_dim(keys, inner * block, block, 0)
            value_block = lax.dynamic_slice_in_dim(values, inner * block, block, 0)
            scores = (
                jnp.einsum(
                    "qhgd,shd->hgqs", query_block, key_block, preferred_element_type=jnp.float32
                )
                * scale
            )
            allowed = (index * block + offsets)[:, None] >= (inner * block + offsets)[None, :]
            weights = jnp.where(allowed, jnp.exp(scores), 0.0)
            summed = summed + jnp.einsum(
                "hgqs,shd->hgqd",
                weights.astype(jnp.bfloat16),
                value_block,
                preferred_element_type=jnp.float32,
            )
            return (summed, total + jnp.sum(weights, axis=-1))

        initial = (
            jnp.zeros((key_heads, groups, block, width), jnp.float32),
            jnp.zeros((key_heads, groups, block), jnp.float32),
        )
        summed, total = lax.fori_loop(0, index + 1, key_step, initial)
        result = (summed / total[..., None]).astype(jnp.bfloat16)
        result = result.transpose(2, 0, 1, 3).reshape(block, key_heads * groups * width)
        out_rows = lax.dynamic_update_slice_in_dim(out_rows, result, index * block, 0)
        log_rows = lax.dynamic_update_slice_in_dim(log_rows, jnp.log(total), index * block, 2)
        return (out_rows, log_rows)

    start = (
        jnp.zeros((length, key_heads * groups * width), jnp.bfloat16),
        jnp.zeros((key_heads, groups, length), jnp.float32),
    )
    return lax.fori_loop(0, length // block, query_step, start)


def attend_back(query_rows, pair_rows, out_rows, log_rows, grad_rows, groups, width):
    length = query_rows.shape[0]
    queries, keys, values, key_heads = split_heads(query_rows, pair_rows, groups, width)
    outs = out_rows.reshape(length, key_heads, groups, width)
    grads = grad_rows.reshape(length, key_heads, groups, width)
    correction = jnp.sum(grads.astype(jnp.float32) * outs.astype(jnp.float32), axis=-1)
    block = min(512, length)
    scale = width ** (-0.5)
    offsets = jnp.arange(block)

    def query_step(index, state):
        query_grad, key_grad, value_grad = state
        query_block = lax.dynamic_slice_in_dim(queries, index * block, block, 0)
        grad_block = lax.dynamic_slice_in_dim(grads, index * block, block, 0)
        shift_block = lax.dynamic_slice_in_dim(correction, index * block, block, 0).transpose(
            1, 2, 0
        )
        log_block = lax.dynamic_slice_in_dim(log_rows, index * block, block, 2)

        def key_step(inner, carry):
            block_grad, key_sum, value_sum = carry
            key_block = lax.dynamic_slice_in_dim(keys, inner * block, block, 0)
            value_block = lax.dynamic_slice_in_dim(values, inner * block, block, 0)
            scores = (
                jnp.einsum(
                    "qhgd,shd->hgqs", query_block, key_block, preferred_element_type=jnp.float32
                )
                * scale
            )
            allowed = (index * block + offsets)[:, None] >= (inner * block + offsets)[None, :]
            weights = jnp.where(allowed, jnp.exp(scores - log_block[..., None]), 0.0)
            value_part = jnp.einsum(
                "hgqs,qhgd->shd",
                weights.astype(jnp.bfloat16),
                grad_block,
                preferred_element_type=jnp.float32,
            )
            prob_grad = jnp.einsum(
                "qhgd,shd->hgqs", grad_block, value_block, preferred_element_type=jnp.float32
            )
            score_grad = (weights * (prob_grad - shift_block[..., None]) * scale).astype(
                jnp.bfloat16
            )
            block_grad = block_grad + jnp.einsum(
                "hgqs,shd->qhgd", score_grad, key_block, preferred_element_type=jnp.float32
            )
            key_part = jnp.einsum(
                "hgqs,qhgd->shd", score_grad, query_block, preferred_element_type=jnp.float32
            )
            key_sum = lax.dynamic_update_slice_in_dim(
                key_sum,
                lax.dynamic_slice_in_dim(key_sum, inner * block, block, 0) + key_part,
                inner * block,
                0,
            )
            value_sum = lax.dynamic_update_slice_in_dim(
                value_sum,
                lax.dynamic_slice_in_dim(value_sum, inner * block, block, 0) + value_part,
                inner * block,
                0,
            )
            return (block_grad, key_sum, value_sum)

        initial = (jnp.zeros((block, key_heads, groups, width), jnp.float32), key_grad, value_grad)
        block_grad, key_grad, value_grad = lax.fori_loop(0, index + 1, key_step, initial)
        query_grad = lax.dynamic_update_slice_in_dim(query_grad, block_grad, index * block, 0)
        return (query_grad, key_grad, value_grad)

    state = (
        jnp.zeros((length, key_heads, groups, width), jnp.float32),
        jnp.zeros((length, key_heads, width), jnp.float32),
        jnp.zeros((length, key_heads, width), jnp.float32),
    )
    query_grad, key_grad, value_grad = lax.fori_loop(0, length // block, query_step, state)
    pair_grad = jnp.concatenate(
        [
            key_grad.reshape(length, key_heads * width),
            value_grad.reshape(length, key_heads * width),
        ],
        axis=1,
    )
    return (query_grad.reshape(length, key_heads * groups * width), pair_grad)


def per_device(
    inputs,
    cotangent,
    attention_gain,
    query_weight,
    key_weight,
    value_weight,
    output_weight,
    query_gain,
    key_gain,
    feedforward_gain,
    gate_weight,
    up_weight,
    down_weight,
):
    tokens = inputs.shape[1]
    model = inputs.shape[2]
    width = query_gain.shape[0]
    pair_heads = key_weight.shape[1] // width
    parts = lax.axis_size("seq")
    planes = lax.axis_size("fsdp")
    copies = max(1, parts // pair_heads)
    place = lax.axis_index("seq")
    plane = lax.axis_index("fsdp")
    core = place % 2
    chip_bits = [1 << i for i in range(1, parts.bit_length() - 1)]
    query_cols = model // parts
    local_groups = query_cols // width
    shard = query_weight.shape[0]
    f32, bf16 = jnp.float32, jnp.bfloat16

    def swap(value, bit):
        return lax.ppermute(value, "seq", [(i, i ^ bit) for i in range(parts)])

    def side(bit):
        return (place // bit) % 2

    def line_gather(value):
        ups, downs = [value], [value]
        for step in range(1, planes):
            ups.append(
                lax.ppermute(ups[-1], "fsdp", [(i, i + 1) for i in range(step - 1, planes - 1)])
            )
            downs.append(
                lax.ppermute(downs[-1], "fsdp", [(i, i - 1) for i in range(1, planes - step + 1)])
            )
        return [value] + [
            jnp.where(plane >= k, ups[k], downs[planes - k]) for k in range(1, planes)
        ]

    def line_scatter(slots):
        up = down = None
        for step in range(1, planes):
            send_up, send_down = slots[step], slots[planes - step]
            if step > 1:
                send_up = (send_up.astype(f32) + up.astype(f32)).astype(bf16)
                send_down = (send_down.astype(f32) + down.astype(f32)).astype(bf16)
            up = lax.ppermute(send_up, "fsdp", [(i, i + 1) for i in range(step)])
            down = lax.ppermute(
                send_down, "fsdp", [(i, i - 1) for i in range(planes - 1, planes - 1 - step, -1)]
            )
        return slots[0].astype(f32) + up.astype(f32) + down.astype(f32)

    def plane_gather(value):
        half = value.shape[0] // 2
        pieces = {}
        for color, bits in enumerate((chip_bits, chip_bits[::-1])):
            held = {0: value[color * half : (color + 1) * half]}
            for bit in bits:
                for offset, piece in list(held.items()):
                    held[offset ^ bit] = swap(piece, bit)
            for offset, piece in held.items():
                pieces[(offset, color)] = piece
                pieces[(offset ^ 1, color)] = swap(piece, 1)
        return pieces

    def by_place(pieces):
        (half, columns) = pieces[(0, 0)].shape
        out = jnp.zeros((parts, 2 * half, columns), pieces[(0, 0)].dtype)
        for (offset, color), piece in pieces.items():
            out = lax.dynamic_update_slice(out, piece[None], (place ^ offset, color * half, 0))
        return out

    def by_plane(slots):
        out = jnp.zeros((planes,) + slots[0].shape, slots[0].dtype)
        for k, slot in enumerate(slots):
            out = lax.dynamic_update_slice(
                out, slot[None], ((plane - k) % planes,) + (0,) * slot.ndim
            )
        return out

    def half_rows(value, bit):
        rows = value.shape[0] // 2
        keep = lax.dynamic_slice_in_dim(value, side(bit) * rows, rows, 0)
        give = lax.dynamic_slice_in_dim(value, (1 - side(bit)) * rows, rows, 0)
        return keep, give

    def plane_scatter(value):
        blocks = value.reshape(parts // 2, 2, tokens, value.shape[1])
        give = lax.dynamic_index_in_dim(blocks, 1 - core, 1, keepdims=False)
        keep = lax.dynamic_index_in_dim(blocks, core, 1, keepdims=False)
        keep = (keep.astype(f32) + swap(give, 1).astype(f32)).astype(bf16)
        keep = keep.reshape(parts // 2 * tokens, value.shape[1])
        half = value.shape[1] // 2
        sums = []
        for color, bits in enumerate((chip_bits[::-1], chip_bits)):
            current = keep[:, color * half : (color + 1) * half]
            if color == 1:
                chips = parts // 2
                order = current.reshape((2,) * (chips.bit_length() - 1) + (tokens, half))
                axes = list(range(chips.bit_length() - 1))[::-1]
                order = order.transpose(axes + [len(axes), len(axes) + 1])
                current = order.reshape(chips * tokens, half)
            for position, bit in enumerate(bits):
                own, other = half_rows(current, bit)
                current = own.astype(f32) + swap(other, bit).astype(f32)
                if position < len(bits) - 1:
                    current = current.astype(bf16)
            sums.append(current)
        return jnp.concatenate(sums, axis=1)

    def chip_total(value, bits):
        start = 0
        current = value
        splits = []
        for bit in bits[:-1]:
            keep, give = half_rows(current, bit)
            current = (keep.astype(f32) + swap(give, bit).astype(f32)).astype(bf16)
            splits.append((bit, start))
            start = start + side(bit) * current.shape[0]
        current = (current.astype(f32) + swap(current, bits[-1]).astype(f32)).astype(bf16)
        pieces = [(start, current)]
        for bit, base in splits[::-1]:
            rows = sum(piece.shape[0] for _, piece in pieces)
            mine = base + side(bit) * rows
            theirs = base + (1 - side(bit)) * rows
            pieces = pieces + [
                (theirs + offset - mine, swap(piece, bit)) for offset, piece in pieces
            ]
        return pieces

    def weight_total(value):
        half = value.shape[0] // 2
        columns = value.shape[1]
        out = jnp.zeros((value.shape[0], 2 * columns), f32)
        for color, bits in enumerate((chip_bits, chip_bits[::-1])):
            for offset, piece in chip_total(value[color * half : (color + 1) * half], bits):
                offset = offset + color * half
                out = lax.dynamic_update_slice(out, piece.astype(f32), (offset, core * columns))
                out = lax.dynamic_update_slice(
                    out, swap_rows(piece).astype(f32), (other_core(offset), (1 - core) * columns)
                )
        return out

    def swap_rows(piece):
        return swap(piece, 1)

    def other_core(offset):
        return offset

    rows_in = inputs.reshape(tokens, model)
    cot_rows = cotangent.reshape(tokens, model)

    pair_index = place // copies
    head_weights = jnp.concatenate(
        [
            lax.dynamic_slice(query_weight, (0, place * query_cols), (shard, query_cols)),
            lax.dynamic_slice(key_weight, (0, pair_index * width), (shard, width)),
            lax.dynamic_slice(value_weight, (0, pair_index * width), (shard, width)),
        ],
        axis=1,
    )
    source = rows_in.astype(f32)
    first = rms_factor(source)
    normed_in = (source * first * attention_gain).astype(bf16)
    head_full = by_plane(line_gather(head_weights)).reshape(model, -1)
    normed_all = by_place(plane_gather(normed_in)).reshape(parts * tokens, model)

    proj = matmul(normed_all, head_full)
    query_proj = proj[:, :query_cols]
    key_proj = proj[:, query_cols : query_cols + width]
    values = proj[:, query_cols + width :].astype(bf16)
    cosine, sine = rope_tables(jnp.arange(parts * tokens, dtype=jnp.int32), width)
    queries = prepare(query_proj, query_gain, cosine, sine).astype(bf16)
    keys = prepare(key_proj, key_gain, cosine, sine).astype(bf16)
    pair_rows = jnp.concatenate([keys, values], axis=1)
    out_rows, log_rows = attend_heads(queries, pair_rows, local_groups, width)
    attended = lax.all_to_all(out_rows, "seq", split_axis=0, concat_axis=1, tiled=True)

    piece_rows = shard // parts
    out_piece = lax.dynamic_slice_in_dim(output_weight, place * piece_rows, piece_rows, 0)
    out_column = by_plane(line_gather(out_piece)).reshape(planes * piece_rows, model)
    full_output = by_place(plane_gather(out_column)).reshape(parts, planes, piece_rows, model)
    full_output = full_output.transpose(1, 0, 2, 3).reshape(model, model)

    middle = source + matmul(attended, full_output)
    second = rms_factor(middle)
    normed_mid = (middle * second * feedforward_gain).astype(bf16)

    cot_slots = line_gather(cot_rows)
    cot_all = jnp.concatenate(cot_slots + [swap(slot, 1) for slot in cot_slots], axis=0)
    mid_slots = line_gather(normed_mid)
    mid_all = jnp.concatenate(mid_slots + [swap(slot, 1) for slot in mid_slots], axis=0)
    units = gate_weight.shape[1] // 2
    gate_half = lax.dynamic_slice_in_dim(gate_weight, core * units, units, 1)
    up_half = lax.dynamic_slice_in_dim(up_weight, core * units, units, 1)
    down_half = lax.dynamic_slice_in_dim(down_weight, core * units, units, 1)
    hidden_grad = matmul(cot_all, down_half)
    gate = matmul(mid_all, gate_half)
    lifted = matmul(mid_all, up_half)
    hidden = activate(gate, lifted)
    gate_grad, lifted_grad = gate_back(hidden_grad, gate, lifted)
    mine = planes * tokens

    grad_down = weight_total(inner_rows(cot_all, hidden).astype(bf16))

    def token_total(term):
        keep = term[:mine] + swap(term[mine:].astype(bf16), 1).astype(f32)
        keep = keep.astype(bf16)
        return line_scatter([keep[k * tokens : (k + 1) * tokens] for k in range(planes)])

    mid_grad = token_total(inner_cols(gate_grad, gate_half) + inner_cols(lifted_grad, up_half))
    grad_gate = weight_total(inner_rows(mid_all, gate_grad).astype(bf16))
    grad_up = weight_total(inner_rows(mid_all, lifted_grad).astype(bf16))
    block_rows = middle + token_total(inner_cols(hidden, down_half))

    feedforward_slope = jnp.sum(mid_grad * middle * second, axis=0)
    middle_grad = cot_rows.astype(f32) + norm_back(mid_grad, middle, second, feedforward_gain)
    middle_half = middle_grad.astype(bf16)
    attended_grad = inner_cols(middle_half, full_output).astype(bf16)
    grad_rows = lax.all_to_all(attended_grad, "seq", split_axis=1, concat_axis=0, tiled=True)
    middle_all = by_place(plane_gather(middle_half)).reshape(parts * tokens, model)
    query_back, pair_back = attend_back(
        queries, pair_rows, out_rows, log_rows, grad_rows, local_groups, width
    )
    key_back = pair_back[:, :width]
    value_back = pair_back[:, width:]
    _, query_pull = jax.vjp(
        lambda proj_in, gain_in: prepare(proj_in, gain_in, cosine, sine), query_proj, query_gain
    )
    query_proj_grad, query_slope = query_pull(query_back)
    _, key_pull = jax.vjp(
        lambda proj_in, gain_in: prepare(proj_in, gain_in, cosine, sine), key_proj, key_gain
    )
    key_proj_grad, key_slope = key_pull(key_back)
    halves = jnp.concatenate([query_proj_grad, key_proj_grad, value_back], axis=1).astype(bf16)

    in_grad = plane_scatter(inner_cols(halves, head_full).astype(bf16))
    attention_slope = jnp.sum(in_grad * source * first, axis=0)
    input_rows = (middle_grad + norm_back(in_grad, source, first, attention_gain)).astype(bf16)

    def plane_slots(value, rows):
        return [
            lax.dynamic_slice_in_dim(value, ((plane - k) % planes) * rows, rows, 0)
            for k in range(planes)
        ]

    head_grad = line_scatter(plane_slots(inner_rows(normed_all, halves).astype(bf16), shard))
    head_grads = by_place(plane_gather(head_grad.astype(bf16)))
    grad_query = head_grads[:, :, :query_cols].transpose(1, 0, 2).reshape(shard, -1).astype(f32)
    grad_pair = head_grads[:, :, query_cols:].astype(f32)
    grad_pair = grad_pair.reshape(parts // copies, copies, shard, 2, width).sum(axis=1)
    grad_key = grad_pair[:, :, 0].transpose(1, 0, 2).reshape(shard, -1)
    grad_value = grad_pair[:, :, 1].transpose(1, 0, 2).reshape(shard, -1)

    out_grad = inner_rows(out_rows, middle_all).astype(bf16)
    dealt = lax.all_to_all(
        out_grad.reshape(parts, query_cols // parts, model),
        "seq",
        split_axis=0,
        concat_axis=0,
        tiled=True,
    )
    dealt = dealt.reshape(planes, -1, model)
    out_grad = line_scatter(
        [lax.dynamic_index_in_dim(dealt, (plane - k) % planes, 0, False) for k in range(planes)]
    )
    out_grads = by_place(plane_gather(out_grad.astype(bf16)))
    grad_output = out_grads.reshape(parts, parts // planes, query_cols // parts, model)
    grad_output = grad_output.transpose(1, 0, 2, 3).reshape(shard, model).astype(f32)

    slopes = jnp.concatenate([attention_slope, feedforward_slope, query_slope, key_slope])
    slopes = slopes.reshape(1, -1)
    for bit in range(parts.bit_length() - 1):
        slopes = slopes + swap(slopes, 1 << bit)
    for bit in range(planes.bit_length() - 1):
        slopes = slopes + lax.ppermute(
            slopes, "fsdp", [(i, i ^ (1 << bit)) for i in range(planes)]
        )
    slopes = slopes.reshape(-1)
    attention_slope = slopes[:model]
    feedforward_slope = slopes[model : 2 * model]
    query_slope = slopes[2 * model : 2 * model + width]
    key_slope = slopes[2 * model + width :]
    block_out = block_rows.astype(bf16).reshape(1, tokens, model)
    input_grad = input_rows.reshape(1, tokens, model)
    return (
        block_out,
        input_grad,
        attention_slope,
        grad_query,
        grad_key,
        grad_value,
        grad_output,
        query_slope,
        key_slope,
        feedforward_slope,
        grad_gate,
        grad_up,
        grad_down,
    )


def solution(mesh):
    in_specs = (
        P("fsdp", "seq", None),
        P("fsdp", "seq", None),
        P(),
        P("fsdp", None),
        P("fsdp", None),
        P("fsdp", None),
        P("fsdp", None),
        P(),
        P(),
        P(),
        P(None, "fsdp"),
        P(None, "fsdp"),
        P(None, "fsdp"),
    )
    out_specs = (
        P("fsdp", "seq", None),
        P("fsdp", "seq", None),
        P(),
        P("fsdp", None),
        P("fsdp", None),
        P("fsdp", None),
        P("fsdp", None),
        P(),
        P(),
        P(),
        P(None, "fsdp"),
        P(None, "fsdp"),
        P(None, "fsdp"),
    )
    return jax.shard_map(
        per_device, mesh=mesh, in_specs=in_specs, out_specs=out_specs, check_vma=False
    )
```

```python
import functools

import jax
import jax.numpy as jnp
from jax import lax
from jax.experimental import pallas as pl
from jax.experimental.pallas import tpu as pltpu
from jax.sharding import PartitionSpec as P

EPS = 1e-05
THETA = 1000000.0


def rotate_half(values):
    half = values.shape[-1] // 2
    return jnp.concatenate([-values[..., half:], values[..., :half]], axis=-1)


def rope_tables(positions, width):
    exponents = jnp.arange(width // 2).astype(jnp.float32) * 2.0 / width
    rates = jnp.power(jnp.float32(THETA), -exponents)
    angle = positions.astype(jnp.float32)[:, None] * rates[None, :]
    angle = jnp.concatenate([angle, angle], axis=-1)
    return (jnp.cos(angle), jnp.sin(angle))


def prepare(proj, gain, cosine, sine):
    rows = proj.shape[0]
    width = gain.shape[0]
    split = proj.reshape(rows, -1, width)
    factor = lax.rsqrt(jnp.mean(split * split, axis=-1, keepdims=True) + EPS)
    normed = split * factor * gain
    turned = normed * cosine[:, None, :] + rotate_half(normed) * sine[:, None, :]
    return turned.reshape(rows, -1)


def matmul(left, right):
    return jnp.dot(left, right, preferred_element_type=jnp.float32)


def inner_rows(left, right):
    return lax.dot_general(
        left, right, (((0,), (0,)), ((), ())), preferred_element_type=jnp.float32
    )


def inner_cols(left, right):
    return lax.dot_general(
        left, right, (((1,), (1,)), ((), ())), preferred_element_type=jnp.float32
    )


def rms_factor(values):
    return lax.rsqrt(jnp.mean(values * values, axis=-1, keepdims=True) + EPS)


def norm_back(grad, values, factor, gain):
    scaled = grad * gain
    return factor * (
        scaled - values * factor * factor * jnp.mean(scaled * values, axis=-1, keepdims=True)
    )


def gate_back(hidden_grad, gate, lifted):
    sigma = jax.nn.sigmoid(gate)
    gate_grad = (hidden_grad * lifted * sigma * (1.0 + gate * (1.0 - sigma))).astype(jnp.bfloat16)
    lifted_grad = (hidden_grad * gate * sigma).astype(jnp.bfloat16)
    return (gate_grad, lifted_grad)


def activate(gate, lifted):
    return (gate * jax.nn.sigmoid(gate) * lifted).astype(jnp.bfloat16)


def split_heads(query_rows, pair_rows, groups, width):
    length = query_rows.shape[0]
    key_heads = pair_rows.shape[1] // (2 * width)
    queries = query_rows.reshape(length, key_heads, groups, width)
    keys = pair_rows[:, : key_heads * width].reshape(length, key_heads, width)
    values = pair_rows[:, key_heads * width :].reshape(length, key_heads, width)
    return (queries, keys, values, key_heads)


def attend_heads(query_rows, pair_rows, groups, width):
    length = query_rows.shape[0]
    queries, keys, values, key_heads = split_heads(query_rows, pair_rows, groups, width)
    block = min(512, length)
    scale = width ** (-0.5)
    offsets = jnp.arange(block)

    def query_step(index, state):
        out_rows, log_rows = state
        query_block = lax.dynamic_slice_in_dim(queries, index * block, block, 0)

        def key_step(inner, carry):
            summed, total = carry
            key_block = lax.dynamic_slice_in_dim(keys, inner * block, block, 0)
            value_block = lax.dynamic_slice_in_dim(values, inner * block, block, 0)
            scores = (
                jnp.einsum(
                    "qhgd,shd->hgqs", query_block, key_block, preferred_element_type=jnp.float32
                )
                * scale
            )
            allowed = (index * block + offsets)[:, None] >= (inner * block + offsets)[None, :]
            weights = jnp.where(allowed, jnp.exp(scores), 0.0)
            summed = summed + jnp.einsum(
                "hgqs,shd->hgqd",
                weights.astype(jnp.bfloat16),
                value_block,
                preferred_element_type=jnp.float32,
            )
            return (summed, total + jnp.sum(weights, axis=-1))

        initial = (
            jnp.zeros((key_heads, groups, block, width), jnp.float32),
            jnp.zeros((key_heads, groups, block), jnp.float32),
        )
        summed, total = lax.fori_loop(0, index + 1, key_step, initial)
        result = (summed / total[..., None]).astype(jnp.bfloat16)
        result = result.transpose(2, 0, 1, 3).reshape(block, key_heads * groups * width)
        out_rows = lax.dynamic_update_slice_in_dim(out_rows, result, index * block, 0)
        log_rows = lax.dynamic_update_slice_in_dim(log_rows, jnp.log(total), index * block, 2)
        return (out_rows, log_rows)

    start = (
        jnp.zeros((length, key_heads * groups * width), jnp.bfloat16),
        jnp.zeros((key_heads, groups, length), jnp.float32),
    )
    return lax.fori_loop(0, length // block, query_step, start)


def attend_back(query_rows, pair_rows, out_rows, log_rows, grad_rows, groups, width):
    length = query_rows.shape[0]
    queries, keys, values, key_heads = split_heads(query_rows, pair_rows, groups, width)
    outs = out_rows.reshape(length, key_heads, groups, width)
    grads = grad_rows.reshape(length, key_heads, groups, width)
    correction = jnp.sum(grads.astype(jnp.float32) * outs.astype(jnp.float32), axis=-1)
    block = min(512, length)
    scale = width ** (-0.5)
    offsets = jnp.arange(block)

    def query_step(index, state):
        query_grad, key_grad, value_grad = state
        query_block = lax.dynamic_slice_in_dim(queries, index * block, block, 0)
        grad_block = lax.dynamic_slice_in_dim(grads, index * block, block, 0)
        shift_block = lax.dynamic_slice_in_dim(correction, index * block, block, 0).transpose(
            1, 2, 0
        )
        log_block = lax.dynamic_slice_in_dim(log_rows, index * block, block, 2)

        def key_step(inner, carry):
            block_grad, key_sum, value_sum = carry
            key_block = lax.dynamic_slice_in_dim(keys, inner * block, block, 0)
            value_block = lax.dynamic_slice_in_dim(values, inner * block, block, 0)
            scores = (
                jnp.einsum(
                    "qhgd,shd->hgqs", query_block, key_block, preferred_element_type=jnp.float32
                )
                * scale
            )
            allowed = (index * block + offsets)[:, None] >= (inner * block + offsets)[None, :]
            weights = jnp.where(allowed, jnp.exp(scores - log_block[..., None]), 0.0)
            value_part = jnp.einsum(
                "hgqs,qhgd->shd",
                weights.astype(jnp.bfloat16),
                grad_block,
                preferred_element_type=jnp.float32,
            )
            prob_grad = jnp.einsum(
                "qhgd,shd->hgqs", grad_block, value_block, preferred_element_type=jnp.float32
            )
            score_grad = (weights * (prob_grad - shift_block[..., None]) * scale).astype(
                jnp.bfloat16
            )
            block_grad = block_grad + jnp.einsum(
                "hgqs,shd->qhgd", score_grad, key_block, preferred_element_type=jnp.float32
            )
            key_part = jnp.einsum(
                "hgqs,qhgd->shd", score_grad, query_block, preferred_element_type=jnp.float32
            )
            key_sum = lax.dynamic_update_slice_in_dim(
                key_sum,
                lax.dynamic_slice_in_dim(key_sum, inner * block, block, 0) + key_part,
                inner * block,
                0,
            )
            value_sum = lax.dynamic_update_slice_in_dim(
                value_sum,
                lax.dynamic_slice_in_dim(value_sum, inner * block, block, 0) + value_part,
                inner * block,
                0,
            )
            return (block_grad, key_sum, value_sum)

        initial = (jnp.zeros((block, key_heads, groups, width), jnp.float32), key_grad, value_grad)
        block_grad, key_grad, value_grad = lax.fori_loop(0, index + 1, key_step, initial)
        query_grad = lax.dynamic_update_slice_in_dim(query_grad, block_grad, index * block, 0)
        return (query_grad, key_grad, value_grad)

    state = (
        jnp.zeros((length, key_heads, groups, width), jnp.float32),
        jnp.zeros((length, key_heads, width), jnp.float32),
        jnp.zeros((length, key_heads, width), jnp.float32),
    )
    query_grad, key_grad, value_grad = lax.fori_loop(0, length // block, query_step, state)
    pair_grad = jnp.concatenate(
        [
            key_grad.reshape(length, key_heads * width),
            value_grad.reshape(length, key_heads * width),
        ],
        axis=1,
    )
    return (query_grad.reshape(length, key_heads * groups * width), pair_grad)


MESH = pl.DeviceIdType.MESH


def flip(index, mask, bits):
    for bit in bits:
        if mask & bit:
            index = index + bit - 2 * bit * ((index // bit) % 2)
    return index


class Place:
    def __init__(self, parts, planes):
        self.parts, self.planes = parts, planes
        self.seat = lax.axis_index("seq")
        self.plane = lax.axis_index("fsdp")
        self.core = self.seat % 2
        self.chip = self.seat // 2
        self.seat_bits = [1 << i for i in range(parts.bit_length() - 1)]
        self.chip_bits = self.seat_bits[1:]
        self.plane_bits = [1 << i for i in range(planes.bit_length() - 1)]

    def at(self, mask):
        return flip(self.seat, mask, self.seat_bits)

    def side(self, bit):
        return (self.seat // bit) % 2

    def colors(self):
        return (self.chip_bits, self.chip_bits[::-1])

    def enter(self, masks=(), line=False, plane_masks=()):
        barrier = pltpu.get_barrier_semaphore()
        peers = [{"seq": self.at(mask)} for mask in masks]
        if line:
            peers.append({"fsdp": (self.plane + 1) % self.planes})
            peers.append({"fsdp": (self.plane + self.planes - 1) % self.planes})
        for mask in plane_masks:
            peers.append({"fsdp": flip(self.plane, mask, self.plane_bits)})
        for peer in peers:
            pl.semaphore_signal(barrier, inc=1, device_id=peer, device_id_type=MESH)
        pl.semaphore_wait(barrier, len(peers))


class Wire:
    def __init__(self, sends, receives, locals_):
        self.sends, self.receives, self.locals = sends, receives, locals_
        self.count = self.local_count = 0
        self.open = []

    def remote(self, source, target, device):
        number = self.count
        self.count += 1
        return pltpu.make_async_remote_copy(
            src_ref=source,
            dst_ref=target,
            send_sem=self.sends.at[number],
            recv_sem=self.receives.at[number],
            device_id=device,
            device_id_type=MESH,
        )

    def send(self, source, target, device):
        copy = self.remote(source, target, device)
        copy.start()
        self.open.append(copy)
        return copy

    def local(self, source, target):
        number = self.local_count
        self.local_count += 1
        copy = pltpu.make_async_copy(source, target, self.locals.at[number])
        copy.start()
        return copy

    def close(self):
        for copy in self.open:
            copy.wait_send()


def add_rows(target, left, right, step=64):
    rows = target.shape[0]
    step = min(step, rows)

    def body(index, carry):
        at = pl.ds(pl.multiple_of(index * step, step), step)
        total = left[at, :].astype(jnp.float32) + right[at, :].astype(jnp.float32)
        target[at, :] = total.astype(target.dtype)
        return carry

    lax.fori_loop(0, rows // step, body, 0)


class LineGather:
    def __init__(self, wire, here, source, target, share=None):
        self.here = here
        planes, plane = here.planes, here.plane
        above = {"fsdp": (plane + 1) % planes}
        below = {"fsdp": (plane + planes - 1) % planes}
        self.ups, self.downs = {}, {}
        for step in range(1, planes):
            lower = (plane + planes - step + 1) % planes
            upper = (plane + step - 1) % planes
            first = step == 1
            self.ups[step] = wire.remote(
                source if first else target(lower), target(lower), above
            )
            self.downs[step] = wire.remote(
                source if first else target(upper), target(upper), below
            )
        self.shared = {}
        if share is not None:
            for step in range(1, planes):
                for way, shift in ((0, planes - step), (1, step)):
                    index = (plane + shift) % planes
                    self.shared[(step, way)] = wire.remote(
                        target(index), share(index), {"seq": here.at(1)}
                    )

    def start(self, step):
        planes, plane = self.here.planes, self.here.plane

        @pl.when((plane >= step - 1) & (plane <= planes - 2))
        def _():
            self.ups[step].start()

        @pl.when((plane + step <= planes) & (plane >= 1))
        def _():
            self.downs[step].start()

    def arrive(self, step):
        planes, plane = self.here.planes, self.here.plane

        @pl.when(plane >= step)
        def _():
            self.ups[step].wait_recv()
            if self.shared:
                self.shared[(step, 0)].start()

        @pl.when(plane + step <= planes - 1)
        def _():
            self.downs[step].wait_recv()
            if self.shared:
                self.shared[(step, 1)].start()

    def close(self):
        planes, plane = self.here.planes, self.here.plane
        for (step, way), copy in self.shared.items():

            @pl.when(plane >= step if way == 0 else plane + step <= planes - 1)
            def _(copy=copy):
                copy.wait()

        for step in range(1, planes):

            @pl.when((plane >= step - 1) & (plane <= planes - 2))
            def _(step=step):
                self.ups[step].wait_send()

            @pl.when((plane + step <= planes) & (plane >= 1))
            def _(step=step):
                self.downs[step].wait_send()


class LineScatter:
    def __init__(self, wire, here, term, landing):
        self.wire, self.here, self.term, self.landing = wire, here, term, landing
        planes, plane = here.planes, here.plane
        above = {"fsdp": (plane + 1) % planes}
        below = {"fsdp": (plane + planes - 1) % planes}
        self.ups, self.downs = {}, {}
        for step in range(1, planes):
            self.ups[step] = wire.remote(
                term((plane + planes - step) % planes), landing(0, step - 1), above
            )
            self.downs[step] = wire.remote(
                term((plane + step) % planes), landing(1, step - 1), below
            )

    def step(self, step):
        planes, plane = self.here.planes, self.here.plane
        mirror = planes - 1 - plane
        for way, (position, copies, dest) in enumerate(
            (
                (plane, self.ups, (plane + planes - step) % planes),
                (mirror, self.downs, (plane + step) % planes),
            )
        ):
            if step > 1:

                @pl.when((position >= 1) & (position <= step - 1))
                def _(way=way, copies=copies, dest=dest):
                    copies[step - 1].wait_recv()
                    term = self.term(dest)
                    add_rows(term, term, self.landing(way, step - 2))

            @pl.when(position <= step - 1)
            def _(copies=copies):
                copies[step].start()

    def finish(self, out):
        planes, plane = self.here.planes, self.here.plane
        own = self.term(plane)
        last = planes - 1

        @pl.when(plane >= 1)
        def _():
            self.ups[last].wait_recv()

        @pl.when(plane <= planes - 2)
        def _():
            self.downs[last].wait_recv()

        @pl.when(plane == 0)
        def _():
            add_rows(out, own, self.landing(1, last - 1))

        @pl.when(plane == planes - 1)
        def _():
            add_rows(out, own, self.landing(0, last - 1))

        @pl.when((plane >= 1) & (plane <= planes - 2))
        def _():
            add_rows(own, own, self.landing(0, last - 1))
            add_rows(out, own, self.landing(1, last - 1))

    def close(self):
        planes, plane = self.here.planes, self.here.plane
        mirror = planes - 1 - plane
        for step in range(1, planes):

            @pl.when(plane <= step - 1)
            def _(step=step):
                self.ups[step].wait_send()

            @pl.when(mirror <= step - 1)
            def _(step=step):
                self.downs[step].wait_send()


class PlaneGather:
    def __init__(self, wire, here, source, target):
        self.wire, self.here, self.source, self.target = wire, here, source, target
        self.incoming = {}

    def _send(self, mask, color, bit):
        here = self.here
        target = self.target(here.at(mask), color)
        source = self.source(color) if mask == 0 else target
        self.incoming[(mask ^ bit, color)] = self.wire.send(
            source, target, {"seq": here.at(bit)}
        )

    def start(self):
        for position in range(len(self.here.chip_bits)):
            for color, bits in enumerate(self.here.colors()):
                self._send(0, color, bits[position])
        for color in (0, 1):
            self._send(0, color, 1)

    def forward(self):
        here = self.here
        chips = here.parts // 2
        masks = sorted(
            (mask * 2 for mask in range(1, chips)), key=lambda mask: bin(mask).count("1")
        )
        for mask in masks:
            for color, bits in enumerate(here.colors()):
                self.incoming[(mask, color)].wait_recv()
                last = max(i for i, bit in enumerate(bits) if mask & bit)
                for bit in bits[last + 1 :]:
                    self._send(mask, color, bit)
                self._send(mask, color, 1)

    def finish(self):
        for mask in range(1, self.here.parts, 2):
            for color in (0, 1):
                self.incoming[(mask, color)].wait_recv()


class PlaneScatter:
    def __init__(self, wire, here, product, give, take, current, landing, model):
        self.wire, self.here, self.product = wire, here, product
        self.give, self.take, self.current, self.landing = give, take, current, landing
        self.model = model

    def start(self):
        here = self.here
        chips = here.parts // 2
        self.swaps = {}
        tokens = self.give.shape[1]
        seats = [2 * flip(here.chip, mask, [b // 2 for b in here.chip_bits]) for mask in range(chips)]
        for part in range(self.model // 512):
            columns = slice(part * 512, (part + 1) * 512)
            rows = self.product([seat + 1 - here.core for seat in seats], columns)
            for mask in range(chips):
                self.give[mask, :, columns] = rows[mask * tokens : (mask + 1) * tokens].astype(
                    self.give.dtype
                )
        for mask in range(chips)[::-1]:
            self.swaps[mask] = self.wire.send(
                self.give.at[mask], self.take.at[mask], {"seq": here.at(1)}
            )
        half = self.model // 2
        for part in range(self.model // 512):
            columns = slice(part * 512, (part + 1) * 512)
            rows = self.product([seat + here.core for seat in seats], columns)
            color, inside = divmod(part * 512, half)
            for mask in range(chips):
                self.current[color, mask, :, inside : inside + 512] = rows[
                    mask * tokens : (mask + 1) * tokens
                ].astype(self.current.dtype)

    def join(self):
        half = self.model // 2
        chips = self.here.parts // 2
        for mask in range(chips)[::-1]:
            self.swaps[mask].wait_recv()
            for color in (0, 1):
                mine = self.current.at[color, mask]
                add_rows(mine, mine, self.take.at[mask, :, pl.ds(color * half, half)])

    def stage(self, position):
        here = self.here
        self.moved = {}
        for color, bits in enumerate(here.colors()):
            bit = bits[position]
            done = sum(bits[:position])
            for mask in range(here.parts // 2):
                if mask * 2 & bit and not mask * 2 & done:
                    low = mask ^ (bit // 2)
                    self.moved[(color, low)] = self.wire.send(
                        self.current.at[color, mask],
                        self.landing.at[position, color, low],
                        {"seq": here.at(bit)},
                    )

    def settle(self, position, out):
        half = self.model // 2
        last = position == len(self.here.chip_bits) - 1
        for (color, low), copy in self.moved.items():
            copy.wait_recv()
            mine = self.current.at[color, low]
            if last:
                target = out.at[:, pl.ds(color * half, half)]
            else:
                target = mine
            add_rows(target, mine, self.landing.at[position, color, low])


def head_weights_kernel(parts, planes, x, w, o, x_all, w_all, o_slice, o_all, *sems):
    here = Place(parts, planes)
    wire = Wire(*sems)
    tokens, shard, rows = x.shape[0], w.shape[0], o.shape[0]
    half = tokens // 2
    chips = parts // 2
    chip_masks = [mask * 2 for mask in range(1, chips)]
    here.enter(chip_masks + [1], line=True)
    weights = LineGather(
        wire, here, w, lambda index: w_all.at[pl.ds(pl.multiple_of(index * shard, shard), shard)]
    )
    weights.start(1)
    plane_rows = PlaneGather(
        wire,
        here,
        lambda color: x.at[pl.ds(color * half, half)],
        lambda seat, color: x_all.at[pl.ds(pl.multiple_of(seat * tokens + color * half, half), half)],
    )
    plane_rows.start()
    kept = [
        wire.local(x, x_all.at[pl.ds(pl.multiple_of(here.seat * tokens, tokens), tokens)]),
        wire.local(w, w_all.at[pl.ds(pl.multiple_of(here.plane * shard, shard), shard)]),
        wire.local(o, o_all.at[here.plane]),
    ]
    outer = LineGather(wire, here, o, lambda index: o_all.at[index])
    weights.arrive(1)
    if planes > 2:
        weights.start(2)
    outer.start(1)
    plane_rows.forward()
    for step in range(2, planes):
        weights.arrive(step)
        if step + 1 < planes:
            weights.start(step + 1)
        outer.arrive(step - 1)
        outer.start(step)
    outer.arrive(planes - 1)
    plane_rows.finish()
    for copy in kept:
        copy.wait()
    dealt = []
    spot = o_slice.at[pl.ds(pl.multiple_of(here.chip * rows, rows), rows)]
    for mask in chip_masks:
        chip = here.at(mask) // 2
        dealt.append(wire.send(o_all.at[chip], spot, {"seq": here.at(mask)}))
    own = wire.local(o_all.at[here.chip], spot)
    own.wait()
    for copy in dealt:
        copy.wait_recv()
    wire.close()
    weights.close()
    outer.close()


def out_rows_kernel(
    parts, planes, a, w, c, out, c_all, give, take, current, landing, *sems
):
    here = Place(parts, planes)
    wire = Wire(*sems)
    tokens, model = c.shape
    here.enter([mask for mask in here.seat_bits], line=True)

    def product(seats, columns):
        rows = [a[pl.ds(pl.multiple_of(seat * tokens, tokens), tokens), :] for seat in seats]
        return jnp.dot(
            jnp.concatenate(rows, axis=0), w[:, columns], preferred_element_type=jnp.float32
        )

    mine, theirs = here.core * planes, (1 - here.core) * planes
    cots = LineGather(
        wire,
        here,
        c,
        lambda index: c_all.at[mine + index],
        lambda index: c_all.at[mine + index],
    )
    cots.start(1)
    own = wire.local(c, c_all.at[mine + here.plane])
    across = wire.send(c, c_all.at[mine + here.plane], {"seq": here.at(1)})
    rows = PlaneScatter(wire, here, product, give, take, current, landing, model)
    rows.start()
    rows.join()
    stages = len(here.chip_bits)
    for stage in range(stages):
        rows.stage(stage)
        if stage + 1 < planes:
            cots.arrive(stage + 1)
            if stage + 2 < planes:
                cots.start(stage + 2)
        rows.settle(stage, out)
    for step in range(stages + 1, planes):
        cots.arrive(step)
        if step + 1 < planes:
            cots.start(step + 1)
    own.wait()
    across.wait_recv()
    wire.close()
    cots.close()


def mid_rows_kernel(parts, planes, m, m_all, *sems):
    here = Place(parts, planes)
    wire = Wire(*sems)
    here.enter([1], line=True)
    mine = here.core * planes
    mids = LineGather(
        wire,
        here,
        m,
        lambda index: m_all.at[mine + index],
        lambda index: m_all.at[mine + index],
    )
    mids.start(1)
    own = wire.local(m, m_all.at[mine + here.plane])
    across = wire.send(m, m_all.at[mine + here.plane], {"seq": here.at(1)})
    for step in range(1, planes):
        mids.arrive(step)
        if step + 1 < planes:
            mids.start(step + 1)
    own.wait()
    across.wait_recv()
    wire.close()
    mids.close()


def halve_kernel(parts, planes, p_a, p_b, p_c, part, s_down, s_first, s_second, mid, keep, *rest):
    here = Place(parts, planes)
    stages = len(here.chip_bits) - 1
    landings, rest = rest[:stages], rest[stages:]
    current, take, line_landing, *sems = rest
    wire = Wire(*sems)
    here.enter(here.seat_bits, line=True)
    tokens = mid.shape[0]
    model = p_a.shape[0]
    swaps = TokenSum(wire, here, part, current, take, line_landing)
    swaps.start()
    terms = (p_a, p_b, p_c)
    moved, kept = {}, {}
    rows = model // 4
    for number, term in enumerate(terms):
        for color, bits in enumerate(here.colors()):
            base = color * (model // 2)
            away = pl.multiple_of(base + (1 - here.side(bits[0])) * rows, rows)
            stay = pl.multiple_of(base + here.side(bits[0]) * rows, rows)
            moved[(number, color)] = wire.send(
                term.at[pl.ds(away, rows)],
                landings[0].at[number, color],
                {"seq": here.at(bits[0])},
            )
            kept[(number, color)] = wire.local(
                term.at[pl.ds(stay, rows)], keep.at[number, color]
            )
    swaps.join()
    steps = list(range(1, planes))
    done = 0
    starts = {(number, color): 0 for number in range(3) for color in (0, 1)}
    for stage in range(stages):
        last = stage == stages - 1
        for number in range(3):
            take_steps = len(steps) * (stage * 3 + number + 1) // (stages * 3) - done
            for step in steps[done : done + take_steps]:
                swaps.step(step)
            done += take_steps
            for color, bits in enumerate(here.colors()):
                moved[(number, color)].wait_recv()
                if stage == 0:
                    kept[(number, color)].wait()
                begin = starts[(number, color)]
                mine = keep.at[number, color, pl.ds(begin, rows)]
                if last:
                    target = (
                        s_down.at[color]
                        if number == 0
                        else (s_first, s_second)[color].at[number - 1]
                    )
                    add_rows(target, mine, landings[stage].at[number, color])
                else:
                    add_rows(mine, mine, landings[stage].at[number, color])
                    bit = bits[stage + 1]
                    half = rows // 2
                    away = pl.multiple_of(begin + (1 - here.side(bit)) * half, half)
                    moved[(number, color)] = wire.send(
                        keep.at[number, color, pl.ds(away, half)],
                        landings[stage + 1].at[number, color],
                        {"seq": here.at(bit)},
                    )
                    starts[(number, color)] = pl.multiple_of(begin + here.side(bit) * half, half)
        rows //= 2
    swaps.finish(mid)
    wire.close()
    swaps.close()


class TokenSum:
    def __init__(self, wire, here, part, current, take, landing):
        self.wire, self.here, self.part = wire, here, part
        self.current, self.take = current, take
        self.line = LineScatter(
            wire, here, lambda index: current.at[index], lambda way, step: landing.at[way, step]
        )

    def start(self):
        here, planes = self.here, self.here.planes
        self.across = self.wire.send(
            self.part.at[pl.ds((1 - here.core) * planes, planes)], self.take, {"seq": here.at(1)}
        )
        self.own = self.wire.local(self.part.at[pl.ds(here.core * planes, planes)], self.current)

    def join(self):
        self.own.wait()
        self.across.wait_recv()

        def body(index, carry):
            row = self.current.at[index]
            add_rows(row, row, self.take.at[index])
            return carry

        lax.fori_loop(0, self.here.planes, body, 0)

    def step(self, step):
        self.line.step(step)

    def finish(self, out):
        self.line.finish(out)

    def close(self):
        self.line.close()


def spread_kernel(parts, planes, h, s, part, h_all, t, block, current, take, line_landing, *sems):
    here = Place(parts, planes)
    wire = Wire(*sems)
    here.enter(here.seat_bits, line=True)
    tokens = h.shape[0]
    half = tokens // 2
    rows = PlaneGather(
        wire,
        here,
        lambda color: h.at[pl.ds(color * half, half)],
        lambda seat, color: h_all.at[pl.ds(pl.multiple_of(seat * tokens + color * half, half), half)],
    )
    swaps = TokenSum(wire, here, part, current, take, line_landing)
    rows.start()
    own = wire.local(h, h_all.at[pl.ds(pl.multiple_of(here.seat * tokens, tokens), tokens)])
    swaps.start()
    moved = [
        wire.send(s.at[color], t.at[color], {"seq": here.at(bits[-1])})
        for color, bits in enumerate(here.colors())
    ]
    rows.forward()
    swaps.join()
    for step in range(1, planes):
        swaps.step(step)
    rows.finish()
    for color in (0, 1):
        moved[color].wait_recv()
        add_rows(t.at[color], t.at[color], s.at[color])
    own.wait()
    swaps.finish(block)
    wire.close()
    swaps.close()


def in_rows_kernel(
    parts,
    planes,
    a,
    w,
    head_part,
    out_part,
    out,
    head_sum,
    out_sum,
    give,
    take,
    current,
    landing,
    head_current,
    head_landing,
    dealt,
    out_landing,
    *sems,
):
    here = Place(parts, planes)
    wire = Wire(*sems)
    tokens, model = out.shape
    shard = head_sum.shape[0]
    rows_out = out_sum.shape[0]
    chips = parts // 2
    chip_masks = [mask * 2 for mask in range(1, chips)]
    here.enter(chip_masks + [1], line=True)
    head_own = wire.local(head_part, head_current)
    deals = []
    for mask in chip_masks:
        chip = here.at(mask) // 2
        deals.append(
            wire.send(
                out_part.at[pl.ds(pl.multiple_of(chip * rows_out, rows_out), rows_out)],
                dealt.at[here.chip],
                {"seq": here.at(mask)},
            )
        )
    deal_own = wire.local(
        out_part.at[pl.ds(pl.multiple_of(here.chip * rows_out, rows_out), rows_out)],
        dealt.at[here.chip],
    )

    def product(seats, columns):
        rows = [a[pl.ds(pl.multiple_of(seat * tokens, tokens), tokens), :] for seat in seats]
        return lax.dot_general(
            jnp.concatenate(rows, axis=0),
            w[columns, :],
            (((1,), (1,)), ((), ())),
            preferred_element_type=jnp.float32,
        )

    heads = LineScatter(
        wire, here, lambda index: head_current.at[index], lambda way, step: head_landing.at[way, step]
    )
    outer = LineScatter(
        wire, here, lambda index: dealt.at[index], lambda way, step: out_landing.at[way, step]
    )
    head_own.wait()
    heads.step(1)
    rows = PlaneScatter(wire, here, product, give, take, current, landing, model)
    rows.start()
    deal_own.wait()
    for copy in deals:
        copy.wait_recv()
    outer.step(1)
    rows.join()
    stages = len(here.chip_bits)
    for stage in range(stages):
        rows.stage(stage)
        if stage + 2 < planes:
            heads.step(stage + 2)
            outer.step(stage + 2)
        rows.settle(stage, out)
    for step in range(stages + 2, planes):
        heads.step(step)
        outer.step(step)
    heads.finish(head_sum)
    outer.finish(out_sum)
    wire.close()
    heads.close()
    outer.close()


def collect_kernel(
    parts,
    planes,
    t_down,
    t_first,
    t_second,
    head,
    outer,
    slope,
    grad_down,
    grad_gate,
    grad_up,
    head_all,
    outer_all,
    slope_out,
    near,
    far,
    stage_rows,
    slope_sums,
    slope_landing,
    *sems,
):
    here = Place(parts, planes)
    wire = Wire(*sems)
    here.enter(here.seat_bits, plane_masks=here.plane_bits)
    shard, rows_out = head.shape[0], outer.shape[0]
    chips = parts // 2

    bits = [("seq", bit) for bit in here.seat_bits] + [("fsdp", bit) for bit in here.plane_bits]
    slope_copies = []

    def slope_send(number):
        axis, bit = bits[number]
        index = here.at(bit) if axis == "seq" else flip(here.plane, bit, here.plane_bits)
        source = slope if number == 0 else slope_sums.at[number - 1]
        slope_copies.append(wire.send(source, slope_landing.at[number], {axis: index}))

    def slope_add(number):
        slope_copies[number].wait_recv()
        source = slope if number == 0 else slope_sums.at[number - 1]
        target = slope_out if number == len(bits) - 1 else slope_sums.at[number]
        target[...] = source[...] + slope_landing[number]

    slope_send(0)
    half = shard // 2
    heads = PlaneGather(
        wire,
        here,
        lambda color: head.at[pl.ds(color * half, half)],
        lambda seat, color: head_all.at[seat, pl.ds(color * half, half)],
    )
    half_out = rows_out // 2

    def outer_target(seat, color):
        start = ((seat % 2) * chips + seat // 2) * rows_out + color * half_out
        return outer_all.at[pl.ds(pl.multiple_of(start, half_out), half_out)]

    outers = PlaneGather(
        wire, here, lambda color: outer.at[pl.ds(color * half_out, half_out)], outer_target
    )
    heads.start()
    outers.start()
    own_start = (here.core * chips + here.chip) * rows_out
    own = [
        wire.local(head, head_all.at[here.seat]),
        wire.local(
            outer, outer_all.at[pl.ds(pl.multiple_of(own_start, rows_out), rows_out)]
        ),
    ]

    model = near.shape[1]
    units = near.shape[2]
    size = t_down.shape[1]
    outs = (grad_down, grad_gate, grad_up)
    sources = {}
    incoming = {}
    swaps = {}

    def final(number, color):
        if number == 0:
            return t_down.at[color]
        return (t_first, t_second)[color].at[number - 1]

    def rows_at(start):
        return pl.ds(pl.multiple_of(start, size), size)

    starts = {}
    for color, order in enumerate(here.colors()):
        start = color * (model // 2)
        rows = model // 2
        for bit in order[:-1]:
            rows //= 2
            start = start + here.side(bit) * rows
        starts[color] = start

    def pass_on(number, color, start, source, bit, rows):
        incoming_start = start + rows - 2 * rows * here.side(bit)
        copy = wire.send(
            source, near.at[number, rows_at(start)], {"seq": here.at(bit)}
        )
        return incoming_start, copy

    def swap_core(number, start, source):
        return wire.send(source, far.at[number, rows_at(start)], {"seq": here.at(1)})

    held = {}
    for number in range(3):
        for color, order in enumerate(here.colors()):
            rest = order[:-1]
            source = final(number, color)
            pieces = [(starts[color], source, None)]
            rows = size
            if rest:
                pieces.append(
                    _pending(
                        pass_on(number, color, starts[color], source, rest[-1], rows),
                        near,
                        number,
                        rows_at,
                    )
                )
            swaps[(number, color)] = [(starts[color], swap_core(number, starts[color], source))]
            held[(number, color)] = pieces

    blocks = []
    count = [0]

    def write(number, start, source, column):
        step = stage_rows.shape[1]
        for part in range(size // step):
            slot = count[0] % stage_rows.shape[0]
            if count[0] >= stage_rows.shape[0]:
                blocks[count[0] - stage_rows.shape[0]].wait()
            count[0] += 1

            def body(index, carry):
                at = pl.ds(pl.multiple_of(index * 32, 32), 32)
                from_ = pl.ds(pl.multiple_of(part * step + index * 32, 32), 32)
                stage_rows[slot, at, :] = source[from_, :].astype(jnp.float32)
                return carry

            lax.fori_loop(0, step // 32, body, 0)
            blocks.append(
                wire.local(
                    stage_rows.at[slot],
                    outs[number].at[
                        pl.ds(pl.multiple_of(start + part * step, step), step),
                        pl.ds(pl.multiple_of(column * units, units), units),
                    ],
                )
            )

    slope_add(0)
    if len(bits) > 1:
        slope_send(1)
    heads.forward()
    outers.forward()
    for number in range(1, len(bits)):
        slope_add(number)
        if number + 1 < len(bits):
            slope_send(number + 1)
        if number == 1:
            for color in (0, 1):
                write(0, starts[color], final(0, color), here.core)
    for number in range(3):
        if number > 0:
            for color in (0, 1):
                write(number, starts[color], final(number, color), here.core)
        for color, order in enumerate(here.colors()):
            rest = order[:-1]
            pieces = held[(number, color)]
            position = len(rest) - 1
            rows = size
            while position >= 0:
                fresh = [piece for piece in pieces if piece[2] is not None]
                for piece in fresh:
                    piece[2].wait_recv()
                    swaps[(number, color)].append(
                        (piece[0], swap_core(number, piece[0], piece[1]))
                    )
                    write(number, piece[0], piece[1], here.core)
                pieces = [(start, source, None) for start, source, _ in pieces]
                position -= 1
                rows *= 2
                if position >= 0:
                    bit = rest[position]
                    pieces = pieces + [
                        _pending(
                            pass_on(number, color, start, source, bit, rows), near, number, rows_at
                        )
                        for start, source, _ in pieces
                    ]
        for color in (0, 1):
            for start, copy in swaps[(number, color)]:
                copy.wait_recv()
                write(number, start, far.at[number, rows_at(start)], 1 - here.core)
    heads.finish()
    outers.finish()
    for copy in own:
        copy.wait()
    for copy in blocks[-stage_rows.shape[0] :]:
        copy.wait()
    wire.close()


def _pending(passed, near, number, rows_at):
    start, copy = passed
    return (start, near.at[number, rows_at(start)], copy)


SENDS, LOCALS = 128, 96


def call(kernel, mesh_sizes, number, inputs, in_vmem, outputs, scratch, out_vmem=None):
    vmem = pl.BlockSpec(memory_space=pltpu.VMEM)
    anywhere = pl.BlockSpec(memory_space=pl.ANY)
    out_vmem = out_vmem or [True] * len(outputs)
    semaphores = [
        pltpu.SemaphoreType.DMA((SENDS,)),
        pltpu.SemaphoreType.DMA((SENDS,)),
        pltpu.SemaphoreType.DMA((LOCALS,)),
    ]
    return pl.pallas_call(
        functools.partial(kernel, *mesh_sizes),
        out_shape=[jax.ShapeDtypeStruct(shape, kind) for shape, kind in outputs],
        in_specs=[vmem if inside else anywhere for inside in in_vmem],
        out_specs=[vmem if inside else anywhere for inside in out_vmem],
        scratch_shapes=[pltpu.VMEM(shape, kind) for shape, kind in scratch] + semaphores,
        compiler_params=pltpu.CompilerParams(
            collective_id=number, has_side_effects=True, vmem_limit_bytes=VMEM_BYTES
        ),
    )(*inputs)


VMEM_BYTES = 62 * 1024 * 1024


def per_device(
    inputs,
    cotangent,
    attention_gain,
    query_weight,
    key_weight,
    value_weight,
    output_weight,
    query_gain,
    key_gain,
    feedforward_gain,
    gate_weight,
    up_weight,
    down_weight,
):
    tokens = inputs.shape[1]
    model = inputs.shape[2]
    width = query_gain.shape[0]
    pair_heads = key_weight.shape[1] // width
    parts = lax.axis_size("seq")
    planes = lax.axis_size("fsdp")
    sizes = (parts, planes)
    chips = parts // 2
    copies = max(1, parts // pair_heads)
    place = lax.axis_index("seq")
    plane = lax.axis_index("fsdp")
    core = place % 2
    query_cols = model // parts
    head_cols = query_cols + 2 * width
    local_groups = query_cols // width
    shard = query_weight.shape[0]
    piece_rows = shard // parts
    length = parts * tokens
    units = gate_weight.shape[1] // 2
    f32, bf16 = jnp.float32, jnp.bfloat16
    halvings = chips.bit_length() - 2
    last_rows = model // 2 >> halvings
    rows_in = inputs.reshape(tokens, model)
    cot_rows = cotangent.reshape(tokens, model)

    pair_index = place // copies
    head_weights = jnp.concatenate(
        [
            lax.dynamic_slice(query_weight, (0, place * query_cols), (shard, query_cols)),
            lax.dynamic_slice(key_weight, (0, pair_index * width), (shard, width)),
            lax.dynamic_slice(value_weight, (0, pair_index * width), (shard, width)),
        ],
        axis=1,
    )
    piece_index = core * chips + place // 2
    out_piece = lax.dynamic_slice_in_dim(output_weight, piece_index * piece_rows, piece_rows, 0)
    source = rows_in.astype(f32)
    first = rms_factor(source)
    normed_in = (source * first * attention_gain).astype(bf16)
    normed_all, head_full, out_slice = call(
        head_weights_kernel,
        sizes,
        0,
        (normed_in, head_weights, out_piece),
        (True, True, True),
        [((length, model), bf16), ((model, head_cols), bf16), ((query_cols, model), bf16)],
        [((planes, piece_rows, model), bf16)],
    )

    proj = matmul(normed_all, head_full)
    query_proj = proj[:, :query_cols]
    key_proj = proj[:, query_cols : query_cols + width]
    values = proj[:, query_cols + width :].astype(bf16)
    cosine, sine = rope_tables(jnp.arange(length, dtype=jnp.int32), width)
    queries = prepare(query_proj, query_gain, cosine, sine).astype(bf16)
    keys = prepare(key_proj, key_gain, cosine, sine).astype(bf16)
    pair_rows = jnp.concatenate([keys, values], axis=1)
    out_rows, log_rows = attend_heads(queries, pair_rows, local_groups, width)

    half = model // 2
    scatter_scratch = [
        ((chips, tokens, model), bf16),
        ((chips, tokens, model), bf16),
        ((2, chips, tokens, half), bf16),
        ((halvings + 1, 2, chips, tokens, half), bf16),
    ]
    out_sum, cot_all = call(
        out_rows_kernel,
        sizes,
        1,
        (out_rows, out_slice, cot_rows),
        (True, True, True),
        [((tokens, model), f32), ((2 * planes, tokens, model), bf16)],
        scatter_scratch,
    )
    middle = source + out_sum
    second = rms_factor(middle)
    normed_mid = (middle * second * feedforward_gain).astype(bf16)
    (mid_all,) = call(
        mid_rows_kernel,
        sizes,
        2,
        (normed_mid,),
        (True,),
        [((2 * planes, tokens, model), bf16)],
        [],
    )
    cot_all = cot_all.reshape(-1, model)
    mid_all = mid_all.reshape(-1, model)
    gate_half = lax.dynamic_slice_in_dim(gate_weight, core * units, units, 1)
    up_half = lax.dynamic_slice_in_dim(up_weight, core * units, units, 1)
    down_half = lax.dynamic_slice_in_dim(down_weight, core * units, units, 1)
    hidden_grad = matmul(cot_all, down_half)
    gate = matmul(mid_all, gate_half)
    lifted = matmul(mid_all, up_half)
    hidden = activate(gate, lifted)
    gate_grad, lifted_grad = gate_back(hidden_grad, gate, lifted)

    mid_part = inner_cols(gate_grad, gate_half) + inner_cols(lifted_grad, up_half)
    mid_part = mid_part.astype(bf16).reshape(2 * planes, tokens, model)
    down_part = inner_cols(hidden, down_half).astype(bf16).reshape(2 * planes, tokens, model)
    part_down = inner_rows(cot_all, hidden).astype(bf16)
    part_gate = inner_rows(mid_all, gate_grad).astype(bf16)
    part_up = inner_rows(mid_all, lifted_grad).astype(bf16)

    line_scratch = [
        ((planes, tokens, model), bf16),
        ((planes, tokens, model), bf16),
        ((2, planes - 1, tokens, model), bf16),
    ]
    quarter = model // 4
    s_down, s_first, s_second, mid_grad = call(
        halve_kernel,
        sizes,
        3,
        (part_down, part_gate, part_up, mid_part),
        (False, False, False, False),
        [
            ((2, last_rows, units), bf16),
            ((2, last_rows, units), bf16),
            ((2, last_rows, units), bf16),
            ((tokens, model), f32),
        ],
        [((3, 2, quarter, units), bf16)]
        + [((3, 2, quarter >> stage, units), bf16) for stage in range(halvings)]
        + line_scratch,
    )

    feedforward_slope = jnp.sum(mid_grad * middle * second, axis=0)
    middle_grad = cot_rows.astype(f32) + norm_back(mid_grad, middle, second, feedforward_gain)
    middle_half = middle_grad.astype(bf16)
    middle_all, t_down, down_sum = call(
        spread_kernel,
        sizes,
        4,
        (middle_half, s_down, down_part),
        (True, True, False),
        [((length, model), bf16), ((2, last_rows, units), bf16), ((tokens, model), f32)],
        line_scratch,
    )
    block_rows = middle + down_sum

    def trade(value, bit):
        other = lax.ppermute(value, "seq", [(i, i ^ bit) for i in range(parts)])
        return (value.astype(f32) + other.astype(f32)).astype(bf16)

    t_first = trade(s_first, parts // 2)
    t_second = trade(s_second, 2)

    attended_grad = inner_cols(middle_all, out_slice).astype(bf16)
    query_back, pair_back = attend_back(
        queries, pair_rows, out_rows, log_rows, attended_grad, local_groups, width
    )
    key_back = pair_back[:, :width]
    value_back = pair_back[:, width:]
    _, query_pull = jax.vjp(
        lambda proj_in, gain_in: prepare(proj_in, gain_in, cosine, sine), query_proj, query_gain
    )
    query_proj_grad, query_slope = query_pull(query_back)
    _, key_pull = jax.vjp(
        lambda proj_in, gain_in: prepare(proj_in, gain_in, cosine, sine), key_proj, key_gain
    )
    key_proj_grad, key_slope = key_pull(key_back)
    halves = jnp.concatenate([query_proj_grad, key_proj_grad, value_back], axis=1).astype(bf16)
    head_part = inner_rows(normed_all, halves).astype(bf16).reshape(planes, shard, head_cols)
    out_part = inner_rows(out_rows, middle_all).astype(bf16)

    in_grad, head_sum, outer_sum = call(
        in_rows_kernel,
        sizes,
        5,
        (halves, head_full, head_part, out_part),
        (True, True, False, False),
        [((tokens, model), f32), ((shard, head_cols), bf16), ((piece_rows, model), bf16)],
        scatter_scratch
        + [
            ((planes, shard, head_cols), bf16),
            ((2, planes - 1, shard, head_cols), bf16),
            ((planes, piece_rows, model), bf16),
            ((2, planes - 1, piece_rows, model), bf16),
        ],
    )
    attention_slope = jnp.sum(in_grad * source * first, axis=0)
    input_rows = (middle_grad + norm_back(in_grad, source, first, attention_gain)).astype(bf16)

    slopes = jnp.concatenate([attention_slope, feedforward_slope, query_slope, key_slope])
    slope_cols = -(-slopes.shape[0] // 1024) * 128
    slopes = jnp.pad(slopes, (0, 8 * slope_cols - slopes.shape[0])).reshape(8, slope_cols)
    rounds = (parts * planes).bit_length() - 1
    grad_down, grad_gate, grad_up, head_all, outer_all, slopes = call(
        collect_kernel,
        sizes,
        6,
        (t_down, t_first, t_second, head_sum, outer_sum, slopes),
        (True,) * 6,
        [
            ((model, 2 * units), f32),
            ((model, 2 * units), f32),
            ((model, 2 * units), f32),
            ((parts, shard, head_cols), bf16),
            ((shard, model), bf16),
            ((8, slope_cols), f32),
        ],
        [
            ((3, model, units), bf16),
            ((3, model, units), bf16),
            ((4, 256, units), f32),
            ((rounds, 8, slope_cols), f32),
            ((rounds, 8, slope_cols), f32),
        ],
        [False, False, False, True, True, True],
    )
    grad_query = head_all[:, :, :query_cols].transpose(1, 0, 2).reshape(shard, -1).astype(f32)
    grad_pair = head_all[:, :, query_cols:].astype(f32)
    grad_pair = grad_pair.reshape(parts // copies, copies, shard, 2, width).sum(axis=1)
    grad_key = grad_pair[:, :, 0].transpose(1, 0, 2).reshape(shard, -1)
    grad_value = grad_pair[:, :, 1].transpose(1, 0, 2).reshape(shard, -1)
    grad_output = outer_all.astype(f32)
    slopes = slopes.reshape(-1)
    attention_slope = slopes[:model]
    feedforward_slope = slopes[model : 2 * model]
    query_slope = slopes[2 * model : 2 * model + width]
    key_slope = slopes[2 * model + width : 2 * model + 2 * width]
    block_out = block_rows.astype(bf16).reshape(1, tokens, model)
    input_grad = input_rows.reshape(1, tokens, model)
    return (
        block_out,
        input_grad,
        attention_slope,
        grad_query,
        grad_key,
        grad_value,
        grad_output,
        query_slope,
        key_slope,
        feedforward_slope,
        grad_gate,
        grad_up,
        grad_down,
    )


def solution(mesh):
    in_specs = (
        P("fsdp", "seq", None),
        P("fsdp", "seq", None),
        P(),
        P("fsdp", None),
        P("fsdp", None),
        P("fsdp", None),
        P("fsdp", None),
        P(),
        P(),
        P(),
        P(None, "fsdp"),
        P(None, "fsdp"),
        P(None, "fsdp"),
    )
    out_specs = (
        P("fsdp", "seq", None),
        P("fsdp", "seq", None),
        P(),
        P("fsdp", None),
        P("fsdp", None),
        P("fsdp", None),
        P("fsdp", None),
        P(),
        P(),
        P(),
        P(None, "fsdp"),
        P(None, "fsdp"),
        P(None, "fsdp"),
    )
    return jax.shard_map(
        per_device, mesh=mesh, in_specs=in_specs, out_specs=out_specs, check_vma=False
    )
```

```python
import functools

import jax
import jax.numpy as jnp
from jax import lax
from jax.experimental import pallas as pl
from jax.experimental.pallas import tpu as pltpu
from jax.sharding import PartitionSpec as P

EPS = 1e-05
THETA = 1000000.0


def rotate_half(values):
    half = values.shape[-1] // 2
    return jnp.concatenate([-values[..., half:], values[..., :half]], axis=-1)


def rope_tables(positions, width):
    exponents = jnp.arange(width // 2).astype(jnp.float32) * 2.0 / width
    rates = jnp.power(jnp.float32(THETA), -exponents)
    angle = positions.astype(jnp.float32)[:, None] * rates[None, :]
    angle = jnp.concatenate([angle, angle], axis=-1)
    return (jnp.cos(angle), jnp.sin(angle))


def prepare(proj, gain, cosine, sine):
    rows = proj.shape[0]
    width = gain.shape[0]
    split = proj.reshape(rows, -1, width)
    factor = lax.rsqrt(jnp.mean(split * split, axis=-1, keepdims=True) + EPS)
    normed = split * factor * gain
    turned = normed * cosine[:, None, :] + rotate_half(normed) * sine[:, None, :]
    return turned.reshape(rows, -1)


def matmul(left, right):
    return jnp.dot(left, right, preferred_element_type=jnp.float32)


def inner_rows(left, right):
    return lax.dot_general(
        left, right, (((0,), (0,)), ((), ())), preferred_element_type=jnp.float32
    )


def inner_cols(left, right):
    return lax.dot_general(
        left, right, (((1,), (1,)), ((), ())), preferred_element_type=jnp.float32
    )


def rms_factor(values):
    return lax.rsqrt(jnp.mean(values * values, axis=-1, keepdims=True) + EPS)


def norm_back(grad, values, factor, gain):
    scaled = grad * gain
    return factor * (
        scaled - values * factor * factor * jnp.mean(scaled * values, axis=-1, keepdims=True)
    )


def gate_back(hidden_grad, gate, lifted):
    sigma = jax.nn.sigmoid(gate)
    gate_grad = (hidden_grad * lifted * sigma * (1.0 + gate * (1.0 - sigma))).astype(jnp.bfloat16)
    lifted_grad = (hidden_grad * gate * sigma).astype(jnp.bfloat16)
    return (gate_grad, lifted_grad)


def activate(gate, lifted):
    return (gate * jax.nn.sigmoid(gate) * lifted).astype(jnp.bfloat16)


def split_heads(query_rows, pair_rows, groups, width):
    length = query_rows.shape[0]
    key_heads = pair_rows.shape[1] // (2 * width)
    queries = query_rows.reshape(length, key_heads, groups, width)
    keys = pair_rows[:, : key_heads * width].reshape(length, key_heads, width)
    values = pair_rows[:, key_heads * width :].reshape(length, key_heads, width)
    return (queries, keys, values, key_heads)


def attend_heads(query_rows, pair_rows, groups, width):
    length = query_rows.shape[0]
    queries, keys, values, key_heads = split_heads(query_rows, pair_rows, groups, width)
    block = min(512, length)
    scale = width ** (-0.5)
    offsets = jnp.arange(block)

    def query_step(index, state):
        out_rows, log_rows = state
        query_block = lax.dynamic_slice_in_dim(queries, index * block, block, 0)

        def key_step(inner, carry):
            summed, total = carry
            key_block = lax.dynamic_slice_in_dim(keys, inner * block, block, 0)
            value_block = lax.dynamic_slice_in_dim(values, inner * block, block, 0)
            scores = (
                jnp.einsum(
                    "qhgd,shd->hgqs", query_block, key_block, preferred_element_type=jnp.float32
                )
                * scale
            )
            allowed = (index * block + offsets)[:, None] >= (inner * block + offsets)[None, :]
            weights = jnp.where(allowed, jnp.exp(scores), 0.0)
            summed = summed + jnp.einsum(
                "hgqs,shd->hgqd",
                weights.astype(jnp.bfloat16),
                value_block,
                preferred_element_type=jnp.float32,
            )
            return (summed, total + jnp.sum(weights, axis=-1))

        initial = (
            jnp.zeros((key_heads, groups, block, width), jnp.float32),
            jnp.zeros((key_heads, groups, block), jnp.float32),
        )
        summed, total = lax.fori_loop(0, index + 1, key_step, initial)
        result = (summed / total[..., None]).astype(jnp.bfloat16)
        result = result.transpose(2, 0, 1, 3).reshape(block, key_heads * groups * width)
        out_rows = lax.dynamic_update_slice_in_dim(out_rows, result, index * block, 0)
        log_rows = lax.dynamic_update_slice_in_dim(log_rows, jnp.log(total), index * block, 2)
        return (out_rows, log_rows)

    start = (
        jnp.zeros((length, key_heads * groups * width), jnp.bfloat16),
        jnp.zeros((key_heads, groups, length), jnp.float32),
    )
    return lax.fori_loop(0, length // block, query_step, start)


def attend_back(query_rows, pair_rows, out_rows, log_rows, grad_rows, groups, width):
    length = query_rows.shape[0]
    queries, keys, values, key_heads = split_heads(query_rows, pair_rows, groups, width)
    outs = out_rows.reshape(length, key_heads, groups, width)
    grads = grad_rows.reshape(length, key_heads, groups, width)
    correction = jnp.sum(grads.astype(jnp.float32) * outs.astype(jnp.float32), axis=-1)
    block = min(512, length)
    scale = width ** (-0.5)
    offsets = jnp.arange(block)

    def query_step(index, state):
        query_grad, key_grad, value_grad = state
        query_block = lax.dynamic_slice_in_dim(queries, index * block, block, 0)
        grad_block = lax.dynamic_slice_in_dim(grads, index * block, block, 0)
        shift_block = lax.dynamic_slice_in_dim(correction, index * block, block, 0).transpose(
            1, 2, 0
        )
        log_block = lax.dynamic_slice_in_dim(log_rows, index * block, block, 2)

        def key_step(inner, carry):
            block_grad, key_sum, value_sum = carry
            key_block = lax.dynamic_slice_in_dim(keys, inner * block, block, 0)
            value_block = lax.dynamic_slice_in_dim(values, inner * block, block, 0)
            scores = (
                jnp.einsum(
                    "qhgd,shd->hgqs", query_block, key_block, preferred_element_type=jnp.float32
                )
                * scale
            )
            allowed = (index * block + offsets)[:, None] >= (inner * block + offsets)[None, :]
            weights = jnp.where(allowed, jnp.exp(scores - log_block[..., None]), 0.0)
            value_part = jnp.einsum(
                "hgqs,qhgd->shd",
                weights.astype(jnp.bfloat16),
                grad_block,
                preferred_element_type=jnp.float32,
            )
            prob_grad = jnp.einsum(
                "qhgd,shd->hgqs", grad_block, value_block, preferred_element_type=jnp.float32
            )
            score_grad = (weights * (prob_grad - shift_block[..., None]) * scale).astype(
                jnp.bfloat16
            )
            block_grad = block_grad + jnp.einsum(
                "hgqs,shd->qhgd", score_grad, key_block, preferred_element_type=jnp.float32
            )
            key_part = jnp.einsum(
                "hgqs,qhgd->shd", score_grad, query_block, preferred_element_type=jnp.float32
            )
            key_sum = lax.dynamic_update_slice_in_dim(
                key_sum,
                lax.dynamic_slice_in_dim(key_sum, inner * block, block, 0) + key_part,
                inner * block,
                0,
            )
            value_sum = lax.dynamic_update_slice_in_dim(
                value_sum,
                lax.dynamic_slice_in_dim(value_sum, inner * block, block, 0) + value_part,
                inner * block,
                0,
            )
            return (block_grad, key_sum, value_sum)

        initial = (jnp.zeros((block, key_heads, groups, width), jnp.float32), key_grad, value_grad)
        block_grad, key_grad, value_grad = lax.fori_loop(0, index + 1, key_step, initial)
        query_grad = lax.dynamic_update_slice_in_dim(query_grad, block_grad, index * block, 0)
        return (query_grad, key_grad, value_grad)

    state = (
        jnp.zeros((length, key_heads, groups, width), jnp.float32),
        jnp.zeros((length, key_heads, width), jnp.float32),
        jnp.zeros((length, key_heads, width), jnp.float32),
    )
    query_grad, key_grad, value_grad = lax.fori_loop(0, length // block, query_step, state)
    pair_grad = jnp.concatenate(
        [
            key_grad.reshape(length, key_heads * width),
            value_grad.reshape(length, key_heads * width),
        ],
        axis=1,
    )
    return (query_grad.reshape(length, key_heads * groups * width), pair_grad)


MESH = pl.DeviceIdType.MESH


def flip(index, mask, bits):
    for bit in bits:
        if mask & bit:
            index = index + bit - 2 * bit * ((index // bit) % 2)
    return index


class Place:
    def __init__(self, parts, planes):
        self.parts, self.planes = parts, planes
        self.seat = lax.axis_index("seq")
        self.plane = lax.axis_index("fsdp")
        self.core = self.seat % 2
        self.chip = self.seat // 2
        self.seat_bits = [1 << i for i in range(parts.bit_length() - 1)]
        self.chip_bits = self.seat_bits[1:]
        self.plane_bits = [1 << i for i in range(planes.bit_length() - 1)]

    def at(self, mask):
        return flip(self.seat, mask, self.seat_bits)

    def side(self, bit):
        return (self.seat // bit) % 2

    def colors(self):
        return (self.chip_bits, self.chip_bits[::-1])

    def enter(self, masks=(), line=False, plane_masks=()):
        barrier = pltpu.get_barrier_semaphore()
        peers = [{"seq": self.at(mask)} for mask in masks]
        if line:
            peers.append({"fsdp": (self.plane + 1) % self.planes})
            peers.append({"fsdp": (self.plane + self.planes - 1) % self.planes})
        for mask in plane_masks:
            peers.append({"fsdp": flip(self.plane, mask, self.plane_bits)})
        for peer in peers:
            pl.semaphore_signal(barrier, inc=1, device_id=peer, device_id_type=MESH)
        pl.semaphore_wait(barrier, len(peers))


class Wire:
    def __init__(self, sends, receives, locals_):
        self.sends, self.receives, self.locals = sends, receives, locals_
        self.count = self.local_count = 0
        self.open = []

    def remote(self, source, target, device):
        number = self.count
        self.count += 1
        return pltpu.make_async_remote_copy(
            src_ref=source,
            dst_ref=target,
            send_sem=self.sends.at[number],
            recv_sem=self.receives.at[number],
            device_id=device,
            device_id_type=MESH,
        )

    def send(self, source, target, device):
        copy = self.remote(source, target, device)
        copy.start()
        self.open.append(copy)
        return copy

    def local(self, source, target):
        number = self.local_count
        self.local_count += 1
        copy = pltpu.make_async_copy(source, target, self.locals.at[number])
        copy.start()
        return copy

    def close(self):
        for copy in self.open:
            copy.wait_send()


def add_rows(target, left, right, step=64):
    rows = target.shape[0]
    step = min(step, rows)

    def body(index, carry):
        at = pl.ds(pl.multiple_of(index * step, step), step)
        total = left[at, :].astype(jnp.float32) + right[at, :].astype(jnp.float32)
        target[at, :] = total.astype(target.dtype)
        return carry

    lax.fori_loop(0, rows // step, body, 0)


class LineGather:
    def __init__(self, wire, here, source, target, share=None):
        self.here = here
        planes, plane = here.planes, here.plane
        above = {"fsdp": (plane + 1) % planes}
        below = {"fsdp": (plane + planes - 1) % planes}
        self.ups, self.downs = {}, {}
        for step in range(1, planes):
            lower = (plane + planes - step + 1) % planes
            upper = (plane + step - 1) % planes
            first = step == 1
            self.ups[step] = wire.remote(
                source if first else target(lower), target(lower), above
            )
            self.downs[step] = wire.remote(
                source if first else target(upper), target(upper), below
            )
        self.shared = {}
        if share is not None:
            for step in range(1, planes):
                for way, shift in ((0, planes - step), (1, step)):
                    index = (plane + shift) % planes
                    self.shared[(step, way)] = wire.remote(
                        target(index), share(index), {"seq": here.at(1)}
                    )

    def start(self, step):
        planes, plane = self.here.planes, self.here.plane

        @pl.when((plane >= step - 1) & (plane <= planes - 2))
        def _():
            self.ups[step].start()

        @pl.when((plane + step <= planes) & (plane >= 1))
        def _():
            self.downs[step].start()

    def arrive(self, step):
        planes, plane = self.here.planes, self.here.plane

        @pl.when(plane >= step)
        def _():
            self.ups[step].wait_recv()
            if self.shared:
                self.shared[(step, 0)].start()

        @pl.when(plane + step <= planes - 1)
        def _():
            self.downs[step].wait_recv()
            if self.shared:
                self.shared[(step, 1)].start()

    def close(self):
        planes, plane = self.here.planes, self.here.plane
        for (step, way), copy in self.shared.items():

            @pl.when(plane >= step if way == 0 else plane + step <= planes - 1)
            def _(copy=copy):
                copy.wait()

        for step in range(1, planes):

            @pl.when((plane >= step - 1) & (plane <= planes - 2))
            def _(step=step):
                self.ups[step].wait_send()

            @pl.when((plane + step <= planes) & (plane >= 1))
            def _(step=step):
                self.downs[step].wait_send()


class LineScatter:
    def __init__(self, wire, here, term, landing):
        self.wire, self.here, self.term, self.landing = wire, here, term, landing
        planes, plane = here.planes, here.plane
        above = {"fsdp": (plane + 1) % planes}
        below = {"fsdp": (plane + planes - 1) % planes}
        self.ups, self.downs = {}, {}
        for step in range(1, planes):
            self.ups[step] = wire.remote(
                term((plane + planes - step) % planes), landing(0, step - 1), above
            )
            self.downs[step] = wire.remote(
                term((plane + step) % planes), landing(1, step - 1), below
            )

    def step(self, step):
        planes, plane = self.here.planes, self.here.plane
        mirror = planes - 1 - plane
        for way, (position, copies, dest) in enumerate(
            (
                (plane, self.ups, (plane + planes - step) % planes),
                (mirror, self.downs, (plane + step) % planes),
            )
        ):
            if step > 1:

                @pl.when((position >= 1) & (position <= step - 1))
                def _(way=way, copies=copies, dest=dest):
                    copies[step - 1].wait_recv()
                    term = self.term(dest)
                    add_rows(term, term, self.landing(way, step - 2))

            @pl.when(position <= step - 1)
            def _(copies=copies):
                copies[step].start()

    def finish(self, out):
        planes, plane = self.here.planes, self.here.plane
        own = self.term(plane)
        last = planes - 1

        @pl.when(plane >= 1)
        def _():
            self.ups[last].wait_recv()

        @pl.when(plane <= planes - 2)
        def _():
            self.downs[last].wait_recv()

        @pl.when(plane == 0)
        def _():
            add_rows(out, own, self.landing(1, last - 1))

        @pl.when(plane == planes - 1)
        def _():
            add_rows(out, own, self.landing(0, last - 1))

        @pl.when((plane >= 1) & (plane <= planes - 2))
        def _():
            add_rows(own, own, self.landing(0, last - 1))
            add_rows(out, own, self.landing(1, last - 1))

    def close(self):
        planes, plane = self.here.planes, self.here.plane
        mirror = planes - 1 - plane
        for step in range(1, planes):

            @pl.when(plane <= step - 1)
            def _(step=step):
                self.ups[step].wait_send()

            @pl.when(mirror <= step - 1)
            def _(step=step):
                self.downs[step].wait_send()


class PlaneGather:
    def __init__(self, wire, here, source, target):
        self.wire, self.here, self.source, self.target = wire, here, source, target
        self.incoming = {}

    def _send(self, mask, color, bit):
        here = self.here
        target = self.target(here.at(mask), color)
        source = self.source(color) if mask == 0 else target
        self.incoming[(mask ^ bit, color)] = self.wire.send(
            source, target, {"seq": here.at(bit)}
        )

    def start(self):
        for position in range(len(self.here.chip_bits)):
            for color, bits in enumerate(self.here.colors()):
                self._send(0, color, bits[position])
        for color in (0, 1):
            self._send(0, color, 1)

    def forward(self):
        here = self.here
        chips = here.parts // 2
        masks = sorted(
            (mask * 2 for mask in range(1, chips)), key=lambda mask: bin(mask).count("1")
        )
        for mask in masks:
            for color, bits in enumerate(here.colors()):
                self.incoming[(mask, color)].wait_recv()
                last = max(i for i, bit in enumerate(bits) if mask & bit)
                for bit in bits[last + 1 :]:
                    self._send(mask, color, bit)
                self._send(mask, color, 1)

    def finish(self):
        for mask in range(1, self.here.parts, 2):
            for color in (0, 1):
                self.incoming[(mask, color)].wait_recv()


class PlaneScatter:
    def __init__(self, wire, here, product, give, take, current, landing, model):
        self.wire, self.here, self.product = wire, here, product
        self.give, self.take, self.current, self.landing = give, take, current, landing
        self.model = model

    def start(self):
        here = self.here
        chips = here.parts // 2
        self.swaps = {}
        tokens = self.give.shape[1]
        seats = [2 * flip(here.chip, mask, [b // 2 for b in here.chip_bits]) for mask in range(chips)]
        for part in range(self.model // 512):
            columns = slice(part * 512, (part + 1) * 512)
            rows = self.product([seat + 1 - here.core for seat in seats], columns)
            for mask in range(chips):
                self.give[mask, :, columns] = rows[mask * tokens : (mask + 1) * tokens].astype(
                    self.give.dtype
                )
        for mask in range(chips)[::-1]:
            self.swaps[mask] = self.wire.send(
                self.give.at[mask], self.take.at[mask], {"seq": here.at(1)}
            )
        half = self.model // 2
        for part in range(self.model // 512):
            columns = slice(part * 512, (part + 1) * 512)
            rows = self.product([seat + here.core for seat in seats], columns)
            color, inside = divmod(part * 512, half)
            for mask in range(chips):
                self.current[color, mask, :, inside : inside + 512] = rows[
                    mask * tokens : (mask + 1) * tokens
                ].astype(self.current.dtype)

    def join(self):
        half = self.model // 2
        chips = self.here.parts // 2
        for mask in range(chips)[::-1]:
            self.swaps[mask].wait_recv()
            for color in (0, 1):
                mine = self.current.at[color, mask]
                add_rows(mine, mine, self.take.at[mask, :, pl.ds(color * half, half)])

    def stage(self, position):
        here = self.here
        self.moved = {}
        for color, bits in enumerate(here.colors()):
            bit = bits[position]
            done = sum(bits[:position])
            for mask in range(here.parts // 2):
                if mask * 2 & bit and not mask * 2 & done:
                    low = mask ^ (bit // 2)
                    self.moved[(color, low)] = self.wire.send(
                        self.current.at[color, mask],
                        self.landing.at[position, color, low],
                        {"seq": here.at(bit)},
                    )

    def settle(self, position, out):
        half = self.model // 2
        last = position == len(self.here.chip_bits) - 1
        for (color, low), copy in self.moved.items():
            copy.wait_recv()
            mine = self.current.at[color, low]
            if last:
                target = out.at[:, pl.ds(color * half, half)]
            else:
                target = mine
            add_rows(target, mine, self.landing.at[position, color, low])


def head_weights_kernel(parts, planes, x, w, o, x_all, w_all, o_slice, o_all, *sems):
    here = Place(parts, planes)
    wire = Wire(*sems)
    tokens, shard, rows = x.shape[0], w.shape[0], o.shape[0]
    half = tokens // 2
    chips = parts // 2
    chip_masks = [mask * 2 for mask in range(1, chips)]
    here.enter(chip_masks + [1], line=True)
    weights = LineGather(
        wire, here, w, lambda index: w_all.at[pl.ds(pl.multiple_of(index * shard, shard), shard)]
    )
    weights.start(1)
    plane_rows = PlaneGather(
        wire,
        here,
        lambda color: x.at[pl.ds(color * half, half)],
        lambda seat, color: x_all.at[pl.ds(pl.multiple_of(seat * tokens + color * half, half), half)],
    )
    plane_rows.start()
    kept = [
        wire.local(x, x_all.at[pl.ds(pl.multiple_of(here.seat * tokens, tokens), tokens)]),
        wire.local(w, w_all.at[pl.ds(pl.multiple_of(here.plane * shard, shard), shard)]),
        wire.local(o, o_all.at[here.plane]),
    ]
    outer = LineGather(wire, here, o, lambda index: o_all.at[index])
    weights.arrive(1)
    if planes > 2:
        weights.start(2)
    outer.start(1)
    plane_rows.forward()
    for step in range(2, planes):
        weights.arrive(step)
        if step + 1 < planes:
            weights.start(step + 1)
        outer.arrive(step - 1)
        outer.start(step)
    outer.arrive(planes - 1)
    plane_rows.finish()
    for copy in kept:
        copy.wait()
    dealt = []
    spot = o_slice.at[pl.ds(pl.multiple_of(here.chip * rows, rows), rows)]
    for mask in chip_masks:
        chip = here.at(mask) // 2
        dealt.append(wire.send(o_all.at[chip], spot, {"seq": here.at(mask)}))
    own = wire.local(o_all.at[here.chip], spot)
    own.wait()
    for copy in dealt:
        copy.wait_recv()
    wire.close()
    weights.close()
    outer.close()


def out_rows_kernel(
    parts, planes, a, w, c, out, c_all, give, take, current, landing, *sems
):
    here = Place(parts, planes)
    wire = Wire(*sems)
    tokens, model = c.shape
    here.enter([mask for mask in here.seat_bits], line=True)

    def product(seats, columns):
        rows = [a[pl.ds(pl.multiple_of(seat * tokens, tokens), tokens), :] for seat in seats]
        return jnp.dot(
            jnp.concatenate(rows, axis=0), w[:, columns], preferred_element_type=jnp.float32
        )

    mine, theirs = here.core * planes, (1 - here.core) * planes
    cots = LineGather(
        wire,
        here,
        c,
        lambda index: c_all.at[mine + index],
        lambda index: c_all.at[mine + index],
    )
    cots.start(1)
    own = wire.local(c, c_all.at[mine + here.plane])
    across = wire.send(c, c_all.at[mine + here.plane], {"seq": here.at(1)})
    rows = PlaneScatter(wire, here, product, give, take, current, landing, model)
    rows.start()
    rows.join()
    stages = len(here.chip_bits)
    for stage in range(stages):
        rows.stage(stage)
        if stage + 1 < planes:
            cots.arrive(stage + 1)
            if stage + 2 < planes:
                cots.start(stage + 2)
        rows.settle(stage, out)
    for step in range(stages + 1, planes):
        cots.arrive(step)
        if step + 1 < planes:
            cots.start(step + 1)
    own.wait()
    across.wait_recv()
    wire.close()
    cots.close()


def mid_rows_kernel(parts, planes, m, m_all, *sems):
    here = Place(parts, planes)
    wire = Wire(*sems)
    here.enter([1], line=True)
    mine = here.core * planes
    mids = LineGather(
        wire,
        here,
        m,
        lambda index: m_all.at[mine + index],
        lambda index: m_all.at[mine + index],
    )
    mids.start(1)
    own = wire.local(m, m_all.at[mine + here.plane])
    across = wire.send(m, m_all.at[mine + here.plane], {"seq": here.at(1)})
    for step in range(1, planes):
        mids.arrive(step)
        if step + 1 < planes:
            mids.start(step + 1)
    own.wait()
    across.wait_recv()
    wire.close()
    mids.close()


def halve_kernel(parts, planes, p_a, p_b, p_c, part, s_down, s_first, s_second, mid, keep, *rest):
    here = Place(parts, planes)
    stages = len(here.chip_bits) - 1
    landings, rest = rest[:stages], rest[stages:]
    current, take, line_landing, *sems = rest
    wire = Wire(*sems)
    here.enter(here.seat_bits, line=True)
    tokens = mid.shape[0]
    model = p_a.shape[0]
    swaps = TokenSum(wire, here, part, current, take, line_landing)
    swaps.start()
    terms = (p_a, p_b, p_c)
    moved, kept = {}, {}
    rows = model // 4
    for number, term in enumerate(terms):
        for color, bits in enumerate(here.colors()):
            base = color * (model // 2)
            away = pl.multiple_of(base + (1 - here.side(bits[0])) * rows, rows)
            stay = pl.multiple_of(base + here.side(bits[0]) * rows, rows)
            moved[(number, color)] = wire.send(
                term.at[pl.ds(away, rows)],
                landings[0].at[number, color],
                {"seq": here.at(bits[0])},
            )
            kept[(number, color)] = wire.local(
                term.at[pl.ds(stay, rows)], keep.at[number, color]
            )
    swaps.join()
    steps = list(range(1, planes))
    done = 0
    starts = {(number, color): 0 for number in range(3) for color in (0, 1)}
    for stage in range(stages):
        last = stage == stages - 1
        for number in range(3):
            take_steps = len(steps) * (stage * 3 + number + 1) // (stages * 3) - done
            for step in steps[done : done + take_steps]:
                swaps.step(step)
            done += take_steps
            for color, bits in enumerate(here.colors()):
                moved[(number, color)].wait_recv()
                if stage == 0:
                    kept[(number, color)].wait()
                begin = starts[(number, color)]
                mine = keep.at[number, color, pl.ds(begin, rows)]
                if last:
                    target = (
                        s_down.at[color]
                        if number == 0
                        else (s_first, s_second)[color].at[number - 1]
                    )
                    add_rows(target, mine, landings[stage].at[number, color])
                else:
                    add_rows(mine, mine, landings[stage].at[number, color])
                    bit = bits[stage + 1]
                    half = rows // 2
                    away = pl.multiple_of(begin + (1 - here.side(bit)) * half, half)
                    moved[(number, color)] = wire.send(
                        keep.at[number, color, pl.ds(away, half)],
                        landings[stage + 1].at[number, color],
                        {"seq": here.at(bit)},
                    )
                    starts[(number, color)] = pl.multiple_of(begin + here.side(bit) * half, half)
        rows //= 2
    swaps.finish(mid)
    wire.close()
    swaps.close()


class TokenSum:
    def __init__(self, wire, here, part, current, take, landing):
        self.wire, self.here, self.part = wire, here, part
        self.current, self.take = current, take
        self.line = LineScatter(
            wire, here, lambda index: current.at[index], lambda way, step: landing.at[way, step]
        )

    def start(self):
        here, planes = self.here, self.here.planes
        self.across = self.wire.send(
            self.part.at[pl.ds((1 - here.core) * planes, planes)], self.take, {"seq": here.at(1)}
        )
        self.own = self.wire.local(self.part.at[pl.ds(here.core * planes, planes)], self.current)

    def join(self):
        self.own.wait()
        self.across.wait_recv()

        def body(index, carry):
            row = self.current.at[index]
            add_rows(row, row, self.take.at[index])
            return carry

        lax.fori_loop(0, self.here.planes, body, 0)

    def step(self, step):
        self.line.step(step)

    def finish(self, out):
        self.line.finish(out)

    def close(self):
        self.line.close()


def spread_kernel(parts, planes, h, s, part, h_all, t, block, current, take, line_landing, *sems):
    here = Place(parts, planes)
    wire = Wire(*sems)
    here.enter(here.seat_bits, line=True)
    tokens = h.shape[0]
    half = tokens // 2
    rows = PlaneGather(
        wire,
        here,
        lambda color: h.at[pl.ds(color * half, half)],
        lambda seat, color: h_all.at[pl.ds(pl.multiple_of(seat * tokens + color * half, half), half)],
    )
    swaps = TokenSum(wire, here, part, current, take, line_landing)
    rows.start()
    own = wire.local(h, h_all.at[pl.ds(pl.multiple_of(here.seat * tokens, tokens), tokens)])
    swaps.start()
    moved = [
        wire.send(s.at[color], t.at[color], {"seq": here.at(bits[-1])})
        for color, bits in enumerate(here.colors())
    ]
    rows.forward()
    swaps.join()
    for step in range(1, planes):
        swaps.step(step)
    rows.finish()
    for color in (0, 1):
        moved[color].wait_recv()
        add_rows(t.at[color], t.at[color], s.at[color])
    own.wait()
    swaps.finish(block)
    wire.close()
    swaps.close()


def in_rows_kernel(
    parts,
    planes,
    a,
    w,
    head_part,
    out_part,
    t_down,
    t_first,
    t_second,
    out,
    head_sum,
    out_sum,
    near_down,
    far_down,
    near_gate,
    far_gate,
    give,
    take,
    current,
    landing,
    head_current,
    head_landing,
    dealt,
    out_landing,
    *sems,
):
    here = Place(parts, planes)
    wire = Wire(*sems)
    tokens, model = out.shape
    shard = head_sum.shape[0]
    rows_out = out_sum.shape[0]
    chips = parts // 2
    chip_masks = [mask * 2 for mask in range(1, chips)]
    here.enter(chip_masks + [1], line=True)
    head_own = wire.local(head_part, head_current)
    deals = []
    for mask in chip_masks:
        chip = here.at(mask) // 2
        deals.append(
            wire.send(
                out_part.at[pl.ds(pl.multiple_of(chip * rows_out, rows_out), rows_out)],
                dealt.at[here.chip],
                {"seq": here.at(mask)},
            )
        )
    deal_own = wire.local(
        out_part.at[pl.ds(pl.multiple_of(here.chip * rows_out, rows_out), rows_out)],
        dealt.at[here.chip],
    )

    def product(seats, columns):
        rows = [a[pl.ds(pl.multiple_of(seat * tokens, tokens), tokens), :] for seat in seats]
        return lax.dot_general(
            jnp.concatenate(rows, axis=0),
            w[columns, :],
            (((1,), (1,)), ((), ())),
            preferred_element_type=jnp.float32,
        )

    heads = LineScatter(
        wire, here, lambda index: head_current.at[index], lambda way, step: head_landing.at[way, step]
    )
    outer = LineScatter(
        wire, here, lambda index: dealt.at[index], lambda way, step: out_landing.at[way, step]
    )
    head_own.wait()
    heads.step(1)
    weights = [
        WeightGather(wire, here, (t_down.at[0], t_down.at[1]), near_down, far_down),
        WeightGather(wire, here, (t_first.at[0], t_second.at[0]), near_gate, far_gate),
    ]
    rows = PlaneScatter(wire, here, product, give, take, current, landing, model)
    rows.start()
    deal_own.wait()
    for copy in deals:
        copy.wait_recv()
    outer.step(1)
    rows.join()
    stages = len(here.chip_bits)
    for stage in range(stages):
        rows.stage(stage)
        if stage < 2:
            weights[stage].start()
        if stage + 2 < planes:
            heads.step(stage + 2)
            outer.step(stage + 2)
        rows.settle(stage, out)
    for step in range(stages + 2, planes):
        heads.step(step)
        outer.step(step)
    for weight in weights:
        weight.own()
    for weight in weights:
        weight.forward()
    heads.finish(head_sum)
    outer.finish(out_sum)
    for weight in weights:
        weight.finish()
    wire.close()
    heads.close()
    outer.close()


class WeightGather:
    def __init__(self, wire, here, finals, near, far):
        self.wire, self.here, self.near, self.far = wire, here, near, far
        self.size = finals[0].shape[0]
        model = near.shape[0]
        self.finals = finals
        self.starts = []
        for color, order in enumerate(here.colors()):
            start = color * (model // 2)
            rows = model // 2
            for bit in order[:-1]:
                rows //= 2
                start = start + here.side(bit) * rows
            self.starts.append(start)
        self.swaps, self.kept = [], []

    def _rows(self, start):
        return pl.ds(pl.multiple_of(start, self.size), self.size)

    def _pass(self, start, source, bit, rows):
        copy = self.wire.send(
            source, self.near.at[self._rows(start)], {"seq": self.here.at(bit)}
        )
        start = start + rows - 2 * rows * self.here.side(bit)
        return (start, self.near.at[self._rows(start)], copy)

    def _swap(self, start, source):
        self.swaps.append(
            self.wire.send(source, self.far.at[self._rows(start)], {"seq": self.here.at(1)})
        )

    def start(self):
        self.held = []
        for color, order in enumerate(self.here.colors()):
            source, start = self.finals[color], self.starts[color]
            pieces = [(start, source, None)]
            if order[:-1]:
                pieces.append(self._pass(start, source, order[-2], self.size))
            self.held.append(pieces)

    def own(self):
        for color in (0, 1):
            source, start = self.finals[color], self.starts[color]
            self._swap(start, source)
            self.kept.append(self.wire.local(source, self.near.at[self._rows(start)]))

    def forward(self):
        for color, order in enumerate(self.here.colors()):
            rest = order[:-1]
            pieces = self.held[color]
            rows = self.size
            for position in range(len(rest) - 1, -1, -1):
                for start, source, copy in pieces:
                    if copy is not None:
                        copy.wait_recv()
                        self._swap(start, source)
                pieces = [(start, source, None) for start, source, _ in pieces]
                rows *= 2
                if position > 0:
                    pieces = pieces + [
                        self._pass(start, source, rest[position - 1], rows)
                        for start, source, _ in pieces
                    ]

    def finish(self):
        for copy in self.swaps:
            copy.wait_recv()
        for copy in self.kept:
            copy.wait()


def widen_kernel(near, far, out):
    core = lax.axis_index("seq") % 2
    units = near.shape[1]
    out[:, pl.ds(pl.multiple_of(core * units, units), units)] = near[...].astype(out.dtype)
    out[:, pl.ds(pl.multiple_of((1 - core) * units, units), units)] = far[...].astype(out.dtype)


def collect_kernel(
    parts,
    planes,
    t_first,
    t_second,
    query,
    pair,
    outer,
    slope,
    near,
    far,
    query_all,
    pair_all,
    outer_all,
    slope_out,
    slope_sums,
    slope_landing,
    *sems,
):
    here = Place(parts, planes)
    wire = Wire(*sems)
    here.enter(here.seat_bits, plane_masks=here.plane_bits)
    shard, rows_out = query.shape[0], outer.shape[0]
    chips = parts // 2

    bits = [("seq", bit) for bit in here.seat_bits] + [("fsdp", bit) for bit in here.plane_bits]
    slope_copies = []

    def slope_send(number):
        axis, bit = bits[number]
        index = here.at(bit) if axis == "seq" else flip(here.plane, bit, here.plane_bits)
        source = slope if number == 0 else slope_sums.at[number - 1]
        slope_copies.append(wire.send(source, slope_landing.at[number], {axis: index}))

    def slope_add(number):
        slope_copies[number].wait_recv()
        source = slope if number == 0 else slope_sums.at[number - 1]
        target = slope_out if number == len(bits) - 1 else slope_sums.at[number]
        target[...] = source[...] + slope_landing[number]

    def row_gather(source, target):
        return PlaneGather(wire, here, source, target)

    slope_send(0)
    half, half_out = shard // 2, rows_out // 2
    columns = query.shape[1]
    own_start = (here.core * chips + here.chip) * rows_out
    gathers = [
        row_gather(
            lambda color: query.at[pl.ds(color * half, half)],
            lambda seat, color: query_all.at[
                pl.ds(color * half, half), pl.ds(pl.multiple_of(seat * columns, columns), columns)
            ],
        ),
        row_gather(
            lambda color: pair.at[pl.ds(color * half, half)],
            lambda seat, color: pair_all.at[seat, pl.ds(color * half, half)],
        ),
        row_gather(
            lambda color: outer.at[pl.ds(color * half_out, half_out)],
            lambda seat, color: outer_all.at[
                pl.ds(
                    pl.multiple_of(
                        ((seat % 2) * chips + seat // 2) * rows_out + color * half_out, half_out
                    ),
                    half_out,
                )
            ],
        ),
    ]
    for gather in gathers:
        gather.start()
    weight = WeightGather(wire, here, (t_first.at[1], t_second.at[1]), near, far)
    weight.start()
    own = [
        wire.local(query, query_all.at[:, pl.ds(pl.multiple_of(here.seat * columns, columns), columns)]),
        wire.local(pair, pair_all.at[here.seat]),
        wire.local(outer, outer_all.at[pl.ds(pl.multiple_of(own_start, rows_out), rows_out)]),
    ]
    slope_add(0)
    slope_send(1)
    for gather in gathers:
        gather.forward()
    weight.own()
    for number in range(1, len(bits)):
        slope_add(number)
        if number + 1 < len(bits):
            slope_send(number + 1)
    weight.forward()
    for gather in gathers:
        gather.finish()
    weight.finish()
    for copy in own:
        copy.wait()
    wire.close()


SENDS, LOCALS = 128, 96


def call(kernel, mesh_sizes, number, inputs, in_vmem, outputs, scratch, out_vmem=None):
    vmem = pl.BlockSpec(memory_space=pltpu.VMEM)
    anywhere = pl.BlockSpec(memory_space=pl.ANY)
    out_vmem = out_vmem or [True] * len(outputs)
    semaphores = [
        pltpu.SemaphoreType.DMA((SENDS,)),
        pltpu.SemaphoreType.DMA((SENDS,)),
        pltpu.SemaphoreType.DMA((LOCALS,)),
    ]
    return pl.pallas_call(
        functools.partial(kernel, *mesh_sizes),
        out_shape=[jax.ShapeDtypeStruct(shape, kind) for shape, kind in outputs],
        in_specs=[vmem if inside else anywhere for inside in in_vmem],
        out_specs=[vmem if inside else anywhere for inside in out_vmem],
        scratch_shapes=[pltpu.VMEM(shape, kind) for shape, kind in scratch] + semaphores,
        compiler_params=pltpu.CompilerParams(
            collective_id=number, has_side_effects=True, vmem_limit_bytes=VMEM_BYTES
        ),
    )(*inputs)


def widen(near, far):
    rows, units = near.shape
    step = min(256, rows)
    return pl.pallas_call(
        widen_kernel,
        grid=(rows // step,),
        out_shape=jax.ShapeDtypeStruct((rows, 2 * units), jnp.float32),
        in_specs=[pl.BlockSpec((step, units), lambda index: (index, 0))] * 2,
        out_specs=pl.BlockSpec((step, 2 * units), lambda index: (index, 0)),
        cost_estimate=pl.CostEstimate(
            flops=0, transcendentals=0, bytes_accessed=12 * rows * units
        ),
    )(near, far)


VMEM_BYTES = 62 * 1024 * 1024


def per_device(
    inputs,
    cotangent,
    attention_gain,
    query_weight,
    key_weight,
    value_weight,
    output_weight,
    query_gain,
    key_gain,
    feedforward_gain,
    gate_weight,
    up_weight,
    down_weight,
):
    tokens = inputs.shape[1]
    model = inputs.shape[2]
    width = query_gain.shape[0]
    pair_heads = key_weight.shape[1] // width
    parts = lax.axis_size("seq")
    planes = lax.axis_size("fsdp")
    sizes = (parts, planes)
    chips = parts // 2
    copies = max(1, parts // pair_heads)
    place = lax.axis_index("seq")
    plane = lax.axis_index("fsdp")
    core = place % 2
    query_cols = model // parts
    head_cols = query_cols + 2 * width
    local_groups = query_cols // width
    shard = query_weight.shape[0]
    piece_rows = shard // parts
    length = parts * tokens
    units = gate_weight.shape[1] // 2
    f32, bf16 = jnp.float32, jnp.bfloat16
    halvings = chips.bit_length() - 2
    last_rows = model // 2 >> halvings
    rows_in = inputs.reshape(tokens, model)
    cot_rows = cotangent.reshape(tokens, model)

    pair_index = place // copies
    head_weights = jnp.concatenate(
        [
            lax.dynamic_slice(query_weight, (0, place * query_cols), (shard, query_cols)),
            lax.dynamic_slice(key_weight, (0, pair_index * width), (shard, width)),
            lax.dynamic_slice(value_weight, (0, pair_index * width), (shard, width)),
        ],
        axis=1,
    )
    piece_index = core * chips + place // 2
    out_piece = lax.dynamic_slice_in_dim(output_weight, piece_index * piece_rows, piece_rows, 0)
    source = rows_in.astype(f32)
    first = rms_factor(source)
    normed_in = (source * first * attention_gain).astype(bf16)
    normed_all, head_full, out_slice = call(
        head_weights_kernel,
        sizes,
        0,
        (normed_in, head_weights, out_piece),
        (True, True, True),
        [((length, model), bf16), ((model, head_cols), bf16), ((query_cols, model), bf16)],
        [((planes, piece_rows, model), bf16)],
    )

    proj = matmul(normed_all, head_full)
    query_proj = proj[:, :query_cols]
    key_proj = proj[:, query_cols : query_cols + width]
    values = proj[:, query_cols + width :].astype(bf16)
    cosine, sine = rope_tables(jnp.arange(length, dtype=jnp.int32), width)
    queries = prepare(query_proj, query_gain, cosine, sine).astype(bf16)
    keys = prepare(key_proj, key_gain, cosine, sine).astype(bf16)
    pair_rows = jnp.concatenate([keys, values], axis=1)
    out_rows, log_rows = attend_heads(queries, pair_rows, local_groups, width)

    half = model // 2
    scatter_scratch = [
        ((chips, tokens, model), bf16),
        ((chips, tokens, model), bf16),
        ((2, chips, tokens, half), bf16),
        ((halvings + 1, 2, chips, tokens, half), bf16),
    ]
    out_sum, cot_all = call(
        out_rows_kernel,
        sizes,
        1,
        (out_rows, out_slice, cot_rows),
        (True, True, True),
        [((tokens, model), f32), ((2 * planes, tokens, model), bf16)],
        scatter_scratch,
    )
    middle = source + out_sum
    second = rms_factor(middle)
    normed_mid = (middle * second * feedforward_gain).astype(bf16)
    (mid_all,) = call(
        mid_rows_kernel,
        sizes,
        2,
        (normed_mid,),
        (True,),
        [((2 * planes, tokens, model), bf16)],
        [],
    )
    cot_all = cot_all.reshape(-1, model)
    mid_all = mid_all.reshape(-1, model)
    gate_half = lax.dynamic_slice_in_dim(gate_weight, core * units, units, 1)
    up_half = lax.dynamic_slice_in_dim(up_weight, core * units, units, 1)
    down_half = lax.dynamic_slice_in_dim(down_weight, core * units, units, 1)
    hidden_grad = matmul(cot_all, down_half)
    gate = matmul(mid_all, gate_half)
    lifted = matmul(mid_all, up_half)
    hidden = activate(gate, lifted)
    gate_grad, lifted_grad = gate_back(hidden_grad, gate, lifted)

    mid_part = inner_cols(gate_grad, gate_half) + inner_cols(lifted_grad, up_half)
    mid_part = mid_part.astype(bf16).reshape(2 * planes, tokens, model)
    down_part = inner_cols(hidden, down_half).astype(bf16).reshape(2 * planes, tokens, model)
    part_down = inner_rows(cot_all, hidden).astype(bf16)
    part_gate = inner_rows(mid_all, gate_grad).astype(bf16)
    part_up = inner_rows(mid_all, lifted_grad).astype(bf16)

    line_scratch = [
        ((planes, tokens, model), bf16),
        ((planes, tokens, model), bf16),
        ((2, planes - 1, tokens, model), bf16),
    ]
    quarter = model // 4
    s_down, s_first, s_second, mid_grad = call(
        halve_kernel,
        sizes,
        3,
        (part_down, part_gate, part_up, mid_part),
        (False, False, False, False),
        [
            ((2, last_rows, units), bf16),
            ((2, last_rows, units), bf16),
            ((2, last_rows, units), bf16),
            ((tokens, model), f32),
        ],
        [((3, 2, quarter, units), bf16)]
        + [((3, 2, quarter >> stage, units), bf16) for stage in range(halvings)]
        + line_scratch,
    )

    feedforward_slope = jnp.sum(mid_grad * middle * second, axis=0)
    middle_grad = cot_rows.astype(f32) + norm_back(mid_grad, middle, second, feedforward_gain)
    middle_half = middle_grad.astype(bf16)
    middle_all, t_down, down_sum = call(
        spread_kernel,
        sizes,
        4,
        (middle_half, s_down, down_part),
        (True, True, False),
        [((length, model), bf16), ((2, last_rows, units), bf16), ((tokens, model), f32)],
        line_scratch,
    )
    block_rows = middle + down_sum

    def trade(value, bit):
        other = lax.ppermute(value, "seq", [(i, i ^ bit) for i in range(parts)])
        return (value.astype(f32) + other.astype(f32)).astype(bf16)

    s_first, s_second, middle_all = lax.optimization_barrier((s_first, s_second, middle_all))
    t_first = trade(s_first, parts // 2)
    t_second = trade(s_second, 2)

    attended_grad = inner_cols(middle_all, out_slice).astype(bf16)
    query_back, pair_back = attend_back(
        queries, pair_rows, out_rows, log_rows, attended_grad, local_groups, width
    )
    key_back = pair_back[:, :width]
    value_back = pair_back[:, width:]
    _, query_pull = jax.vjp(
        lambda proj_in, gain_in: prepare(proj_in, gain_in, cosine, sine), query_proj, query_gain
    )
    query_proj_grad, query_slope = query_pull(query_back)
    _, key_pull = jax.vjp(
        lambda proj_in, gain_in: prepare(proj_in, gain_in, cosine, sine), key_proj, key_gain
    )
    key_proj_grad, key_slope = key_pull(key_back)
    halves = jnp.concatenate([query_proj_grad, key_proj_grad, value_back], axis=1).astype(bf16)
    head_part = inner_rows(normed_all, halves).astype(bf16).reshape(planes, shard, head_cols)
    out_part = inner_rows(out_rows, middle_all).astype(bf16)

    side = ((model, units), bf16)
    in_grad, head_sum, outer_sum, near_down, far_down, near_gate, far_gate = call(
        in_rows_kernel,
        sizes,
        5,
        (halves, head_full, head_part, out_part, t_down, t_first, t_second),
        (True, True, False, False, False, False, False),
        [((tokens, model), f32), ((shard, head_cols), bf16), ((piece_rows, model), bf16)]
        + [side] * 4,
        scatter_scratch
        + [
            ((planes, shard, head_cols), bf16),
            ((2, planes - 1, shard, head_cols), bf16),
            ((planes, piece_rows, model), bf16),
            ((2, planes - 1, piece_rows, model), bf16),
        ],
        [True] * 3 + [False] * 4,
    )
    attention_slope = jnp.sum(in_grad * source * first, axis=0)
    input_rows = (middle_grad + norm_back(in_grad, source, first, attention_gain)).astype(bf16)

    slopes = jnp.concatenate([attention_slope, feedforward_slope, query_slope, key_slope])
    slope_cols = -(-slopes.shape[0] // 1024) * 128
    slopes = jnp.pad(slopes, (0, 8 * slope_cols - slopes.shape[0])).reshape(8, slope_cols)
    rounds = (parts * planes).bit_length() - 1
    near_up, far_up, query_all, pair_all, outer_all, slopes = call(
        collect_kernel,
        sizes,
        6,
        (
            t_first,
            t_second,
            head_sum[:, :query_cols],
            head_sum[:, query_cols:],
            outer_sum,
            slopes,
        ),
        (False, False, True, True, True, True),
        [
            side,
            side,
            ((shard, model), bf16),
            ((parts, shard, 2 * width), bf16),
            ((shard, model), bf16),
            ((8, slope_cols), f32),
        ],
        [((rounds, 8, slope_cols), f32), ((rounds, 8, slope_cols), f32)],
        [False, False, True, True, True, True],
    )
    grad_down = widen(near_down, far_down)
    grad_gate = widen(near_gate, far_gate)
    grad_up = widen(near_up, far_up)
    grad_query = query_all.astype(f32)
    grad_pair = pair_all.astype(f32)
    grad_pair = grad_pair.reshape(parts // copies, copies, shard, 2, width).sum(axis=1)
    grad_key = grad_pair[:, :, 0].transpose(1, 0, 2).reshape(shard, -1)
    grad_value = grad_pair[:, :, 1].transpose(1, 0, 2).reshape(shard, -1)
    grad_output = outer_all.astype(f32)
    slopes = slopes.reshape(-1)
    attention_slope = slopes[:model]
    feedforward_slope = slopes[model : 2 * model]
    query_slope = slopes[2 * model : 2 * model + width]
    key_slope = slopes[2 * model + width : 2 * model + 2 * width]
    block_out = block_rows.astype(bf16).reshape(1, tokens, model)
    input_grad = input_rows.reshape(1, tokens, model)
    return (
        block_out,
        input_grad,
        attention_slope,
        grad_query,
        grad_key,
        grad_value,
        grad_output,
        query_slope,
        key_slope,
        feedforward_slope,
        grad_gate,
        grad_up,
        grad_down,
    )


def solution(mesh):
    in_specs = (
        P("fsdp", "seq", None),
        P("fsdp", "seq", None),
        P(),
        P("fsdp", None),
        P("fsdp", None),
        P("fsdp", None),
        P("fsdp", None),
        P(),
        P(),
        P(),
        P(None, "fsdp"),
        P(None, "fsdp"),
        P(None, "fsdp"),
    )
    out_specs = (
        P("fsdp", "seq", None),
        P("fsdp", "seq", None),
        P(),
        P("fsdp", None),
        P("fsdp", None),
        P("fsdp", None),
        P("fsdp", None),
        P(),
        P(),
        P(),
        P(None, "fsdp"),
        P(None, "fsdp"),
        P(None, "fsdp"),
    )
    return jax.shard_map(
        per_device, mesh=mesh, in_specs=in_specs, out_specs=out_specs, check_vma=False
    )
```

```python
import functools

import jax
import jax.numpy as jnp
from jax import lax
from jax.experimental import pallas as pl
from jax.experimental.pallas import tpu as pltpu
from jax.sharding import PartitionSpec as P

EPS = 1e-05
THETA = 1000000.0


def rotate_half(values):
    half = values.shape[-1] // 2
    return jnp.concatenate([-values[..., half:], values[..., :half]], axis=-1)


def rope_tables(positions, width):
    exponents = jnp.arange(width // 2).astype(jnp.float32) * 2.0 / width
    rates = jnp.power(jnp.float32(THETA), -exponents)
    angle = positions.astype(jnp.float32)[:, None] * rates[None, :]
    angle = jnp.concatenate([angle, angle], axis=-1)
    return (jnp.cos(angle), jnp.sin(angle))


def prepare(proj, gain, cosine, sine):
    rows = proj.shape[0]
    width = gain.shape[0]
    split = proj.reshape(rows, -1, width)
    factor = lax.rsqrt(jnp.mean(split * split, axis=-1, keepdims=True) + EPS)
    normed = split * factor * gain
    turned = normed * cosine[:, None, :] + rotate_half(normed) * sine[:, None, :]
    return turned.reshape(rows, -1)


def matmul(left, right):
    return jnp.dot(left, right, preferred_element_type=jnp.float32)


def inner_rows(left, right):
    return lax.dot_general(
        left, right, (((0,), (0,)), ((), ())), preferred_element_type=jnp.float32
    )


def inner_cols(left, right):
    return lax.dot_general(
        left, right, (((1,), (1,)), ((), ())), preferred_element_type=jnp.float32
    )


def rms_factor(values):
    return lax.rsqrt(jnp.mean(values * values, axis=-1, keepdims=True) + EPS)


def norm_back(grad, values, factor, gain):
    scaled = grad * gain
    return factor * (
        scaled - values * factor * factor * jnp.mean(scaled * values, axis=-1, keepdims=True)
    )


def gate_back(hidden_grad, gate, lifted):
    sigma = jax.nn.sigmoid(gate)
    gate_grad = (hidden_grad * lifted * sigma * (1.0 + gate * (1.0 - sigma))).astype(jnp.bfloat16)
    lifted_grad = (hidden_grad * gate * sigma).astype(jnp.bfloat16)
    return (gate_grad, lifted_grad)


def activate(gate, lifted):
    return (gate * jax.nn.sigmoid(gate) * lifted).astype(jnp.bfloat16)


def split_heads(query_rows, pair_rows, groups, width):
    length = query_rows.shape[0]
    key_heads = pair_rows.shape[1] // (2 * width)
    queries = query_rows.reshape(length, key_heads, groups, width)
    keys = pair_rows[:, : key_heads * width].reshape(length, key_heads, width)
    values = pair_rows[:, key_heads * width :].reshape(length, key_heads, width)
    return (queries, keys, values, key_heads)


def attend_heads(query_rows, pair_rows, groups, width):
    length = query_rows.shape[0]
    queries, keys, values, key_heads = split_heads(query_rows, pair_rows, groups, width)
    block = min(512, length)
    scale = width ** (-0.5)
    offsets = jnp.arange(block)

    def query_step(index, state):
        out_rows, log_rows = state
        query_block = lax.dynamic_slice_in_dim(queries, index * block, block, 0)

        def key_step(inner, carry):
            summed, total = carry
            key_block = lax.dynamic_slice_in_dim(keys, inner * block, block, 0)
            value_block = lax.dynamic_slice_in_dim(values, inner * block, block, 0)
            scores = (
                jnp.einsum(
                    "qhgd,shd->hgqs", query_block, key_block, preferred_element_type=jnp.float32
                )
                * scale
            )
            allowed = (index * block + offsets)[:, None] >= (inner * block + offsets)[None, :]
            weights = jnp.where(allowed, jnp.exp(scores), 0.0)
            summed = summed + jnp.einsum(
                "hgqs,shd->hgqd",
                weights.astype(jnp.bfloat16),
                value_block,
                preferred_element_type=jnp.float32,
            )
            return (summed, total + jnp.sum(weights, axis=-1))

        initial = (
            jnp.zeros((key_heads, groups, block, width), jnp.float32),
            jnp.zeros((key_heads, groups, block), jnp.float32),
        )
        summed, total = lax.fori_loop(0, index + 1, key_step, initial)
        result = (summed / total[..., None]).astype(jnp.bfloat16)
        result = result.transpose(2, 0, 1, 3).reshape(block, key_heads * groups * width)
        out_rows = lax.dynamic_update_slice_in_dim(out_rows, result, index * block, 0)
        log_rows = lax.dynamic_update_slice_in_dim(log_rows, jnp.log(total), index * block, 2)
        return (out_rows, log_rows)

    start = (
        jnp.zeros((length, key_heads * groups * width), jnp.bfloat16),
        jnp.zeros((key_heads, groups, length), jnp.float32),
    )
    return lax.fori_loop(0, length // block, query_step, start)


def attend_back(query_rows, pair_rows, out_rows, log_rows, grad_rows, groups, width):
    length = query_rows.shape[0]
    queries, keys, values, key_heads = split_heads(query_rows, pair_rows, groups, width)
    outs = out_rows.reshape(length, key_heads, groups, width)
    grads = grad_rows.reshape(length, key_heads, groups, width)
    correction = jnp.sum(grads.astype(jnp.float32) * outs.astype(jnp.float32), axis=-1)
    block = min(512, length)
    scale = width ** (-0.5)
    offsets = jnp.arange(block)

    def query_step(index, state):
        query_grad, key_grad, value_grad = state
        query_block = lax.dynamic_slice_in_dim(queries, index * block, block, 0)
        grad_block = lax.dynamic_slice_in_dim(grads, index * block, block, 0)
        shift_block = lax.dynamic_slice_in_dim(correction, index * block, block, 0).transpose(
            1, 2, 0
        )
        log_block = lax.dynamic_slice_in_dim(log_rows, index * block, block, 2)

        def key_step(inner, carry):
            block_grad, key_sum, value_sum = carry
            key_block = lax.dynamic_slice_in_dim(keys, inner * block, block, 0)
            value_block = lax.dynamic_slice_in_dim(values, inner * block, block, 0)
            scores = (
                jnp.einsum(
                    "qhgd,shd->hgqs", query_block, key_block, preferred_element_type=jnp.float32
                )
                * scale
            )
            allowed = (index * block + offsets)[:, None] >= (inner * block + offsets)[None, :]
            weights = jnp.where(allowed, jnp.exp(scores - log_block[..., None]), 0.0)
            value_part = jnp.einsum(
                "hgqs,qhgd->shd",
                weights.astype(jnp.bfloat16),
                grad_block,
                preferred_element_type=jnp.float32,
            )
            prob_grad = jnp.einsum(
                "qhgd,shd->hgqs", grad_block, value_block, preferred_element_type=jnp.float32
            )
            score_grad = (weights * (prob_grad - shift_block[..., None]) * scale).astype(
                jnp.bfloat16
            )
            block_grad = block_grad + jnp.einsum(
                "hgqs,shd->qhgd", score_grad, key_block, preferred_element_type=jnp.float32
            )
            key_part = jnp.einsum(
                "hgqs,qhgd->shd", score_grad, query_block, preferred_element_type=jnp.float32
            )
            key_sum = lax.dynamic_update_slice_in_dim(
                key_sum,
                lax.dynamic_slice_in_dim(key_sum, inner * block, block, 0) + key_part,
                inner * block,
                0,
            )
            value_sum = lax.dynamic_update_slice_in_dim(
                value_sum,
                lax.dynamic_slice_in_dim(value_sum, inner * block, block, 0) + value_part,
                inner * block,
                0,
            )
            return (block_grad, key_sum, value_sum)

        initial = (jnp.zeros((block, key_heads, groups, width), jnp.float32), key_grad, value_grad)
        block_grad, key_grad, value_grad = lax.fori_loop(0, index + 1, key_step, initial)
        query_grad = lax.dynamic_update_slice_in_dim(query_grad, block_grad, index * block, 0)
        return (query_grad, key_grad, value_grad)

    state = (
        jnp.zeros((length, key_heads, groups, width), jnp.float32),
        jnp.zeros((length, key_heads, width), jnp.float32),
        jnp.zeros((length, key_heads, width), jnp.float32),
    )
    query_grad, key_grad, value_grad = lax.fori_loop(0, length // block, query_step, state)
    pair_grad = jnp.concatenate(
        [
            key_grad.reshape(length, key_heads * width),
            value_grad.reshape(length, key_heads * width),
        ],
        axis=1,
    )
    return (query_grad.reshape(length, key_heads * groups * width), pair_grad)


MESH = pl.DeviceIdType.MESH


def flip(index, mask, bits):
    for bit in bits:
        if mask & bit:
            index = index + bit - 2 * bit * ((index // bit) % 2)
    return index


class Place:
    def __init__(self, parts, planes):
        self.parts, self.planes = parts, planes
        self.seat = lax.axis_index("seq")
        self.plane = lax.axis_index("fsdp")
        self.core = self.seat % 2
        self.chip = self.seat // 2
        self.seat_bits = [1 << i for i in range(parts.bit_length() - 1)]
        self.chip_bits = self.seat_bits[1:]
        self.plane_bits = [1 << i for i in range(planes.bit_length() - 1)]

    def at(self, mask):
        return flip(self.seat, mask, self.seat_bits)

    def side(self, bit):
        return (self.seat // bit) % 2

    def colors(self):
        return (self.chip_bits, self.chip_bits[::-1])

    def enter(self, masks=(), line=False, plane_masks=()):
        barrier = pltpu.get_barrier_semaphore()
        peers = [{"seq": self.at(mask)} for mask in masks]
        if line:
            peers.append({"fsdp": (self.plane + 1) % self.planes})
            peers.append({"fsdp": (self.plane + self.planes - 1) % self.planes})
        for mask in plane_masks:
            peers.append({"fsdp": flip(self.plane, mask, self.plane_bits)})
        for peer in peers:
            pl.semaphore_signal(barrier, inc=1, device_id=peer, device_id_type=MESH)
        pl.semaphore_wait(barrier, len(peers))


class Wire:
    def __init__(self, sends, receives, locals_):
        self.sends, self.receives, self.locals = sends, receives, locals_
        self.count = self.local_count = 0
        self.open = []

    def remote(self, source, target, device):
        number = self.count
        self.count += 1
        return pltpu.make_async_remote_copy(
            src_ref=source,
            dst_ref=target,
            send_sem=self.sends.at[number],
            recv_sem=self.receives.at[number],
            device_id=device,
            device_id_type=MESH,
        )

    def send(self, source, target, device):
        copy = self.remote(source, target, device)
        copy.start()
        self.open.append(copy)
        return copy

    def local(self, source, target):
        number = self.local_count
        self.local_count += 1
        copy = pltpu.make_async_copy(source, target, self.locals.at[number])
        copy.start()
        return copy

    def sent(self, copy):
        copy.wait_send()
        self.open = [other for other in self.open if other is not copy]

    def close(self):
        for copy in self.open:
            copy.wait_send()


def add_rows(target, left, right, step=64):
    rows = target.shape[0]
    step = min(step, rows)

    def body(index, carry):
        at = pl.ds(pl.multiple_of(index * step, step), step)
        total = left[at, :].astype(jnp.float32) + right[at, :].astype(jnp.float32)
        target[at, :] = total.astype(target.dtype)
        return carry

    lax.fori_loop(0, rows // step, body, 0)


class LineGather:
    def __init__(self, wire, here, source, target, share=None):
        self.here = here
        planes, plane = here.planes, here.plane
        above = {"fsdp": (plane + 1) % planes}
        below = {"fsdp": (plane + planes - 1) % planes}
        self.ups, self.downs = {}, {}
        for step in range(1, planes):
            lower = (plane + planes - step + 1) % planes
            upper = (plane + step - 1) % planes
            first = step == 1
            self.ups[step] = wire.remote(
                source if first else target(lower), target(lower), above
            )
            self.downs[step] = wire.remote(
                source if first else target(upper), target(upper), below
            )
        self.shared = {}
        if share is not None:
            for step in range(1, planes):
                for way, shift in ((0, planes - step), (1, step)):
                    index = (plane + shift) % planes
                    self.shared[(step, way)] = wire.remote(
                        target(index), share(index), {"seq": here.at(1)}
                    )

    def start(self, step):
        planes, plane = self.here.planes, self.here.plane

        @pl.when((plane >= step - 1) & (plane <= planes - 2))
        def _():
            self.ups[step].start()

        @pl.when((plane + step <= planes) & (plane >= 1))
        def _():
            self.downs[step].start()

    def arrive(self, step):
        planes, plane = self.here.planes, self.here.plane

        @pl.when(plane >= step)
        def _():
            self.ups[step].wait_recv()
            if self.shared:
                self.shared[(step, 0)].start()

        @pl.when(plane + step <= planes - 1)
        def _():
            self.downs[step].wait_recv()
            if self.shared:
                self.shared[(step, 1)].start()

    def close(self, shared_taken=False):
        planes, plane = self.here.planes, self.here.plane
        for (step, way), copy in self.shared.items():

            @pl.when(plane >= step if way == 0 else plane + step <= planes - 1)
            def _(copy=copy):
                copy.wait_send()
                if not shared_taken:
                    copy.wait_recv()

        for step in range(1, planes):

            @pl.when((plane >= step - 1) & (plane <= planes - 2))
            def _(step=step):
                self.ups[step].wait_send()

            @pl.when((plane + step <= planes) & (plane >= 1))
            def _(step=step):
                self.downs[step].wait_send()


class Lines:
    def __init__(self, members):
        self.members = members

    def start(self, step):
        for member in self.members:
            member.start(step)

    def pass_on(self, step):
        for member in self.members:
            member.arrive(step)
            if step + 1 < member.here.planes:
                member.start(step + 1)

    def step(self, step):
        for member in self.members:
            member.step(step)

    def close(self, *options):
        for member in self.members:
            member.close(*options)


def gather_lines(wire, here, source, target, share=None, cuts=2):
    rows = source.shape[0] // cuts
    members = []
    for cut in range(cuts):
        at = pl.ds(cut * rows, rows)
        members.append(
            LineGather(
                wire,
                here,
                source.at[at],
                lambda index, at=at: target(index).at[at],
                None if share is None else lambda index, at=at: share(index).at[at],
            )
        )
    return Lines(members)


class LineScatter:
    def __init__(self, wire, here, term, landing):
        self.wire, self.here, self.term, self.landing = wire, here, term, landing
        planes, plane = here.planes, here.plane
        above = {"fsdp": (plane + 1) % planes}
        below = {"fsdp": (plane + planes - 1) % planes}
        self.ups, self.downs = {}, {}
        for step in range(1, planes):
            self.ups[step] = wire.remote(
                term((plane + planes - step) % planes), landing(0, step - 1), above
            )
            self.downs[step] = wire.remote(
                term((plane + step) % planes), landing(1, step - 1), below
            )

    def step(self, step):
        planes, plane = self.here.planes, self.here.plane
        mirror = planes - 1 - plane
        for way, (position, copies, dest) in enumerate(
            (
                (plane, self.ups, (plane + planes - step) % planes),
                (mirror, self.downs, (plane + step) % planes),
            )
        ):
            if step > 1:

                @pl.when((position >= 1) & (position <= step - 1))
                def _(way=way, copies=copies, dest=dest):
                    copies[step - 1].wait_recv()
                    term = self.term(dest)
                    add_rows(term, term, self.landing(way, step - 2))

            @pl.when(position <= step - 1)
            def _(copies=copies):
                copies[step].start()

    def finish(self, out):
        planes, plane = self.here.planes, self.here.plane
        own = self.term(plane)
        last = planes - 1

        @pl.when(plane >= 1)
        def _():
            self.ups[last].wait_recv()

        @pl.when(plane <= planes - 2)
        def _():
            self.downs[last].wait_recv()

        @pl.when(plane == 0)
        def _():
            add_rows(out, own, self.landing(1, last - 1))

        @pl.when(plane == planes - 1)
        def _():
            add_rows(out, own, self.landing(0, last - 1))

        @pl.when((plane >= 1) & (plane <= planes - 2))
        def _():
            add_rows(own, own, self.landing(0, last - 1))
            add_rows(out, own, self.landing(1, last - 1))

    def close(self):
        planes, plane = self.here.planes, self.here.plane
        mirror = planes - 1 - plane
        for step in range(1, planes):

            @pl.when(plane <= step - 1)
            def _(step=step):
                self.ups[step].wait_send()

            @pl.when(mirror <= step - 1)
            def _(step=step):
                self.downs[step].wait_send()


class PlaneGather:
    def __init__(self, wire, here, source, target):
        self.wire, self.here, self.source, self.target = wire, here, source, target
        self.incoming = {}

    def _send(self, mask, color, bit):
        here = self.here
        target = self.target(here.at(mask), color)
        source = self.source(color) if mask == 0 else target
        self.incoming[(mask ^ bit, color)] = self.wire.send(
            source, target, {"seq": here.at(bit)}
        )

    def start(self):
        for position in range(len(self.here.chip_bits)):
            for color, bits in enumerate(self.here.colors()):
                self._send(0, color, bits[position])
        for color in (0, 1):
            self._send(0, color, 1)

    def hop(self, hops):
        here = self.here
        chips = here.parts // 2
        for mask in (mask * 2 for mask in range(1, chips)):
            if bin(mask).count("1") != hops:
                continue
            for color, bits in enumerate(here.colors()):
                self.incoming[(mask, color)].wait_recv()
                last = max(i for i, bit in enumerate(bits) if mask & bit)
                for bit in bits[last + 1 :]:
                    self._send(mask, color, bit)
                self._send(mask, color, 1)

    def hops(self, first=1):
        for hops in range(first, len(self.here.chip_bits) + 1):
            self.hop(hops)

    def finish(self):
        for mask in range(1, self.here.parts, 2):
            for color in (0, 1):
                self.incoming[(mask, color)].wait_recv()


class PlaneScatter:
    def __init__(self, wire, here, product, give, take, current, landing, model):
        self.wire, self.here, self.product = wire, here, product
        self.give, self.take, self.current, self.landing = give, take, current, landing
        self.model = model

    def start(self):
        here = self.here
        chips = here.parts // 2
        self.swaps = {}
        tokens = self.give.shape[1]
        seats = [2 * flip(here.chip, mask, [b // 2 for b in here.chip_bits]) for mask in range(chips)]
        for part in range(self.model // 512):
            columns = slice(part * 512, (part + 1) * 512)
            rows = self.product([seat + 1 - here.core for seat in seats], columns)
            for mask in range(chips):
                self.give[mask, :, columns] = rows[mask * tokens : (mask + 1) * tokens].astype(
                    self.give.dtype
                )
        for mask in range(chips)[::-1]:
            self.swaps[mask] = self.wire.send(
                self.give.at[mask], self.take.at[mask], {"seq": here.at(1)}
            )
        half = self.model // 2
        for part in range(self.model // 512):
            columns = slice(part * 512, (part + 1) * 512)
            rows = self.product([seat + here.core for seat in seats], columns)
            color, inside = divmod(part * 512, half)
            for mask in range(chips):
                self.current[color, mask, :, inside : inside + 512] = rows[
                    mask * tokens : (mask + 1) * tokens
                ].astype(self.current.dtype)

    def join(self):
        half = self.model // 2
        chips = self.here.parts // 2
        for mask in range(chips)[::-1]:
            self.swaps[mask].wait_recv()
            for color in (0, 1):
                mine = self.current.at[color, mask]
                add_rows(mine, mine, self.take.at[mask, :, pl.ds(color * half, half)])

    def stage(self, position):
        here = self.here
        self.moved = {}
        for color, bits in enumerate(here.colors()):
            bit = bits[position]
            done = sum(bits[:position])
            for mask in range(here.parts // 2):
                if mask * 2 & bit and not mask * 2 & done:
                    low = mask ^ (bit // 2)
                    self.moved[(color, low)] = self.wire.send(
                        self.current.at[color, mask],
                        self.landing.at[position, color, low],
                        {"seq": here.at(bit)},
                    )

    def settle(self, position, out):
        half = self.model // 2
        last = position == len(self.here.chip_bits) - 1
        for (color, low), copy in self.moved.items():
            copy.wait_recv()
            mine = self.current.at[color, low]
            if last:
                target = out.at[:, pl.ds(color * half, half)]
            else:
                target = mine
            add_rows(target, mine, self.landing.at[position, color, low])


def head_weights_kernel(parts, planes, x, w, o, x_all, w_all, o_slice, o_all, *sems):
    here = Place(parts, planes)
    wire = Wire(*sems)
    tokens, shard, rows = x.shape[0], w.shape[0], o.shape[0]
    half = tokens // 2
    chips = parts // 2
    chip_masks = [mask * 2 for mask in range(1, chips)]
    here.enter(chip_masks + [1], line=True)
    weights = gather_lines(
        wire, here, w, lambda index: w_all.at[pl.ds(pl.multiple_of(index * shard, shard), shard)]
    )
    weights.start(1)
    plane_rows = PlaneGather(
        wire,
        here,
        lambda color: x.at[pl.ds(color * half, half)],
        lambda seat, color: x_all.at[pl.ds(pl.multiple_of(seat * tokens + color * half, half), half)],
    )
    plane_rows.start()
    kept = [
        wire.local(x, x_all.at[pl.ds(pl.multiple_of(here.seat * tokens, tokens), tokens)]),
        wire.local(w, w_all.at[pl.ds(pl.multiple_of(here.plane * shard, shard), shard)]),
        wire.local(o, o_all.at[here.plane]),
    ]
    outer = gather_lines(wire, here, o, lambda index: o_all.at[index])
    weights.members[0].arrive(1)
    if planes > 2:
        weights.members[0].start(2)
    plane_rows.hop(1)
    weights.members[1].arrive(1)
    if planes > 2:
        weights.members[1].start(2)
    outer.start(1)
    plane_rows.hops(2)
    for step in range(2, planes):
        weights.pass_on(step)
        outer.pass_on(step - 1)
    outer.pass_on(planes - 1)
    plane_rows.finish()
    for copy in kept:
        copy.wait()
    dealt = []
    spot = o_slice.at[pl.ds(pl.multiple_of(here.chip * rows, rows), rows)]
    for mask in chip_masks:
        chip = here.at(mask) // 2
        dealt.append(wire.send(o_all.at[chip], spot, {"seq": here.at(mask)}))
    own = wire.local(o_all.at[here.chip], spot)
    own.wait()
    for copy in dealt:
        copy.wait_recv()
    wire.close()
    weights.close()
    outer.close()


def out_rows_kernel(
    parts, planes, a, w, c, out, c_all, give, take, current, landing, *sems
):
    here = Place(parts, planes)
    wire = Wire(*sems)
    tokens, model = c.shape
    here.enter([mask for mask in here.seat_bits], line=True)

    def product(seats, columns):
        rows = [a[pl.ds(pl.multiple_of(seat * tokens, tokens), tokens), :] for seat in seats]
        return jnp.dot(
            jnp.concatenate(rows, axis=0), w[:, columns], preferred_element_type=jnp.float32
        )

    def spot(index):
        return c_all.at[index, here.core]

    cots = gather_lines(wire, here, c, spot, spot)
    cots.start(1)
    own = wire.local(c, spot(here.plane))
    rows = PlaneScatter(wire, here, product, give, take, current, landing, model)
    rows.start()
    across = wire.send(c, spot(here.plane), {"seq": here.at(1)})
    rows.join()
    rows.stage(0)
    stages = len(here.chip_bits)
    for stage in range(stages):
        if stage + 1 < planes:
            cots.pass_on(stage + 1)
        rows.settle(stage, out)
        if stage + 1 < stages:
            rows.stage(stage + 1)
    for step in range(stages + 1, planes):
        cots.pass_on(step)
    own.wait()
    across.wait_recv()
    wire.close()
    cots.close()


def feed_kernel(
    parts,
    planes,
    m,
    cots,
    gate_weight,
    up_weight,
    down_weight,
    s_down,
    s_first,
    s_second,
    mid,
    down_give,
    down_keep,
    gate_half,
    up_half,
    down_half,
    mids,
    hidden,
    gate_grads,
    lifted_grads,
    away,
    *rest,
):
    here = Place(parts, planes)
    stages = len(here.chip_bits) - 1
    landings, rest = rest[:stages], rest[stages:]
    give, take, current, line_landing, *sems = rest
    wire = Wire(*sems)
    tokens, model = m.shape
    units = gate_half.shape[1]
    own_units = pl.ds(pl.multiple_of(here.core * units, units), units)
    loads = [
        wire.local(whole.at[:, own_units], part)
        for whole, part in (
            (gate_weight, gate_half),
            (up_weight, up_half),
            (down_weight, down_half),
        )
    ]
    here.enter(here.seat_bits, line=True)

    def spot(index):
        return mids.at[index, here.core]

    lines = gather_lines(wire, here, m, spot, spot)
    lines.start(1)
    across = wire.send(m, spot(here.plane), {"seq": here.at(1)})
    own = wire.local(m, spot(here.plane))

    def block(index):
        rows = pl.ds(pl.multiple_of(index * 2 * tokens, 2 * tokens), 2 * tokens)
        mid_rows = mids[index].reshape(2 * tokens, model)
        cot_rows = cots[rows, :]

        def part(number, carry):
            at = pl.ds(pl.multiple_of(number * 256, 256), 256)
            gate = jnp.dot(mid_rows, gate_half[:, at], preferred_element_type=jnp.float32)
            lifted = jnp.dot(mid_rows, up_half[:, at], preferred_element_type=jnp.float32)
            hidden_grad = jnp.dot(cot_rows, down_half[:, at], preferred_element_type=jnp.float32)
            sigma = 1.0 / (1.0 + jnp.exp(-gate))
            active = gate * sigma
            hidden[rows, at] = (active * lifted).astype(hidden.dtype)
            lifted_grads[rows, at] = (hidden_grad * active).astype(hidden.dtype)
            gate_grads[rows, at] = (
                hidden_grad * lifted * sigma * (1.0 + gate * (1.0 - sigma))
            ).astype(hidden.dtype)
            return carry

        lax.fori_loop(0, units // 256, part, 0)

    for load in loads:
        load.wait()
    own.wait()
    across.wait_recv()
    plane = here.plane
    block(plane)
    for step in range(1, planes):
        lines.pass_on(step)
        ups = jnp.where(plane >= step, 1, 0)
        downs = jnp.where(plane + step <= planes - 1, 1, 0)

        def arrived(number, carry, step=step, ups=ups):
            from_up = (number == 0) & (ups == 1)
            for way, chosen in ((0, from_up), (1, jnp.logical_not(from_up))):

                @pl.when(chosen)
                def _(way=way):
                    for line in lines.members:
                        line.shared[(step, way)].wait_recv()

            block(jnp.where(from_up, plane + planes - step, plane + step) % planes)
            return carry

        lax.fori_loop(0, ups + downs, arrived, 0)

    flat_mids = mids.reshape(2 * planes * tokens, model)
    pairs = ((cots, hidden), (flat_mids, gate_grads), (flat_mids, lifted_grads))
    quarter = model // 4
    moved = {}

    def gradient(target, pair, start):
        left, right = pair

        def part(number, carry):
            at = pl.ds(pl.multiple_of(start + number * 256, 256), 256)
            target[pl.ds(pl.multiple_of(number * 256, 256), 256), :] = lax.dot_general(
                left[:, at],
                right[...],
                (((0,), (0,)), ((), ())),
                preferred_element_type=jnp.float32,
            ).astype(target.dtype)
            return carry

        lax.fori_loop(0, quarter // 256, part, 0)

    def first_half(color, mine):
        bit = here.colors()[color][0]
        side = here.side(bit) if mine else 1 - here.side(bit)
        return pl.multiple_of(color * (model // 2) + side * quarter, quarter)

    def send_away(number):
        for color, bits in enumerate(here.colors()):
            gradient(away.at[number, color], pairs[number], first_half(color, False))
            moved[(number, color)] = wire.send(
                away.at[number, color], landings[0].at[number, color], {"seq": here.at(bits[0])}
            )

    def mid_term(target, core):
        rows = [pl.ds(pl.multiple_of((2 * p + core) * tokens, tokens), tokens) for p in range(planes)]
        gates = jnp.concatenate([gate_grads[at, :] for at in rows], axis=0)
        lifts = jnp.concatenate([lifted_grads[at, :] for at in rows], axis=0)

        def part(number, carry):
            at = pl.ds(pl.multiple_of(number * 256, 256), 256)
            term = lax.dot_general(
                gates, gate_half[at, :], (((1,), (1,)), ((), ())), preferred_element_type=jnp.float32
            ) + lax.dot_general(
                lifts, up_half[at, :], (((1,), (1,)), ((), ())), preferred_element_type=jnp.float32
            )
            target[:, :, at] = term.reshape(planes, tokens, 256).astype(target.dtype)
            return carry

        lax.fori_loop(0, model // 256, part, 0)

    def down_term(target, core):
        rows = [pl.ds(pl.multiple_of((2 * p + core) * tokens, tokens), tokens) for p in range(planes)]
        hiddens = jnp.concatenate([hidden[at, :] for at in rows], axis=0)

        def part(number, carry):
            at = pl.ds(pl.multiple_of(number * 256, 256), 256)
            term = lax.dot_general(
                hiddens, down_half[at, :], (((1,), (1,)), ((), ())), preferred_element_type=jnp.float32
            )
            target[:, :, at] = term.reshape(planes, tokens, 256).astype(target.dtype)
            return carry

        lax.fori_loop(0, model // 256, part, 0)

    send_away(0)
    swaps = TokenSum(wire, here, current, take, line_landing)
    mid_term(give, 1 - here.core)
    swaps.start(give)
    send_away(1)
    mid_term(current, here.core)
    swaps.join()
    swaps.step(1)
    send_away(2)
    for step in range(2, planes):
        swaps.step(step)

    def final(number, color):
        if number == 0:
            return s_down.at[color]
        return (s_first, s_second)[color].at[number - 1]

    wire.sent(swaps.across)
    down_term(give, 1 - here.core)
    down_term(take, here.core)
    handed = [wire.local(give, down_give), wire.local(take, down_keep)]
    rows = quarter
    keeps = {}
    for number in range(3):
        for color in (0, 1):
            keep = final(number, color) if stages == 1 else away.at[number, color]
            if stages > 1:
                wire.sent(moved[(number, color)])
            gradient(keep, pairs[number], first_half(color, True))
            keeps[(number, color)] = (keep, 0)
    swaps.finish(mid)
    for stage in range(stages):
        last = stage == stages - 1
        for number in range(3):
            for color, bits in enumerate(here.colors()):
                keep, begin = keeps[(number, color)]
                moved[(number, color)].wait_recv()
                mine = keep.at[pl.ds(begin, rows)]
                if last:
                    add_rows(final(number, color), mine, landings[stage].at[number, color])
                else:
                    add_rows(mine, mine, landings[stage].at[number, color])
                    bit = bits[stage + 1]
                    half = rows // 2
                    gone = pl.multiple_of(begin + (1 - here.side(bit)) * half, half)
                    moved[(number, color)] = wire.send(
                        keep.at[pl.ds(gone, half)],
                        landings[stage + 1].at[number, color],
                        {"seq": here.at(bit)},
                    )
                    keeps[(number, color)] = (
                        keep,
                        pl.multiple_of(begin + here.side(bit) * half, half),
                    )
        rows //= 2
    for copy in handed:
        copy.wait()
    wire.close()
    lines.close(True)
    swaps.close()


class TokenSum:
    def __init__(self, wire, here, current, take, landing):
        self.wire, self.here = wire, here
        self.current, self.take = current, take
        self.cuts = 2
        rows = current.shape[1] // self.cuts
        self.lines = []
        for cut in range(self.cuts):
            at = pl.ds(cut * rows, rows)
            self.lines.append(
                LineScatter(
                    wire,
                    here,
                    lambda index, at=at: current.at[index, at],
                    lambda way, step, at=at: landing.at[way, step, at],
                )
            )

    def start(self, give):
        self.across = self.wire.send(give, self.take, {"seq": self.here.at(1)})

    def join(self):
        self.across.wait_recv()

        def body(index, carry):
            row = self.current.at[index]
            add_rows(row, row, self.take.at[index])
            return carry

        lax.fori_loop(0, self.here.planes, body, 0)

    def step(self, step):
        for line in self.lines:
            line.step(step)

    def finish(self, out):
        rows = out.shape[0] // self.cuts
        for cut, line in enumerate(self.lines):
            line.finish(out.at[pl.ds(cut * rows, rows)])

    def close(self):
        for line in self.lines:
            line.close()


def spread_kernel(
    parts, planes, h, s, give, keep, h_all, t, block, current, take, line_landing, *sems
):
    here = Place(parts, planes)
    wire = Wire(*sems)
    here.enter(here.seat_bits, line=True)
    tokens = h.shape[0]
    half = tokens // 2
    rows = PlaneGather(
        wire,
        here,
        lambda color: h.at[pl.ds(color * half, half)],
        lambda seat, color: h_all.at[pl.ds(pl.multiple_of(seat * tokens + color * half, half), half)],
    )
    swaps = TokenSum(wire, here, current, take, line_landing)
    swaps.start(give)
    kept = wire.local(keep, current)
    rows.start()
    own = wire.local(h, h_all.at[pl.ds(pl.multiple_of(here.seat * tokens, tokens), tokens)])
    kept.wait()
    swaps.join()
    swaps.step(1)
    rows.hop(1)
    moved = [
        wire.send(s.at[color], t.at[color], {"seq": here.at(bits[-1])})
        for color, bits in enumerate(here.colors())
    ]
    for step in range(2, planes):
        if step == 3:
            rows.hops(2)
        swaps.step(step)
    if planes <= 3:
        rows.hops(2)
    rows.finish()
    for color in (0, 1):
        moved[color].wait_recv()
        add_rows(t.at[color], t.at[color], s.at[color])
    own.wait()
    swaps.finish(block)
    wire.close()
    swaps.close()


def in_rows_kernel(
    parts,
    planes,
    a,
    w,
    head_part,
    out_part,
    t_down,
    t_first,
    t_second,
    out,
    head_sum,
    out_sum,
    near_down,
    far_down,
    near_gate,
    far_gate,
    give,
    take,
    current,
    landing,
    head_current,
    head_landing,
    dealt,
    out_landing,
    *sems,
):
    here = Place(parts, planes)
    wire = Wire(*sems)
    tokens, model = out.shape
    shard = head_sum.shape[0]
    rows_out = out_sum.shape[0]
    chips = parts // 2
    chip_masks = [mask * 2 for mask in range(1, chips)]
    here.enter(chip_masks + [1], line=True)
    head_own = wire.local(head_part, head_current)
    deals = []
    for mask in chip_masks:
        chip = here.at(mask) // 2
        deals.append(
            wire.send(
                out_part.at[pl.ds(pl.multiple_of(chip * rows_out, rows_out), rows_out)],
                dealt.at[here.chip],
                {"seq": here.at(mask)},
            )
        )
    deal_own = wire.local(
        out_part.at[pl.ds(pl.multiple_of(here.chip * rows_out, rows_out), rows_out)],
        dealt.at[here.chip],
    )

    def product(seats, columns):
        rows = [a[pl.ds(pl.multiple_of(seat * tokens, tokens), tokens), :] for seat in seats]
        return lax.dot_general(
            jnp.concatenate(rows, axis=0),
            w[columns, :],
            (((1,), (1,)), ((), ())),
            preferred_element_type=jnp.float32,
        )

    heads = LineScatter(
        wire, here, lambda index: head_current.at[index], lambda way, step: head_landing.at[way, step]
    )
    outer = LineScatter(
        wire, here, lambda index: dealt.at[index], lambda way, step: out_landing.at[way, step]
    )
    head_own.wait()
    heads.step(1)
    weights = [
        WeightGather(wire, here, (t_down.at[0], t_down.at[1]), near_down, far_down),
        WeightGather(wire, here, (t_first.at[0], t_second.at[0]), near_gate, far_gate),
    ]
    weights[0].start()
    rows = PlaneScatter(wire, here, product, give, take, current, landing, model)
    rows.start()
    weights[0].own()
    heads.step(2)
    rows.join()
    rows.stage(0)
    deal_own.wait()
    for copy in deals:
        copy.wait_recv()
    outer.step(1)
    stages = len(here.chip_bits)
    for stage in range(stages):
        if stage + 3 < planes:
            heads.step(stage + 3)
        if stage + 2 < planes:
            outer.step(stage + 2)
        if stage == 0:
            weights[0].forward()
        rows.settle(stage, out)
        if stage + 1 < stages:
            rows.stage(stage + 1)
        if stage == 0:
            weights[1].start()
            weights[1].own()
    for step in range(stages + 3, planes):
        heads.step(step)
    for step in range(stages + 2, planes):
        outer.step(step)
    heads.finish(head_sum)
    outer.finish(out_sum)
    weights[1].forward()
    for weight in weights:
        weight.finish()
    wire.close()
    heads.close()
    outer.close()


class WeightGather:
    def __init__(self, wire, here, finals, near, far):
        self.wire, self.here, self.near, self.far = wire, here, near, far
        self.size = finals[0].shape[0]
        model = near.shape[0]
        self.finals = finals
        self.starts = []
        for color, order in enumerate(here.colors()):
            start = color * (model // 2)
            rows = model // 2
            for bit in order[:-1]:
                rows //= 2
                start = start + here.side(bit) * rows
            self.starts.append(start)
        self.swaps, self.kept = [], []

    def _rows(self, start):
        return pl.ds(pl.multiple_of(start, self.size), self.size)

    def _pass(self, start, source, bit, rows):
        copy = self.wire.send(
            source, self.near.at[self._rows(start)], {"seq": self.here.at(bit)}
        )
        start = start + rows - 2 * rows * self.here.side(bit)
        return (start, self.near.at[self._rows(start)], copy)

    def _swap(self, start, source):
        self.swaps.append(
            self.wire.send(source, self.far.at[self._rows(start)], {"seq": self.here.at(1)})
        )

    def start(self):
        self.held = []
        for color, order in enumerate(self.here.colors()):
            source, start = self.finals[color], self.starts[color]
            pieces = [(start, source, None)]
            if order[:-1]:
                pieces.append(self._pass(start, source, order[-2], self.size))
            self.held.append(pieces)

    def own(self):
        for color in (0, 1):
            source, start = self.finals[color], self.starts[color]
            self._swap(start, source)
            self.kept.append(self.wire.local(source, self.near.at[self._rows(start)]))

    def forward(self):
        for color, order in enumerate(self.here.colors()):
            rest = order[:-1]
            pieces = self.held[color]
            rows = self.size
            for position in range(len(rest) - 1, -1, -1):
                for start, source, copy in pieces:
                    if copy is not None:
                        copy.wait_recv()
                        self._swap(start, source)
                pieces = [(start, source, None) for start, source, _ in pieces]
                rows *= 2
                if position > 0:
                    pieces = pieces + [
                        self._pass(start, source, rest[position - 1], rows)
                        for start, source, _ in pieces
                    ]

    def finish(self):
        for copy in self.swaps:
            copy.wait_recv()
        for copy in self.kept:
            copy.wait()


def widen_kernel(near, far, out):
    core = lax.axis_index("seq") % 2
    units = near.shape[1]
    out[:, pl.ds(pl.multiple_of(core * units, units), units)] = near[...].astype(out.dtype)
    out[:, pl.ds(pl.multiple_of((1 - core) * units, units), units)] = far[...].astype(out.dtype)


def collect_kernel(
    parts,
    planes,
    t_first,
    t_second,
    query,
    pair,
    outer,
    slope,
    near,
    far,
    query_all,
    pair_all,
    outer_all,
    slope_out,
    slope_sums,
    slope_landing,
    *sems,
):
    here = Place(parts, planes)
    wire = Wire(*sems)
    here.enter(here.seat_bits, plane_masks=here.plane_bits)
    shard, rows_out = query.shape[0], outer.shape[0]
    chips = parts // 2

    bits = [("seq", bit) for bit in here.seat_bits] + [("fsdp", bit) for bit in here.plane_bits]
    slope_copies = []

    def slope_send(number):
        axis, bit = bits[number]
        index = here.at(bit) if axis == "seq" else flip(here.plane, bit, here.plane_bits)
        source = slope if number == 0 else slope_sums.at[number - 1]
        slope_copies.append(wire.send(source, slope_landing.at[number], {axis: index}))

    def slope_add(number):
        slope_copies[number].wait_recv()
        source = slope if number == 0 else slope_sums.at[number - 1]
        target = slope_out if number == len(bits) - 1 else slope_sums.at[number]
        target[...] = source[...] + slope_landing[number]

    def row_gather(source, target):
        return PlaneGather(wire, here, source, target)

    slope_send(0)
    half, half_out = shard // 2, rows_out // 2
    columns = query.shape[1]
    own_start = (here.core * chips + here.chip) * rows_out
    gathers = [
        row_gather(
            lambda color: query.at[pl.ds(color * half, half)],
            lambda seat, color: query_all.at[
                pl.ds(color * half, half), pl.ds(pl.multiple_of(seat * columns, columns), columns)
            ],
        ),
        row_gather(
            lambda color: pair.at[pl.ds(color * half, half)],
            lambda seat, color: pair_all.at[seat, pl.ds(color * half, half)],
        ),
        row_gather(
            lambda color: outer.at[pl.ds(color * half_out, half_out)],
            lambda seat, color: outer_all.at[
                pl.ds(
                    pl.multiple_of(
                        ((seat % 2) * chips + seat // 2) * rows_out + color * half_out, half_out
                    ),
                    half_out,
                )
            ],
        ),
    ]
    for gather in gathers:
        gather.start()
    weight = WeightGather(wire, here, (t_first.at[1], t_second.at[1]), near, far)
    own = [
        wire.local(query, query_all.at[:, pl.ds(pl.multiple_of(here.seat * columns, columns), columns)]),
        wire.local(pair, pair_all.at[here.seat]),
        wire.local(outer, outer_all.at[pl.ds(pl.multiple_of(own_start, rows_out), rows_out)]),
    ]
    slope_add(0)
    slope_send(1)
    for gather in gathers:
        gather.hop(1)
    weight.start()
    weight.own()
    for number in range(1, len(bits)):
        slope_add(number)
        if number + 1 < len(bits):
            slope_send(number + 1)
        if number == 2:
            for gather in gathers:
                gather.hops(2)
    weight.forward()
    for gather in gathers:
        gather.finish()
    weight.finish()
    for copy in own:
        copy.wait()
    wire.close()


SENDS, LOCALS = 128, 96


def call(kernel, mesh_sizes, number, inputs, in_vmem, outputs, scratch, out_vmem=None):
    vmem = pl.BlockSpec(memory_space=pltpu.VMEM)
    anywhere = pl.BlockSpec(memory_space=pl.ANY)
    out_vmem = out_vmem or [True] * len(outputs)
    semaphores = [
        pltpu.SemaphoreType.DMA((SENDS,)),
        pltpu.SemaphoreType.DMA((SENDS,)),
        pltpu.SemaphoreType.DMA((LOCALS,)),
    ]
    return pl.pallas_call(
        functools.partial(kernel, *mesh_sizes),
        out_shape=[jax.ShapeDtypeStruct(shape, kind) for shape, kind in outputs],
        in_specs=[vmem if inside else anywhere for inside in in_vmem],
        out_specs=[vmem if inside else anywhere for inside in out_vmem],
        scratch_shapes=[pltpu.VMEM(shape, kind) for shape, kind in scratch] + semaphores,
        compiler_params=pltpu.CompilerParams(
            collective_id=number, has_side_effects=True, vmem_limit_bytes=VMEM_BYTES
        ),
    )(*inputs)


def widen(near, far):
    rows, units = near.shape
    step = min(256, rows)
    return pl.pallas_call(
        widen_kernel,
        grid=(rows // step,),
        out_shape=jax.ShapeDtypeStruct((rows, 2 * units), jnp.float32),
        in_specs=[pl.BlockSpec((step, units), lambda index: (index, 0))] * 2,
        out_specs=pl.BlockSpec((step, 2 * units), lambda index: (index, 0)),
        cost_estimate=pl.CostEstimate(
            flops=0, transcendentals=0, bytes_accessed=12 * rows * units
        ),
    )(near, far)


VMEM_BYTES = 67_000_000


def per_device(
    inputs,
    cotangent,
    attention_gain,
    query_weight,
    key_weight,
    value_weight,
    output_weight,
    query_gain,
    key_gain,
    feedforward_gain,
    gate_weight,
    up_weight,
    down_weight,
):
    tokens = inputs.shape[1]
    model = inputs.shape[2]
    width = query_gain.shape[0]
    pair_heads = key_weight.shape[1] // width
    parts = lax.axis_size("seq")
    planes = lax.axis_size("fsdp")
    sizes = (parts, planes)
    chips = parts // 2
    copies = max(1, parts // pair_heads)
    place = lax.axis_index("seq")
    plane = lax.axis_index("fsdp")
    core = place % 2
    query_cols = model // parts
    head_cols = query_cols + 2 * width
    local_groups = query_cols // width
    shard = query_weight.shape[0]
    piece_rows = shard // parts
    length = parts * tokens
    units = gate_weight.shape[1] // 2
    f32, bf16 = jnp.float32, jnp.bfloat16
    halvings = chips.bit_length() - 2
    last_rows = model // 2 >> halvings
    rows_in = inputs.reshape(tokens, model)
    cot_rows = cotangent.reshape(tokens, model)

    pair_index = place // copies
    head_weights = jnp.concatenate(
        [
            lax.dynamic_slice(query_weight, (0, place * query_cols), (shard, query_cols)),
            lax.dynamic_slice(key_weight, (0, pair_index * width), (shard, width)),
            lax.dynamic_slice(value_weight, (0, pair_index * width), (shard, width)),
        ],
        axis=1,
    )
    piece_index = core * chips + place // 2
    out_piece = lax.dynamic_slice_in_dim(output_weight, piece_index * piece_rows, piece_rows, 0)
    source = rows_in.astype(f32)
    first = rms_factor(source)
    normed_in = (source * first * attention_gain).astype(bf16)
    normed_all, head_full, out_slice = call(
        head_weights_kernel,
        sizes,
        0,
        (normed_in, head_weights, out_piece),
        (True, True, True),
        [((length, model), bf16), ((model, head_cols), bf16), ((query_cols, model), bf16)],
        [((planes, piece_rows, model), bf16)],
    )

    proj = matmul(normed_all, head_full)
    query_proj = proj[:, :query_cols]
    key_proj = proj[:, query_cols : query_cols + width]
    values = proj[:, query_cols + width :].astype(bf16)
    cosine, sine = rope_tables(jnp.arange(length, dtype=jnp.int32), width)
    queries = prepare(query_proj, query_gain, cosine, sine).astype(bf16)
    keys = prepare(key_proj, key_gain, cosine, sine).astype(bf16)
    pair_rows = jnp.concatenate([keys, values], axis=1)
    out_rows, log_rows = attend_heads(queries, pair_rows, local_groups, width)

    half = model // 2
    scatter_scratch = [
        ((chips, tokens, model), bf16),
        ((chips, tokens, model), bf16),
        ((2, chips, tokens, half), bf16),
        ((halvings + 1, 2, chips, tokens, half), bf16),
    ]
    out_sum, cot_all = call(
        out_rows_kernel,
        sizes,
        1,
        (out_rows, out_slice, cot_rows),
        (True, True, True),
        [((tokens, model), f32), ((planes, 2, tokens, model), bf16)],
        scatter_scratch,
    )
    middle = source + out_sum
    second = rms_factor(middle)
    normed_mid = (middle * second * feedforward_gain).astype(bf16)
    quarter = model // 4
    rows_shape = (planes, tokens, model)
    line_scratch = [
        (rows_shape, bf16),
        (rows_shape, bf16),
        ((2, planes - 1, tokens, model), bf16),
    ]
    acts = (2 * planes * tokens, units)
    s_down, s_first, s_second, mid_grad, down_give, down_keep = call(
        feed_kernel,
        sizes,
        2,
        (normed_mid, cot_all.reshape(-1, model), gate_weight, up_weight, down_weight),
        (True, True, False, False, False),
        [
            ((2, last_rows, units), bf16),
            ((2, last_rows, units), bf16),
            ((2, last_rows, units), bf16),
            ((tokens, model), f32),
            (rows_shape, bf16),
            (rows_shape, bf16),
        ],
        [((model, units), bf16)] * 3
        + [((planes, 2, tokens, model), bf16)]
        + [(acts, bf16)] * 3
        + [((3, 2, quarter, units), bf16)]
        + [((3, 2, quarter >> stage, units), bf16) for stage in range(halvings)]
        + [(rows_shape, bf16)]
        + line_scratch,
        [True] * 4 + [False] * 2,
    )

    feedforward_slope = jnp.sum(mid_grad * middle * second, axis=0)
    middle_grad = cot_rows.astype(f32) + norm_back(mid_grad, middle, second, feedforward_gain)
    middle_half = middle_grad.astype(bf16)
    middle_all, t_down, down_sum = call(
        spread_kernel,
        sizes,
        4,
        (middle_half, s_down, down_give, down_keep),
        (True, True, False, False),
        [((length, model), bf16), ((2, last_rows, units), bf16), ((tokens, model), f32)],
        line_scratch,
    )
    block_rows = middle + down_sum

    def trade(value, bit):
        other = lax.ppermute(value, "seq", [(i, i ^ bit) for i in range(parts)])
        return (value.astype(f32) + other.astype(f32)).astype(bf16)

    s_first, s_second, middle_all = lax.optimization_barrier((s_first, s_second, middle_all))
    t_first = trade(s_first, parts // 2)
    t_second = trade(s_second, 2)

    attended_grad = inner_cols(middle_all, out_slice).astype(bf16)
    query_back, pair_back = attend_back(
        queries, pair_rows, out_rows, log_rows, attended_grad, local_groups, width
    )
    key_back = pair_back[:, :width]
    value_back = pair_back[:, width:]
    _, query_pull = jax.vjp(
        lambda proj_in, gain_in: prepare(proj_in, gain_in, cosine, sine), query_proj, query_gain
    )
    query_proj_grad, query_slope = query_pull(query_back)
    _, key_pull = jax.vjp(
        lambda proj_in, gain_in: prepare(proj_in, gain_in, cosine, sine), key_proj, key_gain
    )
    key_proj_grad, key_slope = key_pull(key_back)
    halves = jnp.concatenate([query_proj_grad, key_proj_grad, value_back], axis=1).astype(bf16)
    head_part = inner_rows(normed_all, halves).astype(bf16).reshape(planes, shard, head_cols)
    out_part = inner_rows(out_rows, middle_all).astype(bf16)

    side = ((model, units), bf16)
    in_grad, head_sum, outer_sum, near_down, far_down, near_gate, far_gate = call(
        in_rows_kernel,
        sizes,
        5,
        (halves, head_full, head_part, out_part, t_down, t_first, t_second),
        (True, True, False, False, True, True, True),
        [((tokens, model), f32), ((shard, head_cols), bf16), ((piece_rows, model), bf16)]
        + [side] * 4,
        scatter_scratch
        + [
            ((planes, shard, head_cols), bf16),
            ((2, planes - 1, shard, head_cols), bf16),
            ((planes, piece_rows, model), bf16),
            ((2, planes - 1, piece_rows, model), bf16),
        ],
        [True] * 3 + [False] * 4,
    )
    attention_slope = jnp.sum(in_grad * source * first, axis=0)
    input_rows = (middle_grad + norm_back(in_grad, source, first, attention_gain)).astype(bf16)

    slopes = jnp.concatenate([attention_slope, feedforward_slope, query_slope, key_slope])
    slope_cols = -(-slopes.shape[0] // 1024) * 128
    slopes = jnp.pad(slopes, (0, 8 * slope_cols - slopes.shape[0])).reshape(8, slope_cols)
    rounds = (parts * planes).bit_length() - 1
    near_up, far_up, query_all, pair_all, outer_all, slopes = call(
        collect_kernel,
        sizes,
        6,
        (
            t_first,
            t_second,
            head_sum[:, :query_cols],
            head_sum[:, query_cols:],
            outer_sum,
            slopes,
        ),
        (True, True, True, True, True, True),
        [
            side,
            side,
            ((shard, model), bf16),
            ((parts, shard, 2 * width), bf16),
            ((shard, model), bf16),
            ((8, slope_cols), f32),
        ],
        [((rounds, 8, slope_cols), f32), ((rounds, 8, slope_cols), f32)],
        [False, False, True, True, True, True],
    )
    grad_down = widen(near_down, far_down)
    grad_gate = widen(near_gate, far_gate)
    grad_up = widen(near_up, far_up)
    grad_query = query_all.astype(f32)
    grad_pair = pair_all.astype(f32)
    grad_pair = grad_pair.reshape(parts // copies, copies, shard, 2, width).sum(axis=1)
    grad_key = grad_pair[:, :, 0].transpose(1, 0, 2).reshape(shard, -1)
    grad_value = grad_pair[:, :, 1].transpose(1, 0, 2).reshape(shard, -1)
    grad_output = outer_all.astype(f32)
    slopes = slopes.reshape(-1)
    attention_slope = slopes[:model]
    feedforward_slope = slopes[model : 2 * model]
    query_slope = slopes[2 * model : 2 * model + width]
    key_slope = slopes[2 * model + width : 2 * model + 2 * width]
    block_out = block_rows.astype(bf16).reshape(1, tokens, model)
    input_grad = input_rows.reshape(1, tokens, model)
    return (
        block_out,
        input_grad,
        attention_slope,
        grad_query,
        grad_key,
        grad_value,
        grad_output,
        query_slope,
        key_slope,
        feedforward_slope,
        grad_gate,
        grad_up,
        grad_down,
    )


def solution(mesh):
    in_specs = (
        P("fsdp", "seq", None),
        P("fsdp", "seq", None),
        P(),
        P("fsdp", None),
        P("fsdp", None),
        P("fsdp", None),
        P("fsdp", None),
        P(),
        P(),
        P(),
        P(None, "fsdp"),
        P(None, "fsdp"),
        P(None, "fsdp"),
    )
    out_specs = (
        P("fsdp", "seq", None),
        P("fsdp", "seq", None),
        P(),
        P("fsdp", None),
        P("fsdp", None),
        P("fsdp", None),
        P("fsdp", None),
        P(),
        P(),
        P(),
        P(None, "fsdp"),
        P(None, "fsdp"),
        P(None, "fsdp"),
    )
    return jax.shard_map(
        per_device, mesh=mesh, in_specs=in_specs, out_specs=out_specs, check_vma=False
    )
```

```python
import functools

import jax
import jax.numpy as jnp
from jax import lax
from jax.experimental import pallas as pl
from jax.experimental.pallas import tpu as pltpu
from jax.sharding import PartitionSpec as P

EPS = 1e-05
THETA = 1000000.0


def rotate_half(values):
    half = values.shape[-1] // 2
    return jnp.concatenate([-values[..., half:], values[..., :half]], axis=-1)


def rope_tables(positions, width):
    exponents = jnp.arange(width // 2).astype(jnp.float32) * 2.0 / width
    rates = jnp.power(jnp.float32(THETA), -exponents)
    angle = positions.astype(jnp.float32)[:, None] * rates[None, :]
    angle = jnp.concatenate([angle, angle], axis=-1)
    return (jnp.cos(angle), jnp.sin(angle))


def prepare(proj, gain, cosine, sine):
    rows = proj.shape[0]
    width = gain.shape[0]
    split = proj.reshape(rows, -1, width)
    factor = lax.rsqrt(jnp.mean(split * split, axis=-1, keepdims=True) + EPS)
    normed = split * factor * gain
    turned = normed * cosine[:, None, :] + rotate_half(normed) * sine[:, None, :]
    return turned.reshape(rows, -1)


def matmul(left, right):
    return jnp.dot(left, right, preferred_element_type=jnp.float32)


def inner_rows(left, right):
    return lax.dot_general(
        left, right, (((0,), (0,)), ((), ())), preferred_element_type=jnp.float32
    )


def inner_cols(left, right):
    return lax.dot_general(
        left, right, (((1,), (1,)), ((), ())), preferred_element_type=jnp.float32
    )


def rms_factor(values):
    return lax.rsqrt(jnp.mean(values * values, axis=-1, keepdims=True) + EPS)


def norm_back(grad, values, factor, gain):
    scaled = grad * gain
    return factor * (
        scaled - values * factor * factor * jnp.mean(scaled * values, axis=-1, keepdims=True)
    )


def gate_back(hidden_grad, gate, lifted):
    sigma = jax.nn.sigmoid(gate)
    gate_grad = (hidden_grad * lifted * sigma * (1.0 + gate * (1.0 - sigma))).astype(jnp.bfloat16)
    lifted_grad = (hidden_grad * gate * sigma).astype(jnp.bfloat16)
    return (gate_grad, lifted_grad)


def activate(gate, lifted):
    return (gate * jax.nn.sigmoid(gate) * lifted).astype(jnp.bfloat16)


def split_heads(query_rows, pair_rows, groups, width):
    length = query_rows.shape[0]
    key_heads = pair_rows.shape[1] // (2 * width)
    queries = query_rows.reshape(length, key_heads, groups, width)
    keys = pair_rows[:, : key_heads * width].reshape(length, key_heads, width)
    values = pair_rows[:, key_heads * width :].reshape(length, key_heads, width)
    return (queries, keys, values, key_heads)


def attend_heads(query_rows, pair_rows, groups, width):
    length = query_rows.shape[0]
    queries, keys, values, key_heads = split_heads(query_rows, pair_rows, groups, width)
    block = min(512, length)
    scale = width ** (-0.5)
    offsets = jnp.arange(block)

    def query_step(index, state):
        out_rows, log_rows = state
        query_block = lax.dynamic_slice_in_dim(queries, index * block, block, 0)

        def key_step(inner, carry):
            summed, total = carry
            key_block = lax.dynamic_slice_in_dim(keys, inner * block, block, 0)
            value_block = lax.dynamic_slice_in_dim(values, inner * block, block, 0)
            scores = (
                jnp.einsum(
                    "qhgd,shd->hgqs", query_block, key_block, preferred_element_type=jnp.float32
                )
                * scale
            )
            allowed = (index * block + offsets)[:, None] >= (inner * block + offsets)[None, :]
            weights = jnp.where(allowed, jnp.exp(scores), 0.0)
            summed = summed + jnp.einsum(
                "hgqs,shd->hgqd",
                weights.astype(jnp.bfloat16),
                value_block,
                preferred_element_type=jnp.float32,
            )
            return (summed, total + jnp.sum(weights, axis=-1))

        initial = (
            jnp.zeros((key_heads, groups, block, width), jnp.float32),
            jnp.zeros((key_heads, groups, block), jnp.float32),
        )
        summed, total = lax.fori_loop(0, index + 1, key_step, initial)
        result = (summed / total[..., None]).astype(jnp.bfloat16)
        result = result.transpose(2, 0, 1, 3).reshape(block, key_heads * groups * width)
        out_rows = lax.dynamic_update_slice_in_dim(out_rows, result, index * block, 0)
        log_rows = lax.dynamic_update_slice_in_dim(log_rows, jnp.log(total), index * block, 2)
        return (out_rows, log_rows)

    start = (
        jnp.zeros((length, key_heads * groups * width), jnp.bfloat16),
        jnp.zeros((key_heads, groups, length), jnp.float32),
    )
    return lax.fori_loop(0, length // block, query_step, start)


def attend_back(query_rows, pair_rows, out_rows, log_rows, grad_rows, groups, width):
    length = query_rows.shape[0]
    queries, keys, values, key_heads = split_heads(query_rows, pair_rows, groups, width)
    outs = out_rows.reshape(length, key_heads, groups, width)
    grads = grad_rows.reshape(length, key_heads, groups, width)
    correction = jnp.sum(grads.astype(jnp.float32) * outs.astype(jnp.float32), axis=-1)
    block = min(512, length)
    scale = width ** (-0.5)
    offsets = jnp.arange(block)

    def query_step(index, state):
        query_grad, key_grad, value_grad = state
        query_block = lax.dynamic_slice_in_dim(queries, index * block, block, 0)
        grad_block = lax.dynamic_slice_in_dim(grads, index * block, block, 0)
        shift_block = lax.dynamic_slice_in_dim(correction, index * block, block, 0).transpose(
            1, 2, 0
        )
        log_block = lax.dynamic_slice_in_dim(log_rows, index * block, block, 2)

        def key_step(inner, carry):
            block_grad, key_sum, value_sum = carry
            key_block = lax.dynamic_slice_in_dim(keys, inner * block, block, 0)
            value_block = lax.dynamic_slice_in_dim(values, inner * block, block, 0)
            scores = (
                jnp.einsum(
                    "qhgd,shd->hgqs", query_block, key_block, preferred_element_type=jnp.float32
                )
                * scale
            )
            allowed = (index * block + offsets)[:, None] >= (inner * block + offsets)[None, :]
            weights = jnp.where(allowed, jnp.exp(scores - log_block[..., None]), 0.0)
            value_part = jnp.einsum(
                "hgqs,qhgd->shd",
                weights.astype(jnp.bfloat16),
                grad_block,
                preferred_element_type=jnp.float32,
            )
            prob_grad = jnp.einsum(
                "qhgd,shd->hgqs", grad_block, value_block, preferred_element_type=jnp.float32
            )
            score_grad = (weights * (prob_grad - shift_block[..., None]) * scale).astype(
                jnp.bfloat16
            )
            block_grad = block_grad + jnp.einsum(
                "hgqs,shd->qhgd", score_grad, key_block, preferred_element_type=jnp.float32
            )
            key_part = jnp.einsum(
                "hgqs,qhgd->shd", score_grad, query_block, preferred_element_type=jnp.float32
            )
            key_sum = lax.dynamic_update_slice_in_dim(
                key_sum,
                lax.dynamic_slice_in_dim(key_sum, inner * block, block, 0) + key_part,
                inner * block,
                0,
            )
            value_sum = lax.dynamic_update_slice_in_dim(
                value_sum,
                lax.dynamic_slice_in_dim(value_sum, inner * block, block, 0) + value_part,
                inner * block,
                0,
            )
            return (block_grad, key_sum, value_sum)

        initial = (jnp.zeros((block, key_heads, groups, width), jnp.float32), key_grad, value_grad)
        block_grad, key_grad, value_grad = lax.fori_loop(0, index + 1, key_step, initial)
        query_grad = lax.dynamic_update_slice_in_dim(query_grad, block_grad, index * block, 0)
        return (query_grad, key_grad, value_grad)

    state = (
        jnp.zeros((length, key_heads, groups, width), jnp.float32),
        jnp.zeros((length, key_heads, width), jnp.float32),
        jnp.zeros((length, key_heads, width), jnp.float32),
    )
    query_grad, key_grad, value_grad = lax.fori_loop(0, length // block, query_step, state)
    pair_grad = jnp.concatenate(
        [
            key_grad.reshape(length, key_heads * width),
            value_grad.reshape(length, key_heads * width),
        ],
        axis=1,
    )
    return (query_grad.reshape(length, key_heads * groups * width), pair_grad)


MESH = pl.DeviceIdType.MESH


def flip(index, mask, bits):
    for bit in bits:
        if mask & bit:
            index = index + bit - 2 * bit * ((index // bit) % 2)
    return index


class Place:
    def __init__(self, parts, planes):
        self.parts, self.planes = parts, planes
        self.seat = lax.axis_index("seq")
        self.plane = lax.axis_index("fsdp")
        self.core = self.seat % 2
        self.chip = self.seat // 2
        self.seat_bits = [1 << i for i in range(parts.bit_length() - 1)]
        self.chip_bits = self.seat_bits[1:]
        self.plane_bits = [1 << i for i in range(planes.bit_length() - 1)]

    def at(self, mask):
        return flip(self.seat, mask, self.seat_bits)

    def side(self, bit):
        return (self.seat // bit) % 2

    def colors(self):
        return (self.chip_bits, self.chip_bits[::-1])

    def enter(self, masks=(), line=False, plane_masks=()):
        barrier = pltpu.get_barrier_semaphore()
        peers = [{"seq": self.at(mask)} for mask in masks]
        if line:
            peers.append({"fsdp": (self.plane + 1) % self.planes})
            peers.append({"fsdp": (self.plane + self.planes - 1) % self.planes})
        for mask in plane_masks:
            peers.append({"fsdp": flip(self.plane, mask, self.plane_bits)})
        for peer in peers:
            pl.semaphore_signal(barrier, inc=1, device_id=peer, device_id_type=MESH)
        pl.semaphore_wait(barrier, len(peers))


class Wire:
    def __init__(self, sends, receives, locals_):
        self.sends, self.receives, self.locals = sends, receives, locals_
        self.count = self.local_count = 0
        self.open = []

    def remote(self, source, target, device):
        number = self.count
        self.count += 1
        return pltpu.make_async_remote_copy(
            src_ref=source,
            dst_ref=target,
            send_sem=self.sends.at[number],
            recv_sem=self.receives.at[number],
            device_id=device,
            device_id_type=MESH,
        )

    def send(self, source, target, device):
        copy = self.remote(source, target, device)
        copy.start()
        self.open.append(copy)
        return copy

    def quiet(self, source, target):
        number = self.local_count
        self.local_count += 1
        return pltpu.make_async_copy(source, target, self.locals.at[number])

    def local(self, source, target):
        copy = self.quiet(source, target)
        copy.start()
        return copy

    def sent(self, copy):
        copy.wait_send()
        self.open = [other for other in self.open if other is not copy]

    def close(self):
        for copy in self.open:
            copy.wait_send()


def add_rows(target, left, right, step=64):
    rows = target.shape[0]
    step = min(step, rows)

    def body(index, carry):
        at = pl.ds(pl.multiple_of(index * step, step), step)
        total = left[at, :].astype(jnp.float32) + right[at, :].astype(jnp.float32)
        target[at, :] = total.astype(target.dtype)
        return carry

    lax.fori_loop(0, rows // step, body, 0)


class LineGather:
    def __init__(self, wire, here, source, target, share=None):
        self.here = here
        planes, plane = here.planes, here.plane
        above = {"fsdp": (plane + 1) % planes}
        below = {"fsdp": (plane + planes - 1) % planes}
        self.ups, self.downs = {}, {}
        for step in range(1, planes):
            lower = (plane + planes - step + 1) % planes
            upper = (plane + step - 1) % planes
            first = step == 1
            self.ups[step] = wire.remote(
                source if first else target(lower), target(lower), above
            )
            self.downs[step] = wire.remote(
                source if first else target(upper), target(upper), below
            )
        self.shared = {}
        if share is not None:
            for step in range(1, planes):
                for way, shift in ((0, planes - step), (1, step)):
                    index = (plane + shift) % planes
                    self.shared[(step, way)] = wire.remote(
                        target(index), share(index), {"seq": here.at(1)}
                    )

    def start(self, step):
        planes, plane = self.here.planes, self.here.plane

        @pl.when((plane >= step - 1) & (plane <= planes - 2))
        def _():
            self.ups[step].start()

        @pl.when((plane + step <= planes) & (plane >= 1))
        def _():
            self.downs[step].start()

    def arrive(self, step):
        planes, plane = self.here.planes, self.here.plane

        @pl.when(plane >= step)
        def _():
            self.ups[step].wait_recv()
            if self.shared:
                self.shared[(step, 0)].start()

        @pl.when(plane + step <= planes - 1)
        def _():
            self.downs[step].wait_recv()
            if self.shared:
                self.shared[(step, 1)].start()

    def close(self, shared_taken=False):
        planes, plane = self.here.planes, self.here.plane
        for (step, way), copy in self.shared.items():

            @pl.when(plane >= step if way == 0 else plane + step <= planes - 1)
            def _(copy=copy):
                copy.wait_send()
                if not shared_taken:
                    copy.wait_recv()

        for step in range(1, planes):

            @pl.when((plane >= step - 1) & (plane <= planes - 2))
            def _(step=step):
                self.ups[step].wait_send()

            @pl.when((plane + step <= planes) & (plane >= 1))
            def _(step=step):
                self.downs[step].wait_send()


class Lines:
    def __init__(self, members):
        self.members = members

    def start(self, step):
        for member in self.members:
            member.start(step)

    def pass_on(self, step):
        for member in self.members:
            member.arrive(step)
            if step + 1 < member.here.planes:
                member.start(step + 1)

    def step(self, step):
        for member in self.members:
            member.step(step)

    def close(self, *options):
        for member in self.members:
            member.close(*options)


def gather_lines(wire, here, source, target, share=None, cuts=2):
    rows = source.shape[0] // cuts
    members = []
    for cut in range(cuts):
        at = pl.ds(cut * rows, rows)
        members.append(
            LineGather(
                wire,
                here,
                source.at[at],
                lambda index, at=at: target(index).at[at],
                None if share is None else lambda index, at=at: share(index).at[at],
            )
        )
    return Lines(members)


class LineScatter:
    def __init__(self, wire, here, term, landing):
        self.wire, self.here, self.term, self.landing = wire, here, term, landing
        planes, plane = here.planes, here.plane
        above = {"fsdp": (plane + 1) % planes}
        below = {"fsdp": (plane + planes - 1) % planes}
        self.ups, self.downs = {}, {}
        for step in range(1, planes):
            self.ups[step] = wire.remote(
                term((plane + planes - step) % planes), landing(0, step - 1), above
            )
            self.downs[step] = wire.remote(
                term((plane + step) % planes), landing(1, step - 1), below
            )

    def step(self, step):
        planes, plane = self.here.planes, self.here.plane
        mirror = planes - 1 - plane
        for way, (position, copies, dest) in enumerate(
            (
                (plane, self.ups, (plane + planes - step) % planes),
                (mirror, self.downs, (plane + step) % planes),
            )
        ):
            if step > 1:

                @pl.when((position >= 1) & (position <= step - 1))
                def _(way=way, copies=copies, dest=dest):
                    copies[step - 1].wait_recv()
                    term = self.term(dest)
                    add_rows(term, term, self.landing(way, step - 2))

            @pl.when(position <= step - 1)
            def _(copies=copies):
                copies[step].start()

    def finish(self, out):
        planes, plane = self.here.planes, self.here.plane
        own = self.term(plane)
        last = planes - 1

        @pl.when(plane >= 1)
        def _():
            self.ups[last].wait_recv()

        @pl.when(plane <= planes - 2)
        def _():
            self.downs[last].wait_recv()

        @pl.when(plane == 0)
        def _():
            add_rows(out, own, self.landing(1, last - 1))

        @pl.when(plane == planes - 1)
        def _():
            add_rows(out, own, self.landing(0, last - 1))

        @pl.when((plane >= 1) & (plane <= planes - 2))
        def _():
            add_rows(own, own, self.landing(0, last - 1))
            add_rows(out, own, self.landing(1, last - 1))

    def close(self):
        planes, plane = self.here.planes, self.here.plane
        mirror = planes - 1 - plane
        for step in range(1, planes):

            @pl.when(plane <= step - 1)
            def _(step=step):
                self.ups[step].wait_send()

            @pl.when(mirror <= step - 1)
            def _(step=step):
                self.downs[step].wait_send()


class PlaneGather:
    def __init__(self, wire, here, source, target):
        self.wire, self.here, self.source, self.target = wire, here, source, target
        self.incoming = {}

    def _send(self, mask, color, bit):
        here = self.here
        target = self.target(here.at(mask), color)
        source = self.source(color) if mask == 0 else target
        self.incoming[(mask ^ bit, color)] = self.wire.send(
            source, target, {"seq": here.at(bit)}
        )

    def start(self):
        for position in range(len(self.here.chip_bits)):
            for color, bits in enumerate(self.here.colors()):
                self._send(0, color, bits[position])
        for color in (0, 1):
            self._send(0, color, 1)

    def hop(self, hops):
        here = self.here
        chips = here.parts // 2
        for mask in (mask * 2 for mask in range(1, chips)):
            if bin(mask).count("1") != hops:
                continue
            for color, bits in enumerate(here.colors()):
                self.incoming[(mask, color)].wait_recv()
                last = max(i for i, bit in enumerate(bits) if mask & bit)
                for bit in bits[last + 1 :]:
                    self._send(mask, color, bit)
                self._send(mask, color, 1)

    def hops(self, first=1):
        for hops in range(first, len(self.here.chip_bits) + 1):
            self.hop(hops)

    def finish(self):
        for mask in range(1, self.here.parts, 2):
            for color in (0, 1):
                self.incoming[(mask, color)].wait_recv()


class PlaneScatter:
    def __init__(self, wire, here, product, give, take, current, landing, model):
        self.wire, self.here, self.product = wire, here, product
        self.give, self.take, self.current, self.landing = give, take, current, landing
        self.model = model

    def start(self):
        here = self.here
        chips = here.parts // 2
        self.swaps = {}
        tokens = self.give.shape[1]
        seats = [2 * flip(here.chip, mask, [b // 2 for b in here.chip_bits]) for mask in range(chips)]
        for part in range(self.model // 512):
            columns = slice(part * 512, (part + 1) * 512)
            rows = self.product([seat + 1 - here.core for seat in seats], columns)
            for mask in range(chips):
                self.give[mask, :, columns] = rows[mask * tokens : (mask + 1) * tokens].astype(
                    self.give.dtype
                )
        for mask in range(chips)[::-1]:
            self.swaps[mask] = self.wire.send(
                self.give.at[mask], self.take.at[mask], {"seq": here.at(1)}
            )
        half = self.model // 2
        for part in range(self.model // 512):
            columns = slice(part * 512, (part + 1) * 512)
            rows = self.product([seat + here.core for seat in seats], columns)
            color, inside = divmod(part * 512, half)
            for mask in range(chips):
                self.current[color, mask, :, inside : inside + 512] = rows[
                    mask * tokens : (mask + 1) * tokens
                ].astype(self.current.dtype)

    def join(self):
        half = self.model // 2
        chips = self.here.parts // 2
        for mask in range(chips)[::-1]:
            self.swaps[mask].wait_recv()
            for color in (0, 1):
                mine = self.current.at[color, mask]
                add_rows(mine, mine, self.take.at[mask, :, pl.ds(color * half, half)])

    def stage(self, position):
        here = self.here
        self.moved = {}
        for color, bits in enumerate(here.colors()):
            bit = bits[position]
            done = sum(bits[:position])
            for mask in range(here.parts // 2):
                if mask * 2 & bit and not mask * 2 & done:
                    low = mask ^ (bit // 2)
                    self.moved[(color, low)] = self.wire.send(
                        self.current.at[color, mask],
                        self.landing.at[position, color, low],
                        {"seq": here.at(bit)},
                    )

    def settle(self, position, out):
        half = self.model // 2
        last = position == len(self.here.chip_bits) - 1
        for (color, low), copy in self.moved.items():
            copy.wait_recv()
            mine = self.current.at[color, low]
            if last:
                target = out.at[:, pl.ds(color * half, half)]
            else:
                target = mine
            add_rows(target, mine, self.landing.at[position, color, low])


def pick_lanes(low, high, width):
    lane = lax.broadcasted_iota(jnp.int32, low.shape, low.ndim - 1)
    return jnp.where(lane % (2 * width) < width, low, high)


def group_mean(values, group, width):
    high = values.astype(jnp.bfloat16)
    low = (values - high.astype(jnp.float32)).astype(jnp.bfloat16)
    total = jnp.dot(high, group, preferred_element_type=jnp.float32) + jnp.dot(
        low, group, preferred_element_type=jnp.float32
    )
    return total * (1.0 / width)


def turn(values, width):
    lanes = values.shape[1]
    half = width // 2
    return pick_lanes(
        pltpu.roll(values, lanes - half, 1), pltpu.roll(values, half, 1), half
    )


def attend_block(index, block, width, heads, queries, pair, twin, left, right, out_rows, logs):
    rows = pl.ds(index * block, block)
    before = index * block
    columns = 2 * width
    row = lax.broadcasted_iota(jnp.int32, (block, block), 0)
    column = lax.broadcasted_iota(jnp.int32, (block, block), 1)
    allowed = row >= column
    contract = (((1,), (1,)), ((), ()))
    totals = []
    for number in range(heads // 2):
        at = pl.ds(number * columns, columns)
        both = queries[rows, at]
        both = (both.astype(jnp.float32) * width**-0.5).astype(both.dtype)
        zero = jnp.zeros_like(both)
        result = None
        for side, values in ((0, left), (1, right)):
            mine = pick_lanes(both, zero, width) if side == 0 else pick_lanes(zero, both, width)
            scores = lax.dot_general(
                mine, twin[rows, :], contract, preferred_element_type=jnp.float32
            )
            weights = jnp.where(allowed, jnp.exp(scores), 0.0)
            total = jnp.sum(weights, axis=1, keepdims=True)
            summed = jnp.dot(
                weights.astype(jnp.bfloat16), values[rows, :], preferred_element_type=jnp.float32
            )
            if before:
                scores = lax.dot_general(
                    mine, twin[0:before, :], contract, preferred_element_type=jnp.float32
                )
                weights = jnp.exp(scores)
                total = total + jnp.sum(weights, axis=1, keepdims=True)
                summed = summed + jnp.dot(
                    weights.astype(jnp.bfloat16),
                    values[0:before, :],
                    preferred_element_type=jnp.float32,
                )
            totals.append(total)
            part = summed / total
            result = part if result is None else result + part
        out_rows[rows, at] = result.astype(out_rows.dtype)
    lane = lax.broadcasted_iota(jnp.int32, (block, 128), 1)
    table = jnp.ones((block, 128), jnp.float32)
    for number, total in enumerate(totals):
        table = jnp.where(lane == number, total, table)
    logs[:, rows] = jnp.log(table).T[0 : logs.shape[0], :]


def front_kernel(
    width,
    parts,
    planes,
    x,
    w,
    o,
    gain,
    cosine,
    sine,
    group,
    x_all,
    w_all,
    o_slice,
    proj,
    queries,
    pair,
    out_rows,
    logs,
    o_all,
    twin,
    left,
    right,
    *sems,
):
    here = Place(parts, planes)
    wire = Wire(*sems)
    tokens, shard, rows = x.shape[0], w.shape[0], o.shape[0]
    half = tokens // 2
    chips = parts // 2
    chip_masks = [mask * 2 for mask in range(1, chips)]
    here.enter(chip_masks + [1], line=True)
    weights = gather_lines(
        wire, here, w, lambda index: w_all.at[pl.ds(pl.multiple_of(index * shard, shard), shard)]
    )
    weights.start(1)
    plane_rows = PlaneGather(
        wire,
        here,
        lambda color: x.at[pl.ds(color * half, half)],
        lambda seat, color: x_all.at[pl.ds(pl.multiple_of(seat * tokens + color * half, half), half)],
    )
    plane_rows.start()
    kept = [
        wire.local(x, x_all.at[pl.ds(pl.multiple_of(here.seat * tokens, tokens), tokens)]),
        wire.local(w, w_all.at[pl.ds(pl.multiple_of(here.plane * shard, shard), shard)]),
        wire.local(o, o_all.at[here.plane]),
    ]
    outer = gather_lines(wire, here, o, lambda index: o_all.at[index])
    weights.members[0].arrive(1)
    if planes > 2:
        weights.members[0].start(2)
    plane_rows.hop(1)
    weights.members[1].arrive(1)
    if planes > 2:
        weights.members[1].start(2)
    outer.start(1)
    plane_rows.hops(2)
    spot = o_slice.at[pl.ds(pl.multiple_of(here.chip * rows, rows), rows)]
    deals = []
    for mask in chip_masks:
        chip = here.at(mask) // 2
        deals.append((chip, wire.remote(o_all.at[chip], spot, {"seq": here.at(mask)})))
    keep_own = wire.quiet(o_all.at[here.chip], spot)

    def deal(step):
        for chip, copy in deals + [(here.chip, keep_own)]:

            @pl.when((chip == here.plane + step) | (chip + step == here.plane))
            def _(copy=copy):
                copy.start()

    kept[2].wait()
    deal(0)
    for step in range(2, planes):
        weights.pass_on(step)
    plane_rows.finish()
    for copy in kept[:2]:
        copy.wait()
    length = x_all.shape[0]
    block = min(256, length)
    blocks = length // block
    query_cols = queries.shape[1]
    heads = query_cols // width

    def project(index, carry):
        at = pl.ds(pl.multiple_of(index * block, block), block)
        value = jnp.dot(x_all[at, :], w_all[...], preferred_element_type=jnp.float32)
        proj[at, :] = value
        factor = lax.rsqrt(group_mean(value * value, group[...], width) + EPS)
        normed = value * factor * gain[...]
        repeat = value.shape[1] // cosine.shape[1]
        cosines = jnp.concatenate([cosine[at, :]] * repeat, axis=1)
        sines = jnp.concatenate([sine[at, :]] * repeat, axis=1)
        turned = normed * cosines + turn(normed, width) * sines
        queries[at, :] = turned[:, :query_cols].astype(queries.dtype)
        keys, values = turned[:, query_cols:], value[:, query_cols:]
        both = pick_lanes(keys, values, width)
        pair[at, :] = both.astype(pair.dtype)
        swapped = pltpu.roll(both, width, 1)
        twin[at, :] = pick_lanes(both, swapped, width).astype(twin.dtype)
        zero = jnp.zeros_like(both)
        left[at, :] = pick_lanes(swapped, zero, width).astype(left.dtype)
        right[at, :] = pick_lanes(zero, both, width).astype(right.dtype)
        return carry

    lax.fori_loop(0, blocks, project, 0)
    waits = list(range(1, planes))
    for index in range(blocks):
        while waits and waits[0] * blocks <= (index + 1) * planes:
            step = waits.pop(0)
            outer.pass_on(step)
            deal(step)
        attend_block(
            index, block, width, heads, queries, pair, twin, left, right, out_rows, logs
        )
    for step in waits:
        outer.pass_on(step)
        deal(step)
    keep_own.wait()
    for _, copy in deals:
        copy.wait()
    wire.close()
    weights.close()
    outer.close()


def out_rows_kernel(
    parts, planes, a, w, c, out, c_all, give, take, current, landing, *sems
):
    here = Place(parts, planes)
    wire = Wire(*sems)
    tokens, model = c.shape
    here.enter([mask for mask in here.seat_bits], line=True)

    def product(seats, columns):
        rows = [a[pl.ds(pl.multiple_of(seat * tokens, tokens), tokens), :] for seat in seats]
        return jnp.dot(
            jnp.concatenate(rows, axis=0), w[:, columns], preferred_element_type=jnp.float32
        )

    def spot(index):
        return c_all.at[index, here.core]

    cots = gather_lines(wire, here, c, spot, spot)
    cots.start(1)
    own = wire.local(c, spot(here.plane))
    rows = PlaneScatter(wire, here, product, give, take, current, landing, model)
    rows.start()
    across = wire.send(c, spot(here.plane), {"seq": here.at(1)})
    rows.join()
    rows.stage(0)
    stages = len(here.chip_bits)
    for stage in range(stages):
        if stage + 1 < planes:
            cots.pass_on(stage + 1)
        rows.settle(stage, out)
        if stage + 1 < stages:
            rows.stage(stage + 1)
    for step in range(stages + 1, planes):
        cots.pass_on(step)
    own.wait()
    across.wait_recv()
    wire.close()
    cots.close()


def feed_kernel(
    parts,
    planes,
    m,
    cots,
    gate_weight,
    up_weight,
    down_weight,
    s_down,
    s_gate_a,
    s_gate_b,
    s_up_a,
    s_up_b,
    mid,
    down_give,
    down_keep,
    gate_half,
    up_half,
    down_half,
    mids,
    hidden,
    gate_grads,
    lifted_grads,
    away,
    *rest,
):
    here = Place(parts, planes)
    stages = len(here.chip_bits) - 1
    landings, rest = rest[:stages], rest[stages:]
    give, take, current, line_landing, *sems = rest
    wire = Wire(*sems)
    tokens, model = m.shape
    units = gate_half.shape[1]
    own_units = pl.ds(pl.multiple_of(here.core * units, units), units)
    loads = [
        wire.local(whole.at[:, own_units], part)
        for whole, part in (
            (gate_weight, gate_half),
            (up_weight, up_half),
            (down_weight, down_half),
        )
    ]
    here.enter(here.seat_bits, line=True)

    def spot(index):
        return mids.at[index, here.core]

    lines = gather_lines(wire, here, m, spot, spot)
    lines.start(1)
    across = wire.send(m, spot(here.plane), {"seq": here.at(1)})
    own = wire.local(m, spot(here.plane))

    def block(index):
        rows = pl.ds(pl.multiple_of(index * 2 * tokens, 2 * tokens), 2 * tokens)
        mid_rows = mids[index].reshape(2 * tokens, model)
        cot_rows = cots[rows, :]

        def part(number, carry):
            at = pl.ds(pl.multiple_of(number * 256, 256), 256)
            gate = jnp.dot(mid_rows, gate_half[:, at], preferred_element_type=jnp.float32)
            lifted = jnp.dot(mid_rows, up_half[:, at], preferred_element_type=jnp.float32)
            hidden_grad = jnp.dot(cot_rows, down_half[:, at], preferred_element_type=jnp.float32)
            sigma = 1.0 / (1.0 + jnp.exp(-gate))
            active = gate * sigma
            hidden[rows, at] = (active * lifted).astype(hidden.dtype)
            lifted_grads[rows, at] = (hidden_grad * active).astype(hidden.dtype)
            gate_grads[rows, at] = (
                hidden_grad * lifted * sigma * (1.0 + gate * (1.0 - sigma))
            ).astype(hidden.dtype)
            return carry

        lax.fori_loop(0, units // 256, part, 0)

    for load in loads:
        load.wait()
    own.wait()
    across.wait_recv()
    plane = here.plane
    block(plane)
    for step in range(1, planes):
        lines.pass_on(step)
        ups = jnp.where(plane >= step, 1, 0)
        downs = jnp.where(plane + step <= planes - 1, 1, 0)

        def arrived(number, carry, step=step, ups=ups):
            from_up = (number == 0) & (ups == 1)
            for way, chosen in ((0, from_up), (1, jnp.logical_not(from_up))):

                @pl.when(chosen)
                def _(way=way):
                    for line in lines.members:
                        line.shared[(step, way)].wait_recv()

            block(jnp.where(from_up, plane + planes - step, plane + step) % planes)
            return carry

        lax.fori_loop(0, ups + downs, arrived, 0)

    flat_mids = mids.reshape(2 * planes * tokens, model)
    pairs = ((cots, hidden), (flat_mids, gate_grads), (flat_mids, lifted_grads))
    quarter = model // 4
    moved = {}

    def gradient(target, pair, start):
        left, right = pair

        def part(number, carry):
            at = pl.ds(pl.multiple_of(start + number * 256, 256), 256)
            target[pl.ds(pl.multiple_of(number * 256, 256), 256), :] = lax.dot_general(
                left[:, at],
                right[...],
                (((0,), (0,)), ((), ())),
                preferred_element_type=jnp.float32,
            ).astype(target.dtype)
            return carry

        lax.fori_loop(0, quarter // 256, part, 0)

    def first_half(color, mine):
        bit = here.colors()[color][0]
        side = here.side(bit) if mine else 1 - here.side(bit)
        return pl.multiple_of(color * (model // 2) + side * quarter, quarter)

    def send_away(number):
        for color, bits in enumerate(here.colors()):
            gradient(away.at[number, color], pairs[number], first_half(color, False))
            moved[(number, color)] = wire.send(
                away.at[number, color], landings[0].at[number, color], {"seq": here.at(bits[0])}
            )

    def mid_term(target, core):
        rows = [pl.ds(pl.multiple_of((2 * p + core) * tokens, tokens), tokens) for p in range(planes)]
        gates = jnp.concatenate([gate_grads[at, :] for at in rows], axis=0)
        lifts = jnp.concatenate([lifted_grads[at, :] for at in rows], axis=0)

        def part(number, carry):
            at = pl.ds(pl.multiple_of(number * 256, 256), 256)
            term = lax.dot_general(
                gates, gate_half[at, :], (((1,), (1,)), ((), ())), preferred_element_type=jnp.float32
            ) + lax.dot_general(
                lifts, up_half[at, :], (((1,), (1,)), ((), ())), preferred_element_type=jnp.float32
            )
            target[:, :, at] = term.reshape(planes, tokens, 256).astype(target.dtype)
            return carry

        lax.fori_loop(0, model // 256, part, 0)

    def down_term(target, core):
        rows = [pl.ds(pl.multiple_of((2 * p + core) * tokens, tokens), tokens) for p in range(planes)]
        hiddens = jnp.concatenate([hidden[at, :] for at in rows], axis=0)

        def part(number, carry):
            at = pl.ds(pl.multiple_of(number * 256, 256), 256)
            term = lax.dot_general(
                hiddens, down_half[at, :], (((1,), (1,)), ((), ())), preferred_element_type=jnp.float32
            )
            target[:, :, at] = term.reshape(planes, tokens, 256).astype(target.dtype)
            return carry

        lax.fori_loop(0, model // 256, part, 0)

    send_away(0)
    swaps = TokenSum(wire, here, current, take, line_landing)
    mid_term(give, 1 - here.core)
    swaps.start(give)
    send_away(1)
    mid_term(current, here.core)
    swaps.join()
    swaps.step(1)
    send_away(2)
    for step in range(2, planes):
        swaps.step(step)

    def final(number, color):
        if number == 0:
            return s_down.at[color]
        return ((s_gate_a, s_gate_b), (s_up_a, s_up_b))[number - 1][color]

    wire.sent(swaps.across)
    down_term(give, 1 - here.core)
    down_term(take, here.core)
    handed = [wire.local(give, down_give), wire.local(take, down_keep)]
    rows = quarter
    keeps = {}
    for number in range(3):
        for color in (0, 1):
            keep = final(number, color) if stages == 1 else away.at[number, color]
            if stages > 1:
                wire.sent(moved[(number, color)])
            gradient(keep, pairs[number], first_half(color, True))
            keeps[(number, color)] = (keep, 0)
    swaps.finish(mid)
    for stage in range(stages):
        last = stage == stages - 1
        for number in range(3):
            for color, bits in enumerate(here.colors()):
                keep, begin = keeps[(number, color)]
                moved[(number, color)].wait_recv()
                mine = keep.at[pl.ds(begin, rows)]
                if last:
                    add_rows(final(number, color), mine, landings[stage].at[number, color])
                else:
                    add_rows(mine, mine, landings[stage].at[number, color])
                    bit = bits[stage + 1]
                    half = rows // 2
                    gone = pl.multiple_of(begin + (1 - here.side(bit)) * half, half)
                    moved[(number, color)] = wire.send(
                        keep.at[pl.ds(gone, half)],
                        landings[stage + 1].at[number, color],
                        {"seq": here.at(bit)},
                    )
                    keeps[(number, color)] = (
                        keep,
                        pl.multiple_of(begin + here.side(bit) * half, half),
                    )
        rows //= 2
    for copy in handed:
        copy.wait()
    wire.close()
    lines.close(True)
    swaps.close()


class TokenSum:
    def __init__(self, wire, here, current, take, landing):
        self.wire, self.here = wire, here
        self.current, self.take = current, take
        self.cuts = 2
        rows = current.shape[1] // self.cuts
        self.lines = []
        for cut in range(self.cuts):
            at = pl.ds(cut * rows, rows)
            self.lines.append(
                LineScatter(
                    wire,
                    here,
                    lambda index, at=at: current.at[index, at],
                    lambda way, step, at=at: landing.at[way, step, at],
                )
            )

    def start(self, give):
        self.across = self.wire.send(give, self.take, {"seq": self.here.at(1)})

    def join(self):
        self.across.wait_recv()

        def body(index, carry):
            row = self.current.at[index]
            add_rows(row, row, self.take.at[index])
            return carry

        lax.fori_loop(0, self.here.planes, body, 0)

    def step(self, step):
        for line in self.lines:
            line.step(step)

    def finish(self, out):
        rows = out.shape[0] // self.cuts
        for cut, line in enumerate(self.lines):
            line.finish(out.at[pl.ds(cut * rows, rows)])

    def close(self):
        for line in self.lines:
            line.close()


def spread_kernel(
    parts, planes, h, s, give, keep, h_all, t, block, current, take, line_landing, *sems
):
    here = Place(parts, planes)
    wire = Wire(*sems)
    here.enter(here.seat_bits, line=True)
    tokens = h.shape[0]
    half = tokens // 2
    rows = PlaneGather(
        wire,
        here,
        lambda color: h.at[pl.ds(color * half, half)],
        lambda seat, color: h_all.at[pl.ds(pl.multiple_of(seat * tokens + color * half, half), half)],
    )
    swaps = TokenSum(wire, here, current, take, line_landing)
    swaps.start(give)
    kept = wire.local(keep, current)
    rows.start()
    own = wire.local(h, h_all.at[pl.ds(pl.multiple_of(here.seat * tokens, tokens), tokens)])
    kept.wait()
    swaps.join()
    swaps.step(1)
    rows.hop(1)
    moved = [
        wire.send(s.at[color], t.at[color], {"seq": here.at(bits[-1])})
        for color, bits in enumerate(here.colors())
    ]
    for step in range(2, planes):
        if step == 3:
            rows.hops(2)
        swaps.step(step)
    if planes <= 3:
        rows.hops(2)
    rows.finish()
    for color in (0, 1):
        moved[color].wait_recv()
        add_rows(t.at[color], t.at[color], s.at[color])
    own.wait()
    swaps.finish(block)
    wire.close()
    swaps.close()


def final_kernel(
    parts,
    planes,
    a,
    w,
    head_part,
    out_part,
    t_down,
    source,
    factor,
    slope,
    *rest,
):
    sent, rest = rest[:4], rest[4:]
    came, rest = rest[:4], rest[4:]
    out, near, far, query_all, pair_all, outer_all, slope_out, *rest = rest
    joined, rest = rest[:4], rest[4:]
    (
        give,
        take,
        current,
        landing,
        head_current,
        head_landing,
        dealt,
        out_landing,
        head_sum,
        out_sum,
        left,
        right,
        slope_sums,
        slope_landing,
        *sems,
    ) = rest
    here = Place(parts, planes)
    wire = Wire(*sems)
    tokens, model = out.shape
    shard = head_sum.shape[0]
    columns = query_all.shape[1] // parts
    rows_out = out_sum.shape[0]
    chips = parts // 2
    chip_masks = [mask * 2 for mask in range(1, chips)]
    here.enter(chip_masks + [1], line=True, plane_masks=here.plane_bits)
    weights = [
        WeightGather(wire, here, (t_down.at[0], t_down.at[1]), near, far, cut, 2)
        for cut in range(2)
    ]
    head_own = wire.local(head_part, head_current)
    deals = []
    for mask in chip_masks:
        chip = here.at(mask) // 2
        deals.append(
            wire.send(
                out_part.at[pl.ds(pl.multiple_of(chip * rows_out, rows_out), rows_out)],
                dealt.at[here.chip],
                {"seq": here.at(mask)},
            )
        )
    deal_own = wire.local(
        out_part.at[pl.ds(pl.multiple_of(here.chip * rows_out, rows_out), rows_out)],
        dealt.at[here.chip],
    )

    def product(seats, columns):
        rows = [a[pl.ds(pl.multiple_of(seat * tokens, tokens), tokens), :] for seat in seats]
        return lax.dot_general(
            jnp.concatenate(rows, axis=0),
            w[columns, :],
            (((1,), (1,)), ((), ())),
            preferred_element_type=jnp.float32,
        )

    heads = LineScatter(
        wire, here, lambda index: head_current.at[index], lambda way, step: head_landing.at[way, step]
    )
    outer = LineScatter(
        wire, here, lambda index: dealt.at[index], lambda way, step: out_landing.at[way, step]
    )
    head_own.wait()
    heads.step(1)
    rows = PlaneScatter(wire, here, product, give, take, current, landing, model)
    rows.start()
    loads = []
    for number in range(4):
        loads.append(
            (
                wire.local(sent[number], left.at[number]),
                wire.local(came[number], right.at[number]),
            )
        )
    heads.step(2)
    rows.join()
    rows.stage(0)
    weights[0].start()
    weights[0].own()
    deal_own.wait()
    for copy in deals:
        copy.wait_recv()
    outer.step(1)

    stores = []

    def join(number):
        for load in loads[number]:
            load.wait()
        add_rows(left.at[number], left.at[number], right.at[number])
        stores.append(wire.local(left.at[number], joined[number]))

    stages = len(here.chip_bits)
    for step in range(3, planes):
        heads.step(step)
    rows.settle(0, out)
    for stage in range(1, stages):
        rows.stage(stage)
        if stage + 1 < planes:
            outer.step(stage + 1)
        if stage == 1:
            heads.finish(head_sum)
        if stage + 1 < stages:
            rows.settle(stage, out)
    half, half_out = shard // 2, rows_out // 2

    def seat_columns(seat):
        return pl.ds(pl.multiple_of(seat * columns, columns), columns)

    gathers = [
        PlaneGather(
            wire,
            here,
            lambda color: head_sum.at[pl.ds(color * half, half), pl.ds(0, columns)],
            lambda seat, color: query_all.at[pl.ds(color * half, half), seat_columns(seat)],
        ),
        PlaneGather(
            wire,
            here,
            lambda color: head_sum.at[
                pl.ds(color * half, half), pl.ds(columns, pair_all.shape[2])
            ],
            lambda seat, color: pair_all.at[seat, pl.ds(color * half, half)],
        ),
        PlaneGather(
            wire,
            here,
            lambda color: out_sum.at[pl.ds(color * half_out, half_out)],
            lambda seat, color: outer_all.at[
                pl.ds(
                    pl.multiple_of(
                        ((seat % 2) * chips + seat // 2) * rows_out + color * half_out, half_out
                    ),
                    half_out,
                )
            ],
        ),
    ]
    own = []
    for gather in gathers[:2]:
        gather.start()
    own.append(
        wire.local(head_sum.at[:, pl.ds(0, columns)], query_all.at[:, seat_columns(here.seat)])
    )
    own.append(
        wire.local(
            head_sum.at[:, pl.ds(columns, pair_all.shape[2])], pair_all.at[here.seat]
        )
    )

    weights[1].start()
    weights[1].own()
    rows.settle(stages - 1, out)
    slope_sums[0] = slope[...]
    slope_sums[0, 0:1, :] = jnp.sum(out[...] * source[...].astype(jnp.float32) * factor[...], axis=0, keepdims=True)
    bits = [("seq", bit) for bit in here.seat_bits] + [("fsdp", bit) for bit in here.plane_bits]
    slope_copies = []

    def slope_send(number):
        axis, bit = bits[number]
        index = here.at(bit) if axis == "seq" else flip(here.plane, bit, here.plane_bits)
        slope_copies.append(
            wire.send(slope_sums.at[number], slope_landing.at[number], {axis: index})
        )

    def slope_add(number):
        slope_copies[number].wait_recv()
        target = slope_out if number == len(bits) - 1 else slope_sums.at[number + 1]
        target[...] = slope_sums[number] + slope_landing[number]

    slope_send(0)
    for step in range(stages + 1, planes):
        outer.step(step)
    join(0)
    gathers[0].hop(1)
    gathers[1].hop(1)
    slope_add(0)
    slope_send(1)
    outer.finish(out_sum)
    gathers[2].start()
    weights[0].forward()
    own_start = (here.core * chips + here.chip) * rows_out
    own.append(
        wire.local(out_sum, outer_all.at[pl.ds(pl.multiple_of(own_start, rows_out), rows_out)])
    )
    join(1)
    for number in range(1, len(bits)):
        slope_add(number)
        if number + 1 < len(bits):
            slope_send(number + 1)
        if number < 3:
            join(number + 1)
    gathers[2].hop(1)
    for gather in gathers:
        gather.hops(2)
    weights[1].forward()
    for gather in gathers:
        gather.finish()
    for weight in weights:
        weight.finish()
    for copy in own + stores:
        copy.wait()
    wire.close()
    heads.close()
    outer.close()


class WeightGather:
    def __init__(self, wire, here, finals, near, far, cut=0, cuts=1):
        self.wire, self.here, self.near, self.far = wire, here, near, far
        self.size = finals[0].shape[0]
        self.rows = self.size // cuts
        self.shift = cut * self.rows
        model = near.shape[0]
        self.finals = [final.at[pl.ds(self.shift, self.rows)] for final in finals]
        self.starts = []
        for color, order in enumerate(here.colors()):
            start = color * (model // 2)
            rows = model // 2
            for bit in order[:-1]:
                rows //= 2
                start = start + here.side(bit) * rows
            self.starts.append(start)
        self.swaps, self.kept = [], []

    def _rows(self, start):
        return pl.ds(pl.multiple_of(start + self.shift, self.rows), self.rows)

    def _pass(self, start, source, bit, rows):
        copy = self.wire.send(
            source, self.near.at[self._rows(start)], {"seq": self.here.at(bit)}
        )
        start = start + rows - 2 * rows * self.here.side(bit)
        return (start, self.near.at[self._rows(start)], copy)

    def _swap(self, start, source):
        self.swaps.append(
            self.wire.send(source, self.far.at[self._rows(start)], {"seq": self.here.at(1)})
        )

    def start(self):
        self.held = []
        for color, order in enumerate(self.here.colors()):
            source, start = self.finals[color], self.starts[color]
            pieces = [(start, source, None)]
            if order[:-1]:
                pieces.append(self._pass(start, source, order[-2], self.size))
            self.held.append(pieces)

    def own(self):
        for color in (0, 1):
            source, start = self.finals[color], self.starts[color]
            self._swap(start, source)
            self.kept.append(self.wire.local(source, self.near.at[self._rows(start)]))

    def forward(self):
        for color, order in enumerate(self.here.colors()):
            rest = order[:-1]
            pieces = self.held[color]
            rows = self.size
            for position in range(len(rest) - 1, -1, -1):
                for start, source, copy in pieces:
                    if copy is not None:
                        copy.wait_recv()
                        self._swap(start, source)
                pieces = [(start, source, None) for start, source, _ in pieces]
                rows *= 2
                if position > 0:
                    pieces = pieces + [
                        self._pass(start, source, rest[position - 1], rows)
                        for start, source, _ in pieces
                    ]

    def finish(self):
        for copy in self.swaps:
            copy.wait_recv()
        for copy in self.kept:
            copy.wait()


def widen_kernel(near, far, out):
    core = lax.axis_index("seq") % 2
    units = near.shape[1]
    out[:, pl.ds(pl.multiple_of(core * units, units), units)] = near[...].astype(out.dtype)
    out[:, pl.ds(pl.multiple_of((1 - core) * units, units), units)] = far[...].astype(out.dtype)


def widen_pieces_kernel(count, steps, starts, *refs):
    nears, fars, out = refs[:count], refs[count : 2 * count], refs[2 * count]
    core = lax.axis_index("seq") % 2
    units = nears[0].shape[1]
    index = pl.program_id(0)
    for number in range(count):

        @pl.when(index // steps == number)
        def _(near=nears[number], far=fars[number]):
            own = pl.ds(pl.multiple_of(core * units, units), units)
            other = pl.ds(pl.multiple_of((1 - core) * units, units), units)
            out[:, own] = near[...].astype(out.dtype)
            out[:, other] = far[...].astype(out.dtype)


SENDS, LOCALS = 128, 96


def call(kernel, mesh_sizes, number, inputs, in_vmem, outputs, scratch, out_vmem=None):
    vmem = pl.BlockSpec(memory_space=pltpu.VMEM)
    anywhere = pl.BlockSpec(memory_space=pl.ANY)
    out_vmem = out_vmem or [True] * len(outputs)
    semaphores = [
        pltpu.SemaphoreType.DMA((SENDS,)),
        pltpu.SemaphoreType.DMA((SENDS,)),
        pltpu.SemaphoreType.DMA((LOCALS,)),
    ]
    return pl.pallas_call(
        functools.partial(kernel, *mesh_sizes),
        out_shape=[jax.ShapeDtypeStruct(shape, kind) for shape, kind in outputs],
        in_specs=[vmem if inside else anywhere for inside in in_vmem],
        out_specs=[vmem if inside else anywhere for inside in out_vmem],
        scratch_shapes=[pltpu.VMEM(shape, kind) for shape, kind in scratch] + semaphores,
        compiler_params=pltpu.CompilerParams(
            collective_id=number, has_side_effects=True, vmem_limit_bytes=VMEM_BYTES
        ),
    )(*inputs)


def widen(near, far):
    rows, units = near.shape
    step = min(256, rows)
    return pl.pallas_call(
        widen_kernel,
        grid=(rows // step,),
        out_shape=jax.ShapeDtypeStruct((rows, 2 * units), jnp.float32),
        in_specs=[pl.BlockSpec((step, units), lambda index: (index, 0))] * 2,
        out_specs=pl.BlockSpec((step, 2 * units), lambda index: (index, 0)),
        cost_estimate=pl.CostEstimate(
            flops=0, transcendentals=0, bytes_accessed=12 * rows * units
        ),
    )(near, far)


def widen_pieces(pieces, fars):
    rows, units = fars[0].shape
    count = len(fars)
    step = min(256, rows)
    steps = rows // step
    starts = jnp.stack([jnp.asarray(start, jnp.int32) // step for start, _ in pieces])

    def block(number):
        return pl.BlockSpec(
            (step, units),
            lambda index, starts: (jnp.clip(index - number * steps, 0, steps - 1), 0),
        )

    return pl.pallas_call(
        functools.partial(widen_pieces_kernel, count, steps),
        out_shape=jax.ShapeDtypeStruct((count * rows, 2 * units), jnp.float32),
        grid_spec=pltpu.PrefetchScalarGridSpec(
            num_scalar_prefetch=1,
            grid=(count * steps,),
            in_specs=[block(number) for number in range(count)] * 2,
            out_specs=pl.BlockSpec(
                (step, 2 * units), lambda index, starts: (starts[index // steps] + index % steps, 0)
            ),
        ),
        cost_estimate=pl.CostEstimate(
            flops=0, transcendentals=0, bytes_accessed=12 * count * rows * units
        ),
    )(starts, *[value for _, value in pieces], *fars)


VMEM_BYTES = 67_000_000


def per_device(
    inputs,
    cotangent,
    attention_gain,
    query_weight,
    key_weight,
    value_weight,
    output_weight,
    query_gain,
    key_gain,
    feedforward_gain,
    gate_weight,
    up_weight,
    down_weight,
):
    tokens = inputs.shape[1]
    model = inputs.shape[2]
    width = query_gain.shape[0]
    pair_heads = key_weight.shape[1] // width
    parts = lax.axis_size("seq")
    planes = lax.axis_size("fsdp")
    sizes = (parts, planes)
    chips = parts // 2
    copies = max(1, parts // pair_heads)
    place = lax.axis_index("seq")
    plane = lax.axis_index("fsdp")
    core = place % 2
    query_cols = model // parts
    head_cols = query_cols + 2 * width
    local_groups = query_cols // width
    shard = query_weight.shape[0]
    piece_rows = shard // parts
    length = parts * tokens
    units = gate_weight.shape[1] // 2
    f32, bf16 = jnp.float32, jnp.bfloat16
    halvings = chips.bit_length() - 2
    last_rows = model // 2 >> halvings
    rows_in = inputs.reshape(tokens, model)
    cot_rows = cotangent.reshape(tokens, model)

    pair_index = place // copies
    head_weights = jnp.concatenate(
        [
            lax.dynamic_slice(query_weight, (0, place * query_cols), (shard, query_cols)),
            lax.dynamic_slice(key_weight, (0, pair_index * width), (shard, width)),
            lax.dynamic_slice(value_weight, (0, pair_index * width), (shard, width)),
        ],
        axis=1,
    )
    piece_index = core * chips + place // 2
    out_piece = lax.dynamic_slice_in_dim(output_weight, piece_index * piece_rows, piece_rows, 0)
    source = rows_in.astype(f32)
    first = rms_factor(source)
    normed_in = (source * first * attention_gain).astype(bf16)
    cosine, sine = rope_tables(jnp.arange(length, dtype=jnp.int32), width)
    lanes = jnp.arange(2 * width)
    signed = jnp.where(lanes % width < width // 2, -1.0, 1.0) * jnp.concatenate([sine, sine], axis=1)
    heads_of = jnp.arange(head_cols) // width
    group = (heads_of[:, None] == heads_of[None, :]).astype(bf16)
    gain_row = jnp.concatenate([jnp.tile(query_gain, local_groups), key_gain, key_gain])[None, :]
    log_rows_count = -(-local_groups // 8) * 8
    normed_all, head_full, out_slice, proj, queries, pair_rows, out_rows, log_rows = call(
        functools.partial(front_kernel, width),
        sizes,
        0,
        (
            normed_in,
            head_weights,
            out_piece,
            gain_row,
            jnp.concatenate([cosine, cosine], axis=1),
            signed,
            group,
        ),
        (True,) * 7,
        [
            ((length, model), bf16),
            ((model, head_cols), bf16),
            ((query_cols, model), bf16),
            ((length, head_cols), f32),
            ((length, query_cols), bf16),
            ((length, 2 * width), bf16),
            ((length, query_cols), bf16),
            ((log_rows_count, length), f32),
        ],
        [((planes, piece_rows, model), bf16)] + [((length, 2 * width), bf16)] * 3,
    )
    query_proj = proj[:, :query_cols]
    key_proj = proj[:, query_cols : query_cols + width]
    log_rows = log_rows[:local_groups][None]

    half = model // 2
    scatter_scratch = [
        ((chips, tokens, model), bf16),
        ((chips, tokens, model), bf16),
        ((2, chips, tokens, half), bf16),
        ((halvings + 1, 2, chips, tokens, half), bf16),
    ]
    out_sum, cot_all = call(
        out_rows_kernel,
        sizes,
        1,
        (out_rows, out_slice, cot_rows),
        (True, True, True),
        [((tokens, model), f32), ((planes, 2, tokens, model), bf16)],
        scatter_scratch,
    )
    middle = source + out_sum
    second = rms_factor(middle)
    normed_mid = (middle * second * feedforward_gain).astype(bf16)
    quarter = model // 4
    rows_shape = (planes, tokens, model)
    line_scratch = [
        (rows_shape, bf16),
        (rows_shape, bf16),
        ((2, planes - 1, tokens, model), bf16),
    ]
    acts = (2 * planes * tokens, units)
    s_down, s_gate_a, s_gate_b, s_up_a, s_up_b, mid_grad, down_give, down_keep = call(
        feed_kernel,
        sizes,
        2,
        (normed_mid, cot_all.reshape(-1, model), gate_weight, up_weight, down_weight),
        (True, True, False, False, False),
        [((2, last_rows, units), bf16)]
        + [((last_rows, units), bf16)] * 4
        + [
            ((tokens, model), f32),
            (rows_shape, bf16),
            (rows_shape, bf16),
        ],
        [((model, units), bf16)] * 3
        + [((planes, 2, tokens, model), bf16)]
        + [(acts, bf16)] * 3
        + [((3, 2, quarter, units), bf16)]
        + [((3, 2, quarter >> stage, units), bf16) for stage in range(halvings)]
        + [(rows_shape, bf16)]
        + line_scratch,
        [True] * 6 + [False] * 2,
    )

    feedforward_slope = jnp.sum(mid_grad * middle * second, axis=0)
    middle_grad = cot_rows.astype(f32) + norm_back(mid_grad, middle, second, feedforward_gain)
    middle_half = middle_grad.astype(bf16)
    middle_all, t_down, down_sum = call(
        spread_kernel,
        sizes,
        4,
        (middle_half, s_down, down_give, down_keep),
        (True, True, False, False),
        [((length, model), bf16), ((2, last_rows, units), bf16), ((tokens, model), f32)],
        line_scratch,
    )
    block_rows = middle + down_sum

    def swap(value, bit):
        return lax.ppermute(value, "seq", [(i, i ^ bit) for i in range(parts)])

    *sent, middle_all = lax.optimization_barrier((s_gate_a, s_gate_b, s_up_a, s_up_b, middle_all))
    bit_orders = ([2 << i for i in range(halvings + 1)], [chips >> i for i in range(halvings + 1)])
    came = [swap(piece, bit_orders[number % 2][-1]) for number, piece in enumerate(sent)]

    attended_grad = inner_cols(middle_all, out_slice).astype(bf16)
    query_back, pair_back = attend_back(
        queries, pair_rows, out_rows, log_rows, attended_grad, local_groups, width
    )
    key_back = pair_back[:, :width]
    value_back = pair_back[:, width:]
    _, query_pull = jax.vjp(
        lambda proj_in, gain_in: prepare(proj_in, gain_in, cosine, sine), query_proj, query_gain
    )
    query_proj_grad, query_slope = query_pull(query_back)
    _, key_pull = jax.vjp(
        lambda proj_in, gain_in: prepare(proj_in, gain_in, cosine, sine), key_proj, key_gain
    )
    key_proj_grad, key_slope = key_pull(key_back)
    halves = jnp.concatenate([query_proj_grad, key_proj_grad, value_back], axis=1).astype(bf16)
    head_part = inner_rows(normed_all, halves).astype(bf16).reshape(planes, shard, head_cols)
    out_part = inner_rows(out_rows, middle_all).astype(bf16)

    gains = jnp.concatenate([query_slope, key_slope])
    gains = jnp.pad(gains, (0, model - gains.shape[0]))
    slopes = jnp.stack([feedforward_slope, gains])
    slopes = jnp.pad(slopes, ((1, 5), (0, 0)))
    rounds = (parts * planes).bit_length() - 1
    side = ((model, units), bf16)
    piece = ((last_rows, units), bf16)
    in_grad, near_down, far_down, query_all, pair_all, outer_all, slopes, *pieces = call(
        final_kernel,
        sizes,
        5,
        (halves, head_full, head_part, out_part, t_down, rows_in, first, slopes, *sent, *came),
        (True, True, False, False, True, True, True, True) + (False,) * 8,
        [
            ((tokens, model), f32),
            side,
            side,
            ((shard, model), bf16),
            ((parts, shard, 2 * width), bf16),
            ((shard, model), bf16),
            ((8, model), f32),
        ]
        + [piece] * 4,
        scatter_scratch
        + [
            ((planes, shard, head_cols), bf16),
            ((2, planes - 1, shard, head_cols), bf16),
            ((planes, piece_rows, model), bf16),
            ((2, planes - 1, piece_rows, model), bf16),
            ((shard, head_cols), bf16),
            ((piece_rows, model), bf16),
            ((4, last_rows, units), bf16),
            ((4, last_rows, units), bf16),
            ((rounds, 8, model), f32),
            ((rounds, 8, model), f32),
        ],
        [True, False, False] + [True] * 4 + [False] * 4,
    )
    pieces, near_down, far_down, in_grad = lax.optimization_barrier(
        (pieces, near_down, far_down, in_grad)
    )
    input_rows = (middle_grad + norm_back(in_grad, source, first, attention_gain)).astype(bf16)

    def plane_pieces(values):
        whole = []
        for color, order in enumerate(bit_orders):
            start, rows = color * (model // 2), model // 2
            for bit in order[:-1]:
                rows //= 2
                start = start + (place // bit) % 2 * rows
            held = [(start, values[color])]
            rows = last_rows
            for bit in order[-2::-1]:
                held = held + [
                    (start + rows - 2 * rows * ((place // bit) % 2), swap(value, bit))
                    for start, value in held
                ]
                rows *= 2
            whole = whole + held
        return whole

    gate_pieces = plane_pieces(pieces[:2])
    grad_down = widen(near_down, far_down)
    grad_query = query_all.astype(f32)
    grad_pair = pair_all.astype(f32)
    grad_pair = grad_pair.reshape(parts // copies, copies, shard, 2, width).sum(axis=1)
    grad_key = grad_pair[:, :, 0].transpose(1, 0, 2).reshape(shard, -1)
    grad_value = grad_pair[:, :, 1].transpose(1, 0, 2).reshape(shard, -1)
    grad_output = outer_all.astype(f32)
    pieces[2:], gate_pieces, grad_down, grad_query, grad_output, input_rows = (
        lax.optimization_barrier(
            (pieces[2:], gate_pieces, grad_down, grad_query, grad_output, input_rows)
        )
    )
    up_pieces = plane_pieces(pieces[2:])
    grad_gate = widen_pieces(gate_pieces, [swap(value, 1) for _, value in gate_pieces])
    up_pieces, grad_gate = lax.optimization_barrier((up_pieces, grad_gate))
    grad_up = widen_pieces(up_pieces, [swap(value, 1) for _, value in up_pieces])
    attention_slope, feedforward_slope = slopes[0], slopes[1]
    query_slope, key_slope = slopes[2, :width], slopes[2, width : 2 * width]
    block_out = block_rows.astype(bf16).reshape(1, tokens, model)
    input_grad = input_rows.reshape(1, tokens, model)
    return (
        block_out,
        input_grad,
        attention_slope,
        grad_query,
        grad_key,
        grad_value,
        grad_output,
        query_slope,
        key_slope,
        feedforward_slope,
        grad_gate,
        grad_up,
        grad_down,
    )


def solution(mesh):
    in_specs = (
        P("fsdp", "seq", None),
        P("fsdp", "seq", None),
        P(),
        P("fsdp", None),
        P("fsdp", None),
        P("fsdp", None),
        P("fsdp", None),
        P(),
        P(),
        P(),
        P(None, "fsdp"),
        P(None, "fsdp"),
        P(None, "fsdp"),
    )
    out_specs = (
        P("fsdp", "seq", None),
        P("fsdp", "seq", None),
        P(),
        P("fsdp", None),
        P("fsdp", None),
        P("fsdp", None),
        P("fsdp", None),
        P(),
        P(),
        P(),
        P(None, "fsdp"),
        P(None, "fsdp"),
        P(None, "fsdp"),
    )
    return jax.shard_map(
        per_device, mesh=mesh, in_specs=in_specs, out_specs=out_specs, check_vma=False
    )
```

```python
import functools

import jax
import jax.numpy as jnp
from jax import lax
from jax.experimental import pallas as pl
from jax.experimental.pallas import tpu as pltpu
from jax.sharding import PartitionSpec as P

EPS = 1e-05
THETA = 1000000.0


def rotate_half(values):
    half = values.shape[-1] // 2
    return jnp.concatenate([-values[..., half:], values[..., :half]], axis=-1)


def rope_tables(positions, width):
    exponents = jnp.arange(width // 2).astype(jnp.float32) * 2.0 / width
    rates = jnp.power(jnp.float32(THETA), -exponents)
    angle = positions.astype(jnp.float32)[:, None] * rates[None, :]
    angle = jnp.concatenate([angle, angle], axis=-1)
    return (jnp.cos(angle), jnp.sin(angle))


def prepare(proj, gain, cosine, sine):
    rows = proj.shape[0]
    width = gain.shape[0]
    split = proj.reshape(rows, -1, width)
    factor = lax.rsqrt(jnp.mean(split * split, axis=-1, keepdims=True) + EPS)
    normed = split * factor * gain
    turned = normed * cosine[:, None, :] + rotate_half(normed) * sine[:, None, :]
    return turned.reshape(rows, -1)


def matmul(left, right):
    return jnp.dot(left, right, preferred_element_type=jnp.float32)


def inner_rows(left, right):
    return lax.dot_general(
        left, right, (((0,), (0,)), ((), ())), preferred_element_type=jnp.float32
    )


def inner_cols(left, right):
    return lax.dot_general(
        left, right, (((1,), (1,)), ((), ())), preferred_element_type=jnp.float32
    )


def rms_factor(values):
    return lax.rsqrt(jnp.mean(values * values, axis=-1, keepdims=True) + EPS)


def norm_back(grad, values, factor, gain):
    scaled = grad * gain
    return factor * (
        scaled - values * factor * factor * jnp.mean(scaled * values, axis=-1, keepdims=True)
    )


def gate_back(hidden_grad, gate, lifted):
    sigma = jax.nn.sigmoid(gate)
    gate_grad = (hidden_grad * lifted * sigma * (1.0 + gate * (1.0 - sigma))).astype(jnp.bfloat16)
    lifted_grad = (hidden_grad * gate * sigma).astype(jnp.bfloat16)
    return (gate_grad, lifted_grad)


def activate(gate, lifted):
    return (gate * jax.nn.sigmoid(gate) * lifted).astype(jnp.bfloat16)


def split_heads(query_rows, pair_rows, groups, width):
    length = query_rows.shape[0]
    key_heads = pair_rows.shape[1] // (2 * width)
    queries = query_rows.reshape(length, key_heads, groups, width)
    keys = pair_rows[:, : key_heads * width].reshape(length, key_heads, width)
    values = pair_rows[:, key_heads * width :].reshape(length, key_heads, width)
    return (queries, keys, values, key_heads)


def attend_heads(query_rows, pair_rows, groups, width):
    length = query_rows.shape[0]
    queries, keys, values, key_heads = split_heads(query_rows, pair_rows, groups, width)
    block = min(512, length)
    scale = width ** (-0.5)
    offsets = jnp.arange(block)

    def query_step(index, state):
        out_rows, log_rows = state
        query_block = lax.dynamic_slice_in_dim(queries, index * block, block, 0)

        def key_step(inner, carry):
            summed, total = carry
            key_block = lax.dynamic_slice_in_dim(keys, inner * block, block, 0)
            value_block = lax.dynamic_slice_in_dim(values, inner * block, block, 0)
            scores = (
                jnp.einsum(
                    "qhgd,shd->hgqs", query_block, key_block, preferred_element_type=jnp.float32
                )
                * scale
            )
            allowed = (index * block + offsets)[:, None] >= (inner * block + offsets)[None, :]
            weights = jnp.where(allowed, jnp.exp(scores), 0.0)
            summed = summed + jnp.einsum(
                "hgqs,shd->hgqd",
                weights.astype(jnp.bfloat16),
                value_block,
                preferred_element_type=jnp.float32,
            )
            return (summed, total + jnp.sum(weights, axis=-1))

        initial = (
            jnp.zeros((key_heads, groups, block, width), jnp.float32),
            jnp.zeros((key_heads, groups, block), jnp.float32),
        )
        summed, total = lax.fori_loop(0, index + 1, key_step, initial)
        result = (summed / total[..., None]).astype(jnp.bfloat16)
        result = result.transpose(2, 0, 1, 3).reshape(block, key_heads * groups * width)
        out_rows = lax.dynamic_update_slice_in_dim(out_rows, result, index * block, 0)
        log_rows = lax.dynamic_update_slice_in_dim(log_rows, jnp.log(total), index * block, 2)
        return (out_rows, log_rows)

    start = (
        jnp.zeros((length, key_heads * groups * width), jnp.bfloat16),
        jnp.zeros((key_heads, groups, length), jnp.float32),
    )
    return lax.fori_loop(0, length // block, query_step, start)


def attend_back(query_rows, pair_rows, out_rows, log_rows, grad_rows, groups, width):
    length = query_rows.shape[0]
    queries, keys, values, key_heads = split_heads(query_rows, pair_rows, groups, width)
    outs = out_rows.reshape(length, key_heads, groups, width)
    grads = grad_rows.reshape(length, key_heads, groups, width)
    correction = jnp.sum(grads.astype(jnp.float32) * outs.astype(jnp.float32), axis=-1)
    block = min(512, length)
    scale = width ** (-0.5)
    offsets = jnp.arange(block)

    def query_step(index, state):
        query_grad, key_grad, value_grad = state
        query_block = lax.dynamic_slice_in_dim(queries, index * block, block, 0)
        grad_block = lax.dynamic_slice_in_dim(grads, index * block, block, 0)
        shift_block = lax.dynamic_slice_in_dim(correction, index * block, block, 0).transpose(
            1, 2, 0
        )
        log_block = lax.dynamic_slice_in_dim(log_rows, index * block, block, 2)

        def key_step(inner, carry):
            block_grad, key_sum, value_sum = carry
            key_block = lax.dynamic_slice_in_dim(keys, inner * block, block, 0)
            value_block = lax.dynamic_slice_in_dim(values, inner * block, block, 0)
            scores = (
                jnp.einsum(
                    "qhgd,shd->hgqs", query_block, key_block, preferred_element_type=jnp.float32
                )
                * scale
            )
            allowed = (index * block + offsets)[:, None] >= (inner * block + offsets)[None, :]
            weights = jnp.where(allowed, jnp.exp(scores - log_block[..., None]), 0.0)
            value_part = jnp.einsum(
                "hgqs,qhgd->shd",
                weights.astype(jnp.bfloat16),
                grad_block,
                preferred_element_type=jnp.float32,
            )
            prob_grad = jnp.einsum(
                "qhgd,shd->hgqs", grad_block, value_block, preferred_element_type=jnp.float32
            )
            score_grad = (weights * (prob_grad - shift_block[..., None]) * scale).astype(
                jnp.bfloat16
            )
            block_grad = block_grad + jnp.einsum(
                "hgqs,shd->qhgd", score_grad, key_block, preferred_element_type=jnp.float32
            )
            key_part = jnp.einsum(
                "hgqs,qhgd->shd", score_grad, query_block, preferred_element_type=jnp.float32
            )
            key_sum = lax.dynamic_update_slice_in_dim(
                key_sum,
                lax.dynamic_slice_in_dim(key_sum, inner * block, block, 0) + key_part,
                inner * block,
                0,
            )
            value_sum = lax.dynamic_update_slice_in_dim(
                value_sum,
                lax.dynamic_slice_in_dim(value_sum, inner * block, block, 0) + value_part,
                inner * block,
                0,
            )
            return (block_grad, key_sum, value_sum)

        initial = (jnp.zeros((block, key_heads, groups, width), jnp.float32), key_grad, value_grad)
        block_grad, key_grad, value_grad = lax.fori_loop(0, index + 1, key_step, initial)
        query_grad = lax.dynamic_update_slice_in_dim(query_grad, block_grad, index * block, 0)
        return (query_grad, key_grad, value_grad)

    state = (
        jnp.zeros((length, key_heads, groups, width), jnp.float32),
        jnp.zeros((length, key_heads, width), jnp.float32),
        jnp.zeros((length, key_heads, width), jnp.float32),
    )
    query_grad, key_grad, value_grad = lax.fori_loop(0, length // block, query_step, state)
    pair_grad = jnp.concatenate(
        [
            key_grad.reshape(length, key_heads * width),
            value_grad.reshape(length, key_heads * width),
        ],
        axis=1,
    )
    return (query_grad.reshape(length, key_heads * groups * width), pair_grad)


MESH = pl.DeviceIdType.MESH


def flip(index, mask, bits):
    for bit in bits:
        if mask & bit:
            index = index + bit - 2 * bit * ((index // bit) % 2)
    return index


class Place:
    def __init__(self, parts, planes):
        self.parts, self.planes = parts, planes
        self.seat = lax.axis_index("seq")
        self.plane = lax.axis_index("fsdp")
        self.core = self.seat % 2
        self.chip = self.seat // 2
        self.seat_bits = [1 << i for i in range(parts.bit_length() - 1)]
        self.chip_bits = self.seat_bits[1:]
        self.plane_bits = [1 << i for i in range(planes.bit_length() - 1)]

    def at(self, mask):
        return flip(self.seat, mask, self.seat_bits)

    def side(self, bit):
        return (self.seat // bit) % 2

    def colors(self):
        return (self.chip_bits, self.chip_bits[::-1])

    def enter(self, masks=(), line=False, plane_masks=()):
        barrier = pltpu.get_barrier_semaphore()
        peers = [{"seq": self.at(mask)} for mask in masks]
        if line:
            peers.append({"fsdp": (self.plane + 1) % self.planes})
            peers.append({"fsdp": (self.plane + self.planes - 1) % self.planes})
        for mask in plane_masks:
            peers.append({"fsdp": flip(self.plane, mask, self.plane_bits)})
        for peer in peers:
            pl.semaphore_signal(barrier, inc=1, device_id=peer, device_id_type=MESH)
        pl.semaphore_wait(barrier, len(peers))


class Wire:
    def __init__(self, sends, receives, locals_):
        self.sends, self.receives, self.locals = sends, receives, locals_
        self.count = self.local_count = 0
        self.open = []

    def remote(self, source, target, device):
        number = self.count
        self.count += 1
        return pltpu.make_async_remote_copy(
            src_ref=source,
            dst_ref=target,
            send_sem=self.sends.at[number],
            recv_sem=self.receives.at[number],
            device_id=device,
            device_id_type=MESH,
        )

    def send(self, source, target, device):
        copy = self.remote(source, target, device)
        copy.start()
        self.open.append(copy)
        return copy

    def quiet(self, source, target):
        number = self.local_count
        self.local_count += 1
        return pltpu.make_async_copy(source, target, self.locals.at[number])

    def local(self, source, target):
        copy = self.quiet(source, target)
        copy.start()
        return copy

    def sent(self, copy):
        copy.wait_send()
        self.open = [other for other in self.open if other is not copy]

    def close(self):
        for copy in self.open:
            copy.wait_send()


def add_rows(target, left, right, step=64):
    rows = target.shape[0]
    step = min(step, rows)

    def body(index, carry):
        at = pl.ds(pl.multiple_of(index * step, step), step)
        total = left[at, :].astype(jnp.float32) + right[at, :].astype(jnp.float32)
        target[at, :] = total.astype(target.dtype)
        return carry

    lax.fori_loop(0, rows // step, body, 0)


class LineGather:
    def __init__(self, wire, here, source, target, share=None):
        self.here = here
        planes, plane = here.planes, here.plane
        above = {"fsdp": (plane + 1) % planes}
        below = {"fsdp": (plane + planes - 1) % planes}
        self.ups, self.downs = {}, {}
        for step in range(1, planes):
            lower = (plane + planes - step + 1) % planes
            upper = (plane + step - 1) % planes
            first = step == 1
            self.ups[step] = wire.remote(
                source if first else target(lower), target(lower), above
            )
            self.downs[step] = wire.remote(
                source if first else target(upper), target(upper), below
            )
        self.shared = {}
        if share is not None:
            for step in range(1, planes):
                for way, shift in ((0, planes - step), (1, step)):
                    index = (plane + shift) % planes
                    self.shared[(step, way)] = wire.remote(
                        target(index), share(index), {"seq": here.at(1)}
                    )

    def start(self, step):
        planes, plane = self.here.planes, self.here.plane

        @pl.when((plane >= step - 1) & (plane <= planes - 2))
        def _():
            self.ups[step].start()

        @pl.when((plane + step <= planes) & (plane >= 1))
        def _():
            self.downs[step].start()

    def arrive(self, step):
        planes, plane = self.here.planes, self.here.plane

        @pl.when(plane >= step)
        def _():
            self.ups[step].wait_recv()
            if self.shared:
                self.shared[(step, 0)].start()

        @pl.when(plane + step <= planes - 1)
        def _():
            self.downs[step].wait_recv()
            if self.shared:
                self.shared[(step, 1)].start()

    def close(self, shared_taken=False):
        planes, plane = self.here.planes, self.here.plane
        for (step, way), copy in self.shared.items():

            @pl.when(plane >= step if way == 0 else plane + step <= planes - 1)
            def _(copy=copy):
                copy.wait_send()
                if not shared_taken:
                    copy.wait_recv()

        for step in range(1, planes):

            @pl.when((plane >= step - 1) & (plane <= planes - 2))
            def _(step=step):
                self.ups[step].wait_send()

            @pl.when((plane + step <= planes) & (plane >= 1))
            def _(step=step):
                self.downs[step].wait_send()


class Lines:
    def __init__(self, members):
        self.members = members

    def start(self, step):
        for member in self.members:
            member.start(step)

    def pass_on(self, step):
        for member in self.members:
            member.arrive(step)
            if step + 1 < member.here.planes:
                member.start(step + 1)

    def step(self, step):
        for member in self.members:
            member.step(step)

    def close(self, *options):
        for member in self.members:
            member.close(*options)


def gather_lines(wire, here, source, target, share=None, cuts=2):
    rows = source.shape[0] // cuts
    members = []
    for cut in range(cuts):
        at = pl.ds(cut * rows, rows)
        members.append(
            LineGather(
                wire,
                here,
                source.at[at],
                lambda index, at=at: target(index).at[at],
                None if share is None else lambda index, at=at: share(index).at[at],
            )
        )
    return Lines(members)


class LineScatter:
    def __init__(self, wire, here, term, landing):
        self.wire, self.here, self.term, self.landing = wire, here, term, landing
        planes, plane = here.planes, here.plane
        above = {"fsdp": (plane + 1) % planes}
        below = {"fsdp": (plane + planes - 1) % planes}
        self.ups, self.downs = {}, {}
        for step in range(1, planes):
            self.ups[step] = wire.remote(
                term((plane + planes - step) % planes), landing(0, step - 1), above
            )
            self.downs[step] = wire.remote(
                term((plane + step) % planes), landing(1, step - 1), below
            )

    def step(self, step):
        planes, plane = self.here.planes, self.here.plane
        mirror = planes - 1 - plane
        for way, (position, copies, dest) in enumerate(
            (
                (plane, self.ups, (plane + planes - step) % planes),
                (mirror, self.downs, (plane + step) % planes),
            )
        ):
            if step > 1:

                @pl.when((position >= 1) & (position <= step - 1))
                def _(way=way, copies=copies, dest=dest):
                    copies[step - 1].wait_recv()
                    term = self.term(dest)
                    add_rows(term, term, self.landing(way, step - 2))

            @pl.when(position <= step - 1)
            def _(copies=copies):
                copies[step].start()

    def finish(self, out):
        planes, plane = self.here.planes, self.here.plane
        own = self.term(plane)
        last = planes - 1

        @pl.when(plane >= 1)
        def _():
            self.ups[last].wait_recv()

        @pl.when(plane <= planes - 2)
        def _():
            self.downs[last].wait_recv()

        @pl.when(plane == 0)
        def _():
            add_rows(out, own, self.landing(1, last - 1))

        @pl.when(plane == planes - 1)
        def _():
            add_rows(out, own, self.landing(0, last - 1))

        @pl.when((plane >= 1) & (plane <= planes - 2))
        def _():
            add_rows(own, own, self.landing(0, last - 1))
            add_rows(out, own, self.landing(1, last - 1))

    def close(self):
        planes, plane = self.here.planes, self.here.plane
        mirror = planes - 1 - plane
        for step in range(1, planes):

            @pl.when(plane <= step - 1)
            def _(step=step):
                self.ups[step].wait_send()

            @pl.when(mirror <= step - 1)
            def _(step=step):
                self.downs[step].wait_send()


class PlaneGather:
    def __init__(self, wire, here, source, target):
        self.wire, self.here, self.source, self.target = wire, here, source, target
        self.incoming = {}

    def _send(self, mask, color, bit):
        here = self.here
        target = self.target(here.at(mask), color)
        source = self.source(color) if mask == 0 else target
        self.incoming[(mask ^ bit, color)] = self.wire.send(
            source, target, {"seq": here.at(bit)}
        )

    def start(self):
        for position in range(len(self.here.chip_bits)):
            for color, bits in enumerate(self.here.colors()):
                self._send(0, color, bits[position])
        for color in (0, 1):
            self._send(0, color, 1)

    def hop(self, hops):
        here = self.here
        chips = here.parts // 2
        for mask in (mask * 2 for mask in range(1, chips)):
            if bin(mask).count("1") != hops:
                continue
            for color, bits in enumerate(here.colors()):
                self.incoming[(mask, color)].wait_recv()
                last = max(i for i, bit in enumerate(bits) if mask & bit)
                for bit in bits[last + 1 :]:
                    self._send(mask, color, bit)
                self._send(mask, color, 1)

    def hops(self, first=1):
        for hops in range(first, len(self.here.chip_bits) + 1):
            self.hop(hops)

    def finish(self):
        for mask in range(1, self.here.parts, 2):
            for color in (0, 1):
                self.incoming[(mask, color)].wait_recv()


class PlaneScatter:
    def __init__(self, wire, here, product, give, take, current, landing, model):
        self.wire, self.here, self.product = wire, here, product
        self.give, self.take, self.current, self.landing = give, take, current, landing
        self.model = model

    def start(self):
        here = self.here
        chips = here.parts // 2
        self.swaps = {}
        tokens = self.give.shape[1]
        seats = [2 * flip(here.chip, mask, [b // 2 for b in here.chip_bits]) for mask in range(chips)]
        for part in range(self.model // 512):
            columns = slice(part * 512, (part + 1) * 512)
            rows = self.product([seat + 1 - here.core for seat in seats], columns)
            for mask in range(chips):
                self.give[mask, :, columns] = rows[mask * tokens : (mask + 1) * tokens].astype(
                    self.give.dtype
                )
        for mask in range(chips)[::-1]:
            self.swaps[mask] = self.wire.send(
                self.give.at[mask], self.take.at[mask], {"seq": here.at(1)}
            )
        half = self.model // 2
        for part in range(self.model // 512):
            columns = slice(part * 512, (part + 1) * 512)
            rows = self.product([seat + here.core for seat in seats], columns)
            color, inside = divmod(part * 512, half)
            for mask in range(chips):
                self.current[color, mask, :, inside : inside + 512] = rows[
                    mask * tokens : (mask + 1) * tokens
                ].astype(self.current.dtype)

    def join(self):
        half = self.model // 2
        chips = self.here.parts // 2
        for mask in range(chips)[::-1]:
            self.swaps[mask].wait_recv()
            for color in (0, 1):
                mine = self.current.at[color, mask]
                add_rows(mine, mine, self.take.at[mask, :, pl.ds(color * half, half)])

    def stage(self, position):
        here = self.here
        self.moved = {}
        for color, bits in enumerate(here.colors()):
            bit = bits[position]
            done = sum(bits[:position])
            for mask in range(here.parts // 2):
                if mask * 2 & bit and not mask * 2 & done:
                    low = mask ^ (bit // 2)
                    self.moved[(color, low)] = self.wire.send(
                        self.current.at[color, mask],
                        self.landing.at[position, color, low],
                        {"seq": here.at(bit)},
                    )

    def settle(self, position, out):
        half = self.model // 2
        last = position == len(self.here.chip_bits) - 1
        for (color, low), copy in self.moved.items():
            copy.wait_recv()
            mine = self.current.at[color, low]
            if last:
                target = out.at[:, pl.ds(color * half, half)]
            else:
                target = mine
            add_rows(target, mine, self.landing.at[position, color, low])


def pick_lanes(low, high, width):
    lane = lax.broadcasted_iota(jnp.int32, low.shape, low.ndim - 1)
    return jnp.where(lane % (2 * width) < width, low, high)


def group_mean(values, group, width):
    high = values.astype(jnp.bfloat16)
    low = (values - high.astype(jnp.float32)).astype(jnp.bfloat16)
    total = jnp.dot(high, group, preferred_element_type=jnp.float32) + jnp.dot(
        low, group, preferred_element_type=jnp.float32
    )
    return total * (1.0 / width)


def turn(values, width):
    lanes = values.shape[1]
    half = width // 2
    return pick_lanes(
        pltpu.roll(values, lanes - half, 1), pltpu.roll(values, half, 1), half
    )


def attend_block(index, block, width, heads, queries, pair, twin, left, right, out_rows, logs):
    rows = pl.ds(index * block, block)
    before = index * block
    columns = 2 * width
    row = lax.broadcasted_iota(jnp.int32, (block, block), 0)
    column = lax.broadcasted_iota(jnp.int32, (block, block), 1)
    allowed = row >= column
    contract = (((1,), (1,)), ((), ()))
    totals = []
    for number in range(heads // 2):
        at = pl.ds(number * columns, columns)
        both = queries[rows, at]
        both = (both.astype(jnp.float32) * width**-0.5).astype(both.dtype)
        zero = jnp.zeros_like(both)
        result = None
        for side, values in ((0, left), (1, right)):
            mine = pick_lanes(both, zero, width) if side == 0 else pick_lanes(zero, both, width)
            scores = lax.dot_general(
                mine, twin[rows, :], contract, preferred_element_type=jnp.float32
            )
            weights = jnp.where(allowed, jnp.exp(scores), 0.0)
            total = jnp.sum(weights, axis=1, keepdims=True)
            summed = jnp.dot(
                weights.astype(jnp.bfloat16), values[rows, :], preferred_element_type=jnp.float32
            )
            if before:
                scores = lax.dot_general(
                    mine, twin[0:before, :], contract, preferred_element_type=jnp.float32
                )
                weights = jnp.exp(scores)
                total = total + jnp.sum(weights, axis=1, keepdims=True)
                summed = summed + jnp.dot(
                    weights.astype(jnp.bfloat16),
                    values[0:before, :],
                    preferred_element_type=jnp.float32,
                )
            totals.append(total)
            part = summed / total
            result = part if result is None else result + part
        out_rows[rows, at] = result.astype(out_rows.dtype)
    lane = lax.broadcasted_iota(jnp.int32, (block, 128), 1)
    table = jnp.ones((block, 128), jnp.float32)
    for number, total in enumerate(totals):
        table = jnp.where(lane == number, total, table)
    logs[rows, :] = jnp.log(table)


def back_block(
    index, block, width, heads, queries, grads, outs, logs, keys, values, query_back, key_back, value_back
):
    rows = pl.ds(index * block, block)
    before = index * block
    scale = width**-0.5
    row = lax.broadcasted_iota(jnp.int32, (block, block), 0)
    column = lax.broadcasted_iota(jnp.int32, (block, block), 1)
    allowed = row >= column
    across = (((1,), (1,)), ((), ()))
    down = (((0,), (0,)), ((), ()))
    f32 = jnp.float32
    spans = [(rows, True)] + ([(slice(0, before), False)] if before else [])
    for number in range(heads // 2):
        at = pl.ds(number * 2 * width, 2 * width)
        both, both_grad = queries[rows, at], grads[rows, at]
        product = both_grad.astype(f32) * outs[rows, at].astype(f32)
        zero = jnp.zeros_like(both)
        total = None
        for side in (0, 1):
            pick = (
                (lambda value, nothing: pick_lanes(value, nothing, width))
                if side == 0
                else (lambda value, nothing: pick_lanes(nothing, value, width))
            )
            query, grad = pick(both, zero), pick(both_grad, zero)
            scaled = (query.astype(f32) * scale).astype(query.dtype)
            shift = jnp.sum(pick(product, jnp.zeros_like(product)), axis=1, keepdims=True)
            head = 2 * number + side
            log = logs[rows, head : head + 1]
            for span, masked in spans:
                scores = lax.dot_general(
                    scaled, keys[0][span, :], across, preferred_element_type=f32
                )
                weights = jnp.exp(scores - log)
                if masked:
                    weights = jnp.where(allowed, weights, 0.0)
                prob_grad = lax.dot_general(
                    grad, values[0][span, :], across, preferred_element_type=f32
                )
                score_grad = (weights * (prob_grad - shift) * scale).astype(query.dtype)
                part = jnp.dot(score_grad, keys[1 + side][span, :], preferred_element_type=f32)
                total = part if total is None else total + part
                key_back[span, :] += lax.dot_general(
                    score_grad, query, down, preferred_element_type=f32
                )
                value_back[span, :] += lax.dot_general(
                    weights.astype(query.dtype), grad, down, preferred_element_type=f32
                )
        query_back[rows, at] = total


def back_kernel(
    width,
    normed,
    middle,
    out_slice,
    outs,
    logs,
    queries,
    pair,
    proj,
    gain,
    cosine,
    sine,
    group,
    halves,
    head_part,
    out_part,
    slopes,
    grads,
    query_back,
    key_back,
    value_back,
    *twins,
):
    length = normed.shape[0]
    block = min(256, length)
    blocks = length // block
    query_cols = queries.shape[1]
    heads = query_cols // width
    keys, values = twins[:3], twins[3:]
    f32 = jnp.float32
    key_back[...] = jnp.zeros_like(key_back)
    value_back[...] = jnp.zeros_like(value_back)

    def ready(index, carry):
        at = pl.ds(pl.multiple_of(index * block, block), block)
        grads[at, :] = lax.dot_general(
            middle[at, :], out_slice[...], (((1,), (1,)), ((), ())), preferred_element_type=f32
        ).astype(grads.dtype)
        both = pair[at, :].astype(f32)
        swapped = pltpu.roll(both, width, 1)
        zero = jnp.zeros_like(both)
        for refs, low, high in (
            (keys, both, swapped),
            (values, swapped, both),
        ):
            refs[0][at, :] = pick_lanes(low, high, width).astype(refs[0].dtype)
            refs[1][at, :] = pick_lanes(low, zero, width).astype(refs[0].dtype)
            refs[2][at, :] = pick_lanes(zero, high, width).astype(refs[0].dtype)
        return carry

    lax.fori_loop(0, blocks, ready, 0)
    for index in range(blocks):
        back_block(
            index,
            block,
            width,
            heads,
            queries,
            grads,
            outs,
            logs,
            keys,
            values,
            query_back,
            key_back,
            value_back,
        )

    def norms(index, slope):
        at = pl.ds(pl.multiple_of(index * block, block), block)
        key_sum, value_sum = key_back[at, :], value_back[at, :]
        key_sum = key_sum + pltpu.roll(key_sum, width, 1)
        value_sum = value_sum + pltpu.roll(value_sum, width, 1)
        back = jnp.concatenate(
            [query_back[at, :], pick_lanes(key_sum, value_sum, width)], axis=1
        )
        value = proj[at, :]
        factor = lax.rsqrt(group_mean(value * value, group[...], width) + EPS)
        repeat = value.shape[1] // cosine.shape[1]
        cosines = jnp.concatenate([cosine[at, :]] * repeat, axis=1)
        sines = jnp.concatenate([sine[at, :]] * repeat, axis=1)
        turned = back * cosines + turn(back * sines, width)
        slope = slope + jnp.sum(turned * value * factor, axis=0, keepdims=True)
        scaled = turned * gain[...]
        result = factor * (
            scaled - value * factor * factor * group_mean(scaled * value, group[...], width)
        )
        lane = lax.broadcasted_iota(jnp.int32, back.shape, 1)
        result = jnp.where(lane >= query_cols + width, back, result)
        halves[at, :] = result.astype(halves.dtype)
        return slope

    slope = lax.fori_loop(0, blocks, norms, jnp.zeros((1, proj.shape[1]), f32))
    slopes[...] = jnp.broadcast_to(slope, slopes.shape)

    def terms(number, carry):
        at = pl.ds(pl.multiple_of(number * 256, 256), 256)
        down = (((0,), (0,)), ((), ()))
        head_part[at, :] = lax.dot_general(
            normed[:, at], halves[...], down, preferred_element_type=f32
        ).astype(head_part.dtype)
        out_part[:, at] = lax.dot_general(
            outs[...], middle[:, at], down, preferred_element_type=f32
        ).astype(out_part.dtype)
        return carry

    lax.fori_loop(0, normed.shape[1] // 256, terms, 0)


def front_kernel(
    width,
    parts,
    planes,
    x,
    w,
    o,
    gain,
    cosine,
    sine,
    group,
    x_all,
    w_all,
    o_slice,
    proj,
    queries,
    pair,
    out_rows,
    logs,
    o_all,
    twin,
    left,
    right,
    *sems,
):
    here = Place(parts, planes)
    wire = Wire(*sems)
    tokens, shard, rows = x.shape[0], w.shape[0], o.shape[0]
    half = tokens // 2
    chips = parts // 2
    chip_masks = [mask * 2 for mask in range(1, chips)]
    here.enter(chip_masks + [1], line=True)
    weights = gather_lines(
        wire, here, w, lambda index: w_all.at[pl.ds(pl.multiple_of(index * shard, shard), shard)]
    )
    weights.start(1)
    plane_rows = PlaneGather(
        wire,
        here,
        lambda color: x.at[pl.ds(color * half, half)],
        lambda seat, color: x_all.at[pl.ds(pl.multiple_of(seat * tokens + color * half, half), half)],
    )
    plane_rows.start()
    kept = [
        wire.local(x, x_all.at[pl.ds(pl.multiple_of(here.seat * tokens, tokens), tokens)]),
        wire.local(w, w_all.at[pl.ds(pl.multiple_of(here.plane * shard, shard), shard)]),
        wire.local(o, o_all.at[here.plane]),
    ]
    outer = gather_lines(wire, here, o, lambda index: o_all.at[index])
    weights.members[0].arrive(1)
    if planes > 2:
        weights.members[0].start(2)
    plane_rows.hop(1)
    weights.members[1].arrive(1)
    if planes > 2:
        weights.members[1].start(2)
    outer.start(1)
    plane_rows.hops(2)
    spot = o_slice.at[pl.ds(pl.multiple_of(here.chip * rows, rows), rows)]
    deals = []
    for mask in chip_masks:
        chip = here.at(mask) // 2
        deals.append((chip, wire.remote(o_all.at[chip], spot, {"seq": here.at(mask)})))
    keep_own = wire.quiet(o_all.at[here.chip], spot)

    def deal(step):
        for chip, copy in deals + [(here.chip, keep_own)]:

            @pl.when((chip == here.plane + step) | (chip + step == here.plane))
            def _(copy=copy):
                copy.start()

    kept[2].wait()
    deal(0)
    for step in range(2, planes):
        weights.pass_on(step)
    plane_rows.finish()
    for copy in kept[:2]:
        copy.wait()
    length = x_all.shape[0]
    block = min(256, length)
    blocks = length // block
    query_cols = queries.shape[1]
    heads = query_cols // width

    def project(index, carry):
        at = pl.ds(pl.multiple_of(index * block, block), block)
        value = jnp.dot(x_all[at, :], w_all[...], preferred_element_type=jnp.float32)
        proj[at, :] = value
        factor = lax.rsqrt(group_mean(value * value, group[...], width) + EPS)
        normed = value * factor * gain[...]
        repeat = value.shape[1] // cosine.shape[1]
        cosines = jnp.concatenate([cosine[at, :]] * repeat, axis=1)
        sines = jnp.concatenate([sine[at, :]] * repeat, axis=1)
        turned = normed * cosines + turn(normed, width) * sines
        queries[at, :] = turned[:, :query_cols].astype(queries.dtype)
        keys, values = turned[:, query_cols:], value[:, query_cols:]
        both = pick_lanes(keys, values, width)
        pair[at, :] = both.astype(pair.dtype)
        swapped = pltpu.roll(both, width, 1)
        twin[at, :] = pick_lanes(both, swapped, width).astype(twin.dtype)
        zero = jnp.zeros_like(both)
        left[at, :] = pick_lanes(swapped, zero, width).astype(left.dtype)
        right[at, :] = pick_lanes(zero, both, width).astype(right.dtype)
        return carry

    lax.fori_loop(0, blocks, project, 0)
    waits = list(range(1, planes))
    for index in range(blocks):
        while waits and waits[0] * blocks <= (index + 1) * planes:
            step = waits.pop(0)
            outer.pass_on(step)
            deal(step)
        attend_block(
            index, block, width, heads, queries, pair, twin, left, right, out_rows, logs
        )
    for step in waits:
        outer.pass_on(step)
        deal(step)
    keep_own.wait()
    for _, copy in deals:
        copy.wait()
    wire.close()
    weights.close()
    outer.close()


def out_rows_kernel(
    parts, planes, a, w, c, out, c_all, give, take, current, landing, *sems
):
    here = Place(parts, planes)
    wire = Wire(*sems)
    tokens, model = c.shape
    here.enter([mask for mask in here.seat_bits], line=True)

    def product(seats, columns):
        rows = [a[pl.ds(pl.multiple_of(seat * tokens, tokens), tokens), :] for seat in seats]
        return jnp.dot(
            jnp.concatenate(rows, axis=0), w[:, columns], preferred_element_type=jnp.float32
        )

    def spot(index):
        return c_all.at[index, here.core]

    cots = gather_lines(wire, here, c, spot, spot)
    cots.start(1)
    own = wire.local(c, spot(here.plane))
    rows = PlaneScatter(wire, here, product, give, take, current, landing, model)
    rows.start()
    across = wire.send(c, spot(here.plane), {"seq": here.at(1)})
    rows.join()
    rows.stage(0)
    stages = len(here.chip_bits)
    for stage in range(stages):
        if stage + 1 < planes:
            cots.pass_on(stage + 1)
        rows.settle(stage, out)
        if stage + 1 < stages:
            rows.stage(stage + 1)
    for step in range(stages + 1, planes):
        cots.pass_on(step)
    own.wait()
    across.wait_recv()
    wire.close()
    cots.close()


def feed_kernel(
    parts,
    planes,
    m,
    cots,
    gate_weight,
    up_weight,
    down_weight,
    s_down,
    s_gate_a,
    s_gate_b,
    s_up_a,
    s_up_b,
    mid,
    down_give,
    down_keep,
    gate_half,
    up_half,
    down_half,
    mids,
    hidden,
    gate_grads,
    lifted_grads,
    away,
    *rest,
):
    here = Place(parts, planes)
    stages = len(here.chip_bits) - 1
    landings, rest = rest[:stages], rest[stages:]
    give, take, current, line_landing, *sems = rest
    wire = Wire(*sems)
    tokens, model = m.shape
    units = gate_half.shape[1]
    own_units = pl.ds(pl.multiple_of(here.core * units, units), units)
    loads = [
        wire.local(whole.at[:, own_units], part)
        for whole, part in (
            (gate_weight, gate_half),
            (up_weight, up_half),
            (down_weight, down_half),
        )
    ]
    here.enter(here.seat_bits, line=True)

    def spot(index):
        return mids.at[index, here.core]

    lines = gather_lines(wire, here, m, spot, spot)
    lines.start(1)
    across = wire.send(m, spot(here.plane), {"seq": here.at(1)})
    own = wire.local(m, spot(here.plane))

    def block(index):
        rows = pl.ds(pl.multiple_of(index * 2 * tokens, 2 * tokens), 2 * tokens)
        mid_rows = mids[index].reshape(2 * tokens, model)
        cot_rows = cots[rows, :]

        def part(number, carry):
            at = pl.ds(pl.multiple_of(number * 256, 256), 256)
            gate = jnp.dot(mid_rows, gate_half[:, at], preferred_element_type=jnp.float32)
            lifted = jnp.dot(mid_rows, up_half[:, at], preferred_element_type=jnp.float32)
            hidden_grad = jnp.dot(cot_rows, down_half[:, at], preferred_element_type=jnp.float32)
            sigma = 1.0 / (1.0 + jnp.exp(-gate))
            active = gate * sigma
            hidden[rows, at] = (active * lifted).astype(hidden.dtype)
            lifted_grads[rows, at] = (hidden_grad * active).astype(hidden.dtype)
            gate_grads[rows, at] = (
                hidden_grad * lifted * sigma * (1.0 + gate * (1.0 - sigma))
            ).astype(hidden.dtype)
            return carry

        lax.fori_loop(0, units // 256, part, 0)

    for load in loads:
        load.wait()
    own.wait()
    across.wait_recv()
    plane = here.plane
    block(plane)
    for step in range(1, planes):
        lines.pass_on(step)
        ups = jnp.where(plane >= step, 1, 0)
        downs = jnp.where(plane + step <= planes - 1, 1, 0)

        def arrived(number, carry, step=step, ups=ups):
            from_up = (number == 0) & (ups == 1)
            for way, chosen in ((0, from_up), (1, jnp.logical_not(from_up))):

                @pl.when(chosen)
                def _(way=way):
                    for line in lines.members:
                        line.shared[(step, way)].wait_recv()

            block(jnp.where(from_up, plane + planes - step, plane + step) % planes)
            return carry

        lax.fori_loop(0, ups + downs, arrived, 0)

    flat_mids = mids.reshape(2 * planes * tokens, model)
    pairs = ((cots, hidden), (flat_mids, gate_grads), (flat_mids, lifted_grads))
    quarter = model // 4
    moved = {}

    def gradient(target, pair, start):
        left, right = pair

        def part(number, carry):
            at = pl.ds(pl.multiple_of(start + number * 256, 256), 256)
            target[pl.ds(pl.multiple_of(number * 256, 256), 256), :] = lax.dot_general(
                left[:, at],
                right[...],
                (((0,), (0,)), ((), ())),
                preferred_element_type=jnp.float32,
            ).astype(target.dtype)
            return carry

        lax.fori_loop(0, quarter // 256, part, 0)

    def first_half(color, mine):
        bit = here.colors()[color][0]
        side = here.side(bit) if mine else 1 - here.side(bit)
        return pl.multiple_of(color * (model // 2) + side * quarter, quarter)

    def send_away(number):
        for color, bits in enumerate(here.colors()):
            gradient(away.at[number, color], pairs[number], first_half(color, False))
            moved[(number, color)] = wire.send(
                away.at[number, color], landings[0].at[number, color], {"seq": here.at(bits[0])}
            )

    def mid_term(target, core):
        rows = [pl.ds(pl.multiple_of((2 * p + core) * tokens, tokens), tokens) for p in range(planes)]
        gates = jnp.concatenate([gate_grads[at, :] for at in rows], axis=0)
        lifts = jnp.concatenate([lifted_grads[at, :] for at in rows], axis=0)

        def part(number, carry):
            at = pl.ds(pl.multiple_of(number * 256, 256), 256)
            term = lax.dot_general(
                gates, gate_half[at, :], (((1,), (1,)), ((), ())), preferred_element_type=jnp.float32
            ) + lax.dot_general(
                lifts, up_half[at, :], (((1,), (1,)), ((), ())), preferred_element_type=jnp.float32
            )
            target[:, :, at] = term.reshape(planes, tokens, 256).astype(target.dtype)
            return carry

        lax.fori_loop(0, model // 256, part, 0)

    def down_term(target, core):
        rows = [pl.ds(pl.multiple_of((2 * p + core) * tokens, tokens), tokens) for p in range(planes)]
        hiddens = jnp.concatenate([hidden[at, :] for at in rows], axis=0)

        def part(number, carry):
            at = pl.ds(pl.multiple_of(number * 256, 256), 256)
            term = lax.dot_general(
                hiddens, down_half[at, :], (((1,), (1,)), ((), ())), preferred_element_type=jnp.float32
            )
            target[:, :, at] = term.reshape(planes, tokens, 256).astype(target.dtype)
            return carry

        lax.fori_loop(0, model // 256, part, 0)

    send_away(0)
    swaps = TokenSum(wire, here, current, take, line_landing)
    mid_term(give, 1 - here.core)
    swaps.start(give)
    send_away(1)
    mid_term(current, here.core)
    swaps.join()
    swaps.step(1)
    send_away(2)
    for step in range(2, planes):
        swaps.step(step)

    def final(number, color):
        if number == 0:
            return s_down.at[color]
        return ((s_gate_a, s_gate_b), (s_up_a, s_up_b))[number - 1][color]

    wire.sent(swaps.across)
    down_term(give, 1 - here.core)
    down_term(take, here.core)
    handed = [wire.local(give, down_give), wire.local(take, down_keep)]
    rows = quarter
    keeps = {}
    for number in range(3):
        for color in (0, 1):
            keep = final(number, color) if stages == 1 else away.at[number, color]
            if stages > 1:
                wire.sent(moved[(number, color)])
            gradient(keep, pairs[number], first_half(color, True))
            keeps[(number, color)] = (keep, 0)
    swaps.finish(mid)
    for stage in range(stages):
        last = stage == stages - 1
        for number in range(3):
            for color, bits in enumerate(here.colors()):
                keep, begin = keeps[(number, color)]
                moved[(number, color)].wait_recv()
                mine = keep.at[pl.ds(begin, rows)]
                if last:
                    add_rows(final(number, color), mine, landings[stage].at[number, color])
                else:
                    add_rows(mine, mine, landings[stage].at[number, color])
                    bit = bits[stage + 1]
                    half = rows // 2
                    gone = pl.multiple_of(begin + (1 - here.side(bit)) * half, half)
                    moved[(number, color)] = wire.send(
                        keep.at[pl.ds(gone, half)],
                        landings[stage + 1].at[number, color],
                        {"seq": here.at(bit)},
                    )
                    keeps[(number, color)] = (
                        keep,
                        pl.multiple_of(begin + here.side(bit) * half, half),
                    )
        rows //= 2
    for copy in handed:
        copy.wait()
    wire.close()
    lines.close(True)
    swaps.close()


class TokenSum:
    def __init__(self, wire, here, current, take, landing):
        self.wire, self.here = wire, here
        self.current, self.take = current, take
        self.cuts = 2
        rows = current.shape[1] // self.cuts
        self.lines = []
        for cut in range(self.cuts):
            at = pl.ds(cut * rows, rows)
            self.lines.append(
                LineScatter(
                    wire,
                    here,
                    lambda index, at=at: current.at[index, at],
                    lambda way, step, at=at: landing.at[way, step, at],
                )
            )

    def start(self, give):
        self.across = self.wire.send(give, self.take, {"seq": self.here.at(1)})

    def join(self):
        self.across.wait_recv()

        def body(index, carry):
            row = self.current.at[index]
            add_rows(row, row, self.take.at[index])
            return carry

        lax.fori_loop(0, self.here.planes, body, 0)

    def step(self, step):
        for line in self.lines:
            line.step(step)

    def finish(self, out):
        rows = out.shape[0] // self.cuts
        for cut, line in enumerate(self.lines):
            line.finish(out.at[pl.ds(cut * rows, rows)])

    def close(self):
        for line in self.lines:
            line.close()


def spread_kernel(
    parts, planes, h, s, give, keep, h_all, t, block, current, take, line_landing, *sems
):
    here = Place(parts, planes)
    wire = Wire(*sems)
    here.enter(here.seat_bits, line=True)
    tokens = h.shape[0]
    half = tokens // 2
    rows = PlaneGather(
        wire,
        here,
        lambda color: h.at[pl.ds(color * half, half)],
        lambda seat, color: h_all.at[pl.ds(pl.multiple_of(seat * tokens + color * half, half), half)],
    )
    swaps = TokenSum(wire, here, current, take, line_landing)
    swaps.start(give)
    kept = wire.local(keep, current)
    rows.start()
    own = wire.local(h, h_all.at[pl.ds(pl.multiple_of(here.seat * tokens, tokens), tokens)])
    kept.wait()
    swaps.join()
    swaps.step(1)
    rows.hop(1)
    moved = [
        wire.send(s.at[color], t.at[color], {"seq": here.at(bits[-1])})
        for color, bits in enumerate(here.colors())
    ]
    for step in range(2, planes):
        if step == 3:
            rows.hops(2)
        swaps.step(step)
    if planes <= 3:
        rows.hops(2)
    rows.finish()
    for color in (0, 1):
        moved[color].wait_recv()
        add_rows(t.at[color], t.at[color], s.at[color])
    own.wait()
    swaps.finish(block)
    wire.close()
    swaps.close()


def final_kernel(
    parts,
    planes,
    a,
    w,
    head_part,
    out_part,
    t_down,
    source,
    factor,
    slope,
    *rest,
):
    sent, rest = rest[:4], rest[4:]
    came, rest = rest[:4], rest[4:]
    out, near, far, query_all, pair_all, outer_all, slope_out, *rest = rest
    joined, rest = rest[:4], rest[4:]
    (
        give,
        take,
        current,
        landing,
        head_current,
        head_landing,
        dealt,
        out_landing,
        head_sum,
        out_sum,
        left,
        right,
        slope_sums,
        slope_landing,
        *sems,
    ) = rest
    here = Place(parts, planes)
    wire = Wire(*sems)
    tokens, model = out.shape
    shard = head_sum.shape[0]
    columns = query_all.shape[1] // parts
    rows_out = out_sum.shape[0]
    chips = parts // 2
    chip_masks = [mask * 2 for mask in range(1, chips)]
    here.enter(chip_masks + [1], line=True, plane_masks=here.plane_bits)
    weights = [
        WeightGather(wire, here, (t_down.at[0], t_down.at[1]), near, far, cut, 2)
        for cut in range(2)
    ]
    head_own = wire.local(head_part, head_current)
    deals = []
    for mask in chip_masks:
        chip = here.at(mask) // 2
        deals.append(
            wire.send(
                out_part.at[pl.ds(pl.multiple_of(chip * rows_out, rows_out), rows_out)],
                dealt.at[here.chip],
                {"seq": here.at(mask)},
            )
        )
    deal_own = wire.local(
        out_part.at[pl.ds(pl.multiple_of(here.chip * rows_out, rows_out), rows_out)],
        dealt.at[here.chip],
    )

    def product(seats, columns):
        rows = [a[pl.ds(pl.multiple_of(seat * tokens, tokens), tokens), :] for seat in seats]
        return lax.dot_general(
            jnp.concatenate(rows, axis=0),
            w[columns, :],
            (((1,), (1,)), ((), ())),
            preferred_element_type=jnp.float32,
        )

    heads = LineScatter(
        wire, here, lambda index: head_current.at[index], lambda way, step: head_landing.at[way, step]
    )
    outer = LineScatter(
        wire, here, lambda index: dealt.at[index], lambda way, step: out_landing.at[way, step]
    )
    head_own.wait()
    heads.step(1)
    rows = PlaneScatter(wire, here, product, give, take, current, landing, model)
    rows.start()
    loads = []
    for number in range(4):
        loads.append(
            (
                wire.local(sent[number], left.at[number]),
                wire.local(came[number], right.at[number]),
            )
        )
    heads.step(2)
    rows.join()
    rows.stage(0)
    weights[0].start()
    weights[0].own()
    deal_own.wait()
    for copy in deals:
        copy.wait_recv()
    outer.step(1)

    stores = []

    def join(number):
        for load in loads[number]:
            load.wait()
        add_rows(left.at[number], left.at[number], right.at[number])
        stores.append(wire.local(left.at[number], joined[number]))

    stages = len(here.chip_bits)
    for step in range(3, planes):
        heads.step(step)
    rows.settle(0, out)
    for stage in range(1, stages):
        rows.stage(stage)
        if stage + 1 < planes:
            outer.step(stage + 1)
        if stage == 1:
            heads.finish(head_sum)
        if stage + 1 < stages:
            rows.settle(stage, out)
    half, half_out = shard // 2, rows_out // 2

    def seat_columns(seat):
        return pl.ds(pl.multiple_of(seat * columns, columns), columns)

    gathers = [
        PlaneGather(
            wire,
            here,
            lambda color: head_sum.at[pl.ds(color * half, half), pl.ds(0, columns)],
            lambda seat, color: query_all.at[pl.ds(color * half, half), seat_columns(seat)],
        ),
        PlaneGather(
            wire,
            here,
            lambda color: head_sum.at[
                pl.ds(color * half, half), pl.ds(columns, pair_all.shape[2])
            ],
            lambda seat, color: pair_all.at[seat, pl.ds(color * half, half)],
        ),
        PlaneGather(
            wire,
            here,
            lambda color: out_sum.at[pl.ds(color * half_out, half_out)],
            lambda seat, color: outer_all.at[
                pl.ds(
                    pl.multiple_of(
                        ((seat % 2) * chips + seat // 2) * rows_out + color * half_out, half_out
                    ),
                    half_out,
                )
            ],
        ),
    ]
    own = []
    for gather in gathers[:2]:
        gather.start()
    own.append(
        wire.local(head_sum.at[:, pl.ds(0, columns)], query_all.at[:, seat_columns(here.seat)])
    )
    own.append(
        wire.local(
            head_sum.at[:, pl.ds(columns, pair_all.shape[2])], pair_all.at[here.seat]
        )
    )

    weights[1].start()
    weights[1].own()
    rows.settle(stages - 1, out)
    slope_sums[0] = slope[...]
    slope_sums[0, 0:1, :] = jnp.sum(out[...] * source[...].astype(jnp.float32) * factor[...], axis=0, keepdims=True)
    bits = [("seq", bit) for bit in here.seat_bits] + [("fsdp", bit) for bit in here.plane_bits]
    slope_copies = []

    def slope_send(number):
        axis, bit = bits[number]
        index = here.at(bit) if axis == "seq" else flip(here.plane, bit, here.plane_bits)
        slope_copies.append(
            wire.send(slope_sums.at[number], slope_landing.at[number], {axis: index})
        )

    def slope_add(number):
        slope_copies[number].wait_recv()
        target = slope_out if number == len(bits) - 1 else slope_sums.at[number + 1]
        target[...] = slope_sums[number] + slope_landing[number]

    slope_send(0)
    for step in range(stages + 1, planes):
        outer.step(step)
    join(0)
    gathers[0].hop(1)
    gathers[1].hop(1)
    slope_add(0)
    slope_send(1)
    outer.finish(out_sum)
    gathers[2].start()
    weights[0].forward()
    own_start = (here.core * chips + here.chip) * rows_out
    own.append(
        wire.local(out_sum, outer_all.at[pl.ds(pl.multiple_of(own_start, rows_out), rows_out)])
    )
    join(1)
    for number in range(1, len(bits)):
        slope_add(number)
        if number + 1 < len(bits):
            slope_send(number + 1)
        if number < 3:
            join(number + 1)
    gathers[2].hop(1)
    for gather in gathers:
        gather.hops(2)
    weights[1].forward()
    for gather in gathers:
        gather.finish()
    for weight in weights:
        weight.finish()
    for copy in own + stores:
        copy.wait()
    wire.close()
    heads.close()
    outer.close()


class WeightGather:
    def __init__(self, wire, here, finals, near, far, cut=0, cuts=1):
        self.wire, self.here, self.near, self.far = wire, here, near, far
        self.size = finals[0].shape[0]
        self.rows = self.size // cuts
        self.shift = cut * self.rows
        model = near.shape[0]
        self.finals = [final.at[pl.ds(self.shift, self.rows)] for final in finals]
        self.starts = []
        for color, order in enumerate(here.colors()):
            start = color * (model // 2)
            rows = model // 2
            for bit in order[:-1]:
                rows //= 2
                start = start + here.side(bit) * rows
            self.starts.append(start)
        self.swaps, self.kept = [], []

    def _rows(self, start):
        return pl.ds(pl.multiple_of(start + self.shift, self.rows), self.rows)

    def _pass(self, start, source, bit, rows):
        copy = self.wire.send(
            source, self.near.at[self._rows(start)], {"seq": self.here.at(bit)}
        )
        start = start + rows - 2 * rows * self.here.side(bit)
        return (start, self.near.at[self._rows(start)], copy)

    def _swap(self, start, source):
        self.swaps.append(
            self.wire.send(source, self.far.at[self._rows(start)], {"seq": self.here.at(1)})
        )

    def start(self):
        self.held = []
        for color, order in enumerate(self.here.colors()):
            source, start = self.finals[color], self.starts[color]
            pieces = [(start, source, None)]
            if order[:-1]:
                pieces.append(self._pass(start, source, order[-2], self.size))
            self.held.append(pieces)

    def own(self):
        for color in (0, 1):
            source, start = self.finals[color], self.starts[color]
            self._swap(start, source)
            self.kept.append(self.wire.local(source, self.near.at[self._rows(start)]))

    def forward(self):
        for color, order in enumerate(self.here.colors()):
            rest = order[:-1]
            pieces = self.held[color]
            rows = self.size
            for position in range(len(rest) - 1, -1, -1):
                for start, source, copy in pieces:
                    if copy is not None:
                        copy.wait_recv()
                        self._swap(start, source)
                pieces = [(start, source, None) for start, source, _ in pieces]
                rows *= 2
                if position > 0:
                    pieces = pieces + [
                        self._pass(start, source, rest[position - 1], rows)
                        for start, source, _ in pieces
                    ]

    def finish(self):
        for copy in self.swaps:
            copy.wait_recv()
        for copy in self.kept:
            copy.wait()


def widen_kernel(near, far, out):
    core = lax.axis_index("seq") % 2
    units = near.shape[1]
    out[:, pl.ds(pl.multiple_of(core * units, units), units)] = near[...].astype(out.dtype)
    out[:, pl.ds(pl.multiple_of((1 - core) * units, units), units)] = far[...].astype(out.dtype)


def widen_pieces_kernel(count, steps, starts, *refs):
    nears, fars, out = refs[:count], refs[count : 2 * count], refs[2 * count]
    core = lax.axis_index("seq") % 2
    units = nears[0].shape[1]
    index = pl.program_id(0)
    for number in range(count):

        @pl.when(index // steps == number)
        def _(near=nears[number], far=fars[number]):
            own = pl.ds(pl.multiple_of(core * units, units), units)
            other = pl.ds(pl.multiple_of((1 - core) * units, units), units)
            out[:, own] = near[...].astype(out.dtype)
            out[:, other] = far[...].astype(out.dtype)


SENDS, LOCALS = 128, 96


def call(kernel, mesh_sizes, number, inputs, in_vmem, outputs, scratch, out_vmem=None):
    vmem = pl.BlockSpec(memory_space=pltpu.VMEM)
    anywhere = pl.BlockSpec(memory_space=pl.ANY)
    out_vmem = out_vmem or [True] * len(outputs)
    semaphores = [
        pltpu.SemaphoreType.DMA((SENDS,)),
        pltpu.SemaphoreType.DMA((SENDS,)),
        pltpu.SemaphoreType.DMA((LOCALS,)),
    ]
    return pl.pallas_call(
        functools.partial(kernel, *mesh_sizes),
        out_shape=[jax.ShapeDtypeStruct(shape, kind) for shape, kind in outputs],
        in_specs=[vmem if inside else anywhere for inside in in_vmem],
        out_specs=[vmem if inside else anywhere for inside in out_vmem],
        scratch_shapes=[pltpu.VMEM(shape, kind) for shape, kind in scratch] + semaphores,
        compiler_params=pltpu.CompilerParams(
            collective_id=number, has_side_effects=True, vmem_limit_bytes=VMEM_BYTES
        ),
    )(*inputs)


def widen(near, far):
    rows, units = near.shape
    step = min(256, rows)
    return pl.pallas_call(
        widen_kernel,
        grid=(rows // step,),
        out_shape=jax.ShapeDtypeStruct((rows, 2 * units), jnp.float32),
        in_specs=[pl.BlockSpec((step, units), lambda index: (index, 0))] * 2,
        out_specs=pl.BlockSpec((step, 2 * units), lambda index: (index, 0)),
        cost_estimate=pl.CostEstimate(
            flops=0, transcendentals=0, bytes_accessed=12 * rows * units
        ),
    )(near, far)


def widen_pieces(pieces, fars):
    rows, units = fars[0].shape
    count = len(fars)
    step = min(256, rows)
    steps = rows // step
    starts = jnp.stack([jnp.asarray(start, jnp.int32) // step for start, _ in pieces])

    def block(number):
        return pl.BlockSpec(
            (step, units),
            lambda index, starts: (jnp.clip(index - number * steps, 0, steps - 1), 0),
        )

    return pl.pallas_call(
        functools.partial(widen_pieces_kernel, count, steps),
        out_shape=jax.ShapeDtypeStruct((count * rows, 2 * units), jnp.float32),
        grid_spec=pltpu.PrefetchScalarGridSpec(
            num_scalar_prefetch=1,
            grid=(count * steps,),
            in_specs=[block(number) for number in range(count)] * 2,
            out_specs=pl.BlockSpec(
                (step, 2 * units), lambda index, starts: (starts[index // steps] + index % steps, 0)
            ),
        ),
        cost_estimate=pl.CostEstimate(
            flops=0, transcendentals=0, bytes_accessed=12 * count * rows * units
        ),
    )(starts, *[value for _, value in pieces], *fars)


VMEM_BYTES = 67_000_000


def per_device(
    inputs,
    cotangent,
    attention_gain,
    query_weight,
    key_weight,
    value_weight,
    output_weight,
    query_gain,
    key_gain,
    feedforward_gain,
    gate_weight,
    up_weight,
    down_weight,
):
    tokens = inputs.shape[1]
    model = inputs.shape[2]
    width = query_gain.shape[0]
    pair_heads = key_weight.shape[1] // width
    parts = lax.axis_size("seq")
    planes = lax.axis_size("fsdp")
    sizes = (parts, planes)
    chips = parts // 2
    copies = max(1, parts // pair_heads)
    place = lax.axis_index("seq")
    plane = lax.axis_index("fsdp")
    core = place % 2
    query_cols = model // parts
    head_cols = query_cols + 2 * width
    local_groups = query_cols // width
    shard = query_weight.shape[0]
    piece_rows = shard // parts
    length = parts * tokens
    units = gate_weight.shape[1] // 2
    f32, bf16 = jnp.float32, jnp.bfloat16
    halvings = chips.bit_length() - 2
    last_rows = model // 2 >> halvings
    rows_in = inputs.reshape(tokens, model)
    cot_rows = cotangent.reshape(tokens, model)

    pair_index = place // copies
    head_weights = jnp.concatenate(
        [
            lax.dynamic_slice(query_weight, (0, place * query_cols), (shard, query_cols)),
            lax.dynamic_slice(key_weight, (0, pair_index * width), (shard, width)),
            lax.dynamic_slice(value_weight, (0, pair_index * width), (shard, width)),
        ],
        axis=1,
    )
    piece_index = core * chips + place // 2
    out_piece = lax.dynamic_slice_in_dim(output_weight, piece_index * piece_rows, piece_rows, 0)
    source = rows_in.astype(f32)
    first = rms_factor(source)
    normed_in = (source * first * attention_gain).astype(bf16)
    cosine, sine = rope_tables(jnp.arange(length, dtype=jnp.int32), width)
    lanes = jnp.arange(2 * width)
    signed = jnp.where(lanes % width < width // 2, -1.0, 1.0) * jnp.concatenate([sine, sine], axis=1)
    heads_of = jnp.arange(head_cols) // width
    group = (heads_of[:, None] == heads_of[None, :]).astype(bf16)
    gain_row = jnp.concatenate([jnp.tile(query_gain, local_groups), key_gain, key_gain])[None, :]
    tables = (gain_row, jnp.concatenate([cosine, cosine], axis=1), signed, group)
    normed_all, head_full, out_slice, proj, queries, pair_rows, out_rows, log_rows = call(
        functools.partial(front_kernel, width),
        sizes,
        0,
        (normed_in, head_weights, out_piece, *tables),
        (True,) * 7,
        [
            ((length, model), bf16),
            ((model, head_cols), bf16),
            ((query_cols, model), bf16),
            ((length, head_cols), f32),
            ((length, query_cols), bf16),
            ((length, 2 * width), bf16),
            ((length, query_cols), bf16),
            ((length, 128), f32),
        ],
        [((planes, piece_rows, model), bf16)] + [((length, 2 * width), bf16)] * 3,
    )

    half = model // 2
    scatter_scratch = [
        ((chips, tokens, model), bf16),
        ((chips, tokens, model), bf16),
        ((2, chips, tokens, half), bf16),
        ((halvings + 1, 2, chips, tokens, half), bf16),
    ]
    out_sum, cot_all = call(
        out_rows_kernel,
        sizes,
        1,
        (out_rows, out_slice, cot_rows),
        (True, True, True),
        [((tokens, model), f32), ((planes, 2, tokens, model), bf16)],
        scatter_scratch,
    )
    middle = source + out_sum
    second = rms_factor(middle)
    normed_mid = (middle * second * feedforward_gain).astype(bf16)
    quarter = model // 4
    rows_shape = (planes, tokens, model)
    line_scratch = [
        (rows_shape, bf16),
        (rows_shape, bf16),
        ((2, planes - 1, tokens, model), bf16),
    ]
    acts = (2 * planes * tokens, units)
    s_down, s_gate_a, s_gate_b, s_up_a, s_up_b, mid_grad, down_give, down_keep = call(
        feed_kernel,
        sizes,
        2,
        (normed_mid, cot_all.reshape(-1, model), gate_weight, up_weight, down_weight),
        (True, True, False, False, False),
        [((2, last_rows, units), bf16)]
        + [((last_rows, units), bf16)] * 4
        + [
            ((tokens, model), f32),
            (rows_shape, bf16),
            (rows_shape, bf16),
        ],
        [((model, units), bf16)] * 3
        + [((planes, 2, tokens, model), bf16)]
        + [(acts, bf16)] * 3
        + [((3, 2, quarter, units), bf16)]
        + [((3, 2, quarter >> stage, units), bf16) for stage in range(halvings)]
        + [(rows_shape, bf16)]
        + line_scratch,
        [True] * 6 + [False] * 2,
    )

    feedforward_slope = jnp.sum(mid_grad * middle * second, axis=0)
    middle_grad = cot_rows.astype(f32) + norm_back(mid_grad, middle, second, feedforward_gain)
    middle_half = middle_grad.astype(bf16)
    middle_all, t_down, down_sum = call(
        spread_kernel,
        sizes,
        4,
        (middle_half, s_down, down_give, down_keep),
        (True, True, False, False),
        [((length, model), bf16), ((2, last_rows, units), bf16), ((tokens, model), f32)],
        line_scratch,
    )
    block_rows = middle + down_sum

    def swap(value, bit):
        return lax.ppermute(value, "seq", [(i, i ^ bit) for i in range(parts)])

    *sent, middle_all = lax.optimization_barrier((s_gate_a, s_gate_b, s_up_a, s_up_b, middle_all))
    bit_orders = ([2 << i for i in range(halvings + 1)], [chips >> i for i in range(halvings + 1)])
    came = [swap(piece, bit_orders[number % 2][-1]) for number, piece in enumerate(sent)]

    vmem = pl.BlockSpec(memory_space=pltpu.VMEM)
    halves, head_part, out_part, head_slopes = pl.pallas_call(
        functools.partial(back_kernel, width),
        out_shape=[
            jax.ShapeDtypeStruct((length, head_cols), bf16),
            jax.ShapeDtypeStruct((model, head_cols), bf16),
            jax.ShapeDtypeStruct((query_cols, model), bf16),
            jax.ShapeDtypeStruct((8, head_cols), f32),
        ],
        in_specs=[vmem] * 12,
        out_specs=[vmem] * 4,
        scratch_shapes=[
            pltpu.VMEM((length, query_cols), bf16),
            pltpu.VMEM((length, query_cols), f32),
            pltpu.VMEM((length, 2 * width), f32),
            pltpu.VMEM((length, 2 * width), f32),
        ]
        + [pltpu.VMEM((length, 2 * width), bf16)] * 6,
        compiler_params=pltpu.CompilerParams(vmem_limit_bytes=VMEM_BYTES),
        cost_estimate=pl.CostEstimate(
            flops=10 * length * model * head_cols,
            transcendentals=length * length * local_groups,
            bytes_accessed=16 * length * model,
        ),
    )(
        normed_all,
        middle_all,
        out_slice,
        out_rows,
        log_rows,
        queries,
        pair_rows,
        proj,
        *tables,
    )
    head_part = head_part.reshape(planes, shard, head_cols)
    query_slope = head_slopes[0, :query_cols].reshape(local_groups, width).sum(axis=0)
    key_slope = head_slopes[0, query_cols : query_cols + width]

    gains = jnp.concatenate([query_slope, key_slope])
    gains = jnp.pad(gains, (0, model - gains.shape[0]))
    slopes = jnp.stack([feedforward_slope, gains])
    slopes = jnp.pad(slopes, ((1, 5), (0, 0)))
    rounds = (parts * planes).bit_length() - 1
    side = ((model, units), bf16)
    piece = ((last_rows, units), bf16)
    in_grad, near_down, far_down, query_all, pair_all, outer_all, slopes, *pieces = call(
        final_kernel,
        sizes,
        5,
        (halves, head_full, head_part, out_part, t_down, rows_in, first, slopes, *sent, *came),
        (True, True, False, False, True, True, True, True) + (False,) * 8,
        [
            ((tokens, model), f32),
            side,
            side,
            ((shard, model), bf16),
            ((parts, shard, 2 * width), bf16),
            ((shard, model), bf16),
            ((8, model), f32),
        ]
        + [piece] * 4,
        scatter_scratch
        + [
            ((planes, shard, head_cols), bf16),
            ((2, planes - 1, shard, head_cols), bf16),
            ((planes, piece_rows, model), bf16),
            ((2, planes - 1, piece_rows, model), bf16),
            ((shard, head_cols), bf16),
            ((piece_rows, model), bf16),
            ((4, last_rows, units), bf16),
            ((4, last_rows, units), bf16),
            ((rounds, 8, model), f32),
            ((rounds, 8, model), f32),
        ],
        [True, False, False] + [True] * 4 + [False] * 4,
    )
    pieces, near_down, far_down, in_grad = lax.optimization_barrier(
        (pieces, near_down, far_down, in_grad)
    )
    input_rows = (middle_grad + norm_back(in_grad, source, first, attention_gain)).astype(bf16)

    def plane_pieces(values):
        whole = []
        for color, order in enumerate(bit_orders):
            start, rows = color * (model // 2), model // 2
            for bit in order[:-1]:
                rows //= 2
                start = start + (place // bit) % 2 * rows
            held = [(start, values[color])]
            rows = last_rows
            for bit in order[-2::-1]:
                held = held + [
                    (start + rows - 2 * rows * ((place // bit) % 2), swap(value, bit))
                    for start, value in held
                ]
                rows *= 2
            whole = whole + held
        return whole

    gate_pieces = plane_pieces(pieces[:2])
    grad_down = widen(near_down, far_down)
    grad_query = query_all.astype(f32)
    grad_pair = pair_all.astype(f32)
    grad_pair = grad_pair.reshape(parts // copies, copies, shard, 2, width).sum(axis=1)
    grad_key = grad_pair[:, :, 0].transpose(1, 0, 2).reshape(shard, -1)
    grad_value = grad_pair[:, :, 1].transpose(1, 0, 2).reshape(shard, -1)
    grad_output = outer_all.astype(f32)
    written = (grad_down, grad_query, grad_key, grad_value, grad_output, input_rows)
    pieces[2:], gate_pieces, written = lax.optimization_barrier((pieces[2:], gate_pieces, written))
    grad_down, grad_query, grad_key, grad_value, grad_output, input_rows = written
    up_pieces = plane_pieces(pieces[2:])
    grad_gate = widen_pieces(gate_pieces, [swap(value, 1) for _, value in gate_pieces])
    up_pieces, grad_gate = lax.optimization_barrier((up_pieces, grad_gate))
    grad_up = widen_pieces(up_pieces, [swap(value, 1) for _, value in up_pieces])
    attention_slope, feedforward_slope = slopes[0], slopes[1]
    query_slope, key_slope = slopes[2, :width], slopes[2, width : 2 * width]
    block_out = block_rows.astype(bf16).reshape(1, tokens, model)
    input_grad = input_rows.reshape(1, tokens, model)
    return (
        block_out,
        input_grad,
        attention_slope,
        grad_query,
        grad_key,
        grad_value,
        grad_output,
        query_slope,
        key_slope,
        feedforward_slope,
        grad_gate,
        grad_up,
        grad_down,
    )


def solution(mesh):
    in_specs = (
        P("fsdp", "seq", None),
        P("fsdp", "seq", None),
        P(),
        P("fsdp", None),
        P("fsdp", None),
        P("fsdp", None),
        P("fsdp", None),
        P(),
        P(),
        P(),
        P(None, "fsdp"),
        P(None, "fsdp"),
        P(None, "fsdp"),
    )
    out_specs = (
        P("fsdp", "seq", None),
        P("fsdp", "seq", None),
        P(),
        P("fsdp", None),
        P("fsdp", None),
        P("fsdp", None),
        P("fsdp", None),
        P(),
        P(),
        P(),
        P(None, "fsdp"),
        P(None, "fsdp"),
        P(None, "fsdp"),
    )
    return jax.shard_map(
        per_device, mesh=mesh, in_specs=in_specs, out_specs=out_specs, check_vma=False
    )
```

```python
import functools

import jax
import jax.numpy as jnp
from jax import lax
from jax.experimental import pallas as pl
from jax.experimental.pallas import tpu as pltpu
from jax.sharding import PartitionSpec as P

EPS = 1e-05
THETA = 1000000.0


def rotate_half(values):
    half = values.shape[-1] // 2
    return jnp.concatenate([-values[..., half:], values[..., :half]], axis=-1)


def rope_tables(positions, width):
    exponents = jnp.arange(width // 2).astype(jnp.float32) * 2.0 / width
    rates = jnp.power(jnp.float32(THETA), -exponents)
    angle = positions.astype(jnp.float32)[:, None] * rates[None, :]
    angle = jnp.concatenate([angle, angle], axis=-1)
    return (jnp.cos(angle), jnp.sin(angle))


def prepare(proj, gain, cosine, sine):
    rows = proj.shape[0]
    width = gain.shape[0]
    split = proj.reshape(rows, -1, width)
    factor = lax.rsqrt(jnp.mean(split * split, axis=-1, keepdims=True) + EPS)
    normed = split * factor * gain
    turned = normed * cosine[:, None, :] + rotate_half(normed) * sine[:, None, :]
    return turned.reshape(rows, -1)


def matmul(left, right):
    return jnp.dot(left, right, preferred_element_type=jnp.float32)


def inner_rows(left, right):
    return lax.dot_general(
        left, right, (((0,), (0,)), ((), ())), preferred_element_type=jnp.float32
    )


def inner_cols(left, right):
    return lax.dot_general(
        left, right, (((1,), (1,)), ((), ())), preferred_element_type=jnp.float32
    )


def rms_factor(values):
    return lax.rsqrt(jnp.mean(values * values, axis=-1, keepdims=True) + EPS)


def norm_back(grad, values, factor, gain):
    scaled = grad * gain
    return factor * (
        scaled - values * factor * factor * jnp.mean(scaled * values, axis=-1, keepdims=True)
    )


def gate_back(hidden_grad, gate, lifted):
    sigma = jax.nn.sigmoid(gate)
    gate_grad = (hidden_grad * lifted * sigma * (1.0 + gate * (1.0 - sigma))).astype(jnp.bfloat16)
    lifted_grad = (hidden_grad * gate * sigma).astype(jnp.bfloat16)
    return (gate_grad, lifted_grad)


def activate(gate, lifted):
    return (gate * jax.nn.sigmoid(gate) * lifted).astype(jnp.bfloat16)


def split_heads(query_rows, pair_rows, groups, width):
    length = query_rows.shape[0]
    key_heads = pair_rows.shape[1] // (2 * width)
    queries = query_rows.reshape(length, key_heads, groups, width)
    keys = pair_rows[:, : key_heads * width].reshape(length, key_heads, width)
    values = pair_rows[:, key_heads * width :].reshape(length, key_heads, width)
    return (queries, keys, values, key_heads)


def attend_heads(query_rows, pair_rows, groups, width):
    length = query_rows.shape[0]
    queries, keys, values, key_heads = split_heads(query_rows, pair_rows, groups, width)
    block = min(512, length)
    scale = width ** (-0.5)
    offsets = jnp.arange(block)

    def query_step(index, state):
        out_rows, log_rows = state
        query_block = lax.dynamic_slice_in_dim(queries, index * block, block, 0)

        def key_step(inner, carry):
            summed, total = carry
            key_block = lax.dynamic_slice_in_dim(keys, inner * block, block, 0)
            value_block = lax.dynamic_slice_in_dim(values, inner * block, block, 0)
            scores = (
                jnp.einsum(
                    "qhgd,shd->hgqs", query_block, key_block, preferred_element_type=jnp.float32
                )
                * scale
            )
            allowed = (index * block + offsets)[:, None] >= (inner * block + offsets)[None, :]
            weights = jnp.where(allowed, jnp.exp(scores), 0.0)
            summed = summed + jnp.einsum(
                "hgqs,shd->hgqd",
                weights.astype(jnp.bfloat16),
                value_block,
                preferred_element_type=jnp.float32,
            )
            return (summed, total + jnp.sum(weights, axis=-1))

        initial = (
            jnp.zeros((key_heads, groups, block, width), jnp.float32),
            jnp.zeros((key_heads, groups, block), jnp.float32),
        )
        summed, total = lax.fori_loop(0, index + 1, key_step, initial)
        result = (summed / total[..., None]).astype(jnp.bfloat16)
        result = result.transpose(2, 0, 1, 3).reshape(block, key_heads * groups * width)
        out_rows = lax.dynamic_update_slice_in_dim(out_rows, result, index * block, 0)
        log_rows = lax.dynamic_update_slice_in_dim(log_rows, jnp.log(total), index * block, 2)
        return (out_rows, log_rows)

    start = (
        jnp.zeros((length, key_heads * groups * width), jnp.bfloat16),
        jnp.zeros((key_heads, groups, length), jnp.float32),
    )
    return lax.fori_loop(0, length // block, query_step, start)


def attend_back(query_rows, pair_rows, out_rows, log_rows, grad_rows, groups, width):
    length = query_rows.shape[0]
    queries, keys, values, key_heads = split_heads(query_rows, pair_rows, groups, width)
    outs = out_rows.reshape(length, key_heads, groups, width)
    grads = grad_rows.reshape(length, key_heads, groups, width)
    correction = jnp.sum(grads.astype(jnp.float32) * outs.astype(jnp.float32), axis=-1)
    block = min(512, length)
    scale = width ** (-0.5)
    offsets = jnp.arange(block)

    def query_step(index, state):
        query_grad, key_grad, value_grad = state
        query_block = lax.dynamic_slice_in_dim(queries, index * block, block, 0)
        grad_block = lax.dynamic_slice_in_dim(grads, index * block, block, 0)
        shift_block = lax.dynamic_slice_in_dim(correction, index * block, block, 0).transpose(
            1, 2, 0
        )
        log_block = lax.dynamic_slice_in_dim(log_rows, index * block, block, 2)

        def key_step(inner, carry):
            block_grad, key_sum, value_sum = carry
            key_block = lax.dynamic_slice_in_dim(keys, inner * block, block, 0)
            value_block = lax.dynamic_slice_in_dim(values, inner * block, block, 0)
            scores = (
                jnp.einsum(
                    "qhgd,shd->hgqs", query_block, key_block, preferred_element_type=jnp.float32
                )
                * scale
            )
            allowed = (index * block + offsets)[:, None] >= (inner * block + offsets)[None, :]
            weights = jnp.where(allowed, jnp.exp(scores - log_block[..., None]), 0.0)
            value_part = jnp.einsum(
                "hgqs,qhgd->shd",
                weights.astype(jnp.bfloat16),
                grad_block,
                preferred_element_type=jnp.float32,
            )
            prob_grad = jnp.einsum(
                "qhgd,shd->hgqs", grad_block, value_block, preferred_element_type=jnp.float32
            )
            score_grad = (weights * (prob_grad - shift_block[..., None]) * scale).astype(
                jnp.bfloat16
            )
            block_grad = block_grad + jnp.einsum(
                "hgqs,shd->qhgd", score_grad, key_block, preferred_element_type=jnp.float32
            )
            key_part = jnp.einsum(
                "hgqs,qhgd->shd", score_grad, query_block, preferred_element_type=jnp.float32
            )
            key_sum = lax.dynamic_update_slice_in_dim(
                key_sum,
                lax.dynamic_slice_in_dim(key_sum, inner * block, block, 0) + key_part,
                inner * block,
                0,
            )
            value_sum = lax.dynamic_update_slice_in_dim(
                value_sum,
                lax.dynamic_slice_in_dim(value_sum, inner * block, block, 0) + value_part,
                inner * block,
                0,
            )
            return (block_grad, key_sum, value_sum)

        initial = (jnp.zeros((block, key_heads, groups, width), jnp.float32), key_grad, value_grad)
        block_grad, key_grad, value_grad = lax.fori_loop(0, index + 1, key_step, initial)
        query_grad = lax.dynamic_update_slice_in_dim(query_grad, block_grad, index * block, 0)
        return (query_grad, key_grad, value_grad)

    state = (
        jnp.zeros((length, key_heads, groups, width), jnp.float32),
        jnp.zeros((length, key_heads, width), jnp.float32),
        jnp.zeros((length, key_heads, width), jnp.float32),
    )
    query_grad, key_grad, value_grad = lax.fori_loop(0, length // block, query_step, state)
    pair_grad = jnp.concatenate(
        [
            key_grad.reshape(length, key_heads * width),
            value_grad.reshape(length, key_heads * width),
        ],
        axis=1,
    )
    return (query_grad.reshape(length, key_heads * groups * width), pair_grad)


MESH = pl.DeviceIdType.MESH


def flip(index, mask, bits):
    for bit in bits:
        if mask & bit:
            index = index + bit - 2 * bit * ((index // bit) % 2)
    return index


class Place:
    def __init__(self, parts, planes):
        self.parts, self.planes = parts, planes
        self.seat = lax.axis_index("seq")
        self.plane = lax.axis_index("fsdp")
        self.core = self.seat % 2
        self.chip = self.seat // 2
        self.seat_bits = [1 << i for i in range(parts.bit_length() - 1)]
        self.chip_bits = self.seat_bits[1:]
        self.plane_bits = [1 << i for i in range(planes.bit_length() - 1)]

    def at(self, mask):
        return flip(self.seat, mask, self.seat_bits)

    def side(self, bit):
        return (self.seat // bit) % 2

    def colors(self):
        return (self.chip_bits, self.chip_bits[::-1])

    def enter(self, masks=(), line=False, plane_masks=()):
        barrier = pltpu.get_barrier_semaphore()
        peers = [{"seq": self.at(mask)} for mask in masks]
        if line:
            peers.append({"fsdp": (self.plane + 1) % self.planes})
            peers.append({"fsdp": (self.plane + self.planes - 1) % self.planes})
        for mask in plane_masks:
            peers.append({"fsdp": flip(self.plane, mask, self.plane_bits)})
        for peer in peers:
            pl.semaphore_signal(barrier, inc=1, device_id=peer, device_id_type=MESH)
        pl.semaphore_wait(barrier, len(peers))


class Wire:
    def __init__(self, sends, receives, locals_):
        self.sends, self.receives, self.locals = sends, receives, locals_
        self.count = self.local_count = 0
        self.open = []

    def remote(self, source, target, device):
        number = self.count
        self.count += 1
        return pltpu.make_async_remote_copy(
            src_ref=source,
            dst_ref=target,
            send_sem=self.sends.at[number],
            recv_sem=self.receives.at[number],
            device_id=device,
            device_id_type=MESH,
        )

    def send(self, source, target, device):
        copy = self.remote(source, target, device)
        copy.start()
        self.open.append(copy)
        return copy

    def quiet(self, source, target):
        number = self.local_count
        self.local_count += 1
        return pltpu.make_async_copy(source, target, self.locals.at[number])

    def local(self, source, target):
        copy = self.quiet(source, target)
        copy.start()
        return copy

    def sent(self, copy):
        copy.wait_send()
        self.open = [other for other in self.open if other is not copy]

    def close(self):
        for copy in self.open:
            copy.wait_send()


def add_rows(target, left, right, step=64):
    rows = target.shape[0]
    step = min(step, rows)

    def body(index, carry):
        at = pl.ds(pl.multiple_of(index * step, step), step)
        total = left[at, :].astype(jnp.float32) + right[at, :].astype(jnp.float32)
        target[at, :] = total.astype(target.dtype)
        return carry

    lax.fori_loop(0, rows // step, body, 0)


class LineGather:
    def __init__(self, wire, here, source, target, share=None):
        self.here = here
        planes, plane = here.planes, here.plane
        above = {"fsdp": (plane + 1) % planes}
        below = {"fsdp": (plane + planes - 1) % planes}
        self.ups, self.downs = {}, {}
        for step in range(1, planes):
            lower = (plane + planes - step + 1) % planes
            upper = (plane + step - 1) % planes
            first = step == 1
            self.ups[step] = wire.remote(
                source if first else target(lower), target(lower), above
            )
            self.downs[step] = wire.remote(
                source if first else target(upper), target(upper), below
            )
        self.shared = {}
        if share is not None:
            for step in range(1, planes):
                for way, shift in ((0, planes - step), (1, step)):
                    index = (plane + shift) % planes
                    self.shared[(step, way)] = wire.remote(
                        target(index), share(index), {"seq": here.at(1)}
                    )

    def start(self, step):
        planes, plane = self.here.planes, self.here.plane

        @pl.when((plane >= step - 1) & (plane <= planes - 2))
        def _():
            self.ups[step].start()

        @pl.when((plane + step <= planes) & (plane >= 1))
        def _():
            self.downs[step].start()

    def arrive(self, step):
        planes, plane = self.here.planes, self.here.plane

        @pl.when(plane >= step)
        def _():
            self.ups[step].wait_recv()
            if self.shared:
                self.shared[(step, 0)].start()

        @pl.when(plane + step <= planes - 1)
        def _():
            self.downs[step].wait_recv()
            if self.shared:
                self.shared[(step, 1)].start()

    def close(self, shared_taken=False):
        planes, plane = self.here.planes, self.here.plane
        for (step, way), copy in self.shared.items():

            @pl.when(plane >= step if way == 0 else plane + step <= planes - 1)
            def _(copy=copy):
                copy.wait_send()
                if not shared_taken:
                    copy.wait_recv()

        for step in range(1, planes):

            @pl.when((plane >= step - 1) & (plane <= planes - 2))
            def _(step=step):
                self.ups[step].wait_send()

            @pl.when((plane + step <= planes) & (plane >= 1))
            def _(step=step):
                self.downs[step].wait_send()


class Lines:
    def __init__(self, members):
        self.members = members

    def start(self, step):
        for member in self.members:
            member.start(step)

    def pass_on(self, step):
        for member in self.members:
            member.arrive(step)
            if step + 1 < member.here.planes:
                member.start(step + 1)

    def step(self, step):
        for member in self.members:
            member.step(step)

    def close(self, *options):
        for member in self.members:
            member.close(*options)


def gather_lines(wire, here, source, target, share=None, cuts=2):
    rows = source.shape[0] // cuts
    members = []
    for cut in range(cuts):
        at = pl.ds(cut * rows, rows)
        members.append(
            LineGather(
                wire,
                here,
                source.at[at],
                lambda index, at=at: target(index).at[at],
                None if share is None else lambda index, at=at: share(index).at[at],
            )
        )
    return Lines(members)


class LineScatter:
    def __init__(self, wire, here, term, landing):
        self.wire, self.here, self.term, self.landing = wire, here, term, landing
        planes, plane = here.planes, here.plane
        above = {"fsdp": (plane + 1) % planes}
        below = {"fsdp": (plane + planes - 1) % planes}
        self.ups, self.downs = {}, {}
        for step in range(1, planes):
            self.ups[step] = wire.remote(
                term((plane + planes - step) % planes), landing(0, step - 1), above
            )
            self.downs[step] = wire.remote(
                term((plane + step) % planes), landing(1, step - 1), below
            )

    def step(self, step):
        planes, plane = self.here.planes, self.here.plane
        mirror = planes - 1 - plane
        for way, (position, copies, dest) in enumerate(
            (
                (plane, self.ups, (plane + planes - step) % planes),
                (mirror, self.downs, (plane + step) % planes),
            )
        ):
            if step > 1:

                @pl.when((position >= 1) & (position <= step - 1))
                def _(way=way, copies=copies, dest=dest):
                    copies[step - 1].wait_recv()
                    term = self.term(dest)
                    add_rows(term, term, self.landing(way, step - 2))

            @pl.when(position <= step - 1)
            def _(copies=copies):
                copies[step].start()

    def finish(self, out):
        planes, plane = self.here.planes, self.here.plane
        own = self.term(plane)
        last = planes - 1

        @pl.when(plane >= 1)
        def _():
            self.ups[last].wait_recv()

        @pl.when(plane <= planes - 2)
        def _():
            self.downs[last].wait_recv()

        @pl.when(plane == 0)
        def _():
            add_rows(out, own, self.landing(1, last - 1))

        @pl.when(plane == planes - 1)
        def _():
            add_rows(out, own, self.landing(0, last - 1))

        @pl.when((plane >= 1) & (plane <= planes - 2))
        def _():
            add_rows(own, own, self.landing(0, last - 1))
            add_rows(out, own, self.landing(1, last - 1))

    def close(self):
        planes, plane = self.here.planes, self.here.plane
        mirror = planes - 1 - plane
        for step in range(1, planes):

            @pl.when(plane <= step - 1)
            def _(step=step):
                self.ups[step].wait_send()

            @pl.when(mirror <= step - 1)
            def _(step=step):
                self.downs[step].wait_send()


class PlaneGather:
    def __init__(self, wire, here, source, target):
        self.wire, self.here, self.source, self.target = wire, here, source, target
        self.incoming = {}

    def _send(self, mask, color, bit):
        here = self.here
        target = self.target(here.at(mask), color)
        source = self.source(color) if mask == 0 else target
        self.incoming[(mask ^ bit, color)] = self.wire.send(
            source, target, {"seq": here.at(bit)}
        )

    def start(self):
        for position in range(len(self.here.chip_bits)):
            for color, bits in enumerate(self.here.colors()):
                self._send(0, color, bits[position])
        for color in (0, 1):
            self._send(0, color, 1)

    def hop(self, hops):
        here = self.here
        chips = here.parts // 2
        for mask in (mask * 2 for mask in range(1, chips)):
            if bin(mask).count("1") != hops:
                continue
            for color, bits in enumerate(here.colors()):
                self.incoming[(mask, color)].wait_recv()
                last = max(i for i, bit in enumerate(bits) if mask & bit)
                for bit in bits[last + 1 :]:
                    self._send(mask, color, bit)
                self._send(mask, color, 1)

    def hops(self, first=1):
        for hops in range(first, len(self.here.chip_bits) + 1):
            self.hop(hops)

    def finish(self):
        for mask in range(1, self.here.parts, 2):
            for color in (0, 1):
                self.incoming[(mask, color)].wait_recv()


class PlaneScatter:
    def __init__(self, wire, here, product, give, take, current, landing, model):
        self.wire, self.here, self.product = wire, here, product
        self.give, self.take, self.current, self.landing = give, take, current, landing
        self.model = model

    def start(self):
        here = self.here
        chips = here.parts // 2
        self.swaps = {}
        tokens = self.give.shape[1]
        seats = [2 * flip(here.chip, mask, [b // 2 for b in here.chip_bits]) for mask in range(chips)]
        for part in range(self.model // 512):
            columns = slice(part * 512, (part + 1) * 512)
            rows = self.product([seat + 1 - here.core for seat in seats], columns)
            for mask in range(chips):
                self.give[mask, :, columns] = rows[mask * tokens : (mask + 1) * tokens].astype(
                    self.give.dtype
                )
        for mask in range(chips)[::-1]:
            self.swaps[mask] = self.wire.send(
                self.give.at[mask], self.take.at[mask], {"seq": here.at(1)}
            )
        half = self.model // 2
        for part in range(self.model // 512):
            columns = slice(part * 512, (part + 1) * 512)
            rows = self.product([seat + here.core for seat in seats], columns)
            color, inside = divmod(part * 512, half)
            for mask in range(chips):
                self.current[color, mask, :, inside : inside + 512] = rows[
                    mask * tokens : (mask + 1) * tokens
                ].astype(self.current.dtype)

    def join(self):
        half = self.model // 2
        chips = self.here.parts // 2
        for mask in range(chips)[::-1]:
            self.swaps[mask].wait_recv()
            for color in (0, 1):
                mine = self.current.at[color, mask]
                add_rows(mine, mine, self.take.at[mask, :, pl.ds(color * half, half)])

    def stage(self, position):
        here = self.here
        self.moved = {}
        for color, bits in enumerate(here.colors()):
            bit = bits[position]
            done = sum(bits[:position])
            for mask in range(here.parts // 2):
                if mask * 2 & bit and not mask * 2 & done:
                    low = mask ^ (bit // 2)
                    self.moved[(color, low)] = self.wire.send(
                        self.current.at[color, mask],
                        self.landing.at[position, color, low],
                        {"seq": here.at(bit)},
                    )

    def settle(self, position, out):
        half = self.model // 2
        last = position == len(self.here.chip_bits) - 1
        for (color, low), copy in self.moved.items():
            copy.wait_recv()
            mine = self.current.at[color, low]
            if last:
                target = out.at[:, pl.ds(color * half, half)]
            else:
                target = mine
            add_rows(target, mine, self.landing.at[position, color, low])


def pick_lanes(low, high, width):
    lane = lax.broadcasted_iota(jnp.int32, low.shape, low.ndim - 1)
    return jnp.where(lane % (2 * width) < width, low, high)


def group_mean(values, group, width):
    high = values.astype(jnp.bfloat16)
    low = (values - high.astype(jnp.float32)).astype(jnp.bfloat16)
    total = jnp.dot(high, group, preferred_element_type=jnp.float32) + jnp.dot(
        low, group, preferred_element_type=jnp.float32
    )
    return total * (1.0 / width)


def turn(values, width):
    lanes = values.shape[1]
    half = width // 2
    return pick_lanes(
        pltpu.roll(values, lanes - half, 1), pltpu.roll(values, half, 1), half
    )


def attend_block(index, block, width, heads, queries, pair, twin, left, right, out_rows, logs):
    rows = pl.ds(index * block, block)
    before = index * block
    columns = 2 * width
    row = lax.broadcasted_iota(jnp.int32, (block, block), 0)
    column = lax.broadcasted_iota(jnp.int32, (block, block), 1)
    allowed = row >= column
    contract = (((1,), (1,)), ((), ()))
    totals = []
    for number in range(heads // 2):
        at = pl.ds(number * columns, columns)
        both = queries[rows, at]
        both = (both.astype(jnp.float32) * width**-0.5).astype(both.dtype)
        zero = jnp.zeros_like(both)
        result = None
        for side, values in ((0, left), (1, right)):
            mine = pick_lanes(both, zero, width) if side == 0 else pick_lanes(zero, both, width)
            scores = lax.dot_general(
                mine, twin[rows, :], contract, preferred_element_type=jnp.float32
            )
            weights = jnp.where(allowed, jnp.exp(scores), 0.0)
            total = jnp.sum(weights, axis=1, keepdims=True)
            summed = jnp.dot(
                weights.astype(jnp.bfloat16), values[rows, :], preferred_element_type=jnp.float32
            )
            if before:
                scores = lax.dot_general(
                    mine, twin[0:before, :], contract, preferred_element_type=jnp.float32
                )
                weights = jnp.exp(scores)
                total = total + jnp.sum(weights, axis=1, keepdims=True)
                summed = summed + jnp.dot(
                    weights.astype(jnp.bfloat16),
                    values[0:before, :],
                    preferred_element_type=jnp.float32,
                )
            totals.append(total)
            part = summed / total
            result = part if result is None else result + part
        out_rows[rows, at] = result.astype(out_rows.dtype)
    lane = lax.broadcasted_iota(jnp.int32, (block, 128), 1)
    table = jnp.ones((block, 128), jnp.float32)
    for number, total in enumerate(totals):
        table = jnp.where(lane == number, total, table)
    logs[rows, :] = jnp.log(table)


def back_block(
    index, block, width, heads, queries, grads, outs, logs, keys, values, query_back, key_back, value_back
):
    rows = pl.ds(index * block, block)
    before = index * block
    scale = width**-0.5
    row = lax.broadcasted_iota(jnp.int32, (block, block), 0)
    column = lax.broadcasted_iota(jnp.int32, (block, block), 1)
    allowed = row >= column
    across = (((1,), (1,)), ((), ()))
    down = (((0,), (0,)), ((), ()))
    f32 = jnp.float32
    spans = [(rows, True)] + ([(slice(0, before), False)] if before else [])
    for number in range(heads // 2):
        at = pl.ds(number * 2 * width, 2 * width)
        both, both_grad = queries[rows, at], grads[rows, at]
        product = both_grad.astype(f32) * outs[rows, at].astype(f32)
        zero = jnp.zeros_like(both)
        total = None
        for side in (0, 1):
            pick = (
                (lambda value, nothing: pick_lanes(value, nothing, width))
                if side == 0
                else (lambda value, nothing: pick_lanes(nothing, value, width))
            )
            query, grad = pick(both, zero), pick(both_grad, zero)
            scaled = (query.astype(f32) * scale).astype(query.dtype)
            shift = jnp.sum(pick(product, jnp.zeros_like(product)), axis=1, keepdims=True)
            head = 2 * number + side
            log = logs[rows, head : head + 1]
            for span, masked in spans:
                scores = lax.dot_general(
                    scaled, keys[0][span, :], across, preferred_element_type=f32
                )
                weights = jnp.exp(scores - log)
                if masked:
                    weights = jnp.where(allowed, weights, 0.0)
                prob_grad = lax.dot_general(
                    grad, values[0][span, :], across, preferred_element_type=f32
                )
                score_grad = (weights * (prob_grad - shift) * scale).astype(query.dtype)
                part = jnp.dot(score_grad, keys[1 + side][span, :], preferred_element_type=f32)
                total = part if total is None else total + part
                key_back[span, :] += lax.dot_general(
                    score_grad, query, down, preferred_element_type=f32
                )
                value_back[span, :] += lax.dot_general(
                    weights.astype(query.dtype), grad, down, preferred_element_type=f32
                )
        query_back[rows, at] = total


def back_kernel(
    width,
    normed,
    middle,
    out_slice,
    outs,
    logs,
    queries,
    pair,
    proj,
    gain,
    cosine,
    sine,
    group,
    halves,
    head_part,
    out_part,
    slopes,
    grads,
    query_back,
    key_back,
    value_back,
    *twins,
):
    length = normed.shape[0]
    block = min(256, length)
    blocks = length // block
    query_cols = queries.shape[1]
    heads = query_cols // width
    keys, values = twins[:3], twins[3:]
    f32 = jnp.float32
    key_back[...] = jnp.zeros_like(key_back)
    value_back[...] = jnp.zeros_like(value_back)

    def ready(index, carry):
        at = pl.ds(pl.multiple_of(index * block, block), block)
        grads[at, :] = lax.dot_general(
            middle[at, :], out_slice[...], (((1,), (1,)), ((), ())), preferred_element_type=f32
        ).astype(grads.dtype)
        both = pair[at, :].astype(f32)
        swapped = pltpu.roll(both, width, 1)
        zero = jnp.zeros_like(both)
        for refs, low, high in (
            (keys, both, swapped),
            (values, swapped, both),
        ):
            refs[0][at, :] = pick_lanes(low, high, width).astype(refs[0].dtype)
            refs[1][at, :] = pick_lanes(low, zero, width).astype(refs[0].dtype)
            refs[2][at, :] = pick_lanes(zero, high, width).astype(refs[0].dtype)
        return carry

    lax.fori_loop(0, blocks, ready, 0)
    for index in range(blocks):
        back_block(
            index,
            block,
            width,
            heads,
            queries,
            grads,
            outs,
            logs,
            keys,
            values,
            query_back,
            key_back,
            value_back,
        )

    def norms(index, slope):
        at = pl.ds(pl.multiple_of(index * block, block), block)
        key_sum, value_sum = key_back[at, :], value_back[at, :]
        key_sum = key_sum + pltpu.roll(key_sum, width, 1)
        value_sum = value_sum + pltpu.roll(value_sum, width, 1)
        back = jnp.concatenate(
            [query_back[at, :], pick_lanes(key_sum, value_sum, width)], axis=1
        )
        value = proj[at, :]
        factor = lax.rsqrt(group_mean(value * value, group[...], width) + EPS)
        repeat = value.shape[1] // cosine.shape[1]
        cosines = jnp.concatenate([cosine[at, :]] * repeat, axis=1)
        sines = jnp.concatenate([sine[at, :]] * repeat, axis=1)
        turned = back * cosines + turn(back * sines, width)
        slope = slope + jnp.sum(turned * value * factor, axis=0, keepdims=True)
        scaled = turned * gain[...]
        result = factor * (
            scaled - value * factor * factor * group_mean(scaled * value, group[...], width)
        )
        lane = lax.broadcasted_iota(jnp.int32, back.shape, 1)
        result = jnp.where(lane >= query_cols + width, back, result)
        halves[at, :] = result.astype(halves.dtype)
        return slope

    slope = lax.fori_loop(0, blocks, norms, jnp.zeros((1, proj.shape[1]), f32))
    slopes[...] = jnp.broadcast_to(slope, slopes.shape)

    def terms(number, carry):
        at = pl.ds(pl.multiple_of(number * 256, 256), 256)
        down = (((0,), (0,)), ((), ()))
        head_part[at, :] = lax.dot_general(
            normed[:, at], halves[...], down, preferred_element_type=f32
        ).astype(head_part.dtype)
        out_part[:, at] = lax.dot_general(
            outs[...], middle[:, at], down, preferred_element_type=f32
        ).astype(out_part.dtype)
        return carry

    lax.fori_loop(0, normed.shape[1] // 256, terms, 0)


def row_blocks(rows, step, work):
    def body(index, carry):
        work(pl.ds(pl.multiple_of(index * step, step), step))
        return carry

    lax.fori_loop(0, rows // step, body, 0)


def front_kernel(
    width,
    copies,
    parts,
    planes,
    x,
    c,
    query_weight,
    key_weight,
    value_weight,
    output_weight,
    in_gain,
    mid_gain,
    gain,
    rates,
    x_all,
    w_all,
    o_slice,
    proj,
    queries,
    pair,
    out_rows,
    logs,
    cosine,
    sine,
    group,
    middle,
    mid,
    c_all,
    o_all,
    twin,
    left,
    right,
    key_block,
    value_block,
    give,
    take,
    current,
    landing,
    *sems,
):
    here = Place(parts, planes)
    wire = Wire(*sems)
    tokens, model = x.shape
    shard = query_weight.shape[0]
    query_cols = queries.shape[1]
    rows = o_all.shape[1]
    half = tokens // 2
    chips = parts // 2
    f32 = jnp.float32
    chip_masks = [mask * 2 for mask in range(1, chips)]
    pair_head = here.seat // copies
    own_shard = pl.ds(pl.multiple_of(here.plane * shard, shard), shard)
    head_block = pl.ds(pl.multiple_of(pair_head // 2 * 2 * width, 2 * width), 2 * width)
    loads = [
        wire.local(key_weight.at[:, head_block], key_block),
        wire.local(value_weight.at[:, head_block], value_block),
        wire.local(
            query_weight.at[:, pl.ds(pl.multiple_of(here.seat * query_cols, query_cols), query_cols)],
            w_all.at[own_shard, pl.ds(0, query_cols)],
        ),
    ]
    piece = (here.core * chips + here.chip) * rows
    o = output_weight.at[pl.ds(pl.multiple_of(piece, rows), rows)]
    here.enter(chip_masks + [1], line=True)
    o_own = wire.local(o, o_all.at[here.plane])
    for load in loads[:2]:
        load.wait()
    upper = (pair_head % 2) * jnp.ones((1, 1), jnp.int32)
    keys, values = key_block[...].astype(f32), value_block[...].astype(f32)
    keys = jnp.where(upper == 1, pltpu.roll(keys, width, 1), keys)
    values = jnp.where(upper == 1, values, pltpu.roll(values, width, 1))
    w_all[own_shard, query_cols:] = pick_lanes(keys, values, width).astype(w_all.dtype)
    loads[2].wait()
    weights = gather_lines(
        wire,
        here,
        w_all.at[own_shard],
        lambda index: w_all.at[pl.ds(pl.multiple_of(index * shard, shard), shard)],
    )
    weights.start(1)

    def norm_rows(at):
        value = x[at, :].astype(f32)
        factor = lax.rsqrt(jnp.mean(value * value, axis=-1, keepdims=True) + EPS)
        own_at = pl.ds(pl.multiple_of(here.seat * tokens + at.start, 32), 32)
        x_all[own_at, :] = (value * factor * in_gain[...]).astype(x_all.dtype)

    row_blocks(tokens, 32, norm_rows)

    def seat_rows(seat, color):
        return x_all.at[pl.ds(pl.multiple_of(seat * tokens + color * half, half), half)]

    plane_rows = PlaneGather(
        wire, here, lambda color: seat_rows(here.seat, color), seat_rows
    )
    plane_rows.start()
    outer = gather_lines(wire, here, o, lambda index: o_all.at[index])

    def c_spot(index):
        return c_all.at[index, here.core]

    cots = gather_lines(wire, here, c, c_spot, c_spot)
    c_own = wire.local(c, c_spot(here.plane))

    lane = lax.broadcasted_iota(jnp.int32, (32, 2 * width), 1)
    row = lax.broadcasted_iota(jnp.int32, (32, 2 * width), 0)
    sign = jnp.where(lane % width < width // 2, -1.0, 1.0)

    def table_rows(at):
        angle = (row + at.start).astype(f32) * rates[...]
        cosine[at, :] = jnp.cos(angle)
        sine[at, :] = jnp.sin(angle) * sign

    columns = group.shape[0]
    group[...] = jnp.where(
        lax.broadcasted_iota(jnp.int32, (columns, columns), 0) // width
        == lax.broadcasted_iota(jnp.int32, (columns, columns), 1) // width,
        1.0,
        0.0,
    ).astype(group.dtype)
    length = x_all.shape[0]
    row_blocks(length // 2, 32, table_rows)
    weights.members[0].arrive(1)
    if planes > 2:
        weights.members[0].start(2)
    plane_rows.hop(1)
    weights.members[1].arrive(1)
    if planes > 2:
        weights.members[1].start(2)
    outer.start(1)
    row_blocks(
        length // 2, 32, lambda at: table_rows(pl.ds(at.start + length // 2, at.size))
    )
    plane_rows.hops(2)
    spot = o_slice.at[pl.ds(pl.multiple_of(here.chip * rows, rows), rows)]
    deals = []
    for mask in chip_masks:
        chip = here.at(mask) // 2
        deals.append((chip, wire.remote(o_all.at[chip], spot, {"seq": here.at(mask)})))
    keep_own = wire.quiet(o_all.at[here.chip], spot)

    def deal(step):
        for chip, copy in deals + [(here.chip, keep_own)]:

            @pl.when((chip == here.plane + step) | (chip + step == here.plane))
            def _(copy=copy):
                copy.start()

    o_own.wait()
    deal(0)
    for step in range(2, planes):
        weights.pass_on(step)
    plane_rows.finish()
    block = min(256, length)
    blocks = length // block
    heads = query_cols // width

    def project(index, carry):
        at = pl.ds(pl.multiple_of(index * block, block), block)
        value = jnp.dot(x_all[at, :], w_all[...], preferred_element_type=f32)
        proj[at, :] = value
        factor = lax.rsqrt(group_mean(value * value, group[...], width) + EPS)
        normed = value * factor * gain[...]
        repeat = value.shape[1] // cosine.shape[1]
        cosines = jnp.concatenate([cosine[at, :]] * repeat, axis=1)
        sines = jnp.concatenate([sine[at, :]] * repeat, axis=1)
        turned = normed * cosines + turn(normed, width) * sines
        queries[at, :] = turned[:, :query_cols].astype(queries.dtype)
        keys, values = turned[:, query_cols:], value[:, query_cols:]
        both = pick_lanes(keys, values, width)
        pair[at, :] = both.astype(pair.dtype)
        swapped = pltpu.roll(both, width, 1)
        twin[at, :] = pick_lanes(both, swapped, width).astype(twin.dtype)
        zero = jnp.zeros_like(both)
        left[at, :] = pick_lanes(swapped, zero, width).astype(left.dtype)
        right[at, :] = pick_lanes(zero, both, width).astype(right.dtype)
        return carry

    lax.fori_loop(0, blocks, project, 0)
    across = wire.send(c, c_spot(here.plane), {"seq": here.at(1)})
    waits = list(range(1, planes))
    cot_waits = list(range(1, planes))
    for index in range(blocks):
        while waits and waits[0] * blocks <= (index + 1) * planes:
            step = waits.pop(0)
            outer.pass_on(step)
            deal(step)
            if not waits or (step == 2 and planes > 3):
                if len(waits) == planes - 3 or planes <= 3:
                    cots.start(1)
        attend_block(
            index, block, width, heads, queries, pair, twin, left, right, out_rows, logs
        )
    for step in waits:
        outer.pass_on(step)
        deal(step)
    cots.pass_on(cot_waits.pop(0))
    keep_own.wait()
    for _, copy in deals:
        copy.wait()

    def product(seats, at):
        chosen = [
            out_rows[pl.ds(pl.multiple_of(seat * tokens, tokens), tokens), :] for seat in seats
        ]
        return jnp.dot(
            jnp.concatenate(chosen, axis=0), o_slice[:, at], preferred_element_type=f32
        )

    sums = PlaneScatter(wire, here, product, give, take, current, landing, model)
    sums.start()
    sums.join()
    sums.stage(0)
    stages = len(here.chip_bits)
    for stage in range(stages):
        if cot_waits:
            cots.pass_on(cot_waits.pop(0))
        sums.settle(stage, middle)
        if stage + 1 < stages:
            sums.stage(stage + 1)

    def mid_rows(at):
        value = x[at, :].astype(f32) + middle[at, :]
        middle[at, :] = value
        factor = lax.rsqrt(jnp.mean(value * value, axis=-1, keepdims=True) + EPS)
        mid[at, :] = (value * factor * mid_gain[...]).astype(mid.dtype)

    row_blocks(tokens, 32, mid_rows)
    for step in cot_waits:
        cots.pass_on(step)
    c_own.wait()
    across.wait_recv()
    wire.close()
    weights.close()
    outer.close()
    cots.close()


def feed_kernel(
    parts,
    planes,
    m,
    cots,
    middle,
    mid_gain,
    gate_weight,
    up_weight,
    down_weight,
    s_down,
    s_gate_a,
    s_gate_b,
    s_up_a,
    s_up_b,
    mid,
    mid_half,
    mid_slope,
    down_give,
    down_keep,
    gate_half,
    up_half,
    down_half,
    mids,
    hidden,
    gate_grads,
    lifted_grads,
    away,
    *rest,
):
    here = Place(parts, planes)
    stages = len(here.chip_bits) - 1
    landings, rest = rest[:stages], rest[stages:]
    give, take, current, line_landing, *sems = rest
    wire = Wire(*sems)
    tokens, model = m.shape
    units = gate_half.shape[1]
    own_units = pl.ds(pl.multiple_of(here.core * units, units), units)
    loads = [
        wire.local(whole.at[:, own_units], part)
        for whole, part in (
            (gate_weight, gate_half),
            (up_weight, up_half),
            (down_weight, down_half),
        )
    ]
    here.enter(here.seat_bits, line=True)

    def spot(index):
        return mids.at[index, here.core]

    lines = gather_lines(wire, here, m, spot, spot)
    lines.start(1)
    across = wire.send(m, spot(here.plane), {"seq": here.at(1)})
    own = wire.local(m, spot(here.plane))

    def block(index):
        rows = pl.ds(pl.multiple_of(index * 2 * tokens, 2 * tokens), 2 * tokens)
        mid_rows = mids[index].reshape(2 * tokens, model)
        cot_rows = cots[rows, :]

        def part(number, carry):
            at = pl.ds(pl.multiple_of(number * 256, 256), 256)
            gate = jnp.dot(mid_rows, gate_half[:, at], preferred_element_type=jnp.float32)
            lifted = jnp.dot(mid_rows, up_half[:, at], preferred_element_type=jnp.float32)
            hidden_grad = jnp.dot(cot_rows, down_half[:, at], preferred_element_type=jnp.float32)
            sigma = 1.0 / (1.0 + jnp.exp(-gate))
            active = gate * sigma
            hidden[rows, at] = (active * lifted).astype(hidden.dtype)
            lifted_grads[rows, at] = (hidden_grad * active).astype(hidden.dtype)
            gate_grads[rows, at] = (
                hidden_grad * lifted * sigma * (1.0 + gate * (1.0 - sigma))
            ).astype(hidden.dtype)
            return carry

        lax.fori_loop(0, units // 256, part, 0)

    for load in loads:
        load.wait()
    own.wait()
    across.wait_recv()
    plane = here.plane
    block(plane)
    for step in range(1, planes):
        lines.pass_on(step)
        ups = jnp.where(plane >= step, 1, 0)
        downs = jnp.where(plane + step <= planes - 1, 1, 0)

        def arrived(number, carry, step=step, ups=ups):
            from_up = (number == 0) & (ups == 1)
            for way, chosen in ((0, from_up), (1, jnp.logical_not(from_up))):

                @pl.when(chosen)
                def _(way=way):
                    for line in lines.members:
                        line.shared[(step, way)].wait_recv()

            block(jnp.where(from_up, plane + planes - step, plane + step) % planes)
            return carry

        lax.fori_loop(0, ups + downs, arrived, 0)

    flat_mids = mids.reshape(2 * planes * tokens, model)
    pairs = ((cots, hidden), (flat_mids, gate_grads), (flat_mids, lifted_grads))
    quarter = model // 4
    moved = {}

    def gradient(target, pair, start):
        left, right = pair

        def part(number, carry):
            at = pl.ds(pl.multiple_of(start + number * 256, 256), 256)
            target[pl.ds(pl.multiple_of(number * 256, 256), 256), :] = lax.dot_general(
                left[:, at],
                right[...],
                (((0,), (0,)), ((), ())),
                preferred_element_type=jnp.float32,
            ).astype(target.dtype)
            return carry

        lax.fori_loop(0, quarter // 256, part, 0)

    def first_half(color, mine):
        bit = here.colors()[color][0]
        side = here.side(bit) if mine else 1 - here.side(bit)
        return pl.multiple_of(color * (model // 2) + side * quarter, quarter)

    def send_away(number):
        for color, bits in enumerate(here.colors()):
            gradient(away.at[number, color], pairs[number], first_half(color, False))
            moved[(number, color)] = wire.send(
                away.at[number, color], landings[0].at[number, color], {"seq": here.at(bits[0])}
            )

    def mid_term(target, core):
        rows = [pl.ds(pl.multiple_of((2 * p + core) * tokens, tokens), tokens) for p in range(planes)]
        gates = jnp.concatenate([gate_grads[at, :] for at in rows], axis=0)
        lifts = jnp.concatenate([lifted_grads[at, :] for at in rows], axis=0)

        def part(number, carry):
            at = pl.ds(pl.multiple_of(number * 256, 256), 256)
            term = lax.dot_general(
                gates, gate_half[at, :], (((1,), (1,)), ((), ())), preferred_element_type=jnp.float32
            ) + lax.dot_general(
                lifts, up_half[at, :], (((1,), (1,)), ((), ())), preferred_element_type=jnp.float32
            )
            target[:, :, at] = term.reshape(planes, tokens, 256).astype(target.dtype)
            return carry

        lax.fori_loop(0, model // 256, part, 0)

    def down_term(target, core):
        rows = [pl.ds(pl.multiple_of((2 * p + core) * tokens, tokens), tokens) for p in range(planes)]
        hiddens = jnp.concatenate([hidden[at, :] for at in rows], axis=0)

        def part(number, carry):
            at = pl.ds(pl.multiple_of(number * 256, 256), 256)
            term = lax.dot_general(
                hiddens, down_half[at, :], (((1,), (1,)), ((), ())), preferred_element_type=jnp.float32
            )
            target[:, :, at] = term.reshape(planes, tokens, 256).astype(target.dtype)
            return carry

        lax.fori_loop(0, model // 256, part, 0)

    send_away(0)
    swaps = TokenSum(wire, here, current, take, line_landing)
    mid_term(give, 1 - here.core)
    swaps.start(give)
    send_away(1)
    mid_term(current, here.core)
    swaps.join()
    swaps.step(1)
    send_away(2)
    for step in range(2, planes):
        swaps.step(step)

    def final(number, color):
        if number == 0:
            return s_down.at[color]
        return ((s_gate_a, s_gate_b), (s_up_a, s_up_b))[number - 1][color]

    wire.sent(swaps.across)
    down_term(give, 1 - here.core)
    down_term(take, here.core)
    handed = [wire.local(give, down_give), wire.local(take, down_keep)]
    rows = quarter
    keeps = {}
    for number in range(3):
        for color in (0, 1):
            keep = final(number, color) if stages == 1 else away.at[number, color]
            if stages > 1:
                wire.sent(moved[(number, color)])
            gradient(keep, pairs[number], first_half(color, True))
            keeps[(number, color)] = (keep, 0)
    swaps.finish(mid)
    f32 = jnp.float32

    def norm_back_rows(index, slope):
        at = pl.ds(pl.multiple_of(index * 32, 32), 32)
        own_cots = (here.plane * 2 + here.core) * tokens + index * 32
        grad, value = mid[at, :], middle[at, :]
        factor = lax.rsqrt(jnp.mean(value * value, axis=-1, keepdims=True) + EPS)
        scaled = grad * mid_gain[...]
        back = factor * (
            scaled
            - value * factor * factor * jnp.mean(scaled * value, axis=-1, keepdims=True)
        )
        result = cots[pl.ds(pl.multiple_of(own_cots, 32), 32), :].astype(f32) + back
        mid[at, :] = result
        mid_half[at, :] = result.astype(mid_half.dtype)
        return slope + jnp.sum(grad * value * factor, axis=0, keepdims=True)

    mid_slope[...] = lax.fori_loop(
        0, tokens // 32, norm_back_rows, jnp.zeros((1, model), f32)
    )
    for stage in range(stages):
        last = stage == stages - 1
        for number in range(3):
            for color, bits in enumerate(here.colors()):
                keep, begin = keeps[(number, color)]
                moved[(number, color)].wait_recv()
                mine = keep.at[pl.ds(begin, rows)]
                if last:
                    add_rows(final(number, color), mine, landings[stage].at[number, color])
                else:
                    add_rows(mine, mine, landings[stage].at[number, color])
                    bit = bits[stage + 1]
                    half = rows // 2
                    gone = pl.multiple_of(begin + (1 - here.side(bit)) * half, half)
                    moved[(number, color)] = wire.send(
                        keep.at[pl.ds(gone, half)],
                        landings[stage + 1].at[number, color],
                        {"seq": here.at(bit)},
                    )
                    keeps[(number, color)] = (
                        keep,
                        pl.multiple_of(begin + here.side(bit) * half, half),
                    )
        rows //= 2
    for copy in handed:
        copy.wait()
    wire.close()
    lines.close(True)
    swaps.close()


class TokenSum:
    def __init__(self, wire, here, current, take, landing):
        self.wire, self.here = wire, here
        self.current, self.take = current, take
        self.cuts = 2
        rows = current.shape[1] // self.cuts
        self.lines = []
        for cut in range(self.cuts):
            at = pl.ds(cut * rows, rows)
            self.lines.append(
                LineScatter(
                    wire,
                    here,
                    lambda index, at=at: current.at[index, at],
                    lambda way, step, at=at: landing.at[way, step, at],
                )
            )

    def start(self, give):
        self.across = self.wire.send(give, self.take, {"seq": self.here.at(1)})

    def join(self):
        self.across.wait_recv()

        def body(index, carry):
            row = self.current.at[index]
            add_rows(row, row, self.take.at[index])
            return carry

        lax.fori_loop(0, self.here.planes, body, 0)

    def step(self, step):
        for line in self.lines:
            line.step(step)

    def finish(self, out):
        rows = out.shape[0] // self.cuts
        for cut, line in enumerate(self.lines):
            line.finish(out.at[pl.ds(cut * rows, rows)])

    def close(self):
        for line in self.lines:
            line.close()


def spread_kernel(
    parts, planes, h, s, give, keep, h_all, t, block, current, take, line_landing, *sems
):
    here = Place(parts, planes)
    wire = Wire(*sems)
    here.enter(here.seat_bits, line=True)
    tokens = h.shape[0]
    half = tokens // 2
    rows = PlaneGather(
        wire,
        here,
        lambda color: h.at[pl.ds(color * half, half)],
        lambda seat, color: h_all.at[pl.ds(pl.multiple_of(seat * tokens + color * half, half), half)],
    )
    swaps = TokenSum(wire, here, current, take, line_landing)
    swaps.start(give)
    kept = wire.local(keep, current)
    rows.start()
    own = wire.local(h, h_all.at[pl.ds(pl.multiple_of(here.seat * tokens, tokens), tokens)])
    kept.wait()
    swaps.join()
    swaps.step(1)
    rows.hop(1)
    moved = [
        wire.send(s.at[color], t.at[color], {"seq": here.at(bits[-1])})
        for color, bits in enumerate(here.colors())
    ]
    for step in range(2, planes):
        if step == 3:
            rows.hops(2)
        swaps.step(step)
    if planes <= 3:
        rows.hops(2)
    rows.finish()
    for color in (0, 1):
        moved[color].wait_recv()
        add_rows(t.at[color], t.at[color], s.at[color])
    own.wait()
    swaps.finish(block)
    wire.close()
    swaps.close()


def final_kernel(
    parts,
    planes,
    a,
    w,
    head_part,
    out_part,
    t_down,
    source,
    slope,
    *rest,
):
    sent, rest = rest[:4], rest[4:]
    came, rest = rest[:4], rest[4:]
    out, near, far, query_all, pair_all, outer_all, slope_out, *rest = rest
    joined, rest = rest[:4], rest[4:]
    (
        give,
        take,
        current,
        landing,
        head_current,
        head_landing,
        dealt,
        out_landing,
        head_sum,
        out_sum,
        left,
        right,
        slope_sums,
        slope_landing,
        *sems,
    ) = rest
    here = Place(parts, planes)
    wire = Wire(*sems)
    tokens, model = out.shape
    shard = head_sum.shape[0]
    columns = query_all.shape[1] // parts
    rows_out = out_sum.shape[0]
    chips = parts // 2
    chip_masks = [mask * 2 for mask in range(1, chips)]
    here.enter(chip_masks + [1], line=True, plane_masks=here.plane_bits)
    weights = [
        WeightGather(wire, here, (t_down.at[0], t_down.at[1]), near, far, cut, 2)
        for cut in range(2)
    ]
    head_own = wire.local(head_part, head_current)
    deals = []
    for mask in chip_masks:
        chip = here.at(mask) // 2
        deals.append(
            wire.send(
                out_part.at[pl.ds(pl.multiple_of(chip * rows_out, rows_out), rows_out)],
                dealt.at[here.chip],
                {"seq": here.at(mask)},
            )
        )
    deal_own = wire.local(
        out_part.at[pl.ds(pl.multiple_of(here.chip * rows_out, rows_out), rows_out)],
        dealt.at[here.chip],
    )

    def product(seats, columns):
        rows = [a[pl.ds(pl.multiple_of(seat * tokens, tokens), tokens), :] for seat in seats]
        return lax.dot_general(
            jnp.concatenate(rows, axis=0),
            w[columns, :],
            (((1,), (1,)), ((), ())),
            preferred_element_type=jnp.float32,
        )

    heads = LineScatter(
        wire, here, lambda index: head_current.at[index], lambda way, step: head_landing.at[way, step]
    )
    outer = LineScatter(
        wire, here, lambda index: dealt.at[index], lambda way, step: out_landing.at[way, step]
    )
    head_own.wait()
    heads.step(1)
    rows = PlaneScatter(wire, here, product, give, take, current, landing, model)
    rows.start()
    loads = []
    for number in range(4):
        loads.append(
            (
                wire.local(sent[number], left.at[number]),
                wire.local(came[number], right.at[number]),
            )
        )
    heads.step(2)
    rows.join()
    rows.stage(0)
    weights[0].start()
    weights[0].own()
    deal_own.wait()
    for copy in deals:
        copy.wait_recv()
    outer.step(1)

    stores = []

    def join(number):
        for load in loads[number]:
            load.wait()
        add_rows(left.at[number], left.at[number], right.at[number])
        stores.append(wire.local(left.at[number], joined[number]))

    stages = len(here.chip_bits)
    for step in range(3, planes):
        heads.step(step)
    rows.settle(0, out)
    for stage in range(1, stages):
        rows.stage(stage)
        if stage + 1 < planes:
            outer.step(stage + 1)
        if stage == 1:
            heads.finish(head_sum)
        if stage + 1 < stages:
            rows.settle(stage, out)
    half, half_out = shard // 2, rows_out // 2

    def seat_columns(seat):
        return pl.ds(pl.multiple_of(seat * columns, columns), columns)

    gathers = [
        PlaneGather(
            wire,
            here,
            lambda color: head_sum.at[pl.ds(color * half, half), pl.ds(0, columns)],
            lambda seat, color: query_all.at[pl.ds(color * half, half), seat_columns(seat)],
        ),
        PlaneGather(
            wire,
            here,
            lambda color: head_sum.at[
                pl.ds(color * half, half), pl.ds(columns, pair_all.shape[2])
            ],
            lambda seat, color: pair_all.at[seat, pl.ds(color * half, half)],
        ),
        PlaneGather(
            wire,
            here,
            lambda color: out_sum.at[pl.ds(color * half_out, half_out)],
            lambda seat, color: outer_all.at[
                pl.ds(
                    pl.multiple_of(
                        ((seat % 2) * chips + seat // 2) * rows_out + color * half_out, half_out
                    ),
                    half_out,
                )
            ],
        ),
    ]
    own = []
    for gather in gathers[:2]:
        gather.start()
    own.append(
        wire.local(head_sum.at[:, pl.ds(0, columns)], query_all.at[:, seat_columns(here.seat)])
    )
    own.append(
        wire.local(
            head_sum.at[:, pl.ds(columns, pair_all.shape[2])], pair_all.at[here.seat]
        )
    )

    weights[1].start()
    weights[1].own()
    rows.settle(stages - 1, out)
    slope_sums[0] = slope[...]
    value = source[...].astype(jnp.float32)
    factor = lax.rsqrt(jnp.mean(value * value, axis=-1, keepdims=True) + EPS)
    slope_sums[0, 0:1, :] = jnp.sum(out[...] * value * factor, axis=0, keepdims=True)
    bits = [("seq", bit) for bit in here.seat_bits] + [("fsdp", bit) for bit in here.plane_bits]
    slope_copies = []

    def slope_send(number):
        axis, bit = bits[number]
        index = here.at(bit) if axis == "seq" else flip(here.plane, bit, here.plane_bits)
        slope_copies.append(
            wire.send(slope_sums.at[number], slope_landing.at[number], {axis: index})
        )

    def slope_add(number):
        slope_copies[number].wait_recv()
        target = slope_out if number == len(bits) - 1 else slope_sums.at[number + 1]
        target[...] = slope_sums[number] + slope_landing[number]

    slope_send(0)
    for step in range(stages + 1, planes):
        outer.step(step)
    join(0)
    gathers[0].hop(1)
    gathers[1].hop(1)
    slope_add(0)
    slope_send(1)
    outer.finish(out_sum)
    gathers[2].start()
    weights[0].forward()
    own_start = (here.core * chips + here.chip) * rows_out
    own.append(
        wire.local(out_sum, outer_all.at[pl.ds(pl.multiple_of(own_start, rows_out), rows_out)])
    )
    join(1)
    for number in range(1, len(bits)):
        slope_add(number)
        if number + 1 < len(bits):
            slope_send(number + 1)
        if number < 3:
            join(number + 1)
    gathers[2].hop(1)
    for gather in gathers:
        gather.hops(2)
    weights[1].forward()
    for gather in gathers:
        gather.finish()
    for weight in weights:
        weight.finish()
    for copy in own + stores:
        copy.wait()
    wire.close()
    heads.close()
    outer.close()


class WeightGather:
    def __init__(self, wire, here, finals, near, far, cut=0, cuts=1):
        self.wire, self.here, self.near, self.far = wire, here, near, far
        self.size = finals[0].shape[0]
        self.rows = self.size // cuts
        self.shift = cut * self.rows
        model = near.shape[0]
        self.finals = [final.at[pl.ds(self.shift, self.rows)] for final in finals]
        self.starts = []
        for color, order in enumerate(here.colors()):
            start = color * (model // 2)
            rows = model // 2
            for bit in order[:-1]:
                rows //= 2
                start = start + here.side(bit) * rows
            self.starts.append(start)
        self.swaps, self.kept = [], []

    def _rows(self, start):
        return pl.ds(pl.multiple_of(start + self.shift, self.rows), self.rows)

    def _pass(self, start, source, bit, rows):
        copy = self.wire.send(
            source, self.near.at[self._rows(start)], {"seq": self.here.at(bit)}
        )
        start = start + rows - 2 * rows * self.here.side(bit)
        return (start, self.near.at[self._rows(start)], copy)

    def _swap(self, start, source):
        self.swaps.append(
            self.wire.send(source, self.far.at[self._rows(start)], {"seq": self.here.at(1)})
        )

    def start(self):
        self.held = []
        for color, order in enumerate(self.here.colors()):
            source, start = self.finals[color], self.starts[color]
            pieces = [(start, source, None)]
            if order[:-1]:
                pieces.append(self._pass(start, source, order[-2], self.size))
            self.held.append(pieces)

    def own(self):
        for color in (0, 1):
            source, start = self.finals[color], self.starts[color]
            self._swap(start, source)
            self.kept.append(self.wire.local(source, self.near.at[self._rows(start)]))

    def forward(self):
        for color, order in enumerate(self.here.colors()):
            rest = order[:-1]
            pieces = self.held[color]
            rows = self.size
            for position in range(len(rest) - 1, -1, -1):
                for start, source, copy in pieces:
                    if copy is not None:
                        copy.wait_recv()
                        self._swap(start, source)
                pieces = [(start, source, None) for start, source, _ in pieces]
                rows *= 2
                if position > 0:
                    pieces = pieces + [
                        self._pass(start, source, rest[position - 1], rows)
                        for start, source, _ in pieces
                    ]

    def finish(self):
        for copy in self.swaps:
            copy.wait_recv()
        for copy in self.kept:
            copy.wait()


def widen_kernel(near, far, out):
    core = lax.axis_index("seq") % 2
    units = near.shape[1]
    out[:, pl.ds(pl.multiple_of(core * units, units), units)] = near[...].astype(out.dtype)
    out[:, pl.ds(pl.multiple_of((1 - core) * units, units), units)] = far[...].astype(out.dtype)


def widen_pieces_kernel(count, steps, starts, *refs):
    nears, fars, out = refs[:count], refs[count : 2 * count], refs[2 * count]
    core = lax.axis_index("seq") % 2
    units = nears[0].shape[1]
    index = pl.program_id(0)
    for number in range(count):

        @pl.when(index // steps == number)
        def _(near=nears[number], far=fars[number]):
            own = pl.ds(pl.multiple_of(core * units, units), units)
            other = pl.ds(pl.multiple_of((1 - core) * units, units), units)
            out[:, own] = near[...].astype(out.dtype)
            out[:, other] = far[...].astype(out.dtype)


SENDS, LOCALS = 192, 32


def call(kernel, mesh_sizes, number, inputs, in_vmem, outputs, scratch, out_vmem=None):
    vmem = pl.BlockSpec(memory_space=pltpu.VMEM)
    anywhere = pl.BlockSpec(memory_space=pl.ANY)
    out_vmem = out_vmem or [True] * len(outputs)
    semaphores = [
        pltpu.SemaphoreType.DMA((SENDS,)),
        pltpu.SemaphoreType.DMA((SENDS,)),
        pltpu.SemaphoreType.DMA((LOCALS,)),
    ]
    return pl.pallas_call(
        functools.partial(kernel, *mesh_sizes),
        out_shape=[jax.ShapeDtypeStruct(shape, kind) for shape, kind in outputs],
        in_specs=[vmem if inside else anywhere for inside in in_vmem],
        out_specs=[vmem if inside else anywhere for inside in out_vmem],
        scratch_shapes=[pltpu.VMEM(shape, kind) for shape, kind in scratch] + semaphores,
        compiler_params=pltpu.CompilerParams(
            collective_id=number, has_side_effects=True, vmem_limit_bytes=VMEM_BYTES
        ),
    )(*inputs)


def widen(near, far):
    rows, units = near.shape
    step = min(256, rows)
    return pl.pallas_call(
        widen_kernel,
        grid=(rows // step,),
        out_shape=jax.ShapeDtypeStruct((rows, 2 * units), jnp.float32),
        in_specs=[pl.BlockSpec((step, units), lambda index: (index, 0))] * 2,
        out_specs=pl.BlockSpec((step, 2 * units), lambda index: (index, 0)),
        cost_estimate=pl.CostEstimate(
            flops=0, transcendentals=0, bytes_accessed=12 * rows * units
        ),
    )(near, far)


def widen_pieces(pieces, fars):
    rows, units = fars[0].shape
    count = len(fars)
    step = min(256, rows)
    steps = rows // step
    starts = jnp.stack([jnp.asarray(start, jnp.int32) // step for start, _ in pieces])

    def block(number):
        return pl.BlockSpec(
            (step, units),
            lambda index, starts: (jnp.clip(index - number * steps, 0, steps - 1), 0),
        )

    return pl.pallas_call(
        functools.partial(widen_pieces_kernel, count, steps),
        out_shape=jax.ShapeDtypeStruct((count * rows, 2 * units), jnp.float32),
        grid_spec=pltpu.PrefetchScalarGridSpec(
            num_scalar_prefetch=1,
            grid=(count * steps,),
            in_specs=[block(number) for number in range(count)] * 2,
            out_specs=pl.BlockSpec(
                (step, 2 * units), lambda index, starts: (starts[index // steps] + index % steps, 0)
            ),
        ),
        cost_estimate=pl.CostEstimate(
            flops=0, transcendentals=0, bytes_accessed=12 * count * rows * units
        ),
    )(starts, *[value for _, value in pieces], *fars)


VMEM_BYTES = 67_000_000


def per_device(
    inputs,
    cotangent,
    attention_gain,
    query_weight,
    key_weight,
    value_weight,
    output_weight,
    query_gain,
    key_gain,
    feedforward_gain,
    gate_weight,
    up_weight,
    down_weight,
):
    tokens = inputs.shape[1]
    model = inputs.shape[2]
    width = query_gain.shape[0]
    pair_heads = key_weight.shape[1] // width
    parts = lax.axis_size("seq")
    planes = lax.axis_size("fsdp")
    sizes = (parts, planes)
    chips = parts // 2
    copies = max(1, parts // pair_heads)
    place = lax.axis_index("seq")
    plane = lax.axis_index("fsdp")
    core = place % 2
    query_cols = model // parts
    head_cols = query_cols + 2 * width
    local_groups = query_cols // width
    shard = query_weight.shape[0]
    piece_rows = shard // parts
    length = parts * tokens
    units = gate_weight.shape[1] // 2
    f32, bf16 = jnp.float32, jnp.bfloat16
    halvings = chips.bit_length() - 2
    last_rows = model // 2 >> halvings
    rows_in = inputs.reshape(tokens, model)
    cot_rows = cotangent.reshape(tokens, model)

    exponents = jnp.arange(width // 2).astype(f32) * 2.0 / width
    rates = jnp.power(jnp.float32(THETA), -exponents)
    rates = jnp.concatenate([rates] * 4)[None, :]
    gain_row = jnp.concatenate([query_gain] * local_groups + [key_gain] * 2)[None, :]
    half = model // 2
    scatter_scratch = [
        ((chips, tokens, model), bf16),
        ((chips, tokens, model), bf16),
        ((2, chips, tokens, half), bf16),
        ((halvings + 1, 2, chips, tokens, half), bf16),
    ]
    mid_gain = feedforward_gain[None, :]
    (
        normed_all,
        head_full,
        out_slice,
        proj,
        queries,
        pair_rows,
        out_rows,
        log_rows,
        cosine,
        sine,
        group,
        middle,
        normed_mid,
        cot_all,
    ) = call(
        functools.partial(front_kernel, width, copies),
        sizes,
        0,
        (
            rows_in,
            cot_rows,
            query_weight,
            key_weight,
            value_weight,
            output_weight,
            attention_gain[None, :],
            mid_gain,
            gain_row,
            rates,
        ),
        (True, True, False, False, False, False, True, True, True, True),
        [
            ((length, model), bf16),
            ((model, head_cols), bf16),
            ((query_cols, model), bf16),
            ((length, head_cols), f32),
            ((length, query_cols), bf16),
            ((length, 2 * width), bf16),
            ((length, query_cols), bf16),
            ((length, 128), f32),
            ((length, 2 * width), f32),
            ((length, 2 * width), f32),
            ((head_cols, head_cols), bf16),
            ((tokens, model), f32),
            ((tokens, model), bf16),
            ((planes, 2, tokens, model), bf16),
        ],
        [((planes, piece_rows, model), bf16)]
        + [((length, 2 * width), bf16)] * 3
        + [((shard, 2 * width), bf16)] * 2
        + scatter_scratch,
    )
    tables = (gain_row, cosine, sine, group)

    quarter = model // 4
    rows_shape = (planes, tokens, model)
    line_scratch = [
        (rows_shape, bf16),
        (rows_shape, bf16),
        ((2, planes - 1, tokens, model), bf16),
    ]
    acts = (2 * planes * tokens, units)
    (
        s_down,
        s_gate_a,
        s_gate_b,
        s_up_a,
        s_up_b,
        middle_grad,
        middle_half,
        mid_slope,
        down_give,
        down_keep,
    ) = call(
        feed_kernel,
        sizes,
        2,
        (
            normed_mid,
            cot_all.reshape(-1, model),
            middle,
            mid_gain,
            gate_weight,
            up_weight,
            down_weight,
        ),
        (True, True, True, True, False, False, False),
        [((2, last_rows, units), bf16)]
        + [((last_rows, units), bf16)] * 4
        + [
            ((tokens, model), f32),
            ((tokens, model), bf16),
            ((1, model), f32),
            (rows_shape, bf16),
            (rows_shape, bf16),
        ],
        [((model, units), bf16)] * 3
        + [((planes, 2, tokens, model), bf16)]
        + [(acts, bf16)] * 3
        + [((3, 2, quarter, units), bf16)]
        + [((3, 2, quarter >> stage, units), bf16) for stage in range(halvings)]
        + [(rows_shape, bf16)]
        + line_scratch,
        [True] * 8 + [False] * 2,
    )

    middle_all, t_down, down_sum = call(
        spread_kernel,
        sizes,
        4,
        (middle_half, s_down, down_give, down_keep),
        (True, True, False, False),
        [((length, model), bf16), ((2, last_rows, units), bf16), ((tokens, model), f32)],
        line_scratch,
    )
    block_rows = middle + down_sum

    def swap(value, bit):
        return lax.ppermute(value, "seq", [(i, i ^ bit) for i in range(parts)])

    *sent, middle_all = lax.optimization_barrier((s_gate_a, s_gate_b, s_up_a, s_up_b, middle_all))
    bit_orders = ([2 << i for i in range(halvings + 1)], [chips >> i for i in range(halvings + 1)])
    came = [swap(piece, bit_orders[number % 2][-1]) for number, piece in enumerate(sent)]

    vmem = pl.BlockSpec(memory_space=pltpu.VMEM)
    halves, head_part, out_part, head_slopes = pl.pallas_call(
        functools.partial(back_kernel, width),
        out_shape=[
            jax.ShapeDtypeStruct((length, head_cols), bf16),
            jax.ShapeDtypeStruct((model, head_cols), bf16),
            jax.ShapeDtypeStruct((query_cols, model), bf16),
            jax.ShapeDtypeStruct((8, head_cols), f32),
        ],
        in_specs=[vmem] * 12,
        out_specs=[vmem] * 4,
        scratch_shapes=[
            pltpu.VMEM((length, query_cols), bf16),
            pltpu.VMEM((length, query_cols), f32),
            pltpu.VMEM((length, 2 * width), f32),
            pltpu.VMEM((length, 2 * width), f32),
        ]
        + [pltpu.VMEM((length, 2 * width), bf16)] * 6,
        compiler_params=pltpu.CompilerParams(vmem_limit_bytes=VMEM_BYTES),
        cost_estimate=pl.CostEstimate(
            flops=10 * length * model * head_cols,
            transcendentals=length * length * local_groups,
            bytes_accessed=16 * length * model,
        ),
    )(
        normed_all,
        middle_all,
        out_slice,
        out_rows,
        log_rows,
        queries,
        pair_rows,
        proj,
        *tables,
    )
    head_part = head_part.reshape(planes, shard, head_cols)
    query_slope = head_slopes[0, :query_cols].reshape(local_groups, width).sum(axis=0)
    key_slope = head_slopes[0, query_cols : query_cols + width]

    gains = jnp.concatenate([query_slope, key_slope])
    gains = jnp.pad(gains, (0, model - gains.shape[0]))
    slopes = jnp.concatenate([jnp.zeros_like(mid_slope), mid_slope, gains[None, :]], axis=0)
    slopes = jnp.pad(slopes, ((0, 5), (0, 0)))
    rounds = (parts * planes).bit_length() - 1
    side = ((model, units), bf16)
    piece = ((last_rows, units), bf16)
    in_grad, near_down, far_down, query_all, pair_all, outer_all, slopes, *pieces = call(
        final_kernel,
        sizes,
        5,
        (halves, head_full, head_part, out_part, t_down, rows_in, slopes, *sent, *came),
        (True, True, False, False, True, True, True) + (False,) * 8,
        [
            ((tokens, model), f32),
            side,
            side,
            ((shard, model), bf16),
            ((parts, shard, 2 * width), bf16),
            ((shard, model), bf16),
            ((8, model), f32),
        ]
        + [piece] * 4,
        scatter_scratch
        + [
            ((planes, shard, head_cols), bf16),
            ((2, planes - 1, shard, head_cols), bf16),
            ((planes, piece_rows, model), bf16),
            ((2, planes - 1, piece_rows, model), bf16),
            ((shard, head_cols), bf16),
            ((piece_rows, model), bf16),
            ((4, last_rows, units), bf16),
            ((4, last_rows, units), bf16),
            ((rounds, 8, model), f32),
            ((rounds, 8, model), f32),
        ],
        [True, False, False] + [True] * 4 + [False] * 4,
    )
    pieces, near_down, far_down, in_grad = lax.optimization_barrier(
        (pieces, near_down, far_down, in_grad)
    )
    source = rows_in.astype(f32)
    first = rms_factor(source)
    input_rows = (middle_grad + norm_back(in_grad, source, first, attention_gain)).astype(bf16)

    def plane_pieces(values):
        whole = []
        for color, order in enumerate(bit_orders):
            start, rows = color * (model // 2), model // 2
            for bit in order[:-1]:
                rows //= 2
                start = start + (place // bit) % 2 * rows
            held = [(start, values[color])]
            rows = last_rows
            for bit in order[-2::-1]:
                held = held + [
                    (start + rows - 2 * rows * ((place // bit) % 2), swap(value, bit))
                    for start, value in held
                ]
                rows *= 2
            whole = whole + held
        return whole

    gate_pieces = plane_pieces(pieces[:2])
    grad_down = widen(near_down, far_down)
    grad_query = query_all.astype(f32)
    grad_pair = pair_all.astype(f32)
    grad_pair = grad_pair.reshape(parts // copies, copies, shard, 2, width).sum(axis=1)
    grad_key = grad_pair[:, :, 0].transpose(1, 0, 2).reshape(shard, -1)
    grad_value = grad_pair[:, :, 1].transpose(1, 0, 2).reshape(shard, -1)
    grad_output = outer_all.astype(f32)
    written = (grad_down, grad_query, grad_key, grad_value, grad_output, input_rows)
    pieces[2:], gate_pieces, written = lax.optimization_barrier((pieces[2:], gate_pieces, written))
    grad_down, grad_query, grad_key, grad_value, grad_output, input_rows = written
    up_pieces = plane_pieces(pieces[2:])
    grad_gate = widen_pieces(gate_pieces, [swap(value, 1) for _, value in gate_pieces])
    up_pieces, grad_gate = lax.optimization_barrier((up_pieces, grad_gate))
    grad_up = widen_pieces(up_pieces, [swap(value, 1) for _, value in up_pieces])
    attention_slope, feedforward_slope = slopes[0], slopes[1]
    query_slope, key_slope = slopes[2, :width], slopes[2, width : 2 * width]
    block_out = block_rows.astype(bf16).reshape(1, tokens, model)
    input_grad = input_rows.reshape(1, tokens, model)
    return (
        block_out,
        input_grad,
        attention_slope,
        grad_query,
        grad_key,
        grad_value,
        grad_output,
        query_slope,
        key_slope,
        feedforward_slope,
        grad_gate,
        grad_up,
        grad_down,
    )


def solution(mesh):
    in_specs = (
        P("fsdp", "seq", None),
        P("fsdp", "seq", None),
        P(),
        P("fsdp", None),
        P("fsdp", None),
        P("fsdp", None),
        P("fsdp", None),
        P(),
        P(),
        P(),
        P(None, "fsdp"),
        P(None, "fsdp"),
        P(None, "fsdp"),
    )
    out_specs = (
        P("fsdp", "seq", None),
        P("fsdp", "seq", None),
        P(),
        P("fsdp", None),
        P("fsdp", None),
        P("fsdp", None),
        P("fsdp", None),
        P(),
        P(),
        P(),
        P(None, "fsdp"),
        P(None, "fsdp"),
        P(None, "fsdp"),
    )
    return jax.shard_map(
        per_device, mesh=mesh, in_specs=in_specs, out_specs=out_specs, check_vma=False
    )
```

```python
import functools

import jax
import jax.numpy as jnp
from jax import lax
from jax.experimental import pallas as pl
from jax.experimental.pallas import tpu as pltpu
from jax.sharding import PartitionSpec as P

EPS = 1e-05
THETA = 1000000.0


def rotate_half(values):
    half = values.shape[-1] // 2
    return jnp.concatenate([-values[..., half:], values[..., :half]], axis=-1)


def rope_tables(positions, width):
    exponents = jnp.arange(width // 2).astype(jnp.float32) * 2.0 / width
    rates = jnp.power(jnp.float32(THETA), -exponents)
    angle = positions.astype(jnp.float32)[:, None] * rates[None, :]
    angle = jnp.concatenate([angle, angle], axis=-1)
    return (jnp.cos(angle), jnp.sin(angle))


def prepare(proj, gain, cosine, sine):
    rows = proj.shape[0]
    width = gain.shape[0]
    split = proj.reshape(rows, -1, width)
    factor = lax.rsqrt(jnp.mean(split * split, axis=-1, keepdims=True) + EPS)
    normed = split * factor * gain
    turned = normed * cosine[:, None, :] + rotate_half(normed) * sine[:, None, :]
    return turned.reshape(rows, -1)


def matmul(left, right):
    return jnp.dot(left, right, preferred_element_type=jnp.float32)


def inner_rows(left, right):
    return lax.dot_general(
        left, right, (((0,), (0,)), ((), ())), preferred_element_type=jnp.float32
    )


def inner_cols(left, right):
    return lax.dot_general(
        left, right, (((1,), (1,)), ((), ())), preferred_element_type=jnp.float32
    )


def rms_factor(values):
    return lax.rsqrt(jnp.mean(values * values, axis=-1, keepdims=True) + EPS)


def norm_back(grad, values, factor, gain):
    scaled = grad * gain
    return factor * (
        scaled - values * factor * factor * jnp.mean(scaled * values, axis=-1, keepdims=True)
    )


def gate_back(hidden_grad, gate, lifted):
    sigma = jax.nn.sigmoid(gate)
    gate_grad = (hidden_grad * lifted * sigma * (1.0 + gate * (1.0 - sigma))).astype(jnp.bfloat16)
    lifted_grad = (hidden_grad * gate * sigma).astype(jnp.bfloat16)
    return (gate_grad, lifted_grad)


def activate(gate, lifted):
    return (gate * jax.nn.sigmoid(gate) * lifted).astype(jnp.bfloat16)


def split_heads(query_rows, pair_rows, groups, width):
    length = query_rows.shape[0]
    key_heads = pair_rows.shape[1] // (2 * width)
    queries = query_rows.reshape(length, key_heads, groups, width)
    keys = pair_rows[:, : key_heads * width].reshape(length, key_heads, width)
    values = pair_rows[:, key_heads * width :].reshape(length, key_heads, width)
    return (queries, keys, values, key_heads)


def attend_heads(query_rows, pair_rows, groups, width):
    length = query_rows.shape[0]
    queries, keys, values, key_heads = split_heads(query_rows, pair_rows, groups, width)
    block = min(512, length)
    scale = width ** (-0.5)
    offsets = jnp.arange(block)

    def query_step(index, state):
        out_rows, log_rows = state
        query_block = lax.dynamic_slice_in_dim(queries, index * block, block, 0)

        def key_step(inner, carry):
            summed, total = carry
            key_block = lax.dynamic_slice_in_dim(keys, inner * block, block, 0)
            value_block = lax.dynamic_slice_in_dim(values, inner * block, block, 0)
            scores = (
                jnp.einsum(
                    "qhgd,shd->hgqs", query_block, key_block, preferred_element_type=jnp.float32
                )
                * scale
            )
            allowed = (index * block + offsets)[:, None] >= (inner * block + offsets)[None, :]
            weights = jnp.where(allowed, jnp.exp(scores), 0.0)
            summed = summed + jnp.einsum(
                "hgqs,shd->hgqd",
                weights.astype(jnp.bfloat16),
                value_block,
                preferred_element_type=jnp.float32,
            )
            return (summed, total + jnp.sum(weights, axis=-1))

        initial = (
            jnp.zeros((key_heads, groups, block, width), jnp.float32),
            jnp.zeros((key_heads, groups, block), jnp.float32),
        )
        summed, total = lax.fori_loop(0, index + 1, key_step, initial)
        result = (summed / total[..., None]).astype(jnp.bfloat16)
        result = result.transpose(2, 0, 1, 3).reshape(block, key_heads * groups * width)
        out_rows = lax.dynamic_update_slice_in_dim(out_rows, result, index * block, 0)
        log_rows = lax.dynamic_update_slice_in_dim(log_rows, jnp.log(total), index * block, 2)
        return (out_rows, log_rows)

    start = (
        jnp.zeros((length, key_heads * groups * width), jnp.bfloat16),
        jnp.zeros((key_heads, groups, length), jnp.float32),
    )
    return lax.fori_loop(0, length // block, query_step, start)


def attend_back(query_rows, pair_rows, out_rows, log_rows, grad_rows, groups, width):
    length = query_rows.shape[0]
    queries, keys, values, key_heads = split_heads(query_rows, pair_rows, groups, width)
    outs = out_rows.reshape(length, key_heads, groups, width)
    grads = grad_rows.reshape(length, key_heads, groups, width)
    correction = jnp.sum(grads.astype(jnp.float32) * outs.astype(jnp.float32), axis=-1)
    block = min(512, length)
    scale = width ** (-0.5)
    offsets = jnp.arange(block)

    def query_step(index, state):
        query_grad, key_grad, value_grad = state
        query_block = lax.dynamic_slice_in_dim(queries, index * block, block, 0)
        grad_block = lax.dynamic_slice_in_dim(grads, index * block, block, 0)
        shift_block = lax.dynamic_slice_in_dim(correction, index * block, block, 0).transpose(
            1, 2, 0
        )
        log_block = lax.dynamic_slice_in_dim(log_rows, index * block, block, 2)

        def key_step(inner, carry):
            block_grad, key_sum, value_sum = carry
            key_block = lax.dynamic_slice_in_dim(keys, inner * block, block, 0)
            value_block = lax.dynamic_slice_in_dim(values, inner * block, block, 0)
            scores = (
                jnp.einsum(
                    "qhgd,shd->hgqs", query_block, key_block, preferred_element_type=jnp.float32
                )
                * scale
            )
            allowed = (index * block + offsets)[:, None] >= (inner * block + offsets)[None, :]
            weights = jnp.where(allowed, jnp.exp(scores - log_block[..., None]), 0.0)
            value_part = jnp.einsum(
                "hgqs,qhgd->shd",
                weights.astype(jnp.bfloat16),
                grad_block,
                preferred_element_type=jnp.float32,
            )
            prob_grad = jnp.einsum(
                "qhgd,shd->hgqs", grad_block, value_block, preferred_element_type=jnp.float32
            )
            score_grad = (weights * (prob_grad - shift_block[..., None]) * scale).astype(
                jnp.bfloat16
            )
            block_grad = block_grad + jnp.einsum(
                "hgqs,shd->qhgd", score_grad, key_block, preferred_element_type=jnp.float32
            )
            key_part = jnp.einsum(
                "hgqs,qhgd->shd", score_grad, query_block, preferred_element_type=jnp.float32
            )
            key_sum = lax.dynamic_update_slice_in_dim(
                key_sum,
                lax.dynamic_slice_in_dim(key_sum, inner * block, block, 0) + key_part,
                inner * block,
                0,
            )
            value_sum = lax.dynamic_update_slice_in_dim(
                value_sum,
                lax.dynamic_slice_in_dim(value_sum, inner * block, block, 0) + value_part,
                inner * block,
                0,
            )
            return (block_grad, key_sum, value_sum)

        initial = (jnp.zeros((block, key_heads, groups, width), jnp.float32), key_grad, value_grad)
        block_grad, key_grad, value_grad = lax.fori_loop(0, index + 1, key_step, initial)
        query_grad = lax.dynamic_update_slice_in_dim(query_grad, block_grad, index * block, 0)
        return (query_grad, key_grad, value_grad)

    state = (
        jnp.zeros((length, key_heads, groups, width), jnp.float32),
        jnp.zeros((length, key_heads, width), jnp.float32),
        jnp.zeros((length, key_heads, width), jnp.float32),
    )
    query_grad, key_grad, value_grad = lax.fori_loop(0, length // block, query_step, state)
    pair_grad = jnp.concatenate(
        [
            key_grad.reshape(length, key_heads * width),
            value_grad.reshape(length, key_heads * width),
        ],
        axis=1,
    )
    return (query_grad.reshape(length, key_heads * groups * width), pair_grad)


MESH = pl.DeviceIdType.MESH


def flip(index, mask, bits):
    for bit in bits:
        if mask & bit:
            index = index + bit - 2 * bit * ((index // bit) % 2)
    return index


class Place:
    def __init__(self, parts, planes):
        self.parts, self.planes = parts, planes
        self.seat = lax.axis_index("seq")
        self.plane = lax.axis_index("fsdp")
        self.core = self.seat % 2
        self.chip = self.seat // 2
        self.seat_bits = [1 << i for i in range(parts.bit_length() - 1)]
        self.chip_bits = self.seat_bits[1:]
        self.plane_bits = [1 << i for i in range(planes.bit_length() - 1)]

    def at(self, mask):
        return flip(self.seat, mask, self.seat_bits)

    def side(self, bit):
        return (self.seat // bit) % 2

    def colors(self):
        return (self.chip_bits, self.chip_bits[::-1])

    def enter(self, masks=(), line=False, plane_masks=()):
        barrier = pltpu.get_barrier_semaphore()
        peers = [{"seq": self.at(mask)} for mask in masks]
        if line:
            peers.append({"fsdp": (self.plane + 1) % self.planes})
            peers.append({"fsdp": (self.plane + self.planes - 1) % self.planes})
        for mask in plane_masks:
            peers.append({"fsdp": flip(self.plane, mask, self.plane_bits)})
        for peer in peers:
            pl.semaphore_signal(barrier, inc=1, device_id=peer, device_id_type=MESH)
        pl.semaphore_wait(barrier, len(peers))


class Wire:
    def __init__(self, sends, receives, locals_):
        self.sends, self.receives, self.locals = sends, receives, locals_
        self.count = self.local_count = 0
        self.open = []

    def remote(self, source, target, device):
        number = self.count
        self.count += 1
        return pltpu.make_async_remote_copy(
            src_ref=source,
            dst_ref=target,
            send_sem=self.sends.at[number],
            recv_sem=self.receives.at[number],
            device_id=device,
            device_id_type=MESH,
        )

    def send(self, source, target, device):
        copy = self.remote(source, target, device)
        copy.start()
        self.open.append(copy)
        return copy

    def quiet(self, source, target):
        number = self.local_count
        self.local_count += 1
        return pltpu.make_async_copy(source, target, self.locals.at[number])

    def local(self, source, target):
        copy = self.quiet(source, target)
        copy.start()
        return copy

    def sent(self, copy):
        copy.wait_send()
        self.open = [other for other in self.open if other is not copy]

    def close(self):
        for copy in self.open:
            copy.wait_send()


def add_rows(target, left, right, step=64):
    rows = target.shape[0]
    step = min(step, rows)

    def body(index, carry):
        at = pl.ds(pl.multiple_of(index * step, step), step)
        total = left[at, :].astype(jnp.float32) + right[at, :].astype(jnp.float32)
        target[at, :] = total.astype(target.dtype)
        return carry

    lax.fori_loop(0, rows // step, body, 0)


class LineGather:
    def __init__(self, wire, here, source, target, share=None):
        self.here = here
        planes, plane = here.planes, here.plane
        above = {"fsdp": (plane + 1) % planes}
        below = {"fsdp": (plane + planes - 1) % planes}
        self.ups, self.downs = {}, {}
        for step in range(1, planes):
            lower = (plane + planes - step + 1) % planes
            upper = (plane + step - 1) % planes
            first = step == 1
            self.ups[step] = wire.remote(
                source if first else target(lower), target(lower), above
            )
            self.downs[step] = wire.remote(
                source if first else target(upper), target(upper), below
            )
        self.shared = {}
        if share is not None:
            for step in range(1, planes):
                for way, shift in ((0, planes - step), (1, step)):
                    index = (plane + shift) % planes
                    self.shared[(step, way)] = wire.remote(
                        target(index), share(index), {"seq": here.at(1)}
                    )

    def start(self, step):
        planes, plane = self.here.planes, self.here.plane

        @pl.when((plane >= step - 1) & (plane <= planes - 2))
        def _():
            self.ups[step].start()

        @pl.when((plane + step <= planes) & (plane >= 1))
        def _():
            self.downs[step].start()

    def arrive(self, step):
        planes, plane = self.here.planes, self.here.plane

        @pl.when(plane >= step)
        def _():
            self.ups[step].wait_recv()
            if self.shared:
                self.shared[(step, 0)].start()

        @pl.when(plane + step <= planes - 1)
        def _():
            self.downs[step].wait_recv()
            if self.shared:
                self.shared[(step, 1)].start()

    def close(self, shared_taken=False):
        planes, plane = self.here.planes, self.here.plane
        for (step, way), copy in self.shared.items():

            @pl.when(plane >= step if way == 0 else plane + step <= planes - 1)
            def _(copy=copy):
                copy.wait_send()
                if not shared_taken:
                    copy.wait_recv()

        for step in range(1, planes):

            @pl.when((plane >= step - 1) & (plane <= planes - 2))
            def _(step=step):
                self.ups[step].wait_send()

            @pl.when((plane + step <= planes) & (plane >= 1))
            def _(step=step):
                self.downs[step].wait_send()


class Lines:
    def __init__(self, members):
        self.members = members

    def start(self, step):
        for member in self.members:
            member.start(step)

    def pass_on(self, step):
        for member in self.members:
            member.arrive(step)
            if step + 1 < member.here.planes:
                member.start(step + 1)

    def step(self, step):
        for member in self.members:
            member.step(step)

    def close(self, *options):
        for member in self.members:
            member.close(*options)


def gather_lines(wire, here, source, target, share=None, cuts=2):
    rows = source.shape[0] // cuts
    members = []
    for cut in range(cuts):
        at = pl.ds(cut * rows, rows)
        members.append(
            LineGather(
                wire,
                here,
                source.at[at],
                lambda index, at=at: target(index).at[at],
                None if share is None else lambda index, at=at: share(index).at[at],
            )
        )
    return Lines(members)


class LineScatter:
    def __init__(self, wire, here, term, landing):
        self.wire, self.here, self.term, self.landing = wire, here, term, landing
        planes, plane = here.planes, here.plane
        above = {"fsdp": (plane + 1) % planes}
        below = {"fsdp": (plane + planes - 1) % planes}
        self.ups, self.downs = {}, {}
        for step in range(1, planes):
            self.ups[step] = wire.remote(
                term((plane + planes - step) % planes), landing(0, step - 1), above
            )
            self.downs[step] = wire.remote(
                term((plane + step) % planes), landing(1, step - 1), below
            )

    def step(self, step):
        planes, plane = self.here.planes, self.here.plane
        mirror = planes - 1 - plane
        for way, (position, copies, dest) in enumerate(
            (
                (plane, self.ups, (plane + planes - step) % planes),
                (mirror, self.downs, (plane + step) % planes),
            )
        ):
            if step > 1:

                @pl.when((position >= 1) & (position <= step - 1))
                def _(way=way, copies=copies, dest=dest):
                    copies[step - 1].wait_recv()
                    term = self.term(dest)
                    add_rows(term, term, self.landing(way, step - 2))

            @pl.when(position <= step - 1)
            def _(copies=copies):
                copies[step].start()

    def finish(self, out):
        planes, plane = self.here.planes, self.here.plane
        own = self.term(plane)
        last = planes - 1

        @pl.when(plane >= 1)
        def _():
            self.ups[last].wait_recv()

        @pl.when(plane <= planes - 2)
        def _():
            self.downs[last].wait_recv()

        @pl.when(plane == 0)
        def _():
            add_rows(out, own, self.landing(1, last - 1))

        @pl.when(plane == planes - 1)
        def _():
            add_rows(out, own, self.landing(0, last - 1))

        @pl.when((plane >= 1) & (plane <= planes - 2))
        def _():
            add_rows(own, own, self.landing(0, last - 1))
            add_rows(out, own, self.landing(1, last - 1))

    def close(self):
        planes, plane = self.here.planes, self.here.plane
        mirror = planes - 1 - plane
        for step in range(1, planes):

            @pl.when(plane <= step - 1)
            def _(step=step):
                self.ups[step].wait_send()

            @pl.when(mirror <= step - 1)
            def _(step=step):
                self.downs[step].wait_send()


class PlaneGather:
    def __init__(self, wire, here, source, target):
        self.wire, self.here, self.source, self.target = wire, here, source, target
        self.incoming = {}

    def _send(self, mask, color, bit):
        here = self.here
        target = self.target(here.at(mask), color)
        source = self.source(color) if mask == 0 else target
        self.incoming[(mask ^ bit, color)] = self.wire.send(
            source, target, {"seq": here.at(bit)}
        )

    def start(self):
        for position in range(len(self.here.chip_bits)):
            for color, bits in enumerate(self.here.colors()):
                self._send(0, color, bits[position])
        for color in (0, 1):
            self._send(0, color, 1)

    def hop(self, hops):
        here = self.here
        chips = here.parts // 2
        for mask in (mask * 2 for mask in range(1, chips)):
            if bin(mask).count("1") != hops:
                continue
            for color, bits in enumerate(here.colors()):
                self.incoming[(mask, color)].wait_recv()
                last = max(i for i, bit in enumerate(bits) if mask & bit)
                for bit in bits[last + 1 :]:
                    self._send(mask, color, bit)
                self._send(mask, color, 1)

    def hops(self, first=1):
        for hops in range(first, len(self.here.chip_bits) + 1):
            self.hop(hops)

    def finish(self):
        for mask in range(1, self.here.parts, 2):
            for color in (0, 1):
                self.incoming[(mask, color)].wait_recv()


class PlaneScatter:
    def __init__(self, wire, here, product, give, take, current, landing, model):
        self.wire, self.here, self.product = wire, here, product
        self.give, self.take, self.current, self.landing = give, take, current, landing
        self.model = model

    def start(self):
        here = self.here
        chips = here.parts // 2
        self.swaps = {}
        tokens = self.give.shape[1]
        seats = [2 * flip(here.chip, mask, [b // 2 for b in here.chip_bits]) for mask in range(chips)]
        for part in range(self.model // 512):
            columns = slice(part * 512, (part + 1) * 512)
            rows = self.product([seat + 1 - here.core for seat in seats], columns)
            for mask in range(chips):
                self.give[mask, :, columns] = rows[mask * tokens : (mask + 1) * tokens].astype(
                    self.give.dtype
                )
        for mask in range(chips)[::-1]:
            self.swaps[mask] = self.wire.send(
                self.give.at[mask], self.take.at[mask], {"seq": here.at(1)}
            )
        half = self.model // 2
        for part in range(self.model // 512):
            columns = slice(part * 512, (part + 1) * 512)
            rows = self.product([seat + here.core for seat in seats], columns)
            color, inside = divmod(part * 512, half)
            for mask in range(chips):
                self.current[color, mask, :, inside : inside + 512] = rows[
                    mask * tokens : (mask + 1) * tokens
                ].astype(self.current.dtype)

    def join(self):
        half = self.model // 2
        chips = self.here.parts // 2
        for mask in range(chips)[::-1]:
            self.swaps[mask].wait_recv()
            for color in (0, 1):
                mine = self.current.at[color, mask]
                add_rows(mine, mine, self.take.at[mask, :, pl.ds(color * half, half)])

    def stage(self, position):
        here = self.here
        self.moved = getattr(self, "moved", {})
        for onward in (True, False):
            for color, bits in enumerate(here.colors()):
                bit = bits[position]
                done = sum(bits[:position])
                for mask in range(here.parts // 2):
                    low = mask ^ (bit // 2)
                    if not mask * 2 & bit or mask * 2 & done:
                        continue
                    if self._onward(position, color, low) != onward:
                        continue
                    self.moved[(position, color, low)] = self.wire.send(
                        self.current.at[color, mask],
                        self.landing.at[position, color, low],
                        {"seq": here.at(bit)},
                    )

    def _onward(self, position, color, low):
        bits = self.here.colors()[color]
        return position + 1 < len(bits) and bool(low * 2 & bits[position + 1])

    def settle(self, position, out, onward):
        half = self.model // 2
        last = position == len(self.here.chip_bits) - 1
        for (stage, color, low), copy in self.moved.items():
            if stage != position or self._onward(position, color, low) != onward:
                continue
            copy.wait_recv()
            mine = self.current.at[color, low]
            target = out.at[:, pl.ds(color * half, half)] if last else mine
            add_rows(target, mine, self.landing.at[position, color, low])


def pick_lanes(low, high, width):
    lane = lax.broadcasted_iota(jnp.int32, low.shape, low.ndim - 1)
    return jnp.where(lane % (2 * width) < width, low, high)


def group_mean(values, group, width):
    high = values.astype(jnp.bfloat16)
    low = (values - high.astype(jnp.float32)).astype(jnp.bfloat16)
    total = jnp.dot(high, group, preferred_element_type=jnp.float32) + jnp.dot(
        low, group, preferred_element_type=jnp.float32
    )
    return total * (1.0 / width)


def turn(values, width):
    lanes = values.shape[1]
    half = width // 2
    return pick_lanes(
        pltpu.roll(values, lanes - half, 1), pltpu.roll(values, half, 1), half
    )


def attend_block(index, block, width, heads, queries, pair, twin, left, right, out_rows, logs):
    rows = pl.ds(index * block, block)
    before = index * block
    columns = 2 * width
    row = lax.broadcasted_iota(jnp.int32, (block, block), 0)
    column = lax.broadcasted_iota(jnp.int32, (block, block), 1)
    allowed = row >= column
    contract = (((1,), (1,)), ((), ()))
    lane = lax.broadcasted_iota(jnp.int32, (block, 128), 1)

    def two_heads(number, table):
        at = pl.ds(pl.multiple_of(number * columns, columns), columns)
        both = queries[rows, at]
        both = (both.astype(jnp.float32) * width**-0.5).astype(both.dtype)
        zero = jnp.zeros_like(both)
        result = None
        for side, values in ((0, left), (1, right)):
            mine = pick_lanes(both, zero, width) if side == 0 else pick_lanes(zero, both, width)
            scores = lax.dot_general(
                mine, twin[rows, :], contract, preferred_element_type=jnp.float32
            )
            weights = jnp.where(allowed, jnp.exp(scores), 0.0)
            total = jnp.sum(weights, axis=1, keepdims=True)
            summed = jnp.dot(
                weights.astype(jnp.bfloat16), values[rows, :], preferred_element_type=jnp.float32
            )
            if before:
                scores = lax.dot_general(
                    mine, twin[0:before, :], contract, preferred_element_type=jnp.float32
                )
                weights = jnp.exp(scores)
                total = total + jnp.sum(weights, axis=1, keepdims=True)
                summed = summed + jnp.dot(
                    weights.astype(jnp.bfloat16),
                    values[0:before, :],
                    preferred_element_type=jnp.float32,
                )
            table = jnp.where(lane == 2 * number + side, total, table)
            part = summed / total
            result = part if result is None else result + part
        out_rows[rows, at] = result.astype(out_rows.dtype)
        return table

    table = lax.fori_loop(0, heads // 2, two_heads, jnp.ones((block, 128), jnp.float32))
    logs[rows, :] = jnp.log(table)


def back_block(
    index, block, width, heads, queries, grads, outs, logs, keys, values, query_back, key_back, value_back
):
    rows = pl.ds(index * block, block)
    before = index * block
    scale = width**-0.5
    row = lax.broadcasted_iota(jnp.int32, (block, block), 0)
    column = lax.broadcasted_iota(jnp.int32, (block, block), 1)
    allowed = row >= column
    lane = lax.broadcasted_iota(jnp.int32, (block, 2 * width), 1)
    across = (((1,), (1,)), ((), ()))
    down = (((0,), (0,)), ((), ()))
    f32 = jnp.float32
    spans = [(rows, True)] + ([(slice(0, before), False)] if before else [])

    def one_head(head, carry):
        number, side = head // 2, head % 2
        at = pl.ds(pl.multiple_of(number * 2 * width, 2 * width), 2 * width)
        mine = lane // width == side
        query = jnp.where(mine, queries[rows, at], 0)
        grad = jnp.where(mine, grads[rows, at], 0)
        scaled = (query.astype(f32) * scale).astype(query.dtype)
        shift = jnp.sum(grad.astype(f32) * outs[rows, at].astype(f32), axis=1, keepdims=True)
        log = jnp.sum(jnp.where(lane == head, logs[rows, :], 0.0), axis=1, keepdims=True)
        total = query_back[rows, at]
        for span, masked in spans:
            scores = lax.dot_general(
                scaled, keys[0, span, :], across, preferred_element_type=f32
            )
            weights = jnp.exp(scores - log)
            if masked:
                weights = jnp.where(allowed, weights, 0.0)
            prob_grad = lax.dot_general(
                grad, values[span, :], across, preferred_element_type=f32
            )
            score_grad = (weights * (prob_grad - shift) * scale).astype(query.dtype)
            total = total + jnp.dot(
                score_grad, keys[1 + side, span, :], preferred_element_type=f32
            )
            key_back[span, :] += lax.dot_general(
                score_grad, query, down, preferred_element_type=f32
            )
            value_back[span, :] += lax.dot_general(
                weights.astype(query.dtype), grad, down, preferred_element_type=f32
            )
        query_back[rows, at] = total
        return carry

    lax.fori_loop(0, heads, one_head, 0)


def back_kernel(
    width,
    normed,
    middle,
    out_slice,
    outs,
    logs,
    queries,
    pair,
    proj,
    gain,
    cosine,
    sine,
    group,
    halves,
    head_part,
    out_part,
    slopes,
    grads,
    query_back,
    key_back,
    value_back,
    keys,
    values,
):
    length = normed.shape[0]
    block = min(256, length)
    blocks = length // block
    query_cols = queries.shape[1]
    heads = query_cols // width
    f32 = jnp.float32
    query_back[...] = jnp.zeros_like(query_back)
    key_back[...] = jnp.zeros_like(key_back)
    value_back[...] = jnp.zeros_like(value_back)

    def ready(index, carry):
        at = pl.ds(pl.multiple_of(index * block, block), block)
        grads[at, :] = lax.dot_general(
            middle[at, :], out_slice[...], (((1,), (1,)), ((), ())), preferred_element_type=f32
        ).astype(grads.dtype)
        both = pair[at, :].astype(f32)
        swapped = pltpu.roll(both, width, 1)
        zero = jnp.zeros_like(both)
        keys[0, at, :] = pick_lanes(both, swapped, width).astype(keys.dtype)
        keys[1, at, :] = pick_lanes(both, zero, width).astype(keys.dtype)
        keys[2, at, :] = pick_lanes(zero, swapped, width).astype(keys.dtype)
        values[at, :] = pick_lanes(swapped, both, width).astype(values.dtype)
        return carry

    lax.fori_loop(0, blocks, ready, 0)
    for index in range(blocks):
        back_block(
            index,
            block,
            width,
            heads,
            queries,
            grads,
            outs,
            logs,
            keys,
            values,
            query_back,
            key_back,
            value_back,
        )

    def norms(index, slope):
        at = pl.ds(pl.multiple_of(index * block, block), block)
        key_sum, value_sum = key_back[at, :], value_back[at, :]
        key_sum = key_sum + pltpu.roll(key_sum, width, 1)
        value_sum = value_sum + pltpu.roll(value_sum, width, 1)
        back = jnp.concatenate(
            [query_back[at, :], pick_lanes(key_sum, value_sum, width)], axis=1
        )
        value = proj[at, :]
        factor = lax.rsqrt(group_mean(value * value, group[...], width) + EPS)
        repeat = value.shape[1] // cosine.shape[1]
        cosines = jnp.concatenate([cosine[at, :]] * repeat, axis=1)
        sines = jnp.concatenate([sine[at, :]] * repeat, axis=1)
        turned = back * cosines + turn(back * sines, width)
        slope = slope + jnp.sum(turned * value * factor, axis=0, keepdims=True)
        scaled = turned * gain[...]
        result = factor * (
            scaled - value * factor * factor * group_mean(scaled * value, group[...], width)
        )
        lane = lax.broadcasted_iota(jnp.int32, back.shape, 1)
        result = jnp.where(lane >= query_cols + width, back, result)
        halves[at, :] = result.astype(halves.dtype)
        return slope

    slope = lax.fori_loop(0, blocks, norms, jnp.zeros((1, proj.shape[1]), f32))
    slopes[...] = jnp.broadcast_to(slope, slopes.shape)

    def terms(number, carry):
        at = pl.ds(pl.multiple_of(number * 256, 256), 256)
        down = (((0,), (0,)), ((), ()))
        head_part[at, :] = lax.dot_general(
            normed[:, at], halves[...], down, preferred_element_type=f32
        ).astype(head_part.dtype)
        out_part[:, at] = lax.dot_general(
            outs[...], middle[:, at], down, preferred_element_type=f32
        ).astype(out_part.dtype)
        return carry

    lax.fori_loop(0, normed.shape[1] // 256, terms, 0)


def row_blocks(rows, step, work):
    def body(index, carry):
        work(pl.ds(pl.multiple_of(index * step, step), step))
        return carry

    lax.fori_loop(0, rows // step, body, 0)


def front_kernel(
    width,
    copies,
    parts,
    planes,
    x,
    c,
    query_weight,
    key_weight,
    value_weight,
    output_weight,
    in_gain,
    mid_gain,
    gain,
    rates,
    x_store,
    w_store,
    o_store,
    proj_store,
    query_store,
    pair_store,
    out_store,
    log_store,
    cosine_store,
    sine_store,
    group_store,
    middle,
    mid,
    c_store,
    x_all,
    w_all,
    o_slice,
    proj,
    queries,
    pair,
    out_rows,
    logs,
    cosine,
    sine,
    group,
    c_all,
    o_all,
    twin,
    left,
    right,
    key_block,
    value_block,
    give,
    take,
    current,
    landing,
    *sems,
):
    here = Place(parts, planes)
    wire = Wire(*sems)
    tokens, model = x.shape
    shard = query_weight.shape[0]
    query_cols = queries.shape[1]
    rows = o_all.shape[1]
    half = tokens // 2
    chips = parts // 2
    f32 = jnp.float32
    chip_masks = [mask * 2 for mask in range(1, chips)]
    pair_head = here.seat // copies
    own_shard = pl.ds(pl.multiple_of(here.plane * shard, shard), shard)
    head_block = pl.ds(pl.multiple_of(pair_head // 2 * 2 * width, 2 * width), 2 * width)
    loads = [
        wire.local(key_weight.at[:, head_block], key_block),
        wire.local(value_weight.at[:, head_block], value_block),
        wire.local(
            query_weight.at[:, pl.ds(pl.multiple_of(here.seat * query_cols, query_cols), query_cols)],
            w_all.at[own_shard, pl.ds(0, query_cols)],
        ),
    ]
    piece = (here.core * chips + here.chip) * rows
    o = output_weight.at[pl.ds(pl.multiple_of(piece, rows), rows)]
    here.enter(chip_masks + [1], line=True)
    o_own = wire.local(o, o_all.at[here.plane])
    for load in loads[:2]:
        load.wait()
    upper = (pair_head % 2) * jnp.ones((1, 1), jnp.int32)
    keys, values = key_block[...].astype(f32), value_block[...].astype(f32)
    keys = jnp.where(upper == 1, pltpu.roll(keys, width, 1), keys)
    values = jnp.where(upper == 1, values, pltpu.roll(values, width, 1))
    w_all[own_shard, query_cols:] = pick_lanes(keys, values, width).astype(w_all.dtype)
    loads[2].wait()
    weights = gather_lines(
        wire,
        here,
        w_all.at[own_shard],
        lambda index: w_all.at[pl.ds(pl.multiple_of(index * shard, shard), shard)],
    )
    weights.start(1)

    def norm_rows(at):
        value = x[at, :].astype(f32)
        factor = lax.rsqrt(jnp.mean(value * value, axis=-1, keepdims=True) + EPS)
        own_at = pl.ds(pl.multiple_of(here.seat * tokens + at.start, 32), 32)
        x_all[own_at, :] = (value * factor * in_gain[...]).astype(x_all.dtype)

    row_blocks(tokens, 32, norm_rows)

    def seat_rows(seat, color):
        return x_all.at[pl.ds(pl.multiple_of(seat * tokens + color * half, half), half)]

    plane_rows = PlaneGather(
        wire, here, lambda color: seat_rows(here.seat, color), seat_rows
    )
    plane_rows.start()
    outer = gather_lines(wire, here, o, lambda index: o_all.at[index])

    def c_spot(index):
        return c_all.at[index, here.core]

    cots = gather_lines(wire, here, c, c_spot, c_spot)
    c_own = wire.local(c, c_spot(here.plane))

    lane = lax.broadcasted_iota(jnp.int32, (32, 2 * width), 1)
    row = lax.broadcasted_iota(jnp.int32, (32, 2 * width), 0)
    sign = jnp.where(lane % width < width // 2, -1.0, 1.0)

    def table_rows(at):
        angle = (row + at.start).astype(f32) * rates[...]
        cosine[at, :] = jnp.cos(angle)
        sine[at, :] = jnp.sin(angle) * sign

    columns = group.shape[0]
    group[...] = jnp.where(
        lax.broadcasted_iota(jnp.int32, (columns, columns), 0) // width
        == lax.broadcasted_iota(jnp.int32, (columns, columns), 1) // width,
        1.0,
        0.0,
    ).astype(group.dtype)
    length = x_all.shape[0]
    row_blocks(length, 32, table_rows)
    weights.members[0].arrive(1)
    if planes > 2:
        weights.members[0].start(2)
    plane_rows.hop(1)
    weights.members[1].arrive(1)
    if planes > 2:
        weights.members[1].start(2)
    outer.start(1)
    plane_rows.hops(2)
    spot = o_slice.at[pl.ds(pl.multiple_of(here.chip * rows, rows), rows)]
    deals = []
    for mask in chip_masks:
        chip = here.at(mask) // 2
        deals.append((chip, wire.remote(o_all.at[chip], spot, {"seq": here.at(mask)})))
    keep_own = wire.quiet(o_all.at[here.chip], spot)

    def deal(step):
        for chip, copy in deals + [(here.chip, keep_own)]:

            @pl.when((chip == here.plane + step) | (chip + step == here.plane))
            def _(copy=copy):
                copy.start()

    o_own.wait()
    deal(0)
    for step in range(2, planes):
        weights.pass_on(step)
    plane_rows.finish()
    stores = [
        wire.local(x_all, x_store),
        wire.local(w_all, w_store),
        wire.local(cosine, cosine_store),
        wire.local(sine, sine_store),
        wire.local(group, group_store),
    ]
    block = min(256, length)
    blocks = length // block
    heads = query_cols // width

    def project(index, carry):
        at = pl.ds(pl.multiple_of(index * block, block), block)
        value = jnp.dot(x_all[at, :], w_all[...], preferred_element_type=f32)
        proj[at, :] = value
        factor = lax.rsqrt(group_mean(value * value, group[...], width) + EPS)
        normed = value * factor * gain[...]
        repeat = value.shape[1] // cosine.shape[1]
        cosines = jnp.concatenate([cosine[at, :]] * repeat, axis=1)
        sines = jnp.concatenate([sine[at, :]] * repeat, axis=1)
        turned = normed * cosines + turn(normed, width) * sines
        queries[at, :] = turned[:, :query_cols].astype(queries.dtype)
        keys, values = turned[:, query_cols:], value[:, query_cols:]
        both = pick_lanes(keys, values, width)
        pair[at, :] = both.astype(pair.dtype)
        swapped = pltpu.roll(both, width, 1)
        twin[at, :] = pick_lanes(both, swapped, width).astype(twin.dtype)
        zero = jnp.zeros_like(both)
        left[at, :] = pick_lanes(swapped, zero, width).astype(left.dtype)
        right[at, :] = pick_lanes(zero, both, width).astype(right.dtype)
        return carry

    lax.fori_loop(0, blocks, project, 0)
    across = wire.send(c, c_spot(here.plane), {"seq": here.at(1)})
    waits = list(range(1, planes))
    cot_waits = list(range(1, planes))
    for index in range(blocks):
        while waits and waits[0] * blocks <= (index + 1) * planes:
            step = waits.pop(0)
            outer.pass_on(step)
            deal(step)
            if not waits or (step == 2 and planes > 3):
                if len(waits) == planes - 3 or planes <= 3:
                    cots.start(1)
        attend_block(
            index, block, width, heads, queries, pair, twin, left, right, out_rows, logs
        )
    for step in waits:
        outer.pass_on(step)
        deal(step)
    cots.pass_on(cot_waits.pop(0))
    keep_own.wait()
    for _, copy in deals:
        copy.wait()

    def product(seats, at):
        chosen = [
            out_rows[pl.ds(pl.multiple_of(seat * tokens, tokens), tokens), :] for seat in seats
        ]
        return jnp.dot(
            jnp.concatenate(chosen, axis=0), o_slice[:, at], preferred_element_type=f32
        )

    stores += [
        wire.local(o_slice, o_store),
        wire.local(proj, proj_store),
        wire.local(queries, query_store),
        wire.local(pair, pair_store),
        wire.local(out_rows, out_store),
        wire.local(logs, log_store),
    ]
    sums = PlaneScatter(wire, here, product, give, take, current, landing, model)
    sums.start()
    sums.join()
    sums.stage(0)
    stages = len(here.chip_bits)
    for stage in range(stages):
        sums.settle(stage, middle, True)
        if stage + 1 < stages:
            sums.stage(stage + 1)
        if cot_waits:
            cots.pass_on(cot_waits.pop(0))
        sums.settle(stage, middle, False)

    def mid_rows(at):
        value = x[at, :].astype(f32) + middle[at, :]
        middle[at, :] = value
        factor = lax.rsqrt(jnp.mean(value * value, axis=-1, keepdims=True) + EPS)
        mid[at, :] = (value * factor * mid_gain[...]).astype(mid.dtype)

    for step in cot_waits:
        cots.pass_on(step)
    cots.close()
    c_own.wait()
    across.wait_recv()
    stores.append(wire.local(c_all, c_store))
    row_blocks(tokens, 32, mid_rows)
    for copy in stores:
        copy.wait()
    wire.close()
    weights.close()
    outer.close()


def feed_kernel(
    parts,
    planes,
    m,
    cots,
    middle,
    mid_gain,
    gate_weight,
    up_weight,
    down_weight,
    s_down,
    s_first,
    s_second,
    mid,
    mid_half,
    mid_slope,
    down_give,
    down_keep,
    gate_half,
    up_half,
    down_half,
    mids,
    hidden,
    unit_grads,
    away,
    *rest,
):
    here = Place(parts, planes)
    stages = len(here.chip_bits) - 1
    landings, rest = rest[:stages], rest[stages:]
    give, take, current, line_landing, *sems = rest
    wire = Wire(*sems)
    tokens, model = m.shape
    units = gate_half.shape[1]
    own_units = pl.ds(pl.multiple_of(here.core * units, units), units)
    loads = [
        wire.local(whole.at[:, own_units], part)
        for whole, part in (
            (gate_weight, gate_half),
            (up_weight, up_half),
            (down_weight, down_half),
        )
    ]
    here.enter(here.seat_bits, line=True)

    def spot(index):
        return mids.at[index, here.core]

    lines = gather_lines(wire, here, m, spot, spot)
    lines.start(1)
    across = wire.send(m, spot(here.plane), {"seq": here.at(1)})
    own = wire.local(m, spot(here.plane))

    def block(index):
        rows = pl.ds(pl.multiple_of(index * 2 * tokens, 2 * tokens), 2 * tokens)
        mid_rows = mids[index].reshape(2 * tokens, model)
        cot_rows = cots[rows, :]

        def part(number, carry):
            at = pl.ds(pl.multiple_of(number * 256, 256), 256)
            gate = jnp.dot(mid_rows, gate_half[:, at], preferred_element_type=jnp.float32)
            lifted = jnp.dot(mid_rows, up_half[:, at], preferred_element_type=jnp.float32)
            hidden_grad = jnp.dot(cot_rows, down_half[:, at], preferred_element_type=jnp.float32)
            sigma = 1.0 / (1.0 + jnp.exp(-gate))
            active = gate * sigma
            hidden[rows, at] = (active * lifted).astype(hidden.dtype)
            unit_grads[1, rows, at] = (hidden_grad * active).astype(hidden.dtype)
            unit_grads[0, rows, at] = (
                hidden_grad * lifted * sigma * (1.0 + gate * (1.0 - sigma))
            ).astype(hidden.dtype)
            return carry

        lax.fori_loop(0, units // 256, part, 0)

    for load in loads:
        load.wait()
    own.wait()
    across.wait_recv()
    plane = here.plane
    block(plane)
    for step in range(1, planes):
        lines.pass_on(step)
        ups = jnp.where(plane >= step, 1, 0)
        downs = jnp.where(plane + step <= planes - 1, 1, 0)

        def arrived(number, carry, step=step, ups=ups):
            from_up = (number == 0) & (ups == 1)
            for way, chosen in ((0, from_up), (1, jnp.logical_not(from_up))):

                @pl.when(chosen)
                def _(way=way):
                    for line in lines.members:
                        line.shared[(step, way)].wait_recv()

            block(jnp.where(from_up, plane + planes - step, plane + step) % planes)
            return carry

        lax.fori_loop(0, ups + downs, arrived, 0)

    flat_mids = mids.reshape(2 * planes * tokens, model)
    quarter = model // 4
    moved = {}

    def gradients(left, right, target, start, count):
        parts_of = quarter // 256

        def part(number, carry):
            k, inside = number // parts_of, number % parts_of * 256
            at = pl.ds(pl.multiple_of(start(k) + inside, 256), 256)
            target(k)[pl.ds(pl.multiple_of(inside, 256), 256), :] = lax.dot_general(
                left[:, at],
                right(k)[...],
                (((0,), (0,)), ((), ())),
                preferred_element_type=jnp.float32,
            ).astype(away.dtype)
            return carry

        lax.fori_loop(0, count * parts_of, part, 0)

    def first_half(color, mine):
        sides = [here.side(bits[0]) if mine else 1 - here.side(bits[0]) for bits in here.colors()]
        if isinstance(color, int):
            side = sides[color]
        else:
            side = sides[0] * (1 - color) + sides[1] * color
        return pl.multiple_of(color * (model // 2) + side * quarter, quarter)

    def send_away(number):
        for color, bits in enumerate(here.colors()):
            moved[(number, color)] = wire.send(
                away.at[number, color], landings[0].at[number, color], {"seq": here.at(bits[0])}
            )

    def mid_term(target, core):
        rows = [pl.ds(pl.multiple_of((2 * p + core) * tokens, tokens), tokens) for p in range(planes)]
        gates = jnp.concatenate([unit_grads[0, at, :] for at in rows], axis=0)
        lifts = jnp.concatenate([unit_grads[1, at, :] for at in rows], axis=0)

        def part(number, carry):
            at = pl.ds(pl.multiple_of(number * 256, 256), 256)
            term = lax.dot_general(
                gates, gate_half[at, :], (((1,), (1,)), ((), ())), preferred_element_type=jnp.float32
            ) + lax.dot_general(
                lifts, up_half[at, :], (((1,), (1,)), ((), ())), preferred_element_type=jnp.float32
            )
            target[:, :, at] = term.reshape(planes, tokens, 256).astype(target.dtype)
            return carry

        lax.fori_loop(0, model // 256, part, 0)

    def down_term(target, core):
        rows = [pl.ds(pl.multiple_of((2 * p + core) * tokens, tokens), tokens) for p in range(planes)]
        hiddens = jnp.concatenate([hidden[at, :] for at in rows], axis=0)

        def part(number, carry):
            at = pl.ds(pl.multiple_of(number * 256, 256), 256)
            term = lax.dot_general(
                hiddens, down_half[at, :], (((1,), (1,)), ((), ())), preferred_element_type=jnp.float32
            )
            target[:, :, at] = term.reshape(planes, tokens, 256).astype(target.dtype)
            return carry

        lax.fori_loop(0, model // 256, part, 0)

    gradients(
        cots,
        lambda k: hidden,
        lambda k: away.at[0, k],
        lambda k: first_half(k, False),
        2,
    )
    send_away(0)
    swaps = TokenSum(wire, here, current, take, line_landing)
    mid_term(give, 1 - here.core)
    swaps.start(give)
    mid_term(current, here.core)
    swaps.join()
    swaps.step(1)
    gradients(
        flat_mids,
        lambda k: unit_grads.at[k // 2],
        lambda k: away.at[1 + k // 2, k % 2],
        lambda k: first_half(k % 2, False),
        4,
    )
    send_away(1)
    send_away(2)
    for step in range(2, planes):
        swaps.step(step)

    def final(number, color):
        if number == 0:
            return s_down.at[color]
        return (s_first, s_second)[color].at[number - 1]

    wire.sent(swaps.across)
    down_term(give, 1 - here.core)
    down_term(take, here.core)
    handed = [wire.local(give, down_give), wire.local(take, down_keep)]
    rows = quarter
    keeps = {}
    if stages > 1:
        for copy in moved.values():
            wire.sent(copy)
    gradients(
        cots,
        lambda k: hidden,
        lambda k: s_down.at[k] if stages == 1 else away.at[0, k],
        lambda k: first_half(k, True),
        2,
    )
    for color in (0, 1):
        gradients(
            flat_mids,
            lambda k: unit_grads.at[k],
            lambda k: (s_first, s_second)[color].at[k] if stages == 1 else away.at[1 + k, color],
            lambda k: first_half(color, True),
            2,
        )
    for number in range(3):
        for color in (0, 1):
            keep = final(number, color) if stages == 1 else away.at[number, color]
            keeps[(number, color)] = (keep, 0)
    swaps.finish(mid)
    f32 = jnp.float32

    def norm_back_rows(index, slope):
        at = pl.ds(pl.multiple_of(index * 32, 32), 32)
        own_cots = (here.plane * 2 + here.core) * tokens + index * 32
        grad, value = mid[at, :], middle[at, :]
        factor = lax.rsqrt(jnp.mean(value * value, axis=-1, keepdims=True) + EPS)
        scaled = grad * mid_gain[...]
        back = factor * (
            scaled
            - value * factor * factor * jnp.mean(scaled * value, axis=-1, keepdims=True)
        )
        result = cots[pl.ds(pl.multiple_of(own_cots, 32), 32), :].astype(f32) + back
        mid[at, :] = result
        mid_half[at, :] = result.astype(mid_half.dtype)
        return slope + jnp.sum(grad * value * factor, axis=0, keepdims=True)

    mid_slope[...] = lax.fori_loop(
        0, tokens // 32, norm_back_rows, jnp.zeros((1, model), f32)
    )
    for stage in range(stages):
        last = stage == stages - 1
        for number in range(3):
            for color, bits in enumerate(here.colors()):
                keep, begin = keeps[(number, color)]
                moved[(number, color)].wait_recv()
                mine = keep.at[pl.ds(begin, rows)]
                if last:
                    add_rows(final(number, color), mine, landings[stage].at[number, color])
                else:
                    add_rows(mine, mine, landings[stage].at[number, color])
                    bit = bits[stage + 1]
                    half = rows // 2
                    gone = pl.multiple_of(begin + (1 - here.side(bit)) * half, half)
                    moved[(number, color)] = wire.send(
                        keep.at[pl.ds(gone, half)],
                        landings[stage + 1].at[number, color],
                        {"seq": here.at(bit)},
                    )
                    keeps[(number, color)] = (
                        keep,
                        pl.multiple_of(begin + here.side(bit) * half, half),
                    )
        rows //= 2
    for copy in handed:
        copy.wait()
    wire.close()
    lines.close(True)
    swaps.close()


class TokenSum:
    def __init__(self, wire, here, current, take, landing):
        self.wire, self.here = wire, here
        self.current, self.take = current, take
        self.cuts = 2
        rows = current.shape[1] // self.cuts
        self.lines = []
        for cut in range(self.cuts):
            at = pl.ds(cut * rows, rows)
            self.lines.append(
                LineScatter(
                    wire,
                    here,
                    lambda index, at=at: current.at[index, at],
                    lambda way, step, at=at: landing.at[way, step, at],
                )
            )

    def start(self, give):
        self.across = self.wire.send(give, self.take, {"seq": self.here.at(1)})

    def join(self):
        self.across.wait_recv()

        def body(index, carry):
            row = self.current.at[index]
            add_rows(row, row, self.take.at[index])
            return carry

        lax.fori_loop(0, self.here.planes, body, 0)

    def step(self, step):
        for line in self.lines:
            line.step(step)

    def finish(self, out):
        rows = out.shape[0] // self.cuts
        for cut, line in enumerate(self.lines):
            line.finish(out.at[pl.ds(cut * rows, rows)])

    def close(self):
        for line in self.lines:
            line.close()


def spread_kernel(
    parts, planes, h, s, give, keep, h_store, t, block, h_all, current, take, line_landing, *sems
):
    here = Place(parts, planes)
    wire = Wire(*sems)
    here.enter(here.seat_bits, line=True)
    tokens = h.shape[0]
    half = tokens // 2
    rows = PlaneGather(
        wire,
        here,
        lambda color: h.at[pl.ds(color * half, half)],
        lambda seat, color: h_all.at[pl.ds(pl.multiple_of(seat * tokens + color * half, half), half)],
    )
    swaps = TokenSum(wire, here, current, take, line_landing)
    swaps.start(give)
    kept = wire.local(keep, current)
    rows.start()
    own = wire.local(h, h_all.at[pl.ds(pl.multiple_of(here.seat * tokens, tokens), tokens)])
    kept.wait()
    swaps.join()
    swaps.step(1)
    rows.hop(1)
    moved = [
        wire.send(s.at[color], t.at[color], {"seq": here.at(bits[-1])})
        for color, bits in enumerate(here.colors())
    ]
    for step in range(2, planes):
        if step == 3:
            rows.hops(2)
        swaps.step(step)
    if planes <= 3:
        rows.hops(2)
    rows.finish()
    own.wait()
    store = wire.local(h_all, h_store)
    for color in (0, 1):
        moved[color].wait_recv()
        add_rows(t.at[color], t.at[color], s.at[color])
    swaps.finish(block)
    store.wait()
    wire.close()
    swaps.close()


def final_kernel(
    parts,
    planes,
    a,
    w,
    head_part,
    out_part,
    t_down,
    source,
    slope,
    *rest,
):
    sent, came, rest = rest[:2], rest[2:4], rest[4:]
    out, near, far, query_all, pair_all, outer_all, slope_out, *rest = rest
    joined, rest = rest[:4], rest[4:]
    (
        give,
        take,
        current,
        landing,
        head_current,
        head_landing,
        dealt,
        out_landing,
        head_sum,
        out_sum,
        left,
        right,
        slope_sums,
        slope_landing,
        *sems,
    ) = rest
    here = Place(parts, planes)
    wire = Wire(*sems)
    tokens, model = out.shape
    shard = head_sum.shape[0]
    columns = query_all.shape[1] // parts
    rows_out = out_sum.shape[0]
    chips = parts // 2
    chip_masks = [mask * 2 for mask in range(1, chips)]
    here.enter(chip_masks + [1], line=True, plane_masks=here.plane_bits)
    weights = [
        WeightGather(wire, here, (t_down.at[0], t_down.at[1]), near, far, cut, 2)
        for cut in range(2)
    ]
    head_own = wire.local(head_part, head_current)
    deals = []
    for mask in chip_masks:
        chip = here.at(mask) // 2
        deals.append(
            wire.send(
                out_part.at[pl.ds(pl.multiple_of(chip * rows_out, rows_out), rows_out)],
                dealt.at[here.chip],
                {"seq": here.at(mask)},
            )
        )
    deal_own = wire.local(
        out_part.at[pl.ds(pl.multiple_of(here.chip * rows_out, rows_out), rows_out)],
        dealt.at[here.chip],
    )

    def product(seats, columns):
        rows = [a[pl.ds(pl.multiple_of(seat * tokens, tokens), tokens), :] for seat in seats]
        return lax.dot_general(
            jnp.concatenate(rows, axis=0),
            w[columns, :],
            (((1,), (1,)), ((), ())),
            preferred_element_type=jnp.float32,
        )

    heads = LineScatter(
        wire, here, lambda index: head_current.at[index], lambda way, step: head_landing.at[way, step]
    )
    outer = LineScatter(
        wire, here, lambda index: dealt.at[index], lambda way, step: out_landing.at[way, step]
    )
    head_own.wait()
    heads.step(1)
    rows = PlaneScatter(wire, here, product, give, take, current, landing, model)
    rows.start()
    loads = []
    for number in range(4):
        loads.append(
            (
                wire.local(sent[number % 2].at[number // 2], left.at[number]),
                wire.local(came[number % 2].at[number // 2], right.at[number]),
            )
        )
    heads.step(2)
    rows.join()
    rows.stage(0)
    weights[0].start()
    weights[0].own()
    deal_own.wait()
    for copy in deals:
        copy.wait_recv()
    outer.step(1)

    stores = []

    def join(number):
        for load in loads[number]:
            load.wait()
        add_rows(left.at[number], left.at[number], right.at[number])
        stores.append(wire.local(left.at[number], joined[number]))

    stages = len(here.chip_bits)
    for step in range(3, planes):
        heads.step(step)
    for stage in range(1, stages):
        rows.settle(stage - 1, out, True)
        rows.stage(stage)
        rows.settle(stage - 1, out, False)
        if stage + 1 < planes:
            outer.step(stage + 1)
        if stage == 1:
            heads.finish(head_sum)
    half, half_out = shard // 2, rows_out // 2

    def seat_columns(seat):
        return pl.ds(pl.multiple_of(seat * columns, columns), columns)

    gathers = [
        PlaneGather(
            wire,
            here,
            lambda color: head_sum.at[pl.ds(color * half, half), pl.ds(0, columns)],
            lambda seat, color: query_all.at[pl.ds(color * half, half), seat_columns(seat)],
        ),
        PlaneGather(
            wire,
            here,
            lambda color: head_sum.at[
                pl.ds(color * half, half), pl.ds(columns, pair_all.shape[2])
            ],
            lambda seat, color: pair_all.at[seat, pl.ds(color * half, half)],
        ),
        PlaneGather(
            wire,
            here,
            lambda color: out_sum.at[pl.ds(color * half_out, half_out)],
            lambda seat, color: outer_all.at[
                pl.ds(
                    pl.multiple_of(
                        ((seat % 2) * chips + seat // 2) * rows_out + color * half_out, half_out
                    ),
                    half_out,
                )
            ],
        ),
    ]
    own = []
    for gather in gathers[:2]:
        gather.start()
    own.append(
        wire.local(head_sum.at[:, pl.ds(0, columns)], query_all.at[:, seat_columns(here.seat)])
    )
    own.append(
        wire.local(
            head_sum.at[:, pl.ds(columns, pair_all.shape[2])], pair_all.at[here.seat]
        )
    )

    weights[1].start()
    weights[1].own()
    rows.settle(stages - 1, out, False)
    slope_sums[0] = slope[...]
    value = source[...].astype(jnp.float32)
    factor = lax.rsqrt(jnp.mean(value * value, axis=-1, keepdims=True) + EPS)
    slope_sums[0, 0:1, :] = jnp.sum(out[...] * value * factor, axis=0, keepdims=True)
    bits = [("seq", bit) for bit in here.seat_bits] + [("fsdp", bit) for bit in here.plane_bits]
    slope_copies = []

    def slope_send(number):
        axis, bit = bits[number]
        index = here.at(bit) if axis == "seq" else flip(here.plane, bit, here.plane_bits)
        slope_copies.append(
            wire.send(slope_sums.at[number], slope_landing.at[number], {axis: index})
        )

    def slope_add(number):
        slope_copies[number].wait_recv()
        target = slope_out if number == len(bits) - 1 else slope_sums.at[number + 1]
        target[...] = slope_sums[number] + slope_landing[number]

    slope_send(0)
    for step in range(stages + 1, planes):
        outer.step(step)
    join(0)
    gathers[0].hop(1)
    gathers[1].hop(1)
    slope_add(0)
    slope_send(1)
    outer.finish(out_sum)
    gathers[2].start()
    weights[0].forward()
    own_start = (here.core * chips + here.chip) * rows_out
    own.append(
        wire.local(out_sum, outer_all.at[pl.ds(pl.multiple_of(own_start, rows_out), rows_out)])
    )
    join(1)
    for number in range(1, len(bits)):
        slope_add(number)
        if number + 1 < len(bits):
            slope_send(number + 1)
        if number < 3:
            join(number + 1)
    gathers[2].hop(1)
    for gather in gathers:
        gather.hops(2)
    weights[1].forward()
    for gather in gathers:
        gather.finish()
    for weight in weights:
        weight.finish()
    for copy in own + stores:
        copy.wait()
    wire.close()
    heads.close()
    outer.close()


class WeightGather:
    def __init__(self, wire, here, finals, near, far, cut=0, cuts=1):
        self.wire, self.here, self.near, self.far = wire, here, near, far
        self.size = finals[0].shape[0]
        self.rows = self.size // cuts
        self.shift = cut * self.rows
        model = near.shape[0]
        self.finals = [final.at[pl.ds(self.shift, self.rows)] for final in finals]
        self.starts = []
        for color, order in enumerate(here.colors()):
            start = color * (model // 2)
            rows = model // 2
            for bit in order[:-1]:
                rows //= 2
                start = start + here.side(bit) * rows
            self.starts.append(start)
        self.swaps, self.kept = [], []

    def _rows(self, start):
        return pl.ds(pl.multiple_of(start + self.shift, self.rows), self.rows)

    def _pass(self, start, source, bit, rows):
        copy = self.wire.send(
            source, self.near.at[self._rows(start)], {"seq": self.here.at(bit)}
        )
        start = start + rows - 2 * rows * self.here.side(bit)
        return (start, self.near.at[self._rows(start)], copy)

    def _swap(self, start, source):
        self.swaps.append(
            self.wire.send(source, self.far.at[self._rows(start)], {"seq": self.here.at(1)})
        )

    def start(self):
        self.held = []
        for color, order in enumerate(self.here.colors()):
            source, start = self.finals[color], self.starts[color]
            pieces = [(start, source, None)]
            if order[:-1]:
                pieces.append(self._pass(start, source, order[-2], self.size))
            self.held.append(pieces)

    def own(self):
        for color in (0, 1):
            source, start = self.finals[color], self.starts[color]
            self._swap(start, source)
            self.kept.append(self.wire.local(source, self.near.at[self._rows(start)]))

    def forward(self):
        for color, order in enumerate(self.here.colors()):
            rest = order[:-1]
            pieces = self.held[color]
            rows = self.size
            for position in range(len(rest) - 1, -1, -1):
                for start, source, copy in pieces:
                    if copy is not None:
                        copy.wait_recv()
                        self._swap(start, source)
                pieces = [(start, source, None) for start, source, _ in pieces]
                rows *= 2
                if position > 0:
                    pieces = pieces + [
                        self._pass(start, source, rest[position - 1], rows)
                        for start, source, _ in pieces
                    ]

    def finish(self):
        for copy in self.swaps:
            copy.wait_recv()
        for copy in self.kept:
            copy.wait()


def widen_kernel(near, far, out):
    core = lax.axis_index("seq") % 2
    units = near.shape[1]
    out[:, pl.ds(pl.multiple_of(core * units, units), units)] = near[...].astype(out.dtype)
    out[:, pl.ds(pl.multiple_of((1 - core) * units, units), units)] = far[...].astype(out.dtype)


def widen_pieces_kernel(count, steps, starts, *refs):
    nears, fars, out = refs[:count], refs[count : 2 * count], refs[-1]
    core = lax.axis_index("seq") % 2
    units = nears[0].shape[1]
    index = pl.program_id(0)
    for number in range(count):

        @pl.when(index // steps == number)
        def _(near=nears[number], far=fars[number]):
            own = pl.ds(pl.multiple_of(core * units, units), units)
            other = pl.ds(pl.multiple_of((1 - core) * units, units), units)
            out[:, own] = near[...].astype(out.dtype)
            out[:, other] = far[...].astype(out.dtype)


def results_kernel(
    copies, width, query, pair, outer, slope, grad_query, grad_key, grad_value, grad_output, *gains
):
    f32 = jnp.float32
    grad_query[...] = query[...].astype(f32)
    grad_output[...] = outer[...].astype(f32)
    columns = 2 * width
    for number in range(pair.shape[0] // (2 * copies)):
        low, high = (
            sum(
                pair[(2 * number + side) * copies + copy].astype(f32) for copy in range(copies)
            )
            for side in (0, 1)
        )
        at = pl.ds(number * columns, columns)
        grad_key[:, at] = pick_lanes(low, pltpu.roll(high, width, 1), width)
        grad_value[:, at] = pick_lanes(pltpu.roll(low, width, 1), high, width)
    in_slope, mid_slope, query_slope, key_slope = gains
    in_slope[...] = slope[0:1, :]
    mid_slope[...] = slope[1:2, :]
    query_slope[...] = slope[2:3, 0:width]
    key_slope[...] = slope[3:4, 0:width]


SENDS, LOCALS = 192, 32


def call(kernel, mesh_sizes, number, inputs, in_vmem, outputs, scratch, out_vmem=None):
    vmem = pl.BlockSpec(memory_space=pltpu.VMEM)
    anywhere = pl.BlockSpec(memory_space=pl.ANY)
    out_vmem = out_vmem or [True] * len(outputs)
    semaphores = [
        pltpu.SemaphoreType.DMA((SENDS,)),
        pltpu.SemaphoreType.DMA((SENDS,)),
        pltpu.SemaphoreType.DMA((LOCALS,)),
    ]
    return pl.pallas_call(
        functools.partial(kernel, *mesh_sizes),
        out_shape=[jax.ShapeDtypeStruct(shape, kind) for shape, kind in outputs],
        in_specs=[vmem if inside else anywhere for inside in in_vmem],
        out_specs=[vmem if inside else anywhere for inside in out_vmem],
        scratch_shapes=[pltpu.VMEM(shape, kind) for shape, kind in scratch] + semaphores,
        compiler_params=pltpu.CompilerParams(
            collective_id=number, has_side_effects=True, vmem_limit_bytes=VMEM_BYTES
        ),
    )(*inputs)


def widen(near, far):
    rows, units = near.shape
    step = min(256, rows)
    return pl.pallas_call(
        widen_kernel,
        grid=(rows // step,),
        out_shape=jax.ShapeDtypeStruct((rows, 2 * units), jnp.float32),
        in_specs=[pl.BlockSpec((step, units), lambda index: (index, 0))] * 2,
        out_specs=pl.BlockSpec((step, 2 * units), lambda index: (index, 0)),
        cost_estimate=pl.CostEstimate(
            flops=0, transcendentals=0, bytes_accessed=12 * rows * units
        ),
    )(near, far)


def widen_pieces(pieces, fars, whole=None, into=None):
    rows, units = fars[0].shape
    count = len(fars)
    step = min(256, rows)
    steps = rows // step
    starts = jnp.stack([jnp.asarray(start, jnp.int32) >> (step.bit_length() - 1) for start, _ in pieces])

    def block(number):
        return pl.BlockSpec(
            (step, units),
            lambda index, starts: (jnp.clip(index - number * steps, 0, steps - 1), 0),
        )

    more = () if into is None else (into,)
    return pl.pallas_call(
        functools.partial(widen_pieces_kernel, count, steps),
        out_shape=jax.ShapeDtypeStruct((whole or count * rows, 2 * units), jnp.float32),
        grid_spec=pltpu.PrefetchScalarGridSpec(
            num_scalar_prefetch=1,
            grid=(count * steps,),
            in_specs=[block(number) for number in range(count)] * 2
            + [pl.BlockSpec(memory_space=pl.ANY) for _ in more],
            out_specs=pl.BlockSpec(
                (step, 2 * units), lambda index, starts: (starts[index // steps] + index % steps, 0)
            ),
        ),
        input_output_aliases={2 * count + 1: 0} if more else {},
        cost_estimate=pl.CostEstimate(
            flops=0, transcendentals=0, bytes_accessed=12 * count * rows * units
        ),
    )(starts, *[value for _, value in pieces], *fars, *more)


def results(copies, width, query, pair, outer, slope):
    shard, model = query.shape
    seats = pair.shape[0]
    step = min(128, shard)
    f32 = jnp.float32
    pair_cols = seats // copies * width
    row = pl.BlockSpec((step, model), lambda index: (index, 0))
    row_pair = pl.BlockSpec((step, pair_cols), lambda index: (index, 0))
    fixed = lambda *shape: pl.BlockSpec(shape, lambda index: (0, 0))
    return pl.pallas_call(
        functools.partial(results_kernel, copies, width),
        grid=(shard // step,),
        out_shape=[
            jax.ShapeDtypeStruct((shard, model), f32),
            jax.ShapeDtypeStruct((shard, pair_cols), f32),
            jax.ShapeDtypeStruct((shard, pair_cols), f32),
            jax.ShapeDtypeStruct((shard, model), f32),
            jax.ShapeDtypeStruct((1, model), f32),
            jax.ShapeDtypeStruct((1, model), f32),
            jax.ShapeDtypeStruct((1, width), f32),
            jax.ShapeDtypeStruct((1, width), f32),
        ],
        in_specs=[
            row,
            pl.BlockSpec((seats, step, 2 * width), lambda index: (0, index, 0)),
            row,
            fixed(8, model),
        ],
        out_specs=[row, row_pair, row_pair, row]
        + [fixed(1, model), fixed(1, model), fixed(1, width), fixed(1, width)],
        cost_estimate=pl.CostEstimate(
            flops=0, transcendentals=0, bytes_accessed=16 * shard * model
        ),
    )(query, pair, outer, slope)


VMEM_BYTES = 67_000_000


def per_device(
    inputs,
    cotangent,
    attention_gain,
    query_weight,
    key_weight,
    value_weight,
    output_weight,
    query_gain,
    key_gain,
    feedforward_gain,
    gate_weight,
    up_weight,
    down_weight,
):
    tokens = inputs.shape[1]
    model = inputs.shape[2]
    width = query_gain.shape[0]
    pair_heads = key_weight.shape[1] // width
    parts = lax.axis_size("seq")
    planes = lax.axis_size("fsdp")
    sizes = (parts, planes)
    chips = parts // 2
    copies = max(1, parts // pair_heads)
    place = lax.axis_index("seq")
    plane = lax.axis_index("fsdp")
    core = place % 2
    query_cols = model // parts
    head_cols = query_cols + 2 * width
    local_groups = query_cols // width
    shard = query_weight.shape[0]
    piece_rows = shard // parts
    length = parts * tokens
    units = gate_weight.shape[1] // 2
    f32, bf16 = jnp.float32, jnp.bfloat16
    halvings = chips.bit_length() - 2
    last_rows = model // 2 >> halvings
    rows_in = inputs.reshape(tokens, model)
    cot_rows = cotangent.reshape(tokens, model)

    exponents = jnp.arange(width // 2).astype(f32) * 2.0 / width
    rates = jnp.power(jnp.float32(THETA), -exponents)
    rates = jnp.concatenate([rates] * 4)[None, :]
    gain_row = jnp.concatenate([query_gain] * local_groups + [key_gain] * 2)[None, :]
    half = model // 2
    scatter_scratch = [
        ((chips, tokens, model), bf16),
        ((chips, tokens, model), bf16),
        ((2, chips, tokens, half), bf16),
        ((halvings + 1, 2, chips, tokens, half), bf16),
    ]
    mid_gain = feedforward_gain[None, :]
    kept = [
        ((length, model), bf16),
        ((model, head_cols), bf16),
        ((query_cols, model), bf16),
        ((length, head_cols), f32),
        ((length, query_cols), bf16),
        ((length, 2 * width), bf16),
        ((length, query_cols), bf16),
        ((length, 128), f32),
        ((length, 2 * width), f32),
        ((length, 2 * width), f32),
        ((head_cols, head_cols), bf16),
        ((planes, 2, tokens, model), bf16),
    ]
    (
        normed_all,
        head_full,
        out_slice,
        proj,
        queries,
        pair_rows,
        out_rows,
        log_rows,
        cosine,
        sine,
        group,
        middle,
        normed_mid,
        cot_all,
    ) = call(
        functools.partial(front_kernel, width, copies),
        sizes,
        0,
        (
            rows_in,
            cot_rows,
            query_weight,
            key_weight,
            value_weight,
            output_weight,
            attention_gain[None, :],
            mid_gain,
            gain_row,
            rates,
        ),
        (True, True, False, False, False, False, True, True, True, True),
        kept[:11] + [((tokens, model), f32), ((tokens, model), bf16)] + kept[11:],
        kept
        + [((planes, piece_rows, model), bf16)]
        + [((length, 2 * width), bf16)] * 3
        + [((shard, 2 * width), bf16)] * 2
        + scatter_scratch,
        [False] * 11 + [True] * 2 + [False],
    )
    tables = (gain_row, cosine, sine, group)

    quarter = model // 4
    rows_shape = (planes, tokens, model)
    line_scratch = [
        (rows_shape, bf16),
        (rows_shape, bf16),
        ((2, planes - 1, tokens, model), bf16),
    ]
    acts = (2 * planes * tokens, units)
    (
        s_down,
        s_first,
        s_second,
        middle_grad,
        middle_half,
        mid_slope,
        down_give,
        down_keep,
    ) = call(
        feed_kernel,
        sizes,
        2,
        (
            normed_mid,
            cot_all.reshape(-1, model),
            middle,
            mid_gain,
            gate_weight,
            up_weight,
            down_weight,
        ),
        (True, True, True, True, False, False, False),
        [((2, last_rows, units), bf16)] * 3
        + [
            ((tokens, model), f32),
            ((tokens, model), bf16),
            ((1, model), f32),
            (rows_shape, bf16),
            (rows_shape, bf16),
        ],
        [((model, units), bf16)] * 3
        + [((planes, 2, tokens, model), bf16)]
        + [(acts, bf16), ((2,) + acts, bf16)]
        + [((3, 2, quarter, units), bf16)]
        + [((3, 2, quarter >> stage, units), bf16) for stage in range(halvings)]
        + [(rows_shape, bf16)]
        + line_scratch,
        [True] * 6 + [False] * 2,
    )

    middle_all, t_down, down_sum = call(
        spread_kernel,
        sizes,
        4,
        (middle_half, s_down, down_give, down_keep),
        (True, True, False, False),
        [((length, model), bf16), ((2, last_rows, units), bf16), ((tokens, model), f32)],
        [((length, model), bf16)] + line_scratch,
        [False, True, True],
    )

    def swap(value, bit):
        return lax.ppermute(value, "seq", [(i, i ^ bit) for i in range(parts)])

    *sent, middle_all = lax.optimization_barrier((s_first, s_second, middle_all))
    bit_orders = ([2 << i for i in range(halvings + 1)], [chips >> i for i in range(halvings + 1)])
    came = [swap(value, order[-1]) for value, order in zip(sent, bit_orders)]

    vmem = pl.BlockSpec(memory_space=pltpu.VMEM)
    halves, head_part, out_part, head_slopes = pl.pallas_call(
        functools.partial(back_kernel, width),
        out_shape=[
            jax.ShapeDtypeStruct((length, head_cols), bf16),
            jax.ShapeDtypeStruct((model, head_cols), bf16),
            jax.ShapeDtypeStruct((query_cols, model), bf16),
            jax.ShapeDtypeStruct((8, head_cols), f32),
        ],
        in_specs=[vmem] * 12,
        out_specs=[vmem] * 4,
        scratch_shapes=[
            pltpu.VMEM((length, query_cols), bf16),
            pltpu.VMEM((length, query_cols), f32),
            pltpu.VMEM((length, 2 * width), f32),
            pltpu.VMEM((length, 2 * width), f32),
        ]
        + [pltpu.VMEM((3, length, 2 * width), bf16), pltpu.VMEM((length, 2 * width), bf16)],
        compiler_params=pltpu.CompilerParams(vmem_limit_bytes=VMEM_BYTES),
        cost_estimate=pl.CostEstimate(
            flops=10 * length * model * head_cols,
            transcendentals=length * length * local_groups,
            bytes_accessed=16 * length * model,
        ),
    )(
        normed_all,
        middle_all,
        out_slice,
        out_rows,
        log_rows,
        queries,
        pair_rows,
        proj,
        *tables,
    )
    head_part = head_part.reshape(planes, shard, head_cols)
    query_slope = head_slopes[:1, :query_cols].reshape(local_groups, width).sum(axis=0)
    key_slope = head_slopes[0, query_cols : query_cols + width]
    gains = jnp.pad(jnp.stack([query_slope, key_slope]), ((0, 0), (0, model - width)))
    slopes = jnp.concatenate(
        [jnp.zeros_like(mid_slope), mid_slope, gains, jnp.zeros((4, model), f32)], axis=0
    )
    rounds = (parts * planes).bit_length() - 1
    side = ((model, units), bf16)
    piece = ((last_rows, units), bf16)
    in_grad, near_down, far_down, query_all, pair_all, outer_all, slopes, *pieces = call(
        final_kernel,
        sizes,
        5,
        (halves, head_full, head_part, out_part, t_down, rows_in, slopes, *sent, *came),
        (True, True, False, False, True, True, True) + (False,) * 4,
        [
            ((tokens, model), f32),
            side,
            side,
            ((shard, model), bf16),
            ((parts, shard, 2 * width), bf16),
            ((shard, model), bf16),
            ((8, model), f32),
        ]
        + [piece] * 4,
        scatter_scratch
        + [
            ((planes, shard, head_cols), bf16),
            ((2, planes - 1, shard, head_cols), bf16),
            ((planes, piece_rows, model), bf16),
            ((2, planes - 1, piece_rows, model), bf16),
            ((shard, head_cols), bf16),
            ((piece_rows, model), bf16),
            ((4, last_rows, units), bf16),
            ((4, last_rows, units), bf16),
            ((rounds, 8, model), f32),
            ((rounds, 8, model), f32),
        ],
        [True, False, False] + [True] * 4 + [False] * 4,
    )
    pieces, near_down, far_down, in_grad = lax.optimization_barrier(
        (pieces, near_down, far_down, in_grad)
    )
    source = rows_in.astype(f32)
    first = rms_factor(source)
    input_rows = (middle_grad + norm_back(in_grad, source, first, attention_gain)).astype(bf16)

    def plane_pieces(values):
        whole = []
        for color, order in enumerate(bit_orders):
            start, rows = color * (model // 2), model // 2
            for bit in order[:-1]:
                rows //= 2
                start = start + (place // bit) % 2 * rows
            held = [(start, values[color])]
            rows = last_rows
            for bit in order[-2::-1]:
                held = held + [
                    (start + rows - 2 * rows * ((place // bit) % 2), swap(value, bit))
                    for start, value in held
                ]
                rows *= 2
            whole = whole + held
        return whole

    gate_pieces = plane_pieces(pieces[:2])
    grad_down = widen(near_down, far_down)
    (
        grad_query,
        grad_key,
        grad_value,
        grad_output,
        attention_slope,
        feedforward_slope,
        query_slope,
        key_slope,
    ) = results(copies, width, query_all, pair_all, outer_all, slopes)
    block_out = (middle + down_sum).astype(bf16).reshape(1, tokens, model)
    pieces[2:], grad_down = lax.optimization_barrier((pieces[2:], grad_down))
    up_pieces = plane_pieces(pieces[2:])
    written = (grad_down, grad_query, grad_key, grad_value, grad_output, input_rows, block_out)
    gate_pieces, written = lax.optimization_barrier((gate_pieces, written))
    grad_down, grad_query, grad_key, grad_value, grad_output, input_rows, block_out = written
    grad_gate = widen_pieces(gate_pieces, [swap(value, 1) for _, value in gate_pieces])
    own = [up_pieces[0], up_pieces[len(up_pieces) // 2]]
    others = [piece for piece in up_pieces if all(piece is not mine for mine in own)]
    grad_up = widen_pieces(own, [swap(value, 1) for _, value in own], model)
    others, grad_gate, grad_up = lax.optimization_barrier((others, grad_gate, grad_up))
    grad_up = widen_pieces(others, [swap(value, 1) for _, value in others], model, grad_up)
    attention_slope, feedforward_slope = attention_slope[0], feedforward_slope[0]
    query_slope, key_slope = query_slope[0], key_slope[0]
    input_grad = input_rows.reshape(1, tokens, model)
    return (
        block_out,
        input_grad,
        attention_slope,
        grad_query,
        grad_key,
        grad_value,
        grad_output,
        query_slope,
        key_slope,
        feedforward_slope,
        grad_gate,
        grad_up,
        grad_down,
    )


def solution(mesh):
    in_specs = (
        P("fsdp", "seq", None),
        P("fsdp", "seq", None),
        P(),
        P("fsdp", None),
        P("fsdp", None),
        P("fsdp", None),
        P("fsdp", None),
        P(),
        P(),
        P(),
        P(None, "fsdp"),
        P(None, "fsdp"),
        P(None, "fsdp"),
    )
    out_specs = (
        P("fsdp", "seq", None),
        P("fsdp", "seq", None),
        P(),
        P("fsdp", None),
        P("fsdp", None),
        P("fsdp", None),
        P("fsdp", None),
        P(),
        P(),
        P(),
        P(None, "fsdp"),
        P(None, "fsdp"),
        P(None, "fsdp"),
    )
    return jax.shard_map(
        per_device, mesh=mesh, in_specs=in_specs, out_specs=out_specs, check_vma=False
    )
```

```python
import functools

import jax
import jax.numpy as jnp
from jax import lax
from jax.experimental import pallas as pl
from jax.experimental.pallas import tpu as pltpu
from jax.sharding import PartitionSpec as P

EPS = 1e-05
THETA = 1000000.0


def rotate_half(values):
    half = values.shape[-1] // 2
    return jnp.concatenate([-values[..., half:], values[..., :half]], axis=-1)


def rope_tables(positions, width):
    exponents = jnp.arange(width // 2).astype(jnp.float32) * 2.0 / width
    rates = jnp.power(jnp.float32(THETA), -exponents)
    angle = positions.astype(jnp.float32)[:, None] * rates[None, :]
    angle = jnp.concatenate([angle, angle], axis=-1)
    return (jnp.cos(angle), jnp.sin(angle))


def prepare(proj, gain, cosine, sine):
    rows = proj.shape[0]
    width = gain.shape[0]
    split = proj.reshape(rows, -1, width)
    factor = lax.rsqrt(jnp.mean(split * split, axis=-1, keepdims=True) + EPS)
    normed = split * factor * gain
    turned = normed * cosine[:, None, :] + rotate_half(normed) * sine[:, None, :]
    return turned.reshape(rows, -1)


def matmul(left, right):
    return jnp.dot(left, right, preferred_element_type=jnp.float32)


def inner_rows(left, right):
    return lax.dot_general(
        left, right, (((0,), (0,)), ((), ())), preferred_element_type=jnp.float32
    )


def inner_cols(left, right):
    return lax.dot_general(
        left, right, (((1,), (1,)), ((), ())), preferred_element_type=jnp.float32
    )


def rms_factor(values):
    return lax.rsqrt(jnp.mean(values * values, axis=-1, keepdims=True) + EPS)


def norm_back(grad, values, factor, gain):
    scaled = grad * gain
    return factor * (
        scaled - values * factor * factor * jnp.mean(scaled * values, axis=-1, keepdims=True)
    )


def gate_back(hidden_grad, gate, lifted):
    sigma = jax.nn.sigmoid(gate)
    gate_grad = (hidden_grad * lifted * sigma * (1.0 + gate * (1.0 - sigma))).astype(jnp.bfloat16)
    lifted_grad = (hidden_grad * gate * sigma).astype(jnp.bfloat16)
    return (gate_grad, lifted_grad)


def activate(gate, lifted):
    return (gate * jax.nn.sigmoid(gate) * lifted).astype(jnp.bfloat16)


def split_heads(query_rows, pair_rows, groups, width):
    length = query_rows.shape[0]
    key_heads = pair_rows.shape[1] // (2 * width)
    queries = query_rows.reshape(length, key_heads, groups, width)
    keys = pair_rows[:, : key_heads * width].reshape(length, key_heads, width)
    values = pair_rows[:, key_heads * width :].reshape(length, key_heads, width)
    return (queries, keys, values, key_heads)


def attend_heads(query_rows, pair_rows, groups, width):
    length = query_rows.shape[0]
    queries, keys, values, key_heads = split_heads(query_rows, pair_rows, groups, width)
    block = min(512, length)
    scale = width ** (-0.5)
    offsets = jnp.arange(block)

    def query_step(index, state):
        out_rows, log_rows = state
        query_block = lax.dynamic_slice_in_dim(queries, index * block, block, 0)

        def key_step(inner, carry):
            summed, total = carry
            key_block = lax.dynamic_slice_in_dim(keys, inner * block, block, 0)
            value_block = lax.dynamic_slice_in_dim(values, inner * block, block, 0)
            scores = (
                jnp.einsum(
                    "qhgd,shd->hgqs", query_block, key_block, preferred_element_type=jnp.float32
                )
                * scale
            )
            allowed = (index * block + offsets)[:, None] >= (inner * block + offsets)[None, :]
            weights = jnp.where(allowed, jnp.exp(scores), 0.0)
            summed = summed + jnp.einsum(
                "hgqs,shd->hgqd",
                weights.astype(jnp.bfloat16),
                value_block,
                preferred_element_type=jnp.float32,
            )
            return (summed, total + jnp.sum(weights, axis=-1))

        initial = (
            jnp.zeros((key_heads, groups, block, width), jnp.float32),
            jnp.zeros((key_heads, groups, block), jnp.float32),
        )
        summed, total = lax.fori_loop(0, index + 1, key_step, initial)
        result = (summed / total[..., None]).astype(jnp.bfloat16)
        result = result.transpose(2, 0, 1, 3).reshape(block, key_heads * groups * width)
        out_rows = lax.dynamic_update_slice_in_dim(out_rows, result, index * block, 0)
        log_rows = lax.dynamic_update_slice_in_dim(log_rows, jnp.log(total), index * block, 2)
        return (out_rows, log_rows)

    start = (
        jnp.zeros((length, key_heads * groups * width), jnp.bfloat16),
        jnp.zeros((key_heads, groups, length), jnp.float32),
    )
    return lax.fori_loop(0, length // block, query_step, start)


def attend_back(query_rows, pair_rows, out_rows, log_rows, grad_rows, groups, width):
    length = query_rows.shape[0]
    queries, keys, values, key_heads = split_heads(query_rows, pair_rows, groups, width)
    outs = out_rows.reshape(length, key_heads, groups, width)
    grads = grad_rows.reshape(length, key_heads, groups, width)
    correction = jnp.sum(grads.astype(jnp.float32) * outs.astype(jnp.float32), axis=-1)
    block = min(512, length)
    scale = width ** (-0.5)
    offsets = jnp.arange(block)

    def query_step(index, state):
        query_grad, key_grad, value_grad = state
        query_block = lax.dynamic_slice_in_dim(queries, index * block, block, 0)
        grad_block = lax.dynamic_slice_in_dim(grads, index * block, block, 0)
        shift_block = lax.dynamic_slice_in_dim(correction, index * block, block, 0).transpose(
            1, 2, 0
        )
        log_block = lax.dynamic_slice_in_dim(log_rows, index * block, block, 2)

        def key_step(inner, carry):
            block_grad, key_sum, value_sum = carry
            key_block = lax.dynamic_slice_in_dim(keys, inner * block, block, 0)
            value_block = lax.dynamic_slice_in_dim(values, inner * block, block, 0)
            scores = (
                jnp.einsum(
                    "qhgd,shd->hgqs", query_block, key_block, preferred_element_type=jnp.float32
                )
                * scale
            )
            allowed = (index * block + offsets)[:, None] >= (inner * block + offsets)[None, :]
            weights = jnp.where(allowed, jnp.exp(scores - log_block[..., None]), 0.0)
            value_part = jnp.einsum(
                "hgqs,qhgd->shd",
                weights.astype(jnp.bfloat16),
                grad_block,
                preferred_element_type=jnp.float32,
            )
            prob_grad = jnp.einsum(
                "qhgd,shd->hgqs", grad_block, value_block, preferred_element_type=jnp.float32
            )
            score_grad = (weights * (prob_grad - shift_block[..., None]) * scale).astype(
                jnp.bfloat16
            )
            block_grad = block_grad + jnp.einsum(
                "hgqs,shd->qhgd", score_grad, key_block, preferred_element_type=jnp.float32
            )
            key_part = jnp.einsum(
                "hgqs,qhgd->shd", score_grad, query_block, preferred_element_type=jnp.float32
            )
            key_sum = lax.dynamic_update_slice_in_dim(
                key_sum,
                lax.dynamic_slice_in_dim(key_sum, inner * block, block, 0) + key_part,
                inner * block,
                0,
            )
            value_sum = lax.dynamic_update_slice_in_dim(
                value_sum,
                lax.dynamic_slice_in_dim(value_sum, inner * block, block, 0) + value_part,
                inner * block,
                0,
            )
            return (block_grad, key_sum, value_sum)

        initial = (jnp.zeros((block, key_heads, groups, width), jnp.float32), key_grad, value_grad)
        block_grad, key_grad, value_grad = lax.fori_loop(0, index + 1, key_step, initial)
        query_grad = lax.dynamic_update_slice_in_dim(query_grad, block_grad, index * block, 0)
        return (query_grad, key_grad, value_grad)

    state = (
        jnp.zeros((length, key_heads, groups, width), jnp.float32),
        jnp.zeros((length, key_heads, width), jnp.float32),
        jnp.zeros((length, key_heads, width), jnp.float32),
    )
    query_grad, key_grad, value_grad = lax.fori_loop(0, length // block, query_step, state)
    pair_grad = jnp.concatenate(
        [
            key_grad.reshape(length, key_heads * width),
            value_grad.reshape(length, key_heads * width),
        ],
        axis=1,
    )
    return (query_grad.reshape(length, key_heads * groups * width), pair_grad)


MESH = pl.DeviceIdType.MESH


def flip(index, mask, bits):
    for bit in bits:
        if mask & bit:
            index = index + bit - 2 * bit * ((index // bit) % 2)
    return index


class Place:
    def __init__(self, parts, planes):
        self.parts, self.planes = parts, planes
        self.seat = lax.axis_index("seq")
        self.plane = lax.axis_index("fsdp")
        self.core = self.seat % 2
        self.chip = self.seat // 2
        self.seat_bits = [1 << i for i in range(parts.bit_length() - 1)]
        self.chip_bits = self.seat_bits[1:]
        self.plane_bits = [1 << i for i in range(planes.bit_length() - 1)]

    def at(self, mask):
        return flip(self.seat, mask, self.seat_bits)

    def side(self, bit):
        return (self.seat // bit) % 2

    def colors(self):
        return (self.chip_bits, self.chip_bits[::-1])

    def enter(self, masks=(), line=False, plane_masks=()):
        barrier = pltpu.get_barrier_semaphore()
        peers = [{"seq": self.at(mask)} for mask in masks]
        if line:
            peers.append({"fsdp": (self.plane + 1) % self.planes})
            peers.append({"fsdp": (self.plane + self.planes - 1) % self.planes})
        for mask in plane_masks:
            peers.append({"fsdp": flip(self.plane, mask, self.plane_bits)})
        for peer in peers:
            pl.semaphore_signal(barrier, inc=1, device_id=peer, device_id_type=MESH)
        pl.semaphore_wait(barrier, len(peers))


class Wire:
    def __init__(self, sends, receives, locals_):
        self.sends, self.receives, self.locals = sends, receives, locals_
        self.count = self.local_count = 0
        self.open = []

    def remote(self, source, target, device):
        number = self.count
        self.count += 1
        return pltpu.make_async_remote_copy(
            src_ref=source,
            dst_ref=target,
            send_sem=self.sends.at[number],
            recv_sem=self.receives.at[number],
            device_id=device,
            device_id_type=MESH,
        )

    def send(self, source, target, device):
        copy = self.remote(source, target, device)
        copy.start()
        self.open.append(copy)
        return copy

    def quiet(self, source, target):
        number = self.local_count
        self.local_count += 1
        return pltpu.make_async_copy(source, target, self.locals.at[number])

    def local(self, source, target):
        copy = self.quiet(source, target)
        copy.start()
        return copy

    def sent(self, copy):
        copy.wait_send()
        self.open = [other for other in self.open if other is not copy]

    def close(self):
        for copy in self.open:
            copy.wait_send()


def add_rows(target, left, right, step=64):
    rows = target.shape[0]
    step = min(step, rows)

    def body(index, carry):
        at = pl.ds(pl.multiple_of(index * step, step), step)
        total = left[at, :].astype(jnp.float32) + right[at, :].astype(jnp.float32)
        target[at, :] = total.astype(target.dtype)
        return carry

    lax.fori_loop(0, rows // step, body, 0)


class LineGather:
    def __init__(self, wire, here, source, target, share=None):
        self.here = here
        planes, plane = here.planes, here.plane
        above = {"fsdp": (plane + 1) % planes}
        below = {"fsdp": (plane + planes - 1) % planes}
        self.ups, self.downs = {}, {}
        for step in range(1, planes):
            lower = (plane + planes - step + 1) % planes
            upper = (plane + step - 1) % planes
            first = step == 1
            self.ups[step] = wire.remote(
                source if first else target(lower), target(lower), above
            )
            self.downs[step] = wire.remote(
                source if first else target(upper), target(upper), below
            )
        self.shared = {}
        if share is not None:
            for step in range(1, planes):
                for way, shift in ((0, planes - step), (1, step)):
                    index = (plane + shift) % planes
                    self.shared[(step, way)] = wire.remote(
                        target(index), share(index), {"seq": here.at(1)}
                    )

    def start(self, step):
        planes, plane = self.here.planes, self.here.plane

        @pl.when((plane >= step - 1) & (plane <= planes - 2))
        def _():
            self.ups[step].start()

        @pl.when((plane + step <= planes) & (plane >= 1))
        def _():
            self.downs[step].start()

    def arrive(self, step):
        planes, plane = self.here.planes, self.here.plane

        @pl.when(plane >= step)
        def _():
            self.ups[step].wait_recv()
            if self.shared:
                self.shared[(step, 0)].start()

        @pl.when(plane + step <= planes - 1)
        def _():
            self.downs[step].wait_recv()
            if self.shared:
                self.shared[(step, 1)].start()

    def close(self, shared_taken=False):
        planes, plane = self.here.planes, self.here.plane
        for (step, way), copy in self.shared.items():

            @pl.when(plane >= step if way == 0 else plane + step <= planes - 1)
            def _(copy=copy):
                copy.wait_send()
                if not shared_taken:
                    copy.wait_recv()

        for step in range(1, planes):

            @pl.when((plane >= step - 1) & (plane <= planes - 2))
            def _(step=step):
                self.ups[step].wait_send()

            @pl.when((plane + step <= planes) & (plane >= 1))
            def _(step=step):
                self.downs[step].wait_send()


class Lines:
    def __init__(self, members):
        self.members = members

    def start(self, step):
        for member in self.members:
            member.start(step)

    def pass_on(self, step):
        for member in self.members:
            member.arrive(step)
            if step + 1 < member.here.planes:
                member.start(step + 1)

    def step(self, step):
        for member in self.members:
            member.step(step)

    def close(self, *options):
        for member in self.members:
            member.close(*options)


def gather_lines(wire, here, source, target, share=None, cuts=2):
    rows = source.shape[0] // cuts
    members = []
    for cut in range(cuts):
        at = pl.ds(cut * rows, rows)
        members.append(
            LineGather(
                wire,
                here,
                source.at[at],
                lambda index, at=at: target(index).at[at],
                None if share is None else lambda index, at=at: share(index).at[at],
            )
        )
    return Lines(members)


class LineScatter:
    def __init__(self, wire, here, term, landing):
        self.wire, self.here, self.term, self.landing = wire, here, term, landing
        planes, plane = here.planes, here.plane
        above = {"fsdp": (plane + 1) % planes}
        below = {"fsdp": (plane + planes - 1) % planes}
        self.ups, self.downs = {}, {}
        for step in range(1, planes):
            self.ups[step] = wire.remote(
                term((plane + planes - step) % planes), landing(0, step - 1), above
            )
            self.downs[step] = wire.remote(
                term((plane + step) % planes), landing(1, step - 1), below
            )

    def step(self, step):
        planes, plane = self.here.planes, self.here.plane
        mirror = planes - 1 - plane
        for way, (position, copies, dest) in enumerate(
            (
                (plane, self.ups, (plane + planes - step) % planes),
                (mirror, self.downs, (plane + step) % planes),
            )
        ):
            if step > 1:

                @pl.when((position >= 1) & (position <= step - 1))
                def _(way=way, copies=copies, dest=dest):
                    copies[step - 1].wait_recv()
                    term = self.term(dest)
                    add_rows(term, term, self.landing(way, step - 2))

            @pl.when(position <= step - 1)
            def _(copies=copies):
                copies[step].start()

    def finish(self, out):
        planes, plane = self.here.planes, self.here.plane
        own = self.term(plane)
        last = planes - 1

        @pl.when(plane >= 1)
        def _():
            self.ups[last].wait_recv()

        @pl.when(plane <= planes - 2)
        def _():
            self.downs[last].wait_recv()

        @pl.when(plane == 0)
        def _():
            add_rows(out, own, self.landing(1, last - 1))

        @pl.when(plane == planes - 1)
        def _():
            add_rows(out, own, self.landing(0, last - 1))

        @pl.when((plane >= 1) & (plane <= planes - 2))
        def _():
            add_rows(own, own, self.landing(0, last - 1))
            add_rows(out, own, self.landing(1, last - 1))

    def close(self):
        planes, plane = self.here.planes, self.here.plane
        mirror = planes - 1 - plane
        for step in range(1, planes):

            @pl.when(plane <= step - 1)
            def _(step=step):
                self.ups[step].wait_send()

            @pl.when(mirror <= step - 1)
            def _(step=step):
                self.downs[step].wait_send()


class PlaneGather:
    def __init__(self, wire, here, source, target):
        self.wire, self.here, self.source, self.target = wire, here, source, target
        self.incoming = {}

    def _send(self, mask, color, bit):
        here = self.here
        target = self.target(here.at(mask), color)
        source = self.source(color) if mask == 0 else target
        self.incoming[(mask ^ bit, color)] = self.wire.send(
            source, target, {"seq": here.at(bit)}
        )

    def start(self):
        for position in range(len(self.here.chip_bits)):
            for color, bits in enumerate(self.here.colors()):
                self._send(0, color, bits[position])
        for color in (0, 1):
            self._send(0, color, 1)

    def hop(self, hops):
        here = self.here
        chips = here.parts // 2
        for mask in (mask * 2 for mask in range(1, chips)):
            if bin(mask).count("1") != hops:
                continue
            for color, bits in enumerate(here.colors()):
                self.incoming[(mask, color)].wait_recv()
                last = max(i for i, bit in enumerate(bits) if mask & bit)
                for bit in bits[last + 1 :]:
                    self._send(mask, color, bit)
                self._send(mask, color, 1)

    def hops(self, first=1):
        for hops in range(first, len(self.here.chip_bits) + 1):
            self.hop(hops)

    def finish(self):
        for mask in range(1, self.here.parts, 2):
            for color in (0, 1):
                self.incoming[(mask, color)].wait_recv()


class PlaneScatter:
    def __init__(self, wire, here, product, give, take, current, landing, model):
        self.wire, self.here, self.product = wire, here, product
        self.give, self.take, self.current, self.landing = give, take, current, landing
        self.model = model

    def start(self):
        here = self.here
        chips = here.parts // 2
        self.swaps = {}
        tokens = self.give.shape[1]
        seats = [2 * flip(here.chip, mask, [b // 2 for b in here.chip_bits]) for mask in range(chips)]
        for part in range(self.model // 512):
            columns = slice(part * 512, (part + 1) * 512)
            rows = self.product([seat + 1 - here.core for seat in seats], columns)
            for mask in range(chips):
                self.give[mask, :, columns] = rows[mask * tokens : (mask + 1) * tokens].astype(
                    self.give.dtype
                )
        for mask in range(chips)[::-1]:
            self.swaps[mask] = self.wire.send(
                self.give.at[mask], self.take.at[mask], {"seq": here.at(1)}
            )
        half = self.model // 2
        for part in range(self.model // 512):
            columns = slice(part * 512, (part + 1) * 512)
            rows = self.product([seat + here.core for seat in seats], columns)
            color, inside = divmod(part * 512, half)
            for mask in range(chips):
                self.current[color, mask, :, inside : inside + 512] = rows[
                    mask * tokens : (mask + 1) * tokens
                ].astype(self.current.dtype)

    def join(self):
        half = self.model // 2
        chips = self.here.parts // 2
        for mask in range(chips)[::-1]:
            self.swaps[mask].wait_recv()
            for color in (0, 1):
                mine = self.current.at[color, mask]
                add_rows(mine, mine, self.take.at[mask, :, pl.ds(color * half, half)])

    def stage(self, position):
        here = self.here
        self.moved = getattr(self, "moved", {})
        for onward in (True, False):
            for color, bits in enumerate(here.colors()):
                bit = bits[position]
                done = sum(bits[:position])
                for mask in range(here.parts // 2):
                    low = mask ^ (bit // 2)
                    if not mask * 2 & bit or mask * 2 & done:
                        continue
                    if self._onward(position, color, low) != onward:
                        continue
                    self.moved[(position, color, low)] = self.wire.send(
                        self.current.at[color, mask],
                        self.landing.at[position, color, low],
                        {"seq": here.at(bit)},
                    )

    def _onward(self, position, color, low):
        bits = self.here.colors()[color]
        return position + 1 < len(bits) and bool(low * 2 & bits[position + 1])

    def settle(self, position, out, onward):
        half = self.model // 2
        last = position == len(self.here.chip_bits) - 1
        for (stage, color, low), copy in self.moved.items():
            if stage != position or self._onward(position, color, low) != onward:
                continue
            copy.wait_recv()
            mine = self.current.at[color, low]
            target = out.at[:, pl.ds(color * half, half)] if last else mine
            add_rows(target, mine, self.landing.at[position, color, low])


def pick_lanes(low, high, width):
    lane = lax.broadcasted_iota(jnp.int32, low.shape, low.ndim - 1)
    return jnp.where(lane % (2 * width) < width, low, high)


def group_mean(values, group, width):
    high = values.astype(jnp.bfloat16)
    low = (values - high.astype(jnp.float32)).astype(jnp.bfloat16)
    total = jnp.dot(high, group, preferred_element_type=jnp.float32) + jnp.dot(
        low, group, preferred_element_type=jnp.float32
    )
    return total * (1.0 / width)


def turn(values, width):
    lanes = values.shape[1]
    half = width // 2
    return pick_lanes(
        pltpu.roll(values, lanes - half, 1), pltpu.roll(values, half, 1), half
    )


def attend_block(index, block, width, heads, queries, pair, twin, left, right, out_rows, logs):
    rows = pl.ds(index * block, block)
    before = index * block
    columns = 2 * width
    row = lax.broadcasted_iota(jnp.int32, (block, block), 0)
    column = lax.broadcasted_iota(jnp.int32, (block, block), 1)
    allowed = row >= column
    contract = (((1,), (1,)), ((), ()))
    lane = lax.broadcasted_iota(jnp.int32, (block, 128), 1)

    def two_heads(number, table):
        at = pl.ds(pl.multiple_of(number * columns, columns), columns)
        both = queries[rows, at]
        both = (both.astype(jnp.float32) * width**-0.5).astype(both.dtype)
        zero = jnp.zeros_like(both)
        result = None
        for side, values in ((0, left), (1, right)):
            mine = pick_lanes(both, zero, width) if side == 0 else pick_lanes(zero, both, width)
            scores = lax.dot_general(
                mine, twin[rows, :], contract, preferred_element_type=jnp.float32
            )
            weights = jnp.where(allowed, jnp.exp(scores), 0.0)
            total = jnp.sum(weights, axis=1, keepdims=True)
            summed = jnp.dot(
                weights.astype(jnp.bfloat16), values[rows, :], preferred_element_type=jnp.float32
            )
            if before:
                scores = lax.dot_general(
                    mine, twin[0:before, :], contract, preferred_element_type=jnp.float32
                )
                weights = jnp.exp(scores)
                total = total + jnp.sum(weights, axis=1, keepdims=True)
                summed = summed + jnp.dot(
                    weights.astype(jnp.bfloat16),
                    values[0:before, :],
                    preferred_element_type=jnp.float32,
                )
            table = jnp.where(lane == 2 * number + side, total, table)
            part = summed / total
            result = part if result is None else result + part
        out_rows[rows, at] = result.astype(out_rows.dtype)
        return table

    table = lax.fori_loop(0, heads // 2, two_heads, jnp.ones((block, 128), jnp.float32))
    logs[rows, :] = jnp.log(table)


def back_block(
    index, block, width, heads, queries, grads, outs, logs, keys, values, query_back, key_back, value_back
):
    rows = pl.ds(index * block, block)
    before = index * block
    scale = width**-0.5
    row = lax.broadcasted_iota(jnp.int32, (block, block), 0)
    column = lax.broadcasted_iota(jnp.int32, (block, block), 1)
    allowed = row >= column
    lane = lax.broadcasted_iota(jnp.int32, (block, 2 * width), 1)
    across = (((1,), (1,)), ((), ()))
    down = (((0,), (0,)), ((), ()))
    f32 = jnp.float32
    spans = [(rows, True)] + ([(slice(0, before), False)] if before else [])

    def one_head(head, carry):
        number, side = head // 2, head % 2
        at = pl.ds(pl.multiple_of(number * 2 * width, 2 * width), 2 * width)
        mine = lane // width == side
        query = jnp.where(mine, queries[rows, at], 0)
        grad = jnp.where(mine, grads[rows, at], 0)
        scaled = (query.astype(f32) * scale).astype(query.dtype)
        shift = jnp.sum(grad.astype(f32) * outs[rows, at].astype(f32), axis=1, keepdims=True)
        log = jnp.sum(jnp.where(lane == head, logs[rows, :], 0.0), axis=1, keepdims=True)
        total = query_back[rows, at]
        for span, masked in spans:
            scores = lax.dot_general(
                scaled, keys[0, span, :], across, preferred_element_type=f32
            )
            weights = jnp.exp(scores - log)
            if masked:
                weights = jnp.where(allowed, weights, 0.0)
            prob_grad = lax.dot_general(
                grad, values[span, :], across, preferred_element_type=f32
            )
            score_grad = (weights * (prob_grad - shift) * scale).astype(query.dtype)
            total = total + jnp.dot(
                score_grad, keys[1 + side, span, :], preferred_element_type=f32
            )
            key_back[span, :] += lax.dot_general(
                score_grad, query, down, preferred_element_type=f32
            )
            value_back[span, :] += lax.dot_general(
                weights.astype(query.dtype), grad, down, preferred_element_type=f32
            )
        query_back[rows, at] = total
        return carry

    lax.fori_loop(0, heads, one_head, 0)


def back_kernel(
    width,
    normed,
    middle,
    out_slice,
    outs,
    logs,
    queries,
    pair,
    proj,
    gain,
    cosine,
    sine,
    group,
    halves,
    head_part,
    out_part,
    slopes,
    grads,
    query_back,
    key_back,
    value_back,
    keys,
    values,
):
    length = normed.shape[0]
    block = min(256, length)
    blocks = length // block
    query_cols = queries.shape[1]
    heads = query_cols // width
    f32 = jnp.float32
    query_back[...] = jnp.zeros_like(query_back)
    key_back[...] = jnp.zeros_like(key_back)
    value_back[...] = jnp.zeros_like(value_back)

    def ready(index, carry):
        at = pl.ds(pl.multiple_of(index * block, block), block)
        grads[at, :] = lax.dot_general(
            middle[at, :], out_slice[...], (((1,), (1,)), ((), ())), preferred_element_type=f32
        ).astype(grads.dtype)
        both = pair[at, :].astype(f32)
        swapped = pltpu.roll(both, width, 1)
        zero = jnp.zeros_like(both)
        keys[0, at, :] = pick_lanes(both, swapped, width).astype(keys.dtype)
        keys[1, at, :] = pick_lanes(both, zero, width).astype(keys.dtype)
        keys[2, at, :] = pick_lanes(zero, swapped, width).astype(keys.dtype)
        values[at, :] = pick_lanes(swapped, both, width).astype(values.dtype)
        return carry

    lax.fori_loop(0, blocks, ready, 0)
    for index in range(blocks):
        back_block(
            index,
            block,
            width,
            heads,
            queries,
            grads,
            outs,
            logs,
            keys,
            values,
            query_back,
            key_back,
            value_back,
        )

    def norms(index, slope):
        at = pl.ds(pl.multiple_of(index * block, block), block)
        key_sum, value_sum = key_back[at, :], value_back[at, :]
        key_sum = key_sum + pltpu.roll(key_sum, width, 1)
        value_sum = value_sum + pltpu.roll(value_sum, width, 1)
        back = jnp.concatenate(
            [query_back[at, :], pick_lanes(key_sum, value_sum, width)], axis=1
        )
        value = proj[at, :]
        factor = lax.rsqrt(group_mean(value * value, group[...], width) + EPS)
        repeat = value.shape[1] // cosine.shape[1]
        cosines = jnp.concatenate([cosine[at, :]] * repeat, axis=1)
        sines = jnp.concatenate([sine[at, :]] * repeat, axis=1)
        turned = back * cosines + turn(back * sines, width)
        slope = slope + jnp.sum(turned * value * factor, axis=0, keepdims=True)
        scaled = turned * gain[...]
        result = factor * (
            scaled - value * factor * factor * group_mean(scaled * value, group[...], width)
        )
        lane = lax.broadcasted_iota(jnp.int32, back.shape, 1)
        result = jnp.where(lane >= query_cols + width, back, result)
        halves[at, :] = result.astype(halves.dtype)
        return slope

    slope = lax.fori_loop(0, blocks, norms, jnp.zeros((1, proj.shape[1]), f32))
    slopes[...] = jnp.broadcast_to(slope, slopes.shape)

    def terms(number, carry):
        at = pl.ds(pl.multiple_of(number * 256, 256), 256)
        down = (((0,), (0,)), ((), ()))
        head_part[at, :] = lax.dot_general(
            normed[:, at], halves[...], down, preferred_element_type=f32
        ).astype(head_part.dtype)
        out_part[:, at] = lax.dot_general(
            outs[...], middle[:, at], down, preferred_element_type=f32
        ).astype(out_part.dtype)
        return carry

    lax.fori_loop(0, normed.shape[1] // 256, terms, 0)


def row_blocks(rows, step, work):
    def body(index, carry):
        work(pl.ds(pl.multiple_of(index * step, step), step))
        return carry

    lax.fori_loop(0, rows // step, body, 0)


def front_kernel(
    width,
    copies,
    parts,
    planes,
    x,
    c,
    query_weight,
    key_weight,
    value_weight,
    output_weight,
    in_gain,
    mid_gain,
    gain,
    rates,
    x_store,
    w_store,
    o_store,
    proj_store,
    query_store,
    pair_store,
    out_store,
    log_store,
    cosine_store,
    sine_store,
    group_store,
    middle,
    mid,
    c_store,
    x_all,
    w_all,
    o_slice,
    proj,
    queries,
    pair,
    out_rows,
    logs,
    cosine,
    sine,
    group,
    c_all,
    o_all,
    twin,
    left,
    right,
    key_block,
    value_block,
    give,
    take,
    current,
    landing,
    *sems,
):
    here = Place(parts, planes)
    wire = Wire(*sems)
    tokens, model = x.shape
    shard = query_weight.shape[0]
    query_cols = queries.shape[1]
    rows = o_all.shape[1]
    half = tokens // 2
    chips = parts // 2
    f32 = jnp.float32
    chip_masks = [mask * 2 for mask in range(1, chips)]
    pair_head = here.seat // copies
    own_shard = pl.ds(pl.multiple_of(here.plane * shard, shard), shard)
    head_block = pl.ds(pl.multiple_of(pair_head // 2 * 2 * width, 2 * width), 2 * width)
    loads = [
        wire.local(key_weight.at[:, head_block], key_block),
        wire.local(value_weight.at[:, head_block], value_block),
        wire.local(
            query_weight.at[:, pl.ds(pl.multiple_of(here.seat * query_cols, query_cols), query_cols)],
            w_all.at[own_shard, pl.ds(0, query_cols)],
        ),
    ]
    piece = (here.core * chips + here.chip) * rows
    o = output_weight.at[pl.ds(pl.multiple_of(piece, rows), rows)]
    here.enter(chip_masks + [1], line=True)
    o_own = wire.local(o, o_all.at[here.plane])
    for load in loads[:2]:
        load.wait()
    upper = (pair_head % 2) * jnp.ones((1, 1), jnp.int32)
    keys, values = key_block[...].astype(f32), value_block[...].astype(f32)
    keys = jnp.where(upper == 1, pltpu.roll(keys, width, 1), keys)
    values = jnp.where(upper == 1, values, pltpu.roll(values, width, 1))
    w_all[own_shard, query_cols:] = pick_lanes(keys, values, width).astype(w_all.dtype)
    loads[2].wait()
    weights = gather_lines(
        wire,
        here,
        w_all.at[own_shard],
        lambda index: w_all.at[pl.ds(pl.multiple_of(index * shard, shard), shard)],
    )
    weights.start(1)

    def norm_rows(at):
        value = x[at, :].astype(f32)
        factor = lax.rsqrt(jnp.mean(value * value, axis=-1, keepdims=True) + EPS)
        own_at = pl.ds(pl.multiple_of(here.seat * tokens + at.start, 32), 32)
        x_all[own_at, :] = (value * factor * in_gain[...]).astype(x_all.dtype)

    row_blocks(tokens, 32, norm_rows)

    def seat_rows(seat, color):
        return x_all.at[pl.ds(pl.multiple_of(seat * tokens + color * half, half), half)]

    plane_rows = PlaneGather(
        wire, here, lambda color: seat_rows(here.seat, color), seat_rows
    )
    plane_rows.start()
    outer = gather_lines(wire, here, o, lambda index: o_all.at[index])

    def c_spot(index):
        return c_all.at[index, here.core]

    cots = gather_lines(wire, here, c, c_spot, c_spot)
    c_own = wire.local(c, c_spot(here.plane))

    lane = lax.broadcasted_iota(jnp.int32, (32, 2 * width), 1)
    row = lax.broadcasted_iota(jnp.int32, (32, 2 * width), 0)
    sign = jnp.where(lane % width < width // 2, -1.0, 1.0)

    def table_rows(at):
        angle = (row + at.start).astype(f32) * rates[...]
        cosine[at, :] = jnp.cos(angle)
        sine[at, :] = jnp.sin(angle) * sign

    columns = group.shape[0]
    group[...] = jnp.where(
        lax.broadcasted_iota(jnp.int32, (columns, columns), 0) // width
        == lax.broadcasted_iota(jnp.int32, (columns, columns), 1) // width,
        1.0,
        0.0,
    ).astype(group.dtype)
    length = x_all.shape[0]
    row_blocks(length, 32, table_rows)
    weights.members[0].arrive(1)
    if planes > 2:
        weights.members[0].start(2)
    plane_rows.hop(1)
    weights.members[1].arrive(1)
    if planes > 2:
        weights.members[1].start(2)
    outer.start(1)
    plane_rows.hops(2)
    spot = o_slice.at[pl.ds(pl.multiple_of(here.chip * rows, rows), rows)]
    deals = []
    for mask in chip_masks:
        chip = here.at(mask) // 2
        deals.append((chip, wire.remote(o_all.at[chip], spot, {"seq": here.at(mask)})))
    keep_own = wire.quiet(o_all.at[here.chip], spot)

    def deal(step):
        for chip, copy in deals + [(here.chip, keep_own)]:

            @pl.when((chip == here.plane + step) | (chip + step == here.plane))
            def _(copy=copy):
                copy.start()

    o_own.wait()
    deal(0)
    plane_rows.finish()
    block = min(256, length)
    blocks = length // block

    for step in range(2, planes):
        weights.pass_on(step)
    stores = [
        wire.local(x_all, x_store),
        wire.local(w_all, w_store),
        wire.local(cosine, cosine_store),
        wire.local(sine, sine_store),
        wire.local(group, group_store),
    ]
    heads = query_cols // width

    def project(index, carry):
        at = pl.ds(pl.multiple_of(index * block, block), block)
        value = jnp.dot(x_all[at, :], w_all[...], preferred_element_type=f32)
        proj[at, :] = value
        factor = lax.rsqrt(group_mean(value * value, group[...], width) + EPS)
        normed = value * factor * gain[...]
        repeat = value.shape[1] // cosine.shape[1]
        cosines = jnp.concatenate([cosine[at, :]] * repeat, axis=1)
        sines = jnp.concatenate([sine[at, :]] * repeat, axis=1)
        turned = normed * cosines + turn(normed, width) * sines
        queries[at, :] = turned[:, :query_cols].astype(queries.dtype)
        keys, values = turned[:, query_cols:], value[:, query_cols:]
        both = pick_lanes(keys, values, width)
        pair[at, :] = both.astype(pair.dtype)
        swapped = pltpu.roll(both, width, 1)
        twin[at, :] = pick_lanes(both, swapped, width).astype(twin.dtype)
        zero = jnp.zeros_like(both)
        left[at, :] = pick_lanes(swapped, zero, width).astype(left.dtype)
        right[at, :] = pick_lanes(zero, both, width).astype(right.dtype)
        return carry

    lax.fori_loop(0, blocks, project, 0)
    across = wire.send(c, c_spot(here.plane), {"seq": here.at(1)})
    waits = list(range(1, planes))
    cot_waits = list(range(1, planes))
    for index in range(blocks):
        while waits and waits[0] * blocks <= (index + 1) * planes:
            step = waits.pop(0)
            outer.pass_on(step)
            deal(step)
            if step == min(2, planes - 1):
                cots.start(1)
        attend_block(
            index, block, width, heads, queries, pair, twin, left, right, out_rows, logs
        )
    for step in waits:
        outer.pass_on(step)
        deal(step)
    cots.pass_on(cot_waits.pop(0))
    keep_own.wait()
    for _, copy in deals:
        copy.wait()

    def product(seats, at):
        chosen = [
            out_rows[pl.ds(pl.multiple_of(seat * tokens, tokens), tokens), :] for seat in seats
        ]
        return jnp.dot(
            jnp.concatenate(chosen, axis=0), o_slice[:, at], preferred_element_type=f32
        )

    stores += [
        wire.local(o_slice, o_store),
        wire.local(proj, proj_store),
        wire.local(queries, query_store),
        wire.local(pair, pair_store),
        wire.local(out_rows, out_store),
        wire.local(logs, log_store),
    ]
    sums = PlaneScatter(wire, here, product, give, take, current, landing, model)
    sums.start()
    sums.join()
    sums.stage(0)
    stages = len(here.chip_bits)
    for stage in range(stages):
        sums.settle(stage, middle, True)
        if stage + 1 < stages:
            sums.stage(stage + 1)
        if cot_waits:
            cots.pass_on(cot_waits.pop(0))
        sums.settle(stage, middle, False)

    def mid_rows(at):
        value = x[at, :].astype(f32) + middle[at, :]
        middle[at, :] = value
        factor = lax.rsqrt(jnp.mean(value * value, axis=-1, keepdims=True) + EPS)
        mid[at, :] = (value * factor * mid_gain[...]).astype(mid.dtype)

    for step in cot_waits:
        cots.pass_on(step)
    cots.close()
    c_own.wait()
    across.wait_recv()
    stores.append(wire.local(c_all, c_store))
    row_blocks(tokens, 32, mid_rows)
    for copy in stores:
        copy.wait()
    wire.close()
    weights.close()
    outer.close()


def feed_kernel(
    parts,
    planes,
    m,
    mid_gain,
    cots_whole,
    middle_whole,
    gate_weight,
    up_weight,
    down_weight,
    mid_half,
    mid_slope,
    mid_store,
    s_down,
    s_early_a,
    s_early_b,
    s_late_a,
    s_late_b,
    down_give,
    down_keep,
    gate_half,
    up_half,
    down_half,
    cots,
    middle,
    mid,
    mids,
    hidden,
    unit_grads,
    away,
    sums,
    *rest,
):
    here = Place(parts, planes)
    stages = len(here.chip_bits) - 1
    landings, rest = rest[:stages], rest[stages:]
    give, take, current, line_landing, *sems = rest
    wire = Wire(*sems)
    tokens, model = m.shape
    units = gate_half.shape[1]
    own_units = pl.ds(pl.multiple_of(here.core * units, units), units)
    here.enter(here.seat_bits, line=True)

    def spot(index):
        return mids.at[index, here.core]

    lines = gather_lines(wire, here, m, spot, spot)
    lines.start(1)
    across = wire.send(m, spot(here.plane), {"seq": here.at(1)})
    own = wire.local(m, spot(here.plane))
    loads = [
        wire.local(whole.at[:, own_units], part)
        for whole, part in (
            (gate_weight, gate_half),
            (up_weight, up_half),
            (down_weight, down_half),
        )
    ]
    loads += [wire.local(cots_whole, cots), wire.local(middle_whole, middle)]

    def block(index):
        rows = pl.ds(pl.multiple_of(index * 2 * tokens, 2 * tokens), 2 * tokens)
        mid_rows = mids[index].reshape(2 * tokens, model)
        cot_rows = cots[rows, :]

        def part(number, carry):
            at = pl.ds(pl.multiple_of(number * 256, 256), 256)
            gate = jnp.dot(mid_rows, gate_half[:, at], preferred_element_type=jnp.float32)
            lifted = jnp.dot(mid_rows, up_half[:, at], preferred_element_type=jnp.float32)
            hidden_grad = jnp.dot(cot_rows, down_half[:, at], preferred_element_type=jnp.float32)
            sigma = 1.0 / (1.0 + jnp.exp(-gate))
            active = gate * sigma
            hidden[rows, at] = (active * lifted).astype(hidden.dtype)
            unit_grads[1, rows, at] = (hidden_grad * active).astype(hidden.dtype)
            unit_grads[0, rows, at] = (
                hidden_grad * lifted * sigma * (1.0 + gate * (1.0 - sigma))
            ).astype(hidden.dtype)
            return carry

        lax.fori_loop(0, units // 256, part, 0)

    for load in loads:
        load.wait()
    own.wait()
    across.wait_recv()
    plane = here.plane

    def arrivals(step, carry):
        for number in range(1, planes):

            @pl.when(step == number)
            def _(number=number):
                lines.pass_on(number)

        own_turn = step == 0
        ups = jnp.where(own_turn | (plane >= step), 1, 0)
        downs = jnp.where(jnp.logical_not(own_turn) & (plane + step <= planes - 1), 1, 0)

        def arrived(number, carry):
            from_up = (number == 0) & (ups == 1)
            for stage in range(1, planes):
                for way, chosen in ((0, from_up), (1, jnp.logical_not(from_up))):

                    @pl.when((step == stage) & chosen)
                    def _(stage=stage, way=way):
                        for line in lines.members:
                            line.shared[(stage, way)].wait_recv()

            block(jnp.where(from_up, plane + planes - step, plane + step) % planes)
            return carry

        lax.fori_loop(0, ups + downs, arrived, 0)
        return carry

    lax.fori_loop(0, planes, arrivals, 0)

    flat_mids = mids.reshape(2 * planes * tokens, model)
    quarter = model // 4
    moved = {}

    def gradients(left, right, target, start, count):
        parts_of = quarter // 256

        def part(number, carry):
            k, inside = number // parts_of, number % parts_of * 256
            at = pl.ds(pl.multiple_of(start(k) + inside, 256), 256)
            target(k)[pl.ds(pl.multiple_of(inside, 256), 256), :] = lax.dot_general(
                left[:, at],
                right(k)[...],
                (((0,), (0,)), ((), ())),
                preferred_element_type=jnp.float32,
            ).astype(away.dtype)
            return carry

        lax.fori_loop(0, count * parts_of, part, 0)

    def first_half(color, mine):
        sides = [here.side(bits[0]) if mine else 1 - here.side(bits[0]) for bits in here.colors()]
        if isinstance(color, int):
            side = sides[color]
        else:
            side = sides[0] * (1 - color) + sides[1] * color
        return pl.multiple_of(color * (model // 2) + side * quarter, quarter)

    def send_away(number):
        for color, bits in enumerate(here.colors()):
            moved[(number, color)] = wire.send(
                away.at[number, color], landings[0].at[number, color], {"seq": here.at(bits[0])}
            )

    def mid_term(target, core):
        rows = [pl.ds(pl.multiple_of((2 * p + core) * tokens, tokens), tokens) for p in range(planes)]
        gates = jnp.concatenate([unit_grads[0, at, :] for at in rows], axis=0)
        lifts = jnp.concatenate([unit_grads[1, at, :] for at in rows], axis=0)

        def part(number, carry):
            at = pl.ds(pl.multiple_of(number * 256, 256), 256)
            term = lax.dot_general(
                gates, gate_half[at, :], (((1,), (1,)), ((), ())), preferred_element_type=jnp.float32
            ) + lax.dot_general(
                lifts, up_half[at, :], (((1,), (1,)), ((), ())), preferred_element_type=jnp.float32
            )
            target[:, :, at] = term.reshape(planes, tokens, 256).astype(target.dtype)
            return carry

        lax.fori_loop(0, model // 256, part, 0)

    def down_term(target, core):
        rows = [pl.ds(pl.multiple_of((2 * p + core) * tokens, tokens), tokens) for p in range(planes)]
        hiddens = jnp.concatenate([hidden[at, :] for at in rows], axis=0)

        def part(number, carry):
            at = pl.ds(pl.multiple_of(number * 256, 256), 256)
            term = lax.dot_general(
                hiddens, down_half[at, :], (((1,), (1,)), ((), ())), preferred_element_type=jnp.float32
            )
            target[:, :, at] = term.reshape(planes, tokens, 256).astype(target.dtype)
            return carry

        lax.fori_loop(0, model // 256, part, 0)

    gradients(
        cots,
        lambda k: hidden,
        lambda k: away.at[0, k],
        lambda k: first_half(k, False),
        2,
    )
    send_away(0)
    swaps = TokenSum(wire, here, current, take, line_landing)
    mid_term(give, 1 - here.core)
    swaps.start(give)
    mid_term(current, here.core)
    swaps.join()
    swaps.step(1)
    gradients(
        flat_mids,
        lambda k: unit_grads.at[k // 2],
        lambda k: away.at[1 + k // 2, k % 2],
        lambda k: first_half(k % 2, False),
        4,
    )
    send_away(1)
    send_away(2)
    for step in range(2, planes):
        swaps.step(step)

    early = s_early_a.shape[0]

    def store(number, color):
        done = sums.at[number, color]
        if number == 0:
            return [wire.local(done, s_down.at[color])]
        late = (s_late_a, s_late_b)[color]
        size = done.shape[0]
        if number == 1:
            return [
                wire.local(done.at[pl.ds(0, early)], (s_early_a, s_early_b)[color]),
                wire.local(done.at[pl.ds(early, size - early)], late.at[pl.ds(0, size - early)]),
            ]
        return [wire.local(done, late.at[pl.ds(size - early, size)])]

    wire.sent(swaps.across)
    down_term(give, 1 - here.core)
    down_term(take, here.core)
    handed = [wire.local(give, down_give), wire.local(take, down_keep)]
    rows = quarter
    keeps = {}
    if stages > 1:
        for copy in moved.values():
            wire.sent(copy)
    keep_in = sums if stages == 1 else away
    gradients(
        cots,
        lambda k: hidden,
        lambda k: keep_in.at[0, k],
        lambda k: first_half(k, True),
        2,
    )
    gradients(
        flat_mids,
        lambda k: unit_grads.at[k // 2],
        lambda k: keep_in.at[1 + k // 2, k % 2],
        lambda k: first_half(k % 2, True),
        4,
    )
    for number in range(3):
        for color in (0, 1):
            keeps[(number, color)] = (keep_in.at[number, color], 0)
    swaps.finish(mid)
    f32 = jnp.float32

    def norm_back_rows(index, slope):
        at = pl.ds(pl.multiple_of(index * 32, 32), 32)
        own_cots = (here.plane * 2 + here.core) * tokens + index * 32
        grad, value = mid[at, :], middle[at, :]
        factor = lax.rsqrt(jnp.mean(value * value, axis=-1, keepdims=True) + EPS)
        scaled = grad * mid_gain[...]
        back = factor * (
            scaled
            - value * factor * factor * jnp.mean(scaled * value, axis=-1, keepdims=True)
        )
        result = cots[pl.ds(pl.multiple_of(own_cots, 32), 32), :].astype(f32) + back
        mid[at, :] = result
        mid_half[at, :] = result.astype(mid_half.dtype)
        return slope + jnp.sum(grad * value * factor, axis=0, keepdims=True)

    mid_slope[...] = lax.fori_loop(
        0, tokens // 32, norm_back_rows, jnp.zeros((1, model), f32)
    )
    handed.append(wire.local(mid, mid_store))
    for stage in range(stages):
        last = stage == stages - 1
        for number in range(3):
            for color, bits in enumerate(here.colors()):
                keep, begin = keeps[(number, color)]
                moved[(number, color)].wait_recv()
                mine = keep.at[pl.ds(begin, rows)]
                if last:
                    add_rows(
                        sums.at[number, color], mine, landings[stage].at[number, color]
                    )
                    handed.extend(store(number, color))
                else:
                    add_rows(mine, mine, landings[stage].at[number, color])
                    bit = bits[stage + 1]
                    half = rows // 2
                    gone = pl.multiple_of(begin + (1 - here.side(bit)) * half, half)
                    moved[(number, color)] = wire.send(
                        keep.at[pl.ds(gone, half)],
                        landings[stage + 1].at[number, color],
                        {"seq": here.at(bit)},
                    )
                    keeps[(number, color)] = (
                        keep,
                        pl.multiple_of(begin + here.side(bit) * half, half),
                    )
        rows //= 2
    for copy in handed:
        copy.wait()
    wire.close()
    lines.close(True)
    swaps.close()


class TokenSum:
    def __init__(self, wire, here, current, take, landing):
        self.wire, self.here = wire, here
        self.current, self.take = current, take
        self.cuts = 2
        rows = current.shape[1] // self.cuts
        self.lines = []
        for cut in range(self.cuts):
            at = pl.ds(cut * rows, rows)
            self.lines.append(
                LineScatter(
                    wire,
                    here,
                    lambda index, at=at: current.at[index, at],
                    lambda way, step, at=at: landing.at[way, step, at],
                )
            )

    def start(self, give):
        self.across = self.wire.send(give, self.take, {"seq": self.here.at(1)})

    def join(self):
        self.across.wait_recv()

        def body(index, carry):
            row = self.current.at[index]
            add_rows(row, row, self.take.at[index])
            return carry

        lax.fori_loop(0, self.here.planes, body, 0)

    def step(self, step):
        for line in self.lines:
            line.step(step)

    def finish(self, out):
        rows = out.shape[0] // self.cuts
        for cut, line in enumerate(self.lines):
            line.finish(out.at[pl.ds(cut * rows, rows)])

    def close(self):
        for line in self.lines:
            line.close()


def spread_kernel(
    parts,
    planes,
    h,
    s,
    early_a,
    early_b,
    give,
    keep,
    h_store,
    t,
    came_a,
    came_b,
    block,
    h_all,
    current,
    take,
    line_landing,
    *sems,
):
    here = Place(parts, planes)
    wire = Wire(*sems)
    here.enter(here.seat_bits, line=True)
    tokens = h.shape[0]
    half = tokens // 2
    rows = PlaneGather(
        wire,
        here,
        lambda color: h.at[pl.ds(color * half, half)],
        lambda seat, color: h_all.at[pl.ds(pl.multiple_of(seat * tokens + color * half, half), half)],
    )
    swaps = TokenSum(wire, here, current, take, line_landing)
    swaps.start(give)
    kept = wire.local(keep, current)
    rows.start()
    own = wire.local(h, h_all.at[pl.ds(pl.multiple_of(here.seat * tokens, tokens), tokens)])
    kept.wait()
    swaps.join()
    swaps.step(1)
    rows.hop(1)
    moved = [
        wire.send(s.at[color], t.at[color], {"seq": here.at(bits[-1])})
        for color, bits in enumerate(here.colors())
    ]
    moved += [
        wire.send(source, target, {"seq": here.at(bits[-1])})
        for source, target, bits in zip((early_a, early_b), (came_a, came_b), here.colors())
    ]
    for step in range(2, planes):
        if step == 3:
            rows.hops(2)
        swaps.step(step)
    if planes <= 3:
        rows.hops(2)
    rows.finish()
    own.wait()
    store = wire.local(h_all, h_store)
    for color in (0, 1):
        moved[color].wait_recv()
        add_rows(t.at[color], t.at[color], s.at[color])
    swaps.finish(block)
    for copy in moved[2:]:
        copy.wait_recv()
    store.wait()
    wire.close()
    swaps.close()


def final_kernel(
    parts,
    planes,
    a,
    w,
    head_part,
    out_part,
    t_down,
    source,
    slope,
    *rest,
):
    sent, came, rest = rest[:4], rest[4:8], rest[8:]
    out, near, far, query_all, pair_all, outer_all, slope_out, *rest = rest
    joined, rest = rest[:4], rest[4:]
    (
        give,
        take,
        current,
        landing,
        head_current,
        head_landing,
        dealt,
        out_landing,
        head_sum,
        out_sum,
        left,
        right,
        slope_sums,
        slope_landing,
        *sems,
    ) = rest
    here = Place(parts, planes)
    wire = Wire(*sems)
    tokens, model = out.shape
    shard = head_sum.shape[0]
    columns = query_all.shape[1] // parts
    rows_out = out_sum.shape[0]
    chips = parts // 2
    chip_masks = [mask * 2 for mask in range(1, chips)]
    here.enter(chip_masks + [1], line=True, plane_masks=here.plane_bits)
    weights = [
        WeightGather(wire, here, (t_down.at[0], t_down.at[1]), near, far, cut, 2)
        for cut in range(2)
    ]
    head_own = wire.local(head_part, head_current)
    deals = []
    for mask in chip_masks:
        chip = here.at(mask) // 2
        deals.append(
            wire.send(
                out_part.at[pl.ds(pl.multiple_of(chip * rows_out, rows_out), rows_out)],
                dealt.at[here.chip],
                {"seq": here.at(mask)},
            )
        )
    deal_own = wire.local(
        out_part.at[pl.ds(pl.multiple_of(here.chip * rows_out, rows_out), rows_out)],
        dealt.at[here.chip],
    )

    def product(seats, columns):
        rows = [a[pl.ds(pl.multiple_of(seat * tokens, tokens), tokens), :] for seat in seats]
        return lax.dot_general(
            jnp.concatenate(rows, axis=0),
            w[columns, :],
            (((1,), (1,)), ((), ())),
            preferred_element_type=jnp.float32,
        )

    heads = LineScatter(
        wire, here, lambda index: head_current.at[index], lambda way, step: head_landing.at[way, step]
    )
    outer = LineScatter(
        wire, here, lambda index: dealt.at[index], lambda way, step: out_landing.at[way, step]
    )
    head_own.wait()
    heads.step(1)
    rows = PlaneScatter(wire, here, product, give, take, current, landing, model)
    rows.start()
    loads = []
    size, early = left.shape[1], sent[0].shape[0]
    for number in range(4):
        color = number % 2
        copies = []
        for pieces, working in ((sent, left), (came, right)):
            first, late = pieces[color], pieces[2 + color]
            if number < 2:
                copies.append(wire.local(first, working.at[number, pl.ds(0, early)]))
                copies.append(
                    wire.local(
                        late.at[pl.ds(0, size - early)],
                        working.at[number, pl.ds(early, size - early)],
                    )
                )
            else:
                copies.append(wire.local(late.at[pl.ds(size - early, size)], working.at[number]))
        loads.append(copies)
    heads.step(2)
    rows.join()
    rows.stage(0)
    weights[0].start()
    weights[0].own()
    deal_own.wait()
    for copy in deals:
        copy.wait_recv()
    outer.step(1)

    stores = []

    def join(number):
        for load in loads[number]:
            load.wait()
        add_rows(left.at[number], left.at[number], right.at[number])
        stores.append(wire.local(left.at[number], joined[number]))

    stages = len(here.chip_bits)
    for step in range(3, planes):
        heads.step(step)
    for stage in range(1, stages):
        rows.settle(stage - 1, out, True)
        rows.stage(stage)
        rows.settle(stage - 1, out, False)
        if stage + 1 < planes:
            outer.step(stage + 1)
        if stage == 1:
            heads.finish(head_sum)
    half, half_out = shard // 2, rows_out // 2

    def seat_columns(seat):
        return pl.ds(pl.multiple_of(seat * columns, columns), columns)

    gathers = [
        PlaneGather(
            wire,
            here,
            lambda color: head_sum.at[pl.ds(color * half, half), pl.ds(0, columns)],
            lambda seat, color: query_all.at[pl.ds(color * half, half), seat_columns(seat)],
        ),
        PlaneGather(
            wire,
            here,
            lambda color: head_sum.at[
                pl.ds(color * half, half), pl.ds(columns, pair_all.shape[2])
            ],
            lambda seat, color: pair_all.at[seat, pl.ds(color * half, half)],
        ),
        PlaneGather(
            wire,
            here,
            lambda color: out_sum.at[pl.ds(color * half_out, half_out)],
            lambda seat, color: outer_all.at[
                pl.ds(
                    pl.multiple_of(
                        ((seat % 2) * chips + seat // 2) * rows_out + color * half_out, half_out
                    ),
                    half_out,
                )
            ],
        ),
    ]
    own = []
    for gather in gathers[:2]:
        gather.start()
    own.append(
        wire.local(head_sum.at[:, pl.ds(0, columns)], query_all.at[:, seat_columns(here.seat)])
    )
    own.append(
        wire.local(
            head_sum.at[:, pl.ds(columns, pair_all.shape[2])], pair_all.at[here.seat]
        )
    )

    weights[1].start()
    weights[1].own()
    rows.settle(stages - 1, out, False)
    slope_sums[0] = slope[...]
    value = source[...].astype(jnp.float32)
    factor = lax.rsqrt(jnp.mean(value * value, axis=-1, keepdims=True) + EPS)
    slope_sums[0, 0:1, :] = jnp.sum(out[...] * value * factor, axis=0, keepdims=True)
    bits = [("seq", bit) for bit in here.seat_bits] + [("fsdp", bit) for bit in here.plane_bits]
    slope_copies = []

    def slope_send(number):
        axis, bit = bits[number]
        index = here.at(bit) if axis == "seq" else flip(here.plane, bit, here.plane_bits)
        slope_copies.append(
            wire.send(slope_sums.at[number], slope_landing.at[number], {axis: index})
        )

    def slope_add(number):
        slope_copies[number].wait_recv()
        target = slope_out if number == len(bits) - 1 else slope_sums.at[number + 1]
        target[...] = slope_sums[number] + slope_landing[number]

    slope_send(0)
    for step in range(stages + 1, planes):
        outer.step(step)
    join(0)
    gathers[0].hop(1)
    gathers[1].hop(1)
    slope_add(0)
    slope_send(1)
    outer.finish(out_sum)
    gathers[2].start()
    weights[0].forward()
    own_start = (here.core * chips + here.chip) * rows_out
    own.append(
        wire.local(out_sum, outer_all.at[pl.ds(pl.multiple_of(own_start, rows_out), rows_out)])
    )
    join(1)
    for number in range(1, len(bits)):
        slope_add(number)
        if number + 1 < len(bits):
            slope_send(number + 1)
        if number < 3:
            join(number + 1)
        if number == 2:
            gathers[0].hops(2)
            gathers[1].hops(2)
        if number == 3:
            gathers[2].hop(1)
    gathers[2].hops(2)
    weights[1].forward()
    for gather in gathers:
        gather.finish()
    for weight in weights:
        weight.finish()
    for copy in own + stores:
        copy.wait()
    wire.close()
    heads.close()
    outer.close()


class WeightGather:
    def __init__(self, wire, here, finals, near, far, cut=0, cuts=1):
        self.wire, self.here, self.near, self.far = wire, here, near, far
        self.size = finals[0].shape[0]
        self.rows = self.size // cuts
        self.shift = cut * self.rows
        model = near.shape[0]
        self.finals = [final.at[pl.ds(self.shift, self.rows)] for final in finals]
        self.starts = []
        for color, order in enumerate(here.colors()):
            start = color * (model // 2)
            rows = model // 2
            for bit in order[:-1]:
                rows //= 2
                start = start + here.side(bit) * rows
            self.starts.append(start)
        self.swaps, self.kept = [], []

    def _rows(self, start):
        return pl.ds(pl.multiple_of(start + self.shift, self.rows), self.rows)

    def _pass(self, start, source, bit, rows):
        copy = self.wire.send(
            source, self.near.at[self._rows(start)], {"seq": self.here.at(bit)}
        )
        start = start + rows - 2 * rows * self.here.side(bit)
        return (start, self.near.at[self._rows(start)], copy)

    def _swap(self, start, source):
        self.swaps.append(
            self.wire.send(source, self.far.at[self._rows(start)], {"seq": self.here.at(1)})
        )

    def start(self):
        self.held = []
        for color, order in enumerate(self.here.colors()):
            source, start = self.finals[color], self.starts[color]
            pieces = [(start, source, None)]
            if order[:-1]:
                pieces.append(self._pass(start, source, order[-2], self.size))
            self.held.append(pieces)

    def own(self):
        for color in (0, 1):
            source, start = self.finals[color], self.starts[color]
            self._swap(start, source)
            self.kept.append(self.wire.local(source, self.near.at[self._rows(start)]))

    def forward(self):
        for color, order in enumerate(self.here.colors()):
            rest = order[:-1]
            pieces = self.held[color]
            rows = self.size
            for position in range(len(rest) - 1, -1, -1):
                for start, source, copy in pieces:
                    if copy is not None:
                        copy.wait_recv()
                        self._swap(start, source)
                pieces = [(start, source, None) for start, source, _ in pieces]
                rows *= 2
                if position > 0:
                    pieces = pieces + [
                        self._pass(start, source, rest[position - 1], rows)
                        for start, source, _ in pieces
                    ]

    def finish(self):
        for copy in self.swaps:
            copy.wait_recv()
        for copy in self.kept:
            copy.wait()


def widen_kernel(near, far, out):
    core = lax.axis_index("seq") % 2
    units = near.shape[1]
    out[:, pl.ds(pl.multiple_of(core * units, units), units)] = near[...].astype(out.dtype)
    out[:, pl.ds(pl.multiple_of((1 - core) * units, units), units)] = far[...].astype(out.dtype)


def widen_pieces_kernel(count, steps, starts, *refs):
    nears, fars, out = refs[:count], refs[count : 2 * count], refs[-1]
    core = lax.axis_index("seq") % 2
    units = nears[0].shape[1]
    index = pl.program_id(0)
    for number in range(count):

        @pl.when(index // steps == number)
        def _(near=nears[number], far=fars[number]):
            own = pl.ds(pl.multiple_of(core * units, units), units)
            other = pl.ds(pl.multiple_of((1 - core) * units, units), units)
            out[:, own] = near[...].astype(out.dtype)
            out[:, other] = far[...].astype(out.dtype)


def results_kernel(
    copies, width, query, pair, outer, slope, grad_query, grad_key, grad_value, grad_output, *gains
):
    f32 = jnp.float32
    grad_query[...] = query[...].astype(f32)
    grad_output[...] = outer[...].astype(f32)
    columns = 2 * width
    for number in range(pair.shape[0] // (2 * copies)):
        low, high = (
            sum(
                pair[(2 * number + side) * copies + copy].astype(f32) for copy in range(copies)
            )
            for side in (0, 1)
        )
        at = pl.ds(number * columns, columns)
        grad_key[:, at] = pick_lanes(low, pltpu.roll(high, width, 1), width)
        grad_value[:, at] = pick_lanes(pltpu.roll(low, width, 1), high, width)
    in_slope, mid_slope, query_slope, key_slope = gains
    in_slope[...] = slope[0:1, :]
    mid_slope[...] = slope[1:2, :]
    query_slope[...] = slope[2:3, 0:width]
    key_slope[...] = slope[3:4, 0:width]


SENDS, LOCALS = 192, 48


def call(kernel, mesh_sizes, number, inputs, in_vmem, outputs, scratch, out_vmem=None):
    vmem = pl.BlockSpec(memory_space=pltpu.VMEM)
    anywhere = pl.BlockSpec(memory_space=pl.ANY)
    out_vmem = out_vmem or [True] * len(outputs)
    semaphores = [
        pltpu.SemaphoreType.DMA((SENDS,)),
        pltpu.SemaphoreType.DMA((SENDS,)),
        pltpu.SemaphoreType.DMA((LOCALS,)),
    ]
    return pl.pallas_call(
        functools.partial(kernel, *mesh_sizes),
        out_shape=[jax.ShapeDtypeStruct(shape, kind) for shape, kind in outputs],
        in_specs=[vmem if inside else anywhere for inside in in_vmem],
        out_specs=[vmem if inside else anywhere for inside in out_vmem],
        scratch_shapes=[pltpu.VMEM(shape, kind) for shape, kind in scratch] + semaphores,
        compiler_params=pltpu.CompilerParams(
            collective_id=number, has_side_effects=True, vmem_limit_bytes=VMEM_BYTES
        ),
    )(*inputs)


def widen(near, far):
    rows, units = near.shape
    step = min(256, rows)
    return pl.pallas_call(
        widen_kernel,
        grid=(rows // step,),
        out_shape=jax.ShapeDtypeStruct((rows, 2 * units), jnp.float32),
        in_specs=[pl.BlockSpec((step, units), lambda index: (index, 0))] * 2,
        out_specs=pl.BlockSpec((step, 2 * units), lambda index: (index, 0)),
        cost_estimate=pl.CostEstimate(
            flops=0, transcendentals=0, bytes_accessed=12 * rows * units
        ),
    )(near, far)


def widen_pieces(pieces, fars, whole=None, into=None):
    rows, units = fars[0].shape
    count = len(fars)
    step = min(256, rows)
    steps = rows // step
    starts = jnp.stack([jnp.asarray(start, jnp.int32) >> (step.bit_length() - 1) for start, _ in pieces])

    def block(number):
        return pl.BlockSpec(
            (step, units),
            lambda index, starts: (jnp.clip(index - number * steps, 0, steps - 1), 0),
        )

    more = () if into is None else (into,)
    return pl.pallas_call(
        functools.partial(widen_pieces_kernel, count, steps),
        out_shape=jax.ShapeDtypeStruct((whole or count * rows, 2 * units), jnp.float32),
        grid_spec=pltpu.PrefetchScalarGridSpec(
            num_scalar_prefetch=1,
            grid=(count * steps,),
            in_specs=[block(number) for number in range(count)] * 2
            + [pl.BlockSpec(memory_space=pl.ANY) for _ in more],
            out_specs=pl.BlockSpec(
                (step, 2 * units), lambda index, starts: (starts[index // steps] + index % steps, 0)
            ),
        ),
        input_output_aliases={2 * count + 1: 0} if more else {},
        cost_estimate=pl.CostEstimate(
            flops=0, transcendentals=0, bytes_accessed=12 * count * rows * units
        ),
    )(starts, *[value for _, value in pieces], *fars, *more)


def results(copies, width, query, pair, outer, slope):
    shard, model = query.shape
    seats = pair.shape[0]
    step = min(128, shard)
    f32 = jnp.float32
    pair_cols = seats // copies * width
    row = pl.BlockSpec((step, model), lambda index: (index, 0))
    row_pair = pl.BlockSpec((step, pair_cols), lambda index: (index, 0))
    fixed = lambda *shape: pl.BlockSpec(shape, lambda index: (0, 0))
    return pl.pallas_call(
        functools.partial(results_kernel, copies, width),
        grid=(shard // step,),
        out_shape=[
            jax.ShapeDtypeStruct((shard, model), f32),
            jax.ShapeDtypeStruct((shard, pair_cols), f32),
            jax.ShapeDtypeStruct((shard, pair_cols), f32),
            jax.ShapeDtypeStruct((shard, model), f32),
            jax.ShapeDtypeStruct((1, model), f32),
            jax.ShapeDtypeStruct((1, model), f32),
            jax.ShapeDtypeStruct((1, width), f32),
            jax.ShapeDtypeStruct((1, width), f32),
        ],
        in_specs=[
            row,
            pl.BlockSpec((seats, step, 2 * width), lambda index: (0, index, 0)),
            row,
            fixed(8, model),
        ],
        out_specs=[row, row_pair, row_pair, row]
        + [fixed(1, model), fixed(1, model), fixed(1, width), fixed(1, width)],
        cost_estimate=pl.CostEstimate(
            flops=0, transcendentals=0, bytes_accessed=16 * shard * model
        ),
    )(query, pair, outer, slope)


VMEM_BYTES = 67_000_000


def per_device(
    inputs,
    cotangent,
    attention_gain,
    query_weight,
    key_weight,
    value_weight,
    output_weight,
    query_gain,
    key_gain,
    feedforward_gain,
    gate_weight,
    up_weight,
    down_weight,
):
    tokens = inputs.shape[1]
    model = inputs.shape[2]
    width = query_gain.shape[0]
    pair_heads = key_weight.shape[1] // width
    parts = lax.axis_size("seq")
    planes = lax.axis_size("fsdp")
    sizes = (parts, planes)
    chips = parts // 2
    copies = max(1, parts // pair_heads)
    place = lax.axis_index("seq")
    plane = lax.axis_index("fsdp")
    core = place % 2
    query_cols = model // parts
    head_cols = query_cols + 2 * width
    local_groups = query_cols // width
    shard = query_weight.shape[0]
    piece_rows = shard // parts
    length = parts * tokens
    units = gate_weight.shape[1] // 2
    f32, bf16 = jnp.float32, jnp.bfloat16
    halvings = chips.bit_length() - 2
    last_rows = model // 2 >> halvings
    rows_in = inputs.reshape(tokens, model)
    cot_rows = cotangent.reshape(tokens, model)

    exponents = jnp.arange(width // 2).astype(f32) * 2.0 / width
    rates = jnp.power(jnp.float32(THETA), -exponents)
    rates = jnp.concatenate([rates] * 4)[None, :]
    gain_row = jnp.concatenate([query_gain] * local_groups + [key_gain] * 2)[None, :]
    half = model // 2
    scatter_scratch = [
        ((chips, tokens, model), bf16),
        ((chips, tokens, model), bf16),
        ((2, chips, tokens, half), bf16),
        ((halvings + 1, 2, chips, tokens, half), bf16),
    ]
    mid_gain = feedforward_gain[None, :]
    kept = [
        ((length, model), bf16),
        ((model, head_cols), bf16),
        ((query_cols, model), bf16),
        ((length, head_cols), f32),
        ((length, query_cols), bf16),
        ((length, 2 * width), bf16),
        ((length, query_cols), bf16),
        ((length, 128), f32),
        ((length, 2 * width), f32),
        ((length, 2 * width), f32),
        ((head_cols, head_cols), bf16),
        ((planes, 2, tokens, model), bf16),
    ]
    (
        normed_all,
        head_full,
        out_slice,
        proj,
        queries,
        pair_rows,
        out_rows,
        log_rows,
        cosine,
        sine,
        group,
        middle,
        normed_mid,
        cot_all,
    ) = call(
        functools.partial(front_kernel, width, copies),
        sizes,
        0,
        (
            rows_in,
            cot_rows,
            query_weight,
            key_weight,
            value_weight,
            output_weight,
            attention_gain[None, :],
            mid_gain,
            gain_row,
            rates,
        ),
        (True, True, False, False, False, False, True, True, True, True),
        kept[:11] + [((tokens, model), f32), ((tokens, model), bf16)] + kept[11:],
        kept
        + [((planes, piece_rows, model), bf16)]
        + [((length, 2 * width), bf16)] * 3
        + [((shard, 2 * width), bf16)] * 2
        + scatter_scratch,
        [False] * 11 + [True] * 2 + [False],
    )
    tables = (gain_row, cosine, sine, group)

    quarter = model // 4
    rows_shape = (planes, tokens, model)
    line_scratch = [
        (rows_shape, bf16),
        (rows_shape, bf16),
        ((2, planes - 1, tokens, model), bf16),
    ]
    acts = (2 * planes * tokens, units)
    early = last_rows // 2
    early_piece, late_piece = ((early, units), bf16), ((2 * last_rows - early, units), bf16)
    (
        middle_half,
        mid_slope,
        middle_grad,
        s_down,
        early_a,
        early_b,
        late_a,
        late_b,
        down_give,
        down_keep,
    ) = call(
        feed_kernel,
        sizes,
        2,
        (
            normed_mid,
            mid_gain,
            cot_all.reshape(-1, model),
            middle,
            gate_weight,
            up_weight,
            down_weight,
        ),
        (True, True, False, False, False, False, False),
        [
            ((tokens, model), bf16),
            ((1, model), f32),
            ((tokens, model), f32),
            ((2, last_rows, units), bf16),
            early_piece,
            early_piece,
            late_piece,
            late_piece,
            (rows_shape, bf16),
            (rows_shape, bf16),
        ],
        [((model, units), bf16)] * 3
        + [
            ((2 * planes * tokens, model), bf16),
            ((tokens, model), f32),
            ((tokens, model), f32),
            ((planes, 2, tokens, model), bf16),
            (acts, bf16),
            ((2,) + acts, bf16),
            ((3, 2, quarter, units), bf16),
            ((3, 2, last_rows, units), bf16),
        ]
        + [((3, 2, quarter >> stage, units), bf16) for stage in range(halvings)]
        + [(rows_shape, bf16)]
        + line_scratch,
        [True] * 2 + [False] * 8,
    )

    middle_all, t_down, came_a, came_b, down_sum = call(
        spread_kernel,
        sizes,
        4,
        (middle_half, s_down, early_a, early_b, down_give, down_keep),
        (True, True, False, False, False, False),
        [
            ((length, model), bf16),
            ((2, last_rows, units), bf16),
            early_piece,
            early_piece,
            ((tokens, model), f32),
        ],
        [((length, model), bf16)] + line_scratch,
        [False, True, False, False, True],
    )

    def swap(value, bit):
        return lax.ppermute(value, "seq", [(i, i ^ bit) for i in range(parts)])

    late_a, late_b, middle_all = lax.optimization_barrier((late_a, late_b, middle_all))
    bit_orders = ([2 << i for i in range(halvings + 1)], [chips >> i for i in range(halvings + 1)])
    sent = [early_a, early_b, late_a, late_b]
    came = [came_a, came_b, swap(late_a, bit_orders[0][-1]), swap(late_b, bit_orders[1][-1])]

    vmem = pl.BlockSpec(memory_space=pltpu.VMEM)
    halves, head_part, out_part, head_slopes = pl.pallas_call(
        functools.partial(back_kernel, width),
        out_shape=[
            jax.ShapeDtypeStruct((length, head_cols), bf16),
            jax.ShapeDtypeStruct((model, head_cols), bf16),
            jax.ShapeDtypeStruct((query_cols, model), bf16),
            jax.ShapeDtypeStruct((8, head_cols), f32),
        ],
        in_specs=[vmem] * 12,
        out_specs=[vmem] * 4,
        scratch_shapes=[
            pltpu.VMEM((length, query_cols), bf16),
            pltpu.VMEM((length, query_cols), f32),
            pltpu.VMEM((length, 2 * width), f32),
            pltpu.VMEM((length, 2 * width), f32),
        ]
        + [pltpu.VMEM((3, length, 2 * width), bf16), pltpu.VMEM((length, 2 * width), bf16)],
        compiler_params=pltpu.CompilerParams(vmem_limit_bytes=VMEM_BYTES),
        cost_estimate=pl.CostEstimate(
            flops=10 * length * model * head_cols,
            transcendentals=length * length * local_groups,
            bytes_accessed=16 * length * model,
        ),
    )(
        normed_all,
        middle_all,
        out_slice,
        out_rows,
        log_rows,
        queries,
        pair_rows,
        proj,
        *tables,
    )
    head_part = head_part.reshape(planes, shard, head_cols)
    query_slope = head_slopes[:1, :query_cols].reshape(local_groups, width).sum(axis=0)
    key_slope = head_slopes[0, query_cols : query_cols + width]
    gains = jnp.pad(jnp.stack([query_slope, key_slope]), ((0, 0), (0, model - width)))
    slopes = jnp.concatenate(
        [jnp.zeros_like(mid_slope), mid_slope, gains, jnp.zeros((4, model), f32)], axis=0
    )
    rounds = (parts * planes).bit_length() - 1
    side = ((model, units), bf16)
    piece = ((last_rows, units), bf16)
    in_grad, near_down, far_down, query_all, pair_all, outer_all, slopes, *pieces = call(
        final_kernel,
        sizes,
        5,
        (halves, head_full, head_part, out_part, t_down, rows_in, slopes, *sent, *came),
        (True, True, False, False, True, True, True) + (False,) * 8,
        [
            ((tokens, model), f32),
            side,
            side,
            ((shard, model), bf16),
            ((parts, shard, 2 * width), bf16),
            ((shard, model), bf16),
            ((8, model), f32),
        ]
        + [piece] * 4,
        scatter_scratch
        + [
            ((planes, shard, head_cols), bf16),
            ((2, planes - 1, shard, head_cols), bf16),
            ((planes, piece_rows, model), bf16),
            ((2, planes - 1, piece_rows, model), bf16),
            ((shard, head_cols), bf16),
            ((piece_rows, model), bf16),
            ((4, last_rows, units), bf16),
            ((4, last_rows, units), bf16),
            ((rounds, 8, model), f32),
            ((rounds, 8, model), f32),
        ],
        [True, False, False] + [True] * 4 + [False] * 4,
    )
    pieces, near_down, far_down, in_grad = lax.optimization_barrier(
        (pieces, near_down, far_down, in_grad)
    )
    source = rows_in.astype(f32)
    first = rms_factor(source)
    input_rows = (middle_grad + norm_back(in_grad, source, first, attention_gain)).astype(bf16)

    def plane_pieces(values):
        whole = []
        for color, order in enumerate(bit_orders):
            start, rows = color * (model // 2), model // 2
            for bit in order[:-1]:
                rows //= 2
                start = start + (place // bit) % 2 * rows
            held = [(start, values[color])]
            rows = last_rows
            for bit in order[-2::-1]:
                held = held + [
                    (start + rows - 2 * rows * ((place // bit) % 2), swap(value, bit))
                    for start, value in held
                ]
                rows *= 2
            whole = whole + held
        return whole

    gate_pieces = plane_pieces(pieces[:2])
    grad_down = widen(near_down, far_down)
    (
        grad_query,
        grad_key,
        grad_value,
        grad_output,
        attention_slope,
        feedforward_slope,
        query_slope,
        key_slope,
    ) = results(copies, width, query_all, pair_all, outer_all, slopes)
    block_out = (middle + down_sum).astype(bf16).reshape(1, tokens, model)
    pieces[2:], grad_down = lax.optimization_barrier((pieces[2:], grad_down))
    up_pieces = plane_pieces(pieces[2:])
    written = (grad_down, grad_query, grad_key, grad_value, grad_output, input_rows, block_out)
    gate_pieces, written = lax.optimization_barrier((gate_pieces, written))
    grad_down, grad_query, grad_key, grad_value, grad_output, input_rows, block_out = written
    grad_gate = widen_pieces(gate_pieces, [swap(value, 1) for _, value in gate_pieces])
    own = [up_pieces[0], up_pieces[len(up_pieces) // 2]]
    others = [piece for piece in up_pieces if all(piece is not mine for mine in own)]
    grad_up = widen_pieces(own, [swap(value, 1) for _, value in own], model)
    others, grad_gate, grad_up = lax.optimization_barrier((others, grad_gate, grad_up))
    grad_up = widen_pieces(others, [swap(value, 1) for _, value in others], model, grad_up)
    attention_slope, feedforward_slope = attention_slope[0], feedforward_slope[0]
    query_slope, key_slope = query_slope[0], key_slope[0]
    input_grad = input_rows.reshape(1, tokens, model)
    return (
        block_out,
        input_grad,
        attention_slope,
        grad_query,
        grad_key,
        grad_value,
        grad_output,
        query_slope,
        key_slope,
        feedforward_slope,
        grad_gate,
        grad_up,
        grad_down,
    )


def solution(mesh):
    in_specs = (
        P("fsdp", "seq", None),
        P("fsdp", "seq", None),
        P(),
        P("fsdp", None),
        P("fsdp", None),
        P("fsdp", None),
        P("fsdp", None),
        P(),
        P(),
        P(),
        P(None, "fsdp"),
        P(None, "fsdp"),
        P(None, "fsdp"),
    )
    out_specs = (
        P("fsdp", "seq", None),
        P("fsdp", "seq", None),
        P(),
        P("fsdp", None),
        P("fsdp", None),
        P("fsdp", None),
        P("fsdp", None),
        P(),
        P(),
        P(),
        P(None, "fsdp"),
        P(None, "fsdp"),
        P(None, "fsdp"),
    )
    return jax.shard_map(
        per_device, mesh=mesh, in_specs=in_specs, out_specs=out_specs, check_vma=False
    )
```

```python
import functools

import jax
import jax.numpy as jnp
from jax import lax
from jax.experimental import pallas as pl
from jax.experimental.pallas import tpu as pltpu
from jax.sharding import PartitionSpec as P

EPS = 1e-05
THETA = 1000000.0


def rotate_half(values):
    half = values.shape[-1] // 2
    return jnp.concatenate([-values[..., half:], values[..., :half]], axis=-1)


def rope_tables(positions, width):
    exponents = jnp.arange(width // 2).astype(jnp.float32) * 2.0 / width
    rates = jnp.power(jnp.float32(THETA), -exponents)
    angle = positions.astype(jnp.float32)[:, None] * rates[None, :]
    angle = jnp.concatenate([angle, angle], axis=-1)
    return (jnp.cos(angle), jnp.sin(angle))


def prepare(proj, gain, cosine, sine):
    rows = proj.shape[0]
    width = gain.shape[0]
    split = proj.reshape(rows, -1, width)
    factor = lax.rsqrt(jnp.mean(split * split, axis=-1, keepdims=True) + EPS)
    normed = split * factor * gain
    turned = normed * cosine[:, None, :] + rotate_half(normed) * sine[:, None, :]
    return turned.reshape(rows, -1)


def matmul(left, right):
    return jnp.dot(left, right, preferred_element_type=jnp.float32)


def inner_rows(left, right):
    return lax.dot_general(
        left, right, (((0,), (0,)), ((), ())), preferred_element_type=jnp.float32
    )


def inner_cols(left, right):
    return lax.dot_general(
        left, right, (((1,), (1,)), ((), ())), preferred_element_type=jnp.float32
    )


def rms_factor(values):
    return lax.rsqrt(jnp.mean(values * values, axis=-1, keepdims=True) + EPS)


def norm_back(grad, values, factor, gain):
    scaled = grad * gain
    return factor * (
        scaled - values * factor * factor * jnp.mean(scaled * values, axis=-1, keepdims=True)
    )


def gate_back(hidden_grad, gate, lifted):
    sigma = jax.nn.sigmoid(gate)
    gate_grad = (hidden_grad * lifted * sigma * (1.0 + gate * (1.0 - sigma))).astype(jnp.bfloat16)
    lifted_grad = (hidden_grad * gate * sigma).astype(jnp.bfloat16)
    return (gate_grad, lifted_grad)


def activate(gate, lifted):
    return (gate * jax.nn.sigmoid(gate) * lifted).astype(jnp.bfloat16)


def split_heads(query_rows, pair_rows, groups, width):
    length = query_rows.shape[0]
    key_heads = pair_rows.shape[1] // (2 * width)
    queries = query_rows.reshape(length, key_heads, groups, width)
    keys = pair_rows[:, : key_heads * width].reshape(length, key_heads, width)
    values = pair_rows[:, key_heads * width :].reshape(length, key_heads, width)
    return (queries, keys, values, key_heads)


def attend_heads(query_rows, pair_rows, groups, width):
    length = query_rows.shape[0]
    queries, keys, values, key_heads = split_heads(query_rows, pair_rows, groups, width)
    block = min(512, length)
    scale = width ** (-0.5)
    offsets = jnp.arange(block)

    def query_step(index, state):
        out_rows, log_rows = state
        query_block = lax.dynamic_slice_in_dim(queries, index * block, block, 0)

        def key_step(inner, carry):
            summed, total = carry
            key_block = lax.dynamic_slice_in_dim(keys, inner * block, block, 0)
            value_block = lax.dynamic_slice_in_dim(values, inner * block, block, 0)
            scores = (
                jnp.einsum(
                    "qhgd,shd->hgqs", query_block, key_block, preferred_element_type=jnp.float32
                )
                * scale
            )
            allowed = (index * block + offsets)[:, None] >= (inner * block + offsets)[None, :]
            weights = jnp.where(allowed, jnp.exp(scores), 0.0)
            summed = summed + jnp.einsum(
                "hgqs,shd->hgqd",
                weights.astype(jnp.bfloat16),
                value_block,
                preferred_element_type=jnp.float32,
            )
            return (summed, total + jnp.sum(weights, axis=-1))

        initial = (
            jnp.zeros((key_heads, groups, block, width), jnp.float32),
            jnp.zeros((key_heads, groups, block), jnp.float32),
        )
        summed, total = lax.fori_loop(0, index + 1, key_step, initial)
        result = (summed / total[..., None]).astype(jnp.bfloat16)
        result = result.transpose(2, 0, 1, 3).reshape(block, key_heads * groups * width)
        out_rows = lax.dynamic_update_slice_in_dim(out_rows, result, index * block, 0)
        log_rows = lax.dynamic_update_slice_in_dim(log_rows, jnp.log(total), index * block, 2)
        return (out_rows, log_rows)

    start = (
        jnp.zeros((length, key_heads * groups * width), jnp.bfloat16),
        jnp.zeros((key_heads, groups, length), jnp.float32),
    )
    return lax.fori_loop(0, length // block, query_step, start)


def attend_back(query_rows, pair_rows, out_rows, log_rows, grad_rows, groups, width):
    length = query_rows.shape[0]
    queries, keys, values, key_heads = split_heads(query_rows, pair_rows, groups, width)
    outs = out_rows.reshape(length, key_heads, groups, width)
    grads = grad_rows.reshape(length, key_heads, groups, width)
    correction = jnp.sum(grads.astype(jnp.float32) * outs.astype(jnp.float32), axis=-1)
    block = min(512, length)
    scale = width ** (-0.5)
    offsets = jnp.arange(block)

    def query_step(index, state):
        query_grad, key_grad, value_grad = state
        query_block = lax.dynamic_slice_in_dim(queries, index * block, block, 0)
        grad_block = lax.dynamic_slice_in_dim(grads, index * block, block, 0)
        shift_block = lax.dynamic_slice_in_dim(correction, index * block, block, 0).transpose(
            1, 2, 0
        )
        log_block = lax.dynamic_slice_in_dim(log_rows, index * block, block, 2)

        def key_step(inner, carry):
            block_grad, key_sum, value_sum = carry
            key_block = lax.dynamic_slice_in_dim(keys, inner * block, block, 0)
            value_block = lax.dynamic_slice_in_dim(values, inner * block, block, 0)
            scores = (
                jnp.einsum(
                    "qhgd,shd->hgqs", query_block, key_block, preferred_element_type=jnp.float32
                )
                * scale
            )
            allowed = (index * block + offsets)[:, None] >= (inner * block + offsets)[None, :]
            weights = jnp.where(allowed, jnp.exp(scores - log_block[..., None]), 0.0)
            value_part = jnp.einsum(
                "hgqs,qhgd->shd",
                weights.astype(jnp.bfloat16),
                grad_block,
                preferred_element_type=jnp.float32,
            )
            prob_grad = jnp.einsum(
                "qhgd,shd->hgqs", grad_block, value_block, preferred_element_type=jnp.float32
            )
            score_grad = (weights * (prob_grad - shift_block[..., None]) * scale).astype(
                jnp.bfloat16
            )
            block_grad = block_grad + jnp.einsum(
                "hgqs,shd->qhgd", score_grad, key_block, preferred_element_type=jnp.float32
            )
            key_part = jnp.einsum(
                "hgqs,qhgd->shd", score_grad, query_block, preferred_element_type=jnp.float32
            )
            key_sum = lax.dynamic_update_slice_in_dim(
                key_sum,
                lax.dynamic_slice_in_dim(key_sum, inner * block, block, 0) + key_part,
                inner * block,
                0,
            )
            value_sum = lax.dynamic_update_slice_in_dim(
                value_sum,
                lax.dynamic_slice_in_dim(value_sum, inner * block, block, 0) + value_part,
                inner * block,
                0,
            )
            return (block_grad, key_sum, value_sum)

        initial = (jnp.zeros((block, key_heads, groups, width), jnp.float32), key_grad, value_grad)
        block_grad, key_grad, value_grad = lax.fori_loop(0, index + 1, key_step, initial)
        query_grad = lax.dynamic_update_slice_in_dim(query_grad, block_grad, index * block, 0)
        return (query_grad, key_grad, value_grad)

    state = (
        jnp.zeros((length, key_heads, groups, width), jnp.float32),
        jnp.zeros((length, key_heads, width), jnp.float32),
        jnp.zeros((length, key_heads, width), jnp.float32),
    )
    query_grad, key_grad, value_grad = lax.fori_loop(0, length // block, query_step, state)
    pair_grad = jnp.concatenate(
        [
            key_grad.reshape(length, key_heads * width),
            value_grad.reshape(length, key_heads * width),
        ],
        axis=1,
    )
    return (query_grad.reshape(length, key_heads * groups * width), pair_grad)


MESH = pl.DeviceIdType.MESH


def flip(index, mask, bits):
    for bit in bits:
        if mask & bit:
            index = index + bit - 2 * bit * ((index // bit) % 2)
    return index


class Place:
    def __init__(self, parts, planes):
        self.parts, self.planes = parts, planes
        self.seat = lax.axis_index("seq")
        self.plane = lax.axis_index("fsdp")
        self.core = self.seat % 2
        self.chip = self.seat // 2
        self.seat_bits = [1 << i for i in range(parts.bit_length() - 1)]
        self.chip_bits = self.seat_bits[1:]
        self.plane_bits = [1 << i for i in range(planes.bit_length() - 1)]

    def at(self, mask):
        return flip(self.seat, mask, self.seat_bits)

    def side(self, bit):
        return (self.seat // bit) % 2

    def colors(self):
        return (self.chip_bits, self.chip_bits[::-1])

    def enter(self, masks=(), line=False, plane_masks=()):
        barrier = pltpu.get_barrier_semaphore()
        peers = [{"seq": self.at(mask)} for mask in masks]
        if line:
            peers.append({"fsdp": (self.plane + 1) % self.planes})
            peers.append({"fsdp": (self.plane + self.planes - 1) % self.planes})
        for mask in plane_masks:
            peers.append({"fsdp": flip(self.plane, mask, self.plane_bits)})
        for peer in peers:
            pl.semaphore_signal(barrier, inc=1, device_id=peer, device_id_type=MESH)
        pl.semaphore_wait(barrier, len(peers))


class Wire:
    def __init__(self, sends, receives, locals_):
        self.sends, self.receives, self.locals = sends, receives, locals_
        self.count = self.local_count = 0
        self.open = []

    def remote(self, source, target, device):
        number = self.count
        self.count += 1
        return pltpu.make_async_remote_copy(
            src_ref=source,
            dst_ref=target,
            send_sem=self.sends.at[number],
            recv_sem=self.receives.at[number],
            device_id=device,
            device_id_type=MESH,
        )

    def send(self, source, target, device):
        copy = self.remote(source, target, device)
        copy.start()
        self.open.append(copy)
        return copy

    def quiet(self, source, target):
        number = self.local_count
        self.local_count += 1
        return pltpu.make_async_copy(source, target, self.locals.at[number])

    def local(self, source, target):
        copy = self.quiet(source, target)
        copy.start()
        return copy

    def sent(self, copy):
        copy.wait_send()
        self.open = [other for other in self.open if other is not copy]

    def close(self):
        for copy in self.open:
            copy.wait_send()


def add_rows(target, left, right, step=64):
    rows = target.shape[0]
    step = min(step, rows)

    def body(index, carry):
        at = pl.ds(pl.multiple_of(index * step, step), step)
        total = left[at, :].astype(jnp.float32) + right[at, :].astype(jnp.float32)
        target[at, :] = total.astype(target.dtype)
        return carry

    lax.fori_loop(0, rows // step, body, 0)


class LineGather:
    def __init__(self, wire, here, source, target, share=None):
        self.here = here
        planes, plane = here.planes, here.plane
        above = {"fsdp": (plane + 1) % planes}
        below = {"fsdp": (plane + planes - 1) % planes}
        self.ups, self.downs = {}, {}
        for step in range(1, planes):
            lower = (plane + planes - step + 1) % planes
            upper = (plane + step - 1) % planes
            first = step == 1
            self.ups[step] = wire.remote(
                source if first else target(lower), target(lower), above
            )
            self.downs[step] = wire.remote(
                source if first else target(upper), target(upper), below
            )
        self.shared = {}
        if share is not None:
            for step in range(1, planes):
                for way, shift in ((0, planes - step), (1, step)):
                    index = (plane + shift) % planes
                    self.shared[(step, way)] = wire.remote(
                        target(index), share(index), {"seq": here.at(1)}
                    )

    def start(self, step):
        planes, plane = self.here.planes, self.here.plane

        @pl.when((plane >= step - 1) & (plane <= planes - 2))
        def _():
            self.ups[step].start()

        @pl.when((plane + step <= planes) & (plane >= 1))
        def _():
            self.downs[step].start()

    def arrive(self, step):
        planes, plane = self.here.planes, self.here.plane

        @pl.when(plane >= step)
        def _():
            self.ups[step].wait_recv()
            if self.shared:
                self.shared[(step, 0)].start()

        @pl.when(plane + step <= planes - 1)
        def _():
            self.downs[step].wait_recv()
            if self.shared:
                self.shared[(step, 1)].start()

    def close(self, shared_taken=False):
        planes, plane = self.here.planes, self.here.plane
        for (step, way), copy in self.shared.items():

            @pl.when(plane >= step if way == 0 else plane + step <= planes - 1)
            def _(copy=copy):
                copy.wait_send()
                if not shared_taken:
                    copy.wait_recv()

        for step in range(1, planes):

            @pl.when((plane >= step - 1) & (plane <= planes - 2))
            def _(step=step):
                self.ups[step].wait_send()

            @pl.when((plane + step <= planes) & (plane >= 1))
            def _(step=step):
                self.downs[step].wait_send()


class Lines:
    def __init__(self, members):
        self.members = members

    def start(self, step):
        for member in self.members:
            member.start(step)

    def pass_on(self, step):
        for member in self.members:
            member.arrive(step)
            if step + 1 < member.here.planes:
                member.start(step + 1)

    def step(self, step):
        for member in self.members:
            member.step(step)

    def close(self, *options):
        for member in self.members:
            member.close(*options)


def gather_lines(wire, here, source, target, share=None, cuts=2):
    rows = source.shape[0] // cuts
    members = []
    for cut in range(cuts):
        at = pl.ds(cut * rows, rows)
        members.append(
            LineGather(
                wire,
                here,
                source.at[at],
                lambda index, at=at: target(index).at[at],
                None if share is None else lambda index, at=at: share(index).at[at],
            )
        )
    return Lines(members)


class LineScatter:
    def __init__(self, wire, here, term, landing):
        self.wire, self.here, self.term, self.landing = wire, here, term, landing
        planes, plane = here.planes, here.plane
        above = {"fsdp": (plane + 1) % planes}
        below = {"fsdp": (plane + planes - 1) % planes}
        self.ups, self.downs = {}, {}
        for step in range(1, planes):
            self.ups[step] = wire.remote(
                term((plane + planes - step) % planes), landing(0, step - 1), above
            )
            self.downs[step] = wire.remote(
                term((plane + step) % planes), landing(1, step - 1), below
            )

    def step(self, step):
        planes, plane = self.here.planes, self.here.plane
        mirror = planes - 1 - plane
        for way, (position, copies, dest) in enumerate(
            (
                (plane, self.ups, (plane + planes - step) % planes),
                (mirror, self.downs, (plane + step) % planes),
            )
        ):
            if step > 1:

                @pl.when((position >= 1) & (position <= step - 1))
                def _(way=way, copies=copies, dest=dest):
                    copies[step - 1].wait_recv()
                    term = self.term(dest)
                    add_rows(term, term, self.landing(way, step - 2))

            @pl.when(position <= step - 1)
            def _(copies=copies):
                copies[step].start()

    def finish(self, out):
        planes, plane = self.here.planes, self.here.plane
        own = self.term(plane)
        last = planes - 1

        @pl.when(plane >= 1)
        def _():
            self.ups[last].wait_recv()

        @pl.when(plane <= planes - 2)
        def _():
            self.downs[last].wait_recv()

        @pl.when(plane == 0)
        def _():
            add_rows(out, own, self.landing(1, last - 1))

        @pl.when(plane == planes - 1)
        def _():
            add_rows(out, own, self.landing(0, last - 1))

        @pl.when((plane >= 1) & (plane <= planes - 2))
        def _():
            add_rows(own, own, self.landing(0, last - 1))
            add_rows(out, own, self.landing(1, last - 1))

    def close(self):
        planes, plane = self.here.planes, self.here.plane
        mirror = planes - 1 - plane
        for step in range(1, planes):

            @pl.when(plane <= step - 1)
            def _(step=step):
                self.ups[step].wait_send()

            @pl.when(mirror <= step - 1)
            def _(step=step):
                self.downs[step].wait_send()


class PlaneGather:
    def __init__(self, wire, here, source, target):
        self.wire, self.here, self.source, self.target = wire, here, source, target
        self.incoming = {}

    def _send(self, mask, color, bit):
        here = self.here
        target = self.target(here.at(mask), color)
        source = self.source(color) if mask == 0 else target
        self.incoming[(mask ^ bit, color)] = self.wire.send(
            source, target, {"seq": here.at(bit)}
        )

    def start(self):
        for position in range(len(self.here.chip_bits)):
            for color, bits in enumerate(self.here.colors()):
                self._send(0, color, bits[position])
        for color in (0, 1):
            self._send(0, color, 1)

    def hop(self, hops):
        here = self.here
        chips = here.parts // 2
        for mask in (mask * 2 for mask in range(1, chips)):
            if bin(mask).count("1") != hops:
                continue
            for color, bits in enumerate(here.colors()):
                self.incoming[(mask, color)].wait_recv()
                last = max(i for i, bit in enumerate(bits) if mask & bit)
                for bit in bits[last + 1 :]:
                    self._send(mask, color, bit)
                self._send(mask, color, 1)

    def hops(self, first=1):
        for hops in range(first, len(self.here.chip_bits) + 1):
            self.hop(hops)

    def finish(self):
        for mask in range(1, self.here.parts, 2):
            for color in (0, 1):
                self.incoming[(mask, color)].wait_recv()


class PlaneScatter:
    def __init__(self, wire, here, product, give, take, current, landing, model):
        self.wire, self.here, self.product = wire, here, product
        self.give, self.take, self.current, self.landing = give, take, current, landing
        self.model = model

    def start(self):
        here = self.here
        chips = here.parts // 2
        self.swaps = {}
        tokens = self.give.shape[1]
        seats = [2 * flip(here.chip, mask, [b // 2 for b in here.chip_bits]) for mask in range(chips)]
        for part in range(self.model // 512):
            columns = slice(part * 512, (part + 1) * 512)
            rows = self.product([seat + 1 - here.core for seat in seats], columns)
            for mask in range(chips):
                self.give[mask, :, columns] = rows[mask * tokens : (mask + 1) * tokens].astype(
                    self.give.dtype
                )
        for mask in range(chips)[::-1]:
            self.swaps[mask] = self.wire.send(
                self.give.at[mask], self.take.at[mask], {"seq": here.at(1)}
            )
        half = self.model // 2
        for part in range(self.model // 512):
            columns = slice(part * 512, (part + 1) * 512)
            rows = self.product([seat + here.core for seat in seats], columns)
            color, inside = divmod(part * 512, half)
            for mask in range(chips):
                self.current[color, mask, :, inside : inside + 512] = rows[
                    mask * tokens : (mask + 1) * tokens
                ].astype(self.current.dtype)

    def join(self):
        half = self.model // 2
        chips = self.here.parts // 2
        for mask in range(chips)[::-1]:
            self.swaps[mask].wait_recv()
            for color in (0, 1):
                mine = self.current.at[color, mask]
                add_rows(mine, mine, self.take.at[mask, :, pl.ds(color * half, half)])

    def stage(self, position):
        here = self.here
        self.moved = getattr(self, "moved", {})
        for onward in (True, False):
            for color, bits in enumerate(here.colors()):
                bit = bits[position]
                done = sum(bits[:position])
                for mask in range(here.parts // 2):
                    low = mask ^ (bit // 2)
                    if not mask * 2 & bit or mask * 2 & done:
                        continue
                    if self._onward(position, color, low) != onward:
                        continue
                    self.moved[(position, color, low)] = self.wire.send(
                        self.current.at[color, mask],
                        self.landing.at[position, color, low],
                        {"seq": here.at(bit)},
                    )

    def _onward(self, position, color, low):
        bits = self.here.colors()[color]
        return position + 1 < len(bits) and bool(low * 2 & bits[position + 1])

    def settle(self, position, out, onward):
        half = self.model // 2
        last = position == len(self.here.chip_bits) - 1
        for (stage, color, low), copy in self.moved.items():
            if stage != position or self._onward(position, color, low) != onward:
                continue
            copy.wait_recv()
            mine = self.current.at[color, low]
            target = out.at[:, pl.ds(color * half, half)] if last else mine
            add_rows(target, mine, self.landing.at[position, color, low])


def pick_lanes(low, high, width):
    lane = lax.broadcasted_iota(jnp.int32, low.shape, low.ndim - 1)
    return jnp.where(lane % (2 * width) < width, low, high)


def group_mean(values, group, width):
    high = values.astype(jnp.bfloat16)
    low = (values - high.astype(jnp.float32)).astype(jnp.bfloat16)
    total = jnp.dot(high, group, preferred_element_type=jnp.float32) + jnp.dot(
        low, group, preferred_element_type=jnp.float32
    )
    return total * (1.0 / width)


def turn(values, width):
    lanes = values.shape[1]
    half = width // 2
    return pick_lanes(
        pltpu.roll(values, lanes - half, 1), pltpu.roll(values, half, 1), half
    )


def attend_block(index, block, width, heads, queries, pair, twin, left, right, out_rows, logs):
    rows = pl.ds(index * block, block)
    before = index * block
    columns = 2 * width
    row = lax.broadcasted_iota(jnp.int32, (block, block), 0)
    column = lax.broadcasted_iota(jnp.int32, (block, block), 1)
    allowed = row >= column
    contract = (((1,), (1,)), ((), ()))
    lane = lax.broadcasted_iota(jnp.int32, (block, 128), 1)

    def two_heads(number, table):
        at = pl.ds(pl.multiple_of(number * columns, columns), columns)
        both = queries[rows, at]
        both = (both.astype(jnp.float32) * width**-0.5).astype(both.dtype)
        zero = jnp.zeros_like(both)
        result = None
        for side, values in ((0, left), (1, right)):
            mine = pick_lanes(both, zero, width) if side == 0 else pick_lanes(zero, both, width)
            scores = lax.dot_general(
                mine, twin[rows, :], contract, preferred_element_type=jnp.float32
            )
            weights = jnp.where(allowed, jnp.exp(scores), 0.0)
            total = jnp.sum(weights, axis=1, keepdims=True)
            summed = jnp.dot(
                weights.astype(jnp.bfloat16), values[rows, :], preferred_element_type=jnp.float32
            )
            if before:
                scores = lax.dot_general(
                    mine, twin[0:before, :], contract, preferred_element_type=jnp.float32
                )
                weights = jnp.exp(scores)
                total = total + jnp.sum(weights, axis=1, keepdims=True)
                summed = summed + jnp.dot(
                    weights.astype(jnp.bfloat16),
                    values[0:before, :],
                    preferred_element_type=jnp.float32,
                )
            table = jnp.where(lane == 2 * number + side, total, table)
            part = summed / total
            result = part if result is None else result + part
        out_rows[rows, at] = result.astype(out_rows.dtype)
        return table

    table = lax.fori_loop(0, heads // 2, two_heads, jnp.ones((block, 128), jnp.float32))
    logs[rows, :] = jnp.log(table)


def back_block(
    index, block, width, heads, queries, grads, outs, logs, keys, values, query_back, key_back, value_back
):
    rows = pl.ds(index * block, block)
    before = index * block
    scale = width**-0.5
    row = lax.broadcasted_iota(jnp.int32, (block, block), 0)
    column = lax.broadcasted_iota(jnp.int32, (block, block), 1)
    allowed = row >= column
    lane = lax.broadcasted_iota(jnp.int32, (block, 2 * width), 1)
    across = (((1,), (1,)), ((), ()))
    down = (((0,), (0,)), ((), ()))
    f32 = jnp.float32
    spans = [(rows, True)] + ([(slice(0, before), False)] if before else [])

    def one_head(head, carry):
        number, side = head // 2, head % 2
        at = pl.ds(pl.multiple_of(number * 2 * width, 2 * width), 2 * width)
        mine = lane // width == side
        query = jnp.where(mine, queries[rows, at], 0)
        grad = jnp.where(mine, grads[rows, at], 0)
        scaled = (query.astype(f32) * scale).astype(query.dtype)
        shift = jnp.sum(grad.astype(f32) * outs[rows, at].astype(f32), axis=1, keepdims=True)
        log = jnp.sum(jnp.where(lane == head, logs[rows, :], 0.0), axis=1, keepdims=True)
        total = query_back[rows, at]
        for span, masked in spans:
            scores = lax.dot_general(
                scaled, keys[0, span, :], across, preferred_element_type=f32
            )
            weights = jnp.exp(scores - log)
            if masked:
                weights = jnp.where(allowed, weights, 0.0)
            prob_grad = lax.dot_general(
                grad, values[span, :], across, preferred_element_type=f32
            )
            score_grad = (weights * (prob_grad - shift) * scale).astype(query.dtype)
            total = total + jnp.dot(
                score_grad, keys[1 + side, span, :], preferred_element_type=f32
            )
            key_back[span, :] += lax.dot_general(
                score_grad, query, down, preferred_element_type=f32
            )
            value_back[span, :] += lax.dot_general(
                weights.astype(query.dtype), grad, down, preferred_element_type=f32
            )
        query_back[rows, at] = total
        return carry

    lax.fori_loop(0, heads, one_head, 0)


def back_kernel(
    width,
    normed,
    middle,
    out_slice,
    outs,
    logs,
    queries,
    pair,
    proj,
    gain,
    cosine,
    sine,
    group,
    halves,
    head_part,
    out_part,
    slopes,
    grads,
    query_back,
    key_back,
    value_back,
    keys,
    values,
):
    length = normed.shape[0]
    block = min(256, length)
    blocks = length // block
    query_cols = queries.shape[1]
    heads = query_cols // width
    f32 = jnp.float32
    query_back[...] = jnp.zeros_like(query_back)
    key_back[...] = jnp.zeros_like(key_back)
    value_back[...] = jnp.zeros_like(value_back)

    def ready(index, carry):
        at = pl.ds(pl.multiple_of(index * block, block), block)
        grads[at, :] = lax.dot_general(
            middle[at, :], out_slice[...], (((1,), (1,)), ((), ())), preferred_element_type=f32
        ).astype(grads.dtype)
        both = pair[at, :].astype(f32)
        swapped = pltpu.roll(both, width, 1)
        zero = jnp.zeros_like(both)
        keys[0, at, :] = pick_lanes(both, swapped, width).astype(keys.dtype)
        keys[1, at, :] = pick_lanes(both, zero, width).astype(keys.dtype)
        keys[2, at, :] = pick_lanes(zero, swapped, width).astype(keys.dtype)
        values[at, :] = pick_lanes(swapped, both, width).astype(values.dtype)
        return carry

    lax.fori_loop(0, blocks, ready, 0)
    for index in range(blocks):
        back_block(
            index,
            block,
            width,
            heads,
            queries,
            grads,
            outs,
            logs,
            keys,
            values,
            query_back,
            key_back,
            value_back,
        )

    def norms(index, slope):
        at = pl.ds(pl.multiple_of(index * block, block), block)
        key_sum, value_sum = key_back[at, :], value_back[at, :]
        key_sum = key_sum + pltpu.roll(key_sum, width, 1)
        value_sum = value_sum + pltpu.roll(value_sum, width, 1)
        back = jnp.concatenate(
            [query_back[at, :], pick_lanes(key_sum, value_sum, width)], axis=1
        )
        value = proj[at, :]
        factor = lax.rsqrt(group_mean(value * value, group[...], width) + EPS)
        repeat = value.shape[1] // cosine.shape[1]
        cosines = jnp.concatenate([cosine[at, :]] * repeat, axis=1)
        sines = jnp.concatenate([sine[at, :]] * repeat, axis=1)
        turned = back * cosines + turn(back * sines, width)
        slope = slope + jnp.sum(turned * value * factor, axis=0, keepdims=True)
        scaled = turned * gain[...]
        result = factor * (
            scaled - value * factor * factor * group_mean(scaled * value, group[...], width)
        )
        lane = lax.broadcasted_iota(jnp.int32, back.shape, 1)
        result = jnp.where(lane >= query_cols + width, back, result)
        halves[at, :] = result.astype(halves.dtype)
        return slope

    slope = lax.fori_loop(0, blocks, norms, jnp.zeros((1, proj.shape[1]), f32))
    slopes[...] = jnp.broadcast_to(slope, slopes.shape)

    def terms(number, carry):
        at = pl.ds(pl.multiple_of(number * 256, 256), 256)
        down = (((0,), (0,)), ((), ()))
        head_part[at, :] = lax.dot_general(
            normed[:, at], halves[...], down, preferred_element_type=f32
        ).astype(head_part.dtype)
        out_part[:, at] = lax.dot_general(
            outs[...], middle[:, at], down, preferred_element_type=f32
        ).astype(out_part.dtype)
        return carry

    lax.fori_loop(0, normed.shape[1] // 256, terms, 0)


def row_blocks(rows, step, work):
    def body(index, carry):
        work(pl.ds(pl.multiple_of(index * step, step), step))
        return carry

    lax.fori_loop(0, rows // step, body, 0)


def front_kernel(
    width,
    copies,
    parts,
    planes,
    x,
    c,
    query_weight,
    key_weight,
    value_weight,
    output_weight,
    in_gain,
    mid_gain,
    gain,
    rates,
    x_store,
    w_store,
    o_store,
    proj_store,
    query_store,
    pair_store,
    out_store,
    log_store,
    cosine_store,
    sine_store,
    group_store,
    middle,
    mid,
    c_store,
    x_all,
    w_all,
    o_slice,
    proj,
    queries,
    pair,
    out_rows,
    logs,
    cosine,
    sine,
    group,
    c_all,
    o_all,
    twin,
    left,
    right,
    key_block,
    value_block,
    give,
    take,
    current,
    landing,
    *sems,
):
    here = Place(parts, planes)
    wire = Wire(*sems)
    tokens, model = x.shape
    shard = query_weight.shape[0]
    query_cols = queries.shape[1]
    rows = o_all.shape[1]
    half = tokens // 2
    chips = parts // 2
    f32 = jnp.float32
    chip_masks = [mask * 2 for mask in range(1, chips)]
    pair_head = here.seat // copies
    own_shard = pl.ds(pl.multiple_of(here.plane * shard, shard), shard)
    head_block = pl.ds(pl.multiple_of(pair_head // 2 * 2 * width, 2 * width), 2 * width)
    loads = [
        wire.local(key_weight.at[:, head_block], key_block),
        wire.local(value_weight.at[:, head_block], value_block),
        wire.local(
            query_weight.at[:, pl.ds(pl.multiple_of(here.seat * query_cols, query_cols), query_cols)],
            w_all.at[own_shard, pl.ds(0, query_cols)],
        ),
    ]
    piece = (here.core * chips + here.chip) * rows
    o = output_weight.at[pl.ds(pl.multiple_of(piece, rows), rows)]
    here.enter(chip_masks + [1], line=True)
    o_own = wire.local(o, o_all.at[here.plane])
    for load in loads[:2]:
        load.wait()
    upper = (pair_head % 2) * jnp.ones((1, 1), jnp.int32)
    keys, values = key_block[...].astype(f32), value_block[...].astype(f32)
    keys = jnp.where(upper == 1, pltpu.roll(keys, width, 1), keys)
    values = jnp.where(upper == 1, values, pltpu.roll(values, width, 1))
    w_all[own_shard, query_cols:] = pick_lanes(keys, values, width).astype(w_all.dtype)
    loads[2].wait()
    weights = gather_lines(
        wire,
        here,
        w_all.at[own_shard],
        lambda index: w_all.at[pl.ds(pl.multiple_of(index * shard, shard), shard)],
    )
    weights.start(1)

    def norm_rows(at):
        value = x[at, :].astype(f32)
        factor = lax.rsqrt(jnp.mean(value * value, axis=-1, keepdims=True) + EPS)
        own_at = pl.ds(pl.multiple_of(here.seat * tokens + at.start, 32), 32)
        x_all[own_at, :] = (value * factor * in_gain[...]).astype(x_all.dtype)

    row_blocks(tokens, 32, norm_rows)

    def seat_rows(seat, color):
        return x_all.at[pl.ds(pl.multiple_of(seat * tokens + color * half, half), half)]

    plane_rows = PlaneGather(
        wire, here, lambda color: seat_rows(here.seat, color), seat_rows
    )
    plane_rows.start()
    outer = gather_lines(wire, here, o, lambda index: o_all.at[index])

    def c_spot(index):
        return c_all.at[index, here.core]

    cots = gather_lines(wire, here, c, c_spot, c_spot)
    c_own = wire.local(c, c_spot(here.plane))

    lane = lax.broadcasted_iota(jnp.int32, (32, 2 * width), 1)
    row = lax.broadcasted_iota(jnp.int32, (32, 2 * width), 0)
    sign = jnp.where(lane % width < width // 2, -1.0, 1.0)

    def table_rows(at):
        angle = (row + at.start).astype(f32) * rates[...]
        cosine[at, :] = jnp.cos(angle)
        sine[at, :] = jnp.sin(angle) * sign

    columns = group.shape[0]
    group[...] = jnp.where(
        lax.broadcasted_iota(jnp.int32, (columns, columns), 0) // width
        == lax.broadcasted_iota(jnp.int32, (columns, columns), 1) // width,
        1.0,
        0.0,
    ).astype(group.dtype)
    length = x_all.shape[0]
    row_blocks(length, 32, table_rows)
    weights.members[0].arrive(1)
    if planes > 2:
        weights.members[0].start(2)
    plane_rows.hop(1)
    weights.members[1].arrive(1)
    if planes > 2:
        weights.members[1].start(2)
    outer.start(1)
    plane_rows.hops(2)
    spot = o_slice.at[pl.ds(pl.multiple_of(here.chip * rows, rows), rows)]
    deals = []
    for mask in chip_masks:
        chip = here.at(mask) // 2
        deals.append((chip, wire.remote(o_all.at[chip], spot, {"seq": here.at(mask)})))
    keep_own = wire.quiet(o_all.at[here.chip], spot)

    def deal(step):
        for chip, copy in deals + [(here.chip, keep_own)]:

            @pl.when((chip == here.plane + step) | (chip + step == here.plane))
            def _(copy=copy):
                copy.start()

    o_own.wait()
    deal(0)
    plane_rows.finish()
    block = min(256, length)
    blocks = length // block

    for step in range(2, planes):
        weights.pass_on(step)
    stores = [
        wire.local(x_all, x_store),
        wire.local(w_all, w_store),
        wire.local(cosine, cosine_store),
        wire.local(sine, sine_store),
        wire.local(group, group_store),
    ]
    heads = query_cols // width

    def project(index, carry):
        at = pl.ds(pl.multiple_of(index * block, block), block)
        value = jnp.dot(x_all[at, :], w_all[...], preferred_element_type=f32)
        proj[at, :] = value
        factor = lax.rsqrt(group_mean(value * value, group[...], width) + EPS)
        normed = value * factor * gain[...]
        repeat = value.shape[1] // cosine.shape[1]
        cosines = jnp.concatenate([cosine[at, :]] * repeat, axis=1)
        sines = jnp.concatenate([sine[at, :]] * repeat, axis=1)
        turned = normed * cosines + turn(normed, width) * sines
        queries[at, :] = turned[:, :query_cols].astype(queries.dtype)
        keys, values = turned[:, query_cols:], value[:, query_cols:]
        both = pick_lanes(keys, values, width)
        pair[at, :] = both.astype(pair.dtype)
        swapped = pltpu.roll(both, width, 1)
        twin[at, :] = pick_lanes(both, swapped, width).astype(twin.dtype)
        zero = jnp.zeros_like(both)
        left[at, :] = pick_lanes(swapped, zero, width).astype(left.dtype)
        right[at, :] = pick_lanes(zero, both, width).astype(right.dtype)
        return carry

    lax.fori_loop(0, blocks, project, 0)
    across = wire.send(c, c_spot(here.plane), {"seq": here.at(1)})
    waits = list(range(1, planes))
    cot_waits = list(range(1, planes))
    for index in range(blocks):
        while waits and waits[0] * blocks <= (index + 1) * planes:
            step = waits.pop(0)
            outer.pass_on(step)
            deal(step)
            if step == min(2, planes - 1):
                cots.start(1)
        attend_block(
            index, block, width, heads, queries, pair, twin, left, right, out_rows, logs
        )
    for step in waits:
        outer.pass_on(step)
        deal(step)
    cots.pass_on(cot_waits.pop(0))
    keep_own.wait()
    for _, copy in deals:
        copy.wait()

    def product(seats, at):
        chosen = [
            out_rows[pl.ds(pl.multiple_of(seat * tokens, tokens), tokens), :] for seat in seats
        ]
        return jnp.dot(
            jnp.concatenate(chosen, axis=0), o_slice[:, at], preferred_element_type=f32
        )

    stores += [
        wire.local(o_slice, o_store),
        wire.local(proj, proj_store),
        wire.local(queries, query_store),
        wire.local(pair, pair_store),
        wire.local(out_rows, out_store),
        wire.local(logs, log_store),
    ]
    sums = PlaneScatter(wire, here, product, give, take, current, landing, model)
    sums.start()
    sums.join()
    sums.stage(0)
    stages = len(here.chip_bits)
    for stage in range(stages):
        sums.settle(stage, middle, True)
        if stage + 1 < stages:
            sums.stage(stage + 1)
        if cot_waits:
            cots.pass_on(cot_waits.pop(0))
        sums.settle(stage, middle, False)

    def mid_rows(at):
        value = x[at, :].astype(f32) + middle[at, :]
        middle[at, :] = value
        factor = lax.rsqrt(jnp.mean(value * value, axis=-1, keepdims=True) + EPS)
        mid[at, :] = (value * factor * mid_gain[...]).astype(mid.dtype)

    for step in cot_waits:
        cots.pass_on(step)
    cots.close()
    c_own.wait()
    across.wait_recv()
    stores.append(wire.local(c_all, c_store))
    row_blocks(tokens, 32, mid_rows)
    for copy in stores:
        copy.wait()
    wire.close()
    weights.close()
    outer.close()


def feed_kernel(
    parts,
    planes,
    m,
    mid_gain,
    cots_whole,
    middle_whole,
    gate_weight,
    up_weight,
    down_weight,
    mid_half,
    mid_slope,
    mid_store,
    s_down,
    s_early_a,
    s_early_b,
    s_late_a,
    s_late_b,
    down_give,
    down_keep,
    gate_half,
    up_half,
    down_half,
    cots,
    middle,
    mid,
    mids,
    hidden,
    unit_grads,
    away,
    sums,
    *rest,
):
    here = Place(parts, planes)
    stages = len(here.chip_bits) - 1
    landings, rest = rest[:stages], rest[stages:]
    give, take, current, line_landing, *sems = rest
    wire = Wire(*sems)
    tokens, model = m.shape
    units = gate_half.shape[1]
    own_units = pl.ds(pl.multiple_of(here.core * units, units), units)
    here.enter(here.seat_bits, line=True)

    def spot(index):
        return mids.at[index, here.core]

    lines = gather_lines(wire, here, m, spot, spot)
    lines.start(1)
    across = wire.send(m, spot(here.plane), {"seq": here.at(1)})
    own = wire.local(m, spot(here.plane))
    loads = [
        wire.local(whole.at[:, own_units], part)
        for whole, part in (
            (gate_weight, gate_half),
            (up_weight, up_half),
            (down_weight, down_half),
        )
    ]
    loads += [wire.local(cots_whole, cots), wire.local(middle_whole, middle)]

    def block(index):
        rows = pl.ds(pl.multiple_of(index * 2 * tokens, 2 * tokens), 2 * tokens)
        mid_rows = mids[index].reshape(2 * tokens, model)
        cot_rows = cots[rows, :]

        def part(number, carry):
            at = pl.ds(pl.multiple_of(number * 256, 256), 256)
            gate = jnp.dot(mid_rows, gate_half[:, at], preferred_element_type=jnp.float32)
            lifted = jnp.dot(mid_rows, up_half[:, at], preferred_element_type=jnp.float32)
            hidden_grad = jnp.dot(cot_rows, down_half[:, at], preferred_element_type=jnp.float32)
            sigma = 1.0 / (1.0 + jnp.exp(-gate))
            active = gate * sigma
            hidden[rows, at] = (active * lifted).astype(hidden.dtype)
            unit_grads[1, rows, at] = (hidden_grad * active).astype(hidden.dtype)
            unit_grads[0, rows, at] = (
                hidden_grad * lifted * sigma * (1.0 + gate * (1.0 - sigma))
            ).astype(hidden.dtype)
            return carry

        lax.fori_loop(0, units // 256, part, 0)

    for load in loads:
        load.wait()
    own.wait()
    across.wait_recv()
    plane = here.plane

    above, below = plane, planes - 1 - plane
    shared_steps = jnp.where(above < below, above, below)

    def arrivals(step, carry):
        for number in range(1, planes):

            @pl.when(step == number)
            def _(number=number):
                lines.pass_on(number)

        entry = step - 1
        paired = entry < 2 * shared_steps
        stage_of = jnp.where(paired, entry // 2 + 1, entry - shared_steps + 1)
        from_up = jnp.where(paired, entry % 2 == 0, above > below)
        for stage in range(1, planes):
            for way, chosen in ((0, from_up), (1, jnp.logical_not(from_up))):

                @pl.when((step > 0) & (stage_of == stage) & chosen)
                def _(stage=stage, way=way):
                    for line in lines.members:
                        line.shared[(stage, way)].wait_recv()

        index = jnp.where(from_up, plane + planes - stage_of, plane + stage_of) % planes
        block(jnp.where(step == 0, plane, index))
        return carry

    lax.fori_loop(0, planes, arrivals, 0)

    flat_mids = mids.reshape(2 * planes * tokens, model)
    quarter = model // 4
    moved = {}

    def gradients(left, right, target, start, count):
        parts_of = quarter // 256

        def part(number, carry):
            k, inside = number // parts_of, number % parts_of * 256
            at = pl.ds(pl.multiple_of(start(k) + inside, 256), 256)
            target(k)[pl.ds(pl.multiple_of(inside, 256), 256), :] = lax.dot_general(
                left[:, at],
                right(k)[...],
                (((0,), (0,)), ((), ())),
                preferred_element_type=jnp.float32,
            ).astype(away.dtype)
            return carry

        lax.fori_loop(0, count * parts_of, part, 0)

    def first_half(color, mine):
        sides = [here.side(bits[0]) if mine else 1 - here.side(bits[0]) for bits in here.colors()]
        if isinstance(color, int):
            side = sides[color]
        else:
            side = sides[0] * (1 - color) + sides[1] * color
        return pl.multiple_of(color * (model // 2) + side * quarter, quarter)

    def send_away(number):
        for color, bits in enumerate(here.colors()):
            moved[(number, color)] = wire.send(
                away.at[number, color], landings[0].at[number, color], {"seq": here.at(bits[0])}
            )

    def mid_term(target, core):
        rows = [pl.ds(pl.multiple_of((2 * p + core) * tokens, tokens), tokens) for p in range(planes)]
        gates = jnp.concatenate([unit_grads[0, at, :] for at in rows], axis=0)
        lifts = jnp.concatenate([unit_grads[1, at, :] for at in rows], axis=0)

        def part(number, carry):
            at = pl.ds(pl.multiple_of(number * 256, 256), 256)
            term = lax.dot_general(
                gates, gate_half[at, :], (((1,), (1,)), ((), ())), preferred_element_type=jnp.float32
            ) + lax.dot_general(
                lifts, up_half[at, :], (((1,), (1,)), ((), ())), preferred_element_type=jnp.float32
            )
            target[:, :, at] = term.reshape(planes, tokens, 256).astype(target.dtype)
            return carry

        lax.fori_loop(0, model // 256, part, 0)

    def down_term(target, core):
        rows = [pl.ds(pl.multiple_of((2 * p + core) * tokens, tokens), tokens) for p in range(planes)]
        hiddens = jnp.concatenate([hidden[at, :] for at in rows], axis=0)

        def part(number, carry):
            at = pl.ds(pl.multiple_of(number * 256, 256), 256)
            term = lax.dot_general(
                hiddens, down_half[at, :], (((1,), (1,)), ((), ())), preferred_element_type=jnp.float32
            )
            target[:, :, at] = term.reshape(planes, tokens, 256).astype(target.dtype)
            return carry

        lax.fori_loop(0, model // 256, part, 0)

    gradients(
        cots,
        lambda k: hidden,
        lambda k: away.at[0, k],
        lambda k: first_half(k, False),
        2,
    )
    send_away(0)
    swaps = TokenSum(wire, here, current, take, line_landing)
    mid_term(give, 1 - here.core)
    swaps.start(give)
    mid_term(current, here.core)
    swaps.join()
    swaps.step(1)
    gradients(
        flat_mids,
        lambda k: unit_grads.at[k // 2],
        lambda k: away.at[1 + k // 2, k % 2],
        lambda k: first_half(k % 2, False),
        4,
    )
    send_away(1)
    send_away(2)
    for step in range(2, planes):
        swaps.step(step)

    early = s_early_a.shape[0]

    def store(number, color):
        done = sums.at[number, color]
        if number == 0:
            return [wire.local(done, s_down.at[color])]
        late = (s_late_a, s_late_b)[color]
        size = done.shape[0]
        if number == 1:
            return [
                wire.local(done.at[pl.ds(0, early)], (s_early_a, s_early_b)[color]),
                wire.local(done.at[pl.ds(early, size - early)], late.at[pl.ds(0, size - early)]),
            ]
        return [wire.local(done, late.at[pl.ds(size - early, size)])]

    wire.sent(swaps.across)
    down_term(give, 1 - here.core)
    down_term(take, here.core)
    handed = [wire.local(give, down_give), wire.local(take, down_keep)]
    rows = quarter
    keeps = {}
    if stages > 1:
        for copy in moved.values():
            wire.sent(copy)
    keep_in = sums if stages == 1 else away
    gradients(
        cots,
        lambda k: hidden,
        lambda k: keep_in.at[0, k],
        lambda k: first_half(k, True),
        2,
    )
    gradients(
        flat_mids,
        lambda k: unit_grads.at[k // 2],
        lambda k: keep_in.at[1 + k // 2, k % 2],
        lambda k: first_half(k % 2, True),
        4,
    )
    for number in range(3):
        for color in (0, 1):
            keeps[(number, color)] = (keep_in.at[number, color], 0)
    swaps.finish(mid)
    f32 = jnp.float32

    def norm_back_rows(index, slope):
        at = pl.ds(pl.multiple_of(index * 32, 32), 32)
        own_cots = (here.plane * 2 + here.core) * tokens + index * 32
        grad, value = mid[at, :], middle[at, :]
        factor = lax.rsqrt(jnp.mean(value * value, axis=-1, keepdims=True) + EPS)
        scaled = grad * mid_gain[...]
        back = factor * (
            scaled
            - value * factor * factor * jnp.mean(scaled * value, axis=-1, keepdims=True)
        )
        result = cots[pl.ds(pl.multiple_of(own_cots, 32), 32), :].astype(f32) + back
        mid[at, :] = result
        mid_half[at, :] = result.astype(mid_half.dtype)
        return slope + jnp.sum(grad * value * factor, axis=0, keepdims=True)

    mid_slope[...] = lax.fori_loop(
        0, tokens // 32, norm_back_rows, jnp.zeros((1, model), f32)
    )
    handed.append(wire.local(mid, mid_store))
    for stage in range(stages):
        last = stage == stages - 1
        for number in range(3):
            for color, bits in enumerate(here.colors()):
                keep, begin = keeps[(number, color)]
                moved[(number, color)].wait_recv()
                mine = keep.at[pl.ds(begin, rows)]
                if last:
                    add_rows(
                        sums.at[number, color], mine, landings[stage].at[number, color]
                    )
                    handed.extend(store(number, color))
                else:
                    add_rows(mine, mine, landings[stage].at[number, color])
                    bit = bits[stage + 1]
                    half = rows // 2
                    gone = pl.multiple_of(begin + (1 - here.side(bit)) * half, half)
                    moved[(number, color)] = wire.send(
                        keep.at[pl.ds(gone, half)],
                        landings[stage + 1].at[number, color],
                        {"seq": here.at(bit)},
                    )
                    keeps[(number, color)] = (
                        keep,
                        pl.multiple_of(begin + here.side(bit) * half, half),
                    )
        rows //= 2
    for copy in handed:
        copy.wait()
    wire.close()
    lines.close(True)
    swaps.close()


class TokenSum:
    def __init__(self, wire, here, current, take, landing):
        self.wire, self.here = wire, here
        self.current, self.take = current, take
        self.cuts = 2
        rows = current.shape[1] // self.cuts
        self.lines = []
        for cut in range(self.cuts):
            at = pl.ds(cut * rows, rows)
            self.lines.append(
                LineScatter(
                    wire,
                    here,
                    lambda index, at=at: current.at[index, at],
                    lambda way, step, at=at: landing.at[way, step, at],
                )
            )

    def start(self, give):
        self.across = self.wire.send(give, self.take, {"seq": self.here.at(1)})

    def join(self):
        self.across.wait_recv()

        def body(index, carry):
            row = self.current.at[index]
            add_rows(row, row, self.take.at[index])
            return carry

        lax.fori_loop(0, self.here.planes, body, 0)

    def step(self, step):
        for line in self.lines:
            line.step(step)

    def finish(self, out):
        rows = out.shape[0] // self.cuts
        for cut, line in enumerate(self.lines):
            line.finish(out.at[pl.ds(cut * rows, rows)])

    def close(self):
        for line in self.lines:
            line.close()


def spread_kernel(
    parts,
    planes,
    h,
    s,
    early_a,
    early_b,
    give,
    keep,
    h_store,
    t,
    came_a,
    came_b,
    block,
    h_all,
    current,
    take,
    line_landing,
    *sems,
):
    here = Place(parts, planes)
    wire = Wire(*sems)
    here.enter(here.seat_bits, line=True)
    tokens = h.shape[0]
    half = tokens // 2
    rows = PlaneGather(
        wire,
        here,
        lambda color: h.at[pl.ds(color * half, half)],
        lambda seat, color: h_all.at[pl.ds(pl.multiple_of(seat * tokens + color * half, half), half)],
    )
    swaps = TokenSum(wire, here, current, take, line_landing)
    swaps.start(give)
    kept = wire.local(keep, current)
    rows.start()
    own = wire.local(h, h_all.at[pl.ds(pl.multiple_of(here.seat * tokens, tokens), tokens)])
    moved = [
        wire.send(s.at[color], t.at[color], {"seq": here.at(bits[-1])})
        for color, bits in enumerate(here.colors())
    ]
    kept.wait()
    swaps.join()
    swaps.step(1)
    rows.hop(1)
    moved += [
        wire.send(source, target, {"seq": here.at(bits[-1])})
        for source, target, bits in zip((early_a, early_b), (came_a, came_b), here.colors())
    ]
    for step in range(2, planes):
        if step == 3:
            rows.hops(2)
        swaps.step(step)
    if planes <= 3:
        rows.hops(2)
    rows.finish()
    own.wait()
    store = wire.local(h_all, h_store)
    for color in (0, 1):
        moved[color].wait_recv()
        add_rows(t.at[color], t.at[color], s.at[color])
    swaps.finish(block)
    for copy in moved[2:]:
        copy.wait_recv()
    store.wait()
    wire.close()
    swaps.close()


def final_kernel(
    parts,
    planes,
    a,
    w,
    head_part,
    out_part,
    t_down,
    source,
    slope,
    *rest,
):
    sent, came, rest = rest[:4], rest[4:8], rest[8:]
    out, near, far, query_all, pair_all, outer_all, slope_out, *rest = rest
    joined, rest = rest[:4], rest[4:]
    (
        give,
        take,
        current,
        landing,
        head_current,
        head_landing,
        dealt,
        out_landing,
        head_sum,
        out_sum,
        left,
        right,
        slope_sums,
        slope_landing,
        *sems,
    ) = rest
    here = Place(parts, planes)
    wire = Wire(*sems)
    tokens, model = out.shape
    shard = head_sum.shape[0]
    columns = query_all.shape[1] // parts
    rows_out = out_sum.shape[0]
    chips = parts // 2
    chip_masks = [mask * 2 for mask in range(1, chips)]
    here.enter(chip_masks + [1], line=True, plane_masks=here.plane_bits)
    weights = [
        WeightGather(wire, here, (t_down.at[0], t_down.at[1]), near, far, cut, 2)
        for cut in range(2)
    ]
    head_own = wire.local(head_part, head_current)
    deals = []
    for mask in chip_masks:
        chip = here.at(mask) // 2
        deals.append(
            wire.send(
                out_part.at[pl.ds(pl.multiple_of(chip * rows_out, rows_out), rows_out)],
                dealt.at[here.chip],
                {"seq": here.at(mask)},
            )
        )
    deal_own = wire.local(
        out_part.at[pl.ds(pl.multiple_of(here.chip * rows_out, rows_out), rows_out)],
        dealt.at[here.chip],
    )

    def product(seats, columns):
        rows = [a[pl.ds(pl.multiple_of(seat * tokens, tokens), tokens), :] for seat in seats]
        return lax.dot_general(
            jnp.concatenate(rows, axis=0),
            w[columns, :],
            (((1,), (1,)), ((), ())),
            preferred_element_type=jnp.float32,
        )

    heads = LineScatter(
        wire, here, lambda index: head_current.at[index], lambda way, step: head_landing.at[way, step]
    )
    outer = LineScatter(
        wire, here, lambda index: dealt.at[index], lambda way, step: out_landing.at[way, step]
    )
    head_own.wait()
    heads.step(1)
    rows = PlaneScatter(wire, here, product, give, take, current, landing, model)
    rows.start()
    loads = []
    size, early = left.shape[1], sent[0].shape[0]
    for number in range(4):
        color = number % 2
        copies = []
        for pieces, working in ((sent, left), (came, right)):
            first, late = pieces[color], pieces[2 + color]
            if number < 2:
                copies.append(wire.local(first, working.at[number, pl.ds(0, early)]))
                copies.append(
                    wire.local(
                        late.at[pl.ds(0, size - early)],
                        working.at[number, pl.ds(early, size - early)],
                    )
                )
            else:
                copies.append(wire.local(late.at[pl.ds(size - early, size)], working.at[number]))
        loads.append(copies)
    heads.step(2)
    rows.join()
    rows.stage(0)
    weights[0].start()
    weights[0].own()
    deal_own.wait()
    for copy in deals:
        copy.wait_recv()
    outer.step(1)

    stores = []

    def join(number):
        for load in loads[number]:
            load.wait()
        add_rows(left.at[number], left.at[number], right.at[number])
        stores.append(wire.local(left.at[number], joined[number]))

    stages = len(here.chip_bits)
    for step in range(3, planes):
        heads.step(step)
    for stage in range(1, stages):
        rows.settle(stage - 1, out, True)
        rows.stage(stage)
        if stage == 1:
            weights[1].start()
            weights[1].own()
        rows.settle(stage - 1, out, False)
        if stage + 1 < planes:
            outer.step(stage + 1)
        if stage == 1:
            heads.finish(head_sum)
    half, half_out = shard // 2, rows_out // 2

    def seat_columns(seat):
        return pl.ds(pl.multiple_of(seat * columns, columns), columns)

    gathers = [
        PlaneGather(
            wire,
            here,
            lambda color: head_sum.at[pl.ds(color * half, half), pl.ds(0, columns)],
            lambda seat, color: query_all.at[pl.ds(color * half, half), seat_columns(seat)],
        ),
        PlaneGather(
            wire,
            here,
            lambda color: head_sum.at[
                pl.ds(color * half, half), pl.ds(columns, pair_all.shape[2])
            ],
            lambda seat, color: pair_all.at[seat, pl.ds(color * half, half)],
        ),
        PlaneGather(
            wire,
            here,
            lambda color: out_sum.at[pl.ds(color * half_out, half_out)],
            lambda seat, color: outer_all.at[
                pl.ds(
                    pl.multiple_of(
                        ((seat % 2) * chips + seat // 2) * rows_out + color * half_out, half_out
                    ),
                    half_out,
                )
            ],
        ),
    ]
    own = []
    for gather in gathers[:2]:
        gather.start()
    own.append(
        wire.local(head_sum.at[:, pl.ds(0, columns)], query_all.at[:, seat_columns(here.seat)])
    )
    own.append(
        wire.local(
            head_sum.at[:, pl.ds(columns, pair_all.shape[2])], pair_all.at[here.seat]
        )
    )

    rows.settle(stages - 1, out, False)
    slope_sums[0] = slope[...]
    value = source[...].astype(jnp.float32)
    factor = lax.rsqrt(jnp.mean(value * value, axis=-1, keepdims=True) + EPS)
    slope_sums[0, 0:1, :] = jnp.sum(out[...] * value * factor, axis=0, keepdims=True)
    bits = [("seq", bit) for bit in here.seat_bits] + [("fsdp", bit) for bit in here.plane_bits]
    slope_copies = []

    def slope_send(number):
        axis, bit = bits[number]
        index = here.at(bit) if axis == "seq" else flip(here.plane, bit, here.plane_bits)
        slope_copies.append(
            wire.send(slope_sums.at[number], slope_landing.at[number], {axis: index})
        )

    def slope_add(number):
        slope_copies[number].wait_recv()
        target = slope_out if number == len(bits) - 1 else slope_sums.at[number + 1]
        target[...] = slope_sums[number] + slope_landing[number]

    slope_send(0)
    for step in range(stages + 1, planes):
        outer.step(step)
    join(0)
    gathers[0].hop(1)
    gathers[1].hop(1)
    slope_add(0)
    slope_send(1)
    outer.finish(out_sum)
    gathers[2].start()
    weights[0].forward()
    own_start = (here.core * chips + here.chip) * rows_out
    own.append(
        wire.local(out_sum, outer_all.at[pl.ds(pl.multiple_of(own_start, rows_out), rows_out)])
    )
    join(1)
    for number in range(1, len(bits)):
        slope_add(number)
        if number + 1 < len(bits):
            slope_send(number + 1)
        if number < 3:
            join(number + 1)
        if number == 2:
            gathers[0].hops(2)
            gathers[1].hops(2)
        if number == 3:
            gathers[2].hop(1)
    gathers[2].hops(2)
    weights[1].forward()
    for gather in gathers:
        gather.finish()
    for weight in weights:
        weight.finish()
    for copy in own + stores:
        copy.wait()
    wire.close()
    heads.close()
    outer.close()


class WeightGather:
    def __init__(self, wire, here, finals, near, far, cut=0, cuts=1):
        self.wire, self.here, self.near, self.far = wire, here, near, far
        self.size = finals[0].shape[0]
        self.rows = self.size // cuts
        self.shift = cut * self.rows
        model = near.shape[0]
        self.finals = [final.at[pl.ds(self.shift, self.rows)] for final in finals]
        self.starts = []
        for color, order in enumerate(here.colors()):
            start = color * (model // 2)
            rows = model // 2
            for bit in order[:-1]:
                rows //= 2
                start = start + here.side(bit) * rows
            self.starts.append(start)
        self.swaps, self.kept = [], []

    def _rows(self, start):
        return pl.ds(pl.multiple_of(start + self.shift, self.rows), self.rows)

    def _pass(self, start, source, bit, rows):
        copy = self.wire.send(
            source, self.near.at[self._rows(start)], {"seq": self.here.at(bit)}
        )
        start = start + rows - 2 * rows * self.here.side(bit)
        return (start, self.near.at[self._rows(start)], copy)

    def _swap(self, start, source):
        self.swaps.append(
            self.wire.send(source, self.far.at[self._rows(start)], {"seq": self.here.at(1)})
        )

    def start(self):
        self.held = []
        for color, order in enumerate(self.here.colors()):
            source, start = self.finals[color], self.starts[color]
            pieces = [(start, source, None)]
            if order[:-1]:
                pieces.append(self._pass(start, source, order[-2], self.size))
            self.held.append(pieces)

    def own(self):
        for color in (0, 1):
            source, start = self.finals[color], self.starts[color]
            self._swap(start, source)
            self.kept.append(self.wire.local(source, self.near.at[self._rows(start)]))

    def forward(self):
        for color, order in enumerate(self.here.colors()):
            rest = order[:-1]
            pieces = self.held[color]
            rows = self.size
            for position in range(len(rest) - 1, -1, -1):
                for start, source, copy in pieces:
                    if copy is not None:
                        copy.wait_recv()
                        self._swap(start, source)
                pieces = [(start, source, None) for start, source, _ in pieces]
                rows *= 2
                if position > 0:
                    pieces = pieces + [
                        self._pass(start, source, rest[position - 1], rows)
                        for start, source, _ in pieces
                    ]

    def finish(self):
        for copy in self.swaps:
            copy.wait_recv()
        for copy in self.kept:
            copy.wait()


def widen_kernel(near, far, out):
    core = lax.axis_index("seq") % 2
    units = near.shape[1]
    out[:, pl.ds(pl.multiple_of(core * units, units), units)] = near[...].astype(out.dtype)
    out[:, pl.ds(pl.multiple_of((1 - core) * units, units), units)] = far[...].astype(out.dtype)


def widen_pieces_kernel(count, steps, starts, *refs):
    nears, fars, out = refs[:count], refs[count : 2 * count], refs[-1]
    core = lax.axis_index("seq") % 2
    units = nears[0].shape[1]
    index = pl.program_id(0)
    for number in range(count):

        @pl.when(index // steps == number)
        def _(near=nears[number], far=fars[number]):
            own = pl.ds(pl.multiple_of(core * units, units), units)
            other = pl.ds(pl.multiple_of((1 - core) * units, units), units)
            out[:, own] = near[...].astype(out.dtype)
            out[:, other] = far[...].astype(out.dtype)


def results_kernel(
    copies, width, query, pair, outer, slope, grad_query, grad_key, grad_value, grad_output, *gains
):
    f32 = jnp.float32
    grad_query[...] = query[...].astype(f32)
    grad_output[...] = outer[...].astype(f32)
    columns = 2 * width
    for number in range(pair.shape[0] // (2 * copies)):
        low, high = (
            sum(
                pair[(2 * number + side) * copies + copy].astype(f32) for copy in range(copies)
            )
            for side in (0, 1)
        )
        at = pl.ds(number * columns, columns)
        grad_key[:, at] = pick_lanes(low, pltpu.roll(high, width, 1), width)
        grad_value[:, at] = pick_lanes(pltpu.roll(low, width, 1), high, width)
    in_slope, mid_slope, query_slope, key_slope = gains
    in_slope[...] = slope[0:1, :]
    mid_slope[...] = slope[1:2, :]
    query_slope[...] = slope[2:3, 0:width]
    key_slope[...] = slope[3:4, 0:width]


SENDS, LOCALS = 192, 48


def call(kernel, mesh_sizes, number, inputs, in_vmem, outputs, scratch, out_vmem=None):
    vmem = pl.BlockSpec(memory_space=pltpu.VMEM)
    anywhere = pl.BlockSpec(memory_space=pl.ANY)
    out_vmem = out_vmem or [True] * len(outputs)
    semaphores = [
        pltpu.SemaphoreType.DMA((SENDS,)),
        pltpu.SemaphoreType.DMA((SENDS,)),
        pltpu.SemaphoreType.DMA((LOCALS,)),
    ]
    return pl.pallas_call(
        functools.partial(kernel, *mesh_sizes),
        out_shape=[jax.ShapeDtypeStruct(shape, kind) for shape, kind in outputs],
        in_specs=[vmem if inside else anywhere for inside in in_vmem],
        out_specs=[vmem if inside else anywhere for inside in out_vmem],
        scratch_shapes=[pltpu.VMEM(shape, kind) for shape, kind in scratch] + semaphores,
        compiler_params=pltpu.CompilerParams(
            collective_id=number, has_side_effects=True, vmem_limit_bytes=VMEM_BYTES
        ),
    )(*inputs)


def widen(near, far):
    rows, units = near.shape
    step = min(512, rows)
    return pl.pallas_call(
        widen_kernel,
        grid=(rows // step,),
        out_shape=jax.ShapeDtypeStruct((rows, 2 * units), jnp.float32),
        in_specs=[pl.BlockSpec((step, units), lambda index: (index, 0))] * 2,
        out_specs=pl.BlockSpec((step, 2 * units), lambda index: (index, 0)),
        compiler_params=pltpu.CompilerParams(vmem_limit_bytes=VMEM_BYTES),
        cost_estimate=pl.CostEstimate(
            flops=0, transcendentals=0, bytes_accessed=12 * rows * units
        ),
    )(near, far)


def widen_pieces(pieces, fars, whole=None, into=None):
    rows, units = fars[0].shape
    count = len(fars)
    step = min(512, rows)
    steps = rows // step
    starts = jnp.stack([jnp.asarray(start, jnp.int32) >> (step.bit_length() - 1) for start, _ in pieces])

    def block(number):
        return pl.BlockSpec(
            (step, units),
            lambda index, starts: (jnp.clip(index - number * steps, 0, steps - 1), 0),
        )

    more = () if into is None else (into,)
    return pl.pallas_call(
        functools.partial(widen_pieces_kernel, count, steps),
        out_shape=jax.ShapeDtypeStruct((whole or count * rows, 2 * units), jnp.float32),
        grid_spec=pltpu.PrefetchScalarGridSpec(
            num_scalar_prefetch=1,
            grid=(count * steps,),
            in_specs=[block(number) for number in range(count)] * 2
            + [pl.BlockSpec(memory_space=pl.ANY) for _ in more],
            out_specs=pl.BlockSpec(
                (step, 2 * units), lambda index, starts: (starts[index // steps] + index % steps, 0)
            ),
        ),
        input_output_aliases={2 * count + 1: 0} if more else {},
        compiler_params=pltpu.CompilerParams(vmem_limit_bytes=VMEM_BYTES),
        cost_estimate=pl.CostEstimate(
            flops=0, transcendentals=0, bytes_accessed=12 * count * rows * units
        ),
    )(starts, *[value for _, value in pieces], *fars, *more)


def results(copies, width, query, pair, outer, slope):
    shard, model = query.shape
    seats = pair.shape[0]
    step = min(128, shard)
    f32 = jnp.float32
    pair_cols = seats // copies * width
    row = pl.BlockSpec((step, model), lambda index: (index, 0))
    row_pair = pl.BlockSpec((step, pair_cols), lambda index: (index, 0))
    fixed = lambda *shape: pl.BlockSpec(shape, lambda index: (0, 0))
    return pl.pallas_call(
        functools.partial(results_kernel, copies, width),
        grid=(shard // step,),
        out_shape=[
            jax.ShapeDtypeStruct((shard, model), f32),
            jax.ShapeDtypeStruct((shard, pair_cols), f32),
            jax.ShapeDtypeStruct((shard, pair_cols), f32),
            jax.ShapeDtypeStruct((shard, model), f32),
            jax.ShapeDtypeStruct((1, model), f32),
            jax.ShapeDtypeStruct((1, model), f32),
            jax.ShapeDtypeStruct((1, width), f32),
            jax.ShapeDtypeStruct((1, width), f32),
        ],
        in_specs=[
            row,
            pl.BlockSpec((seats, step, 2 * width), lambda index: (0, index, 0)),
            row,
            fixed(8, model),
        ],
        out_specs=[row, row_pair, row_pair, row]
        + [fixed(1, model), fixed(1, model), fixed(1, width), fixed(1, width)],
        cost_estimate=pl.CostEstimate(
            flops=0, transcendentals=0, bytes_accessed=16 * shard * model
        ),
    )(query, pair, outer, slope)


VMEM_BYTES = 67_000_000


def per_device(
    inputs,
    cotangent,
    attention_gain,
    query_weight,
    key_weight,
    value_weight,
    output_weight,
    query_gain,
    key_gain,
    feedforward_gain,
    gate_weight,
    up_weight,
    down_weight,
):
    tokens = inputs.shape[1]
    model = inputs.shape[2]
    width = query_gain.shape[0]
    pair_heads = key_weight.shape[1] // width
    parts = lax.axis_size("seq")
    planes = lax.axis_size("fsdp")
    sizes = (parts, planes)
    chips = parts // 2
    copies = max(1, parts // pair_heads)
    place = lax.axis_index("seq")
    plane = lax.axis_index("fsdp")
    core = place % 2
    query_cols = model // parts
    head_cols = query_cols + 2 * width
    local_groups = query_cols // width
    shard = query_weight.shape[0]
    piece_rows = shard // parts
    length = parts * tokens
    units = gate_weight.shape[1] // 2
    f32, bf16 = jnp.float32, jnp.bfloat16
    halvings = chips.bit_length() - 2
    last_rows = model // 2 >> halvings
    rows_in = inputs.reshape(tokens, model)
    cot_rows = cotangent.reshape(tokens, model)

    exponents = jnp.arange(width // 2).astype(f32) * 2.0 / width
    rates = jnp.power(jnp.float32(THETA), -exponents)
    rates = jnp.concatenate([rates] * 4)[None, :]
    gain_row = jnp.concatenate([query_gain] * local_groups + [key_gain] * 2)[None, :]
    half = model // 2
    scatter_scratch = [
        ((chips, tokens, model), bf16),
        ((chips, tokens, model), bf16),
        ((2, chips, tokens, half), bf16),
        ((halvings + 1, 2, chips, tokens, half), bf16),
    ]
    mid_gain = feedforward_gain[None, :]
    kept = [
        ((length, model), bf16),
        ((model, head_cols), bf16),
        ((query_cols, model), bf16),
        ((length, head_cols), f32),
        ((length, query_cols), bf16),
        ((length, 2 * width), bf16),
        ((length, query_cols), bf16),
        ((length, 128), f32),
        ((length, 2 * width), f32),
        ((length, 2 * width), f32),
        ((head_cols, head_cols), bf16),
        ((planes, 2, tokens, model), bf16),
    ]
    (
        normed_all,
        head_full,
        out_slice,
        proj,
        queries,
        pair_rows,
        out_rows,
        log_rows,
        cosine,
        sine,
        group,
        middle,
        normed_mid,
        cot_all,
    ) = call(
        functools.partial(front_kernel, width, copies),
        sizes,
        0,
        (
            rows_in,
            cot_rows,
            query_weight,
            key_weight,
            value_weight,
            output_weight,
            attention_gain[None, :],
            mid_gain,
            gain_row,
            rates,
        ),
        (True, True, False, False, False, False, True, True, True, True),
        kept[:11] + [((tokens, model), f32), ((tokens, model), bf16)] + kept[11:],
        kept
        + [((planes, piece_rows, model), bf16)]
        + [((length, 2 * width), bf16)] * 3
        + [((shard, 2 * width), bf16)] * 2
        + scatter_scratch,
        [False] * 11 + [True] * 2 + [False],
    )
    tables = (gain_row, cosine, sine, group)

    quarter = model // 4
    rows_shape = (planes, tokens, model)
    line_scratch = [
        (rows_shape, bf16),
        (rows_shape, bf16),
        ((2, planes - 1, tokens, model), bf16),
    ]
    acts = (2 * planes * tokens, units)
    early = last_rows // 2
    early_piece, late_piece = ((early, units), bf16), ((2 * last_rows - early, units), bf16)
    (
        middle_half,
        mid_slope,
        middle_grad,
        s_down,
        early_a,
        early_b,
        late_a,
        late_b,
        down_give,
        down_keep,
    ) = call(
        feed_kernel,
        sizes,
        2,
        (
            normed_mid,
            mid_gain,
            cot_all.reshape(-1, model),
            middle,
            gate_weight,
            up_weight,
            down_weight,
        ),
        (True, True, False, False, False, False, False),
        [
            ((tokens, model), bf16),
            ((1, model), f32),
            ((tokens, model), f32),
            ((2, last_rows, units), bf16),
            early_piece,
            early_piece,
            late_piece,
            late_piece,
            (rows_shape, bf16),
            (rows_shape, bf16),
        ],
        [((model, units), bf16)] * 3
        + [
            ((2 * planes * tokens, model), bf16),
            ((tokens, model), f32),
            ((tokens, model), f32),
            ((planes, 2, tokens, model), bf16),
            (acts, bf16),
            ((2,) + acts, bf16),
            ((3, 2, quarter, units), bf16),
            ((3, 2, last_rows, units), bf16),
        ]
        + [((3, 2, quarter >> stage, units), bf16) for stage in range(halvings)]
        + [(rows_shape, bf16)]
        + line_scratch,
        [True] * 2 + [False] * 8,
    )

    middle_all, t_down, came_a, came_b, down_sum = call(
        spread_kernel,
        sizes,
        4,
        (middle_half, s_down, early_a, early_b, down_give, down_keep),
        (True, True, False, False, False, False),
        [
            ((length, model), bf16),
            ((2, last_rows, units), bf16),
            early_piece,
            early_piece,
            ((tokens, model), f32),
        ],
        [((length, model), bf16)] + line_scratch,
        [False, True, False, False, True],
    )

    def swap(value, bit):
        return lax.ppermute(value, "seq", [(i, i ^ bit) for i in range(parts)])

    late_a, late_b, middle_all = lax.optimization_barrier((late_a, late_b, middle_all))
    bit_orders = ([2 << i for i in range(halvings + 1)], [chips >> i for i in range(halvings + 1)])
    sent = [early_a, early_b, late_a, late_b]
    came = [came_a, came_b, swap(late_a, bit_orders[0][-1]), swap(late_b, bit_orders[1][-1])]

    vmem = pl.BlockSpec(memory_space=pltpu.VMEM)
    halves, head_part, out_part, head_slopes = pl.pallas_call(
        functools.partial(back_kernel, width),
        out_shape=[
            jax.ShapeDtypeStruct((length, head_cols), bf16),
            jax.ShapeDtypeStruct((model, head_cols), bf16),
            jax.ShapeDtypeStruct((query_cols, model), bf16),
            jax.ShapeDtypeStruct((8, head_cols), f32),
        ],
        in_specs=[vmem] * 12,
        out_specs=[vmem] * 4,
        scratch_shapes=[
            pltpu.VMEM((length, query_cols), bf16),
            pltpu.VMEM((length, query_cols), f32),
            pltpu.VMEM((length, 2 * width), f32),
            pltpu.VMEM((length, 2 * width), f32),
        ]
        + [pltpu.VMEM((3, length, 2 * width), bf16), pltpu.VMEM((length, 2 * width), bf16)],
        compiler_params=pltpu.CompilerParams(vmem_limit_bytes=VMEM_BYTES),
        cost_estimate=pl.CostEstimate(
            flops=10 * length * model * head_cols,
            transcendentals=length * length * local_groups,
            bytes_accessed=16 * length * model,
        ),
    )(
        normed_all,
        middle_all,
        out_slice,
        out_rows,
        log_rows,
        queries,
        pair_rows,
        proj,
        *tables,
    )
    head_part = head_part.reshape(planes, shard, head_cols)
    query_slope = head_slopes[:1, :query_cols].reshape(local_groups, width).sum(axis=0)
    key_slope = head_slopes[0, query_cols : query_cols + width]
    gains = jnp.pad(jnp.stack([query_slope, key_slope]), ((0, 0), (0, model - width)))
    slopes = jnp.concatenate(
        [jnp.zeros_like(mid_slope), mid_slope, gains, jnp.zeros((4, model), f32)], axis=0
    )
    rounds = (parts * planes).bit_length() - 1
    side = ((model, units), bf16)
    piece = ((last_rows, units), bf16)
    in_grad, near_down, far_down, query_all, pair_all, outer_all, slopes, *pieces = call(
        final_kernel,
        sizes,
        5,
        (halves, head_full, head_part, out_part, t_down, rows_in, slopes, *sent, *came),
        (True, True, False, False, True, True, True) + (False,) * 8,
        [
            ((tokens, model), f32),
            side,
            side,
            ((shard, model), bf16),
            ((parts, shard, 2 * width), bf16),
            ((shard, model), bf16),
            ((8, model), f32),
        ]
        + [piece] * 4,
        scatter_scratch
        + [
            ((planes, shard, head_cols), bf16),
            ((2, planes - 1, shard, head_cols), bf16),
            ((planes, piece_rows, model), bf16),
            ((2, planes - 1, piece_rows, model), bf16),
            ((shard, head_cols), bf16),
            ((piece_rows, model), bf16),
            ((4, last_rows, units), bf16),
            ((4, last_rows, units), bf16),
            ((rounds, 8, model), f32),
            ((rounds, 8, model), f32),
        ],
        [True, False, False] + [True] * 4 + [False] * 4,
    )
    pieces, near_down, far_down, in_grad = lax.optimization_barrier(
        (pieces, near_down, far_down, in_grad)
    )
    source = rows_in.astype(f32)
    first = rms_factor(source)
    input_rows = (middle_grad + norm_back(in_grad, source, first, attention_gain)).astype(bf16)

    def plane_pieces(values):
        whole = []
        for color, order in enumerate(bit_orders):
            start, rows = color * (model // 2), model // 2
            for bit in order[:-1]:
                rows //= 2
                start = start + (place // bit) % 2 * rows
            held = [(start, values[color])]
            rows = last_rows
            for bit in order[-2::-1]:
                held = held + [
                    (start + rows - 2 * rows * ((place // bit) % 2), swap(value, bit))
                    for start, value in held
                ]
                rows *= 2
            whole = whole + held
        return whole

    gate_pieces = plane_pieces(pieces[:2])
    grad_down = widen(near_down, far_down)
    (
        grad_query,
        grad_key,
        grad_value,
        grad_output,
        attention_slope,
        feedforward_slope,
        query_slope,
        key_slope,
    ) = results(copies, width, query_all, pair_all, outer_all, slopes)
    block_out = (middle + down_sum).astype(bf16).reshape(1, tokens, model)
    pieces[2:], grad_down = lax.optimization_barrier((pieces[2:], grad_down))
    up_pieces = plane_pieces(pieces[2:])
    written = (grad_down, grad_query, grad_key, grad_value, grad_output, input_rows, block_out)
    gate_pieces, written = lax.optimization_barrier((gate_pieces, written))
    grad_down, grad_query, grad_key, grad_value, grad_output, input_rows, block_out = written
    grad_gate = widen_pieces(gate_pieces, [swap(value, 1) for _, value in gate_pieces])
    own = [up_pieces[0], up_pieces[len(up_pieces) // 2]]
    others = [piece for piece in up_pieces if all(piece is not mine for mine in own)]
    grad_up = widen_pieces(own, [swap(value, 1) for _, value in own], model)
    others, grad_gate, grad_up = lax.optimization_barrier((others, grad_gate, grad_up))
    grad_up = widen_pieces(others, [swap(value, 1) for _, value in others], model, grad_up)
    attention_slope, feedforward_slope = attention_slope[0], feedforward_slope[0]
    query_slope, key_slope = query_slope[0], key_slope[0]
    input_grad = input_rows.reshape(1, tokens, model)
    return (
        block_out,
        input_grad,
        attention_slope,
        grad_query,
        grad_key,
        grad_value,
        grad_output,
        query_slope,
        key_slope,
        feedforward_slope,
        grad_gate,
        grad_up,
        grad_down,
    )


def solution(mesh):
    in_specs = (
        P("fsdp", "seq", None),
        P("fsdp", "seq", None),
        P(),
        P("fsdp", None),
        P("fsdp", None),
        P("fsdp", None),
        P("fsdp", None),
        P(),
        P(),
        P(),
        P(None, "fsdp"),
        P(None, "fsdp"),
        P(None, "fsdp"),
    )
    out_specs = (
        P("fsdp", "seq", None),
        P("fsdp", "seq", None),
        P(),
        P("fsdp", None),
        P("fsdp", None),
        P("fsdp", None),
        P("fsdp", None),
        P(),
        P(),
        P(),
        P(None, "fsdp"),
        P(None, "fsdp"),
        P(None, "fsdp"),
    )
    return jax.shard_map(
        per_device, mesh=mesh, in_specs=in_specs, out_specs=out_specs, check_vma=False
    )
```

```python
import functools

import jax
import jax.numpy as jnp
from jax import lax
from jax.experimental import pallas as pl
from jax.experimental.pallas import tpu as pltpu
from jax.sharding import PartitionSpec as P

EPS = 1e-05
THETA = 1000000.0


def rotate_half(values):
    half = values.shape[-1] // 2
    return jnp.concatenate([-values[..., half:], values[..., :half]], axis=-1)


def rope_tables(positions, width):
    exponents = jnp.arange(width // 2).astype(jnp.float32) * 2.0 / width
    rates = jnp.power(jnp.float32(THETA), -exponents)
    angle = positions.astype(jnp.float32)[:, None] * rates[None, :]
    angle = jnp.concatenate([angle, angle], axis=-1)
    return (jnp.cos(angle), jnp.sin(angle))


def prepare(proj, gain, cosine, sine):
    rows = proj.shape[0]
    width = gain.shape[0]
    split = proj.reshape(rows, -1, width)
    factor = lax.rsqrt(jnp.mean(split * split, axis=-1, keepdims=True) + EPS)
    normed = split * factor * gain
    turned = normed * cosine[:, None, :] + rotate_half(normed) * sine[:, None, :]
    return turned.reshape(rows, -1)


def matmul(left, right):
    return jnp.dot(left, right, preferred_element_type=jnp.float32)


def inner_rows(left, right):
    return lax.dot_general(
        left, right, (((0,), (0,)), ((), ())), preferred_element_type=jnp.float32
    )


def inner_cols(left, right):
    return lax.dot_general(
        left, right, (((1,), (1,)), ((), ())), preferred_element_type=jnp.float32
    )


def rms_factor(values):
    return lax.rsqrt(jnp.mean(values * values, axis=-1, keepdims=True) + EPS)


def norm_back(grad, values, factor, gain):
    scaled = grad * gain
    return factor * (
        scaled - values * factor * factor * jnp.mean(scaled * values, axis=-1, keepdims=True)
    )


def gate_back(hidden_grad, gate, lifted):
    sigma = jax.nn.sigmoid(gate)
    gate_grad = (hidden_grad * lifted * sigma * (1.0 + gate * (1.0 - sigma))).astype(jnp.bfloat16)
    lifted_grad = (hidden_grad * gate * sigma).astype(jnp.bfloat16)
    return (gate_grad, lifted_grad)


def activate(gate, lifted):
    return (gate * jax.nn.sigmoid(gate) * lifted).astype(jnp.bfloat16)


def split_heads(query_rows, pair_rows, groups, width):
    length = query_rows.shape[0]
    key_heads = pair_rows.shape[1] // (2 * width)
    queries = query_rows.reshape(length, key_heads, groups, width)
    keys = pair_rows[:, : key_heads * width].reshape(length, key_heads, width)
    values = pair_rows[:, key_heads * width :].reshape(length, key_heads, width)
    return (queries, keys, values, key_heads)


def attend_heads(query_rows, pair_rows, groups, width):
    length = query_rows.shape[0]
    queries, keys, values, key_heads = split_heads(query_rows, pair_rows, groups, width)
    block = min(512, length)
    scale = width ** (-0.5)
    offsets = jnp.arange(block)

    def query_step(index, state):
        out_rows, log_rows = state
        query_block = lax.dynamic_slice_in_dim(queries, index * block, block, 0)

        def key_step(inner, carry):
            summed, total = carry
            key_block = lax.dynamic_slice_in_dim(keys, inner * block, block, 0)
            value_block = lax.dynamic_slice_in_dim(values, inner * block, block, 0)
            scores = (
                jnp.einsum(
                    "qhgd,shd->hgqs", query_block, key_block, preferred_element_type=jnp.float32
                )
                * scale
            )
            allowed = (index * block + offsets)[:, None] >= (inner * block + offsets)[None, :]
            weights = jnp.where(allowed, jnp.exp(scores), 0.0)
            summed = summed + jnp.einsum(
                "hgqs,shd->hgqd",
                weights.astype(jnp.bfloat16),
                value_block,
                preferred_element_type=jnp.float32,
            )
            return (summed, total + jnp.sum(weights, axis=-1))

        initial = (
            jnp.zeros((key_heads, groups, block, width), jnp.float32),
            jnp.zeros((key_heads, groups, block), jnp.float32),
        )
        summed, total = lax.fori_loop(0, index + 1, key_step, initial)
        result = (summed / total[..., None]).astype(jnp.bfloat16)
        result = result.transpose(2, 0, 1, 3).reshape(block, key_heads * groups * width)
        out_rows = lax.dynamic_update_slice_in_dim(out_rows, result, index * block, 0)
        log_rows = lax.dynamic_update_slice_in_dim(log_rows, jnp.log(total), index * block, 2)
        return (out_rows, log_rows)

    start = (
        jnp.zeros((length, key_heads * groups * width), jnp.bfloat16),
        jnp.zeros((key_heads, groups, length), jnp.float32),
    )
    return lax.fori_loop(0, length // block, query_step, start)


def attend_back(query_rows, pair_rows, out_rows, log_rows, grad_rows, groups, width):
    length = query_rows.shape[0]
    queries, keys, values, key_heads = split_heads(query_rows, pair_rows, groups, width)
    outs = out_rows.reshape(length, key_heads, groups, width)
    grads = grad_rows.reshape(length, key_heads, groups, width)
    correction = jnp.sum(grads.astype(jnp.float32) * outs.astype(jnp.float32), axis=-1)
    block = min(512, length)
    scale = width ** (-0.5)
    offsets = jnp.arange(block)

    def query_step(index, state):
        query_grad, key_grad, value_grad = state
        query_block = lax.dynamic_slice_in_dim(queries, index * block, block, 0)
        grad_block = lax.dynamic_slice_in_dim(grads, index * block, block, 0)
        shift_block = lax.dynamic_slice_in_dim(correction, index * block, block, 0).transpose(
            1, 2, 0
        )
        log_block = lax.dynamic_slice_in_dim(log_rows, index * block, block, 2)

        def key_step(inner, carry):
            block_grad, key_sum, value_sum = carry
            key_block = lax.dynamic_slice_in_dim(keys, inner * block, block, 0)
            value_block = lax.dynamic_slice_in_dim(values, inner * block, block, 0)
            scores = (
                jnp.einsum(
                    "qhgd,shd->hgqs", query_block, key_block, preferred_element_type=jnp.float32
                )
                * scale
            )
            allowed = (index * block + offsets)[:, None] >= (inner * block + offsets)[None, :]
            weights = jnp.where(allowed, jnp.exp(scores - log_block[..., None]), 0.0)
            value_part = jnp.einsum(
                "hgqs,qhgd->shd",
                weights.astype(jnp.bfloat16),
                grad_block,
                preferred_element_type=jnp.float32,
            )
            prob_grad = jnp.einsum(
                "qhgd,shd->hgqs", grad_block, value_block, preferred_element_type=jnp.float32
            )
            score_grad = (weights * (prob_grad - shift_block[..., None]) * scale).astype(
                jnp.bfloat16
            )
            block_grad = block_grad + jnp.einsum(
                "hgqs,shd->qhgd", score_grad, key_block, preferred_element_type=jnp.float32
            )
            key_part = jnp.einsum(
                "hgqs,qhgd->shd", score_grad, query_block, preferred_element_type=jnp.float32
            )
            key_sum = lax.dynamic_update_slice_in_dim(
                key_sum,
                lax.dynamic_slice_in_dim(key_sum, inner * block, block, 0) + key_part,
                inner * block,
                0,
            )
            value_sum = lax.dynamic_update_slice_in_dim(
                value_sum,
                lax.dynamic_slice_in_dim(value_sum, inner * block, block, 0) + value_part,
                inner * block,
                0,
            )
            return (block_grad, key_sum, value_sum)

        initial = (jnp.zeros((block, key_heads, groups, width), jnp.float32), key_grad, value_grad)
        block_grad, key_grad, value_grad = lax.fori_loop(0, index + 1, key_step, initial)
        query_grad = lax.dynamic_update_slice_in_dim(query_grad, block_grad, index * block, 0)
        return (query_grad, key_grad, value_grad)

    state = (
        jnp.zeros((length, key_heads, groups, width), jnp.float32),
        jnp.zeros((length, key_heads, width), jnp.float32),
        jnp.zeros((length, key_heads, width), jnp.float32),
    )
    query_grad, key_grad, value_grad = lax.fori_loop(0, length // block, query_step, state)
    pair_grad = jnp.concatenate(
        [
            key_grad.reshape(length, key_heads * width),
            value_grad.reshape(length, key_heads * width),
        ],
        axis=1,
    )
    return (query_grad.reshape(length, key_heads * groups * width), pair_grad)


MESH = pl.DeviceIdType.MESH


def flip(index, mask, bits):
    for bit in bits:
        if mask & bit:
            index = index + bit - 2 * bit * ((index // bit) % 2)
    return index


class Place:
    def __init__(self, parts, planes):
        self.parts, self.planes = parts, planes
        self.seat = lax.axis_index("seq")
        self.plane = lax.axis_index("fsdp")
        self.core = self.seat % 2
        self.chip = self.seat // 2
        self.seat_bits = [1 << i for i in range(parts.bit_length() - 1)]
        self.chip_bits = self.seat_bits[1:]
        self.plane_bits = [1 << i for i in range(planes.bit_length() - 1)]

    def at(self, mask):
        return flip(self.seat, mask, self.seat_bits)

    def side(self, bit):
        return (self.seat // bit) % 2

    def colors(self):
        return (self.chip_bits, self.chip_bits[::-1])

    def enter(self, masks=(), line=False, plane_masks=()):
        barrier = pltpu.get_barrier_semaphore()
        peers = [{"seq": self.at(mask)} for mask in masks]
        if line:
            peers.append({"fsdp": (self.plane + 1) % self.planes})
            peers.append({"fsdp": (self.plane + self.planes - 1) % self.planes})
        for mask in plane_masks:
            peers.append({"fsdp": flip(self.plane, mask, self.plane_bits)})
        for peer in peers:
            pl.semaphore_signal(barrier, inc=1, device_id=peer, device_id_type=MESH)
        pl.semaphore_wait(barrier, len(peers))


class Wire:
    def __init__(self, sends, receives, locals_):
        self.sends, self.receives, self.locals = sends, receives, locals_
        self.count = self.local_count = 0
        self.open = []

    def remote(self, source, target, device):
        number = self.count
        self.count += 1
        return pltpu.make_async_remote_copy(
            src_ref=source,
            dst_ref=target,
            send_sem=self.sends.at[number],
            recv_sem=self.receives.at[number],
            device_id=device,
            device_id_type=MESH,
        )

    def send(self, source, target, device):
        copy = self.remote(source, target, device)
        copy.start()
        self.open.append(copy)
        return copy

    def quiet(self, source, target):
        number = self.local_count
        self.local_count += 1
        return pltpu.make_async_copy(source, target, self.locals.at[number])

    def local(self, source, target):
        copy = self.quiet(source, target)
        copy.start()
        return copy

    def sent(self, copy):
        copy.wait_send()
        self.open = [other for other in self.open if other is not copy]

    def close(self):
        for copy in self.open:
            copy.wait_send()


def add_rows(target, left, right, step=64):
    rows = target.shape[0]
    step = min(step, rows)

    def body(index, carry):
        at = pl.ds(pl.multiple_of(index * step, step), step)
        total = left[at, :].astype(jnp.float32) + right[at, :].astype(jnp.float32)
        target[at, :] = total.astype(target.dtype)
        return carry

    lax.fori_loop(0, rows // step, body, 0)


class LineGather:
    def __init__(self, wire, here, source, target, share=None):
        self.here = here
        planes, plane = here.planes, here.plane
        above = {"fsdp": (plane + 1) % planes}
        below = {"fsdp": (plane + planes - 1) % planes}
        self.ups, self.downs = {}, {}
        for step in range(1, planes):
            lower = (plane + planes - step + 1) % planes
            upper = (plane + step - 1) % planes
            first = step == 1
            self.ups[step] = wire.remote(
                source if first else target(lower), target(lower), above
            )
            self.downs[step] = wire.remote(
                source if first else target(upper), target(upper), below
            )
        self.shared = {}
        if share is not None:
            for step in range(1, planes):
                for way, shift in ((0, planes - step), (1, step)):
                    index = (plane + shift) % planes
                    self.shared[(step, way)] = wire.remote(
                        target(index), share(index), {"seq": here.at(1)}
                    )

    def start(self, step):
        planes, plane = self.here.planes, self.here.plane

        @pl.when((plane >= step - 1) & (plane <= planes - 2))
        def _():
            self.ups[step].start()

        @pl.when((plane + step <= planes) & (plane >= 1))
        def _():
            self.downs[step].start()

    def arrive(self, step):
        planes, plane = self.here.planes, self.here.plane

        @pl.when(plane >= step)
        def _():
            self.ups[step].wait_recv()
            if self.shared:
                self.shared[(step, 0)].start()

        @pl.when(plane + step <= planes - 1)
        def _():
            self.downs[step].wait_recv()
            if self.shared:
                self.shared[(step, 1)].start()

    def close(self, shared_taken=False):
        planes, plane = self.here.planes, self.here.plane
        for (step, way), copy in self.shared.items():

            @pl.when(plane >= step if way == 0 else plane + step <= planes - 1)
            def _(copy=copy):
                copy.wait_send()
                if not shared_taken:
                    copy.wait_recv()

        for step in range(1, planes):

            @pl.when((plane >= step - 1) & (plane <= planes - 2))
            def _(step=step):
                self.ups[step].wait_send()

            @pl.when((plane + step <= planes) & (plane >= 1))
            def _(step=step):
                self.downs[step].wait_send()


class Lines:
    def __init__(self, members):
        self.members = members

    def start(self, step):
        for member in self.members:
            member.start(step)

    def pass_on(self, step):
        for member in self.members:
            member.arrive(step)
            if step + 1 < member.here.planes:
                member.start(step + 1)

    def step(self, step):
        for member in self.members:
            member.step(step)

    def close(self, *options):
        for member in self.members:
            member.close(*options)


def gather_lines(wire, here, source, target, share=None, cuts=2):
    rows = source.shape[0] // cuts
    members = []
    for cut in range(cuts):
        at = pl.ds(cut * rows, rows)
        members.append(
            LineGather(
                wire,
                here,
                source.at[at],
                lambda index, at=at: target(index).at[at],
                None if share is None else lambda index, at=at: share(index).at[at],
            )
        )
    return Lines(members)


class LineScatter:
    def __init__(self, wire, here, term, landing):
        self.wire, self.here, self.term, self.landing = wire, here, term, landing
        planes, plane = here.planes, here.plane
        above = {"fsdp": (plane + 1) % planes}
        below = {"fsdp": (plane + planes - 1) % planes}
        self.ups, self.downs = {}, {}
        for step in range(1, planes):
            self.ups[step] = wire.remote(
                term((plane + planes - step) % planes), landing(0, step - 1), above
            )
            self.downs[step] = wire.remote(
                term((plane + step) % planes), landing(1, step - 1), below
            )

    def step(self, step):
        planes, plane = self.here.planes, self.here.plane
        mirror = planes - 1 - plane
        for way, (position, copies, dest) in enumerate(
            (
                (plane, self.ups, (plane + planes - step) % planes),
                (mirror, self.downs, (plane + step) % planes),
            )
        ):
            if step > 1:

                @pl.when((position >= 1) & (position <= step - 1))
                def _(way=way, copies=copies, dest=dest):
                    copies[step - 1].wait_recv()
                    term = self.term(dest)
                    add_rows(term, term, self.landing(way, step - 2))

            @pl.when(position <= step - 1)
            def _(copies=copies):
                copies[step].start()

    def finish(self, out):
        planes, plane = self.here.planes, self.here.plane
        own = self.term(plane)
        last = planes - 1

        @pl.when(plane >= 1)
        def _():
            self.ups[last].wait_recv()

        @pl.when(plane <= planes - 2)
        def _():
            self.downs[last].wait_recv()

        @pl.when(plane == 0)
        def _():
            add_rows(out, own, self.landing(1, last - 1))

        @pl.when(plane == planes - 1)
        def _():
            add_rows(out, own, self.landing(0, last - 1))

        @pl.when((plane >= 1) & (plane <= planes - 2))
        def _():
            add_rows(own, own, self.landing(0, last - 1))
            add_rows(out, own, self.landing(1, last - 1))

    def close(self):
        planes, plane = self.here.planes, self.here.plane
        mirror = planes - 1 - plane
        for step in range(1, planes):

            @pl.when(plane <= step - 1)
            def _(step=step):
                self.ups[step].wait_send()

            @pl.when(mirror <= step - 1)
            def _(step=step):
                self.downs[step].wait_send()


class PlaneGather:
    def __init__(self, wire, here, source, target):
        self.wire, self.here, self.source, self.target = wire, here, source, target
        self.incoming = {}

    def _send(self, mask, color, bit):
        here = self.here
        target = self.target(here.at(mask), color)
        source = self.source(color) if mask == 0 else target
        self.incoming[(mask ^ bit, color)] = self.wire.send(
            source, target, {"seq": here.at(bit)}
        )

    def start(self):
        for position in range(len(self.here.chip_bits)):
            for color, bits in enumerate(self.here.colors()):
                self._send(0, color, bits[position])
        for color in (0, 1):
            self._send(0, color, 1)

    def hop(self, hops):
        here = self.here
        chips = here.parts // 2
        for mask in (mask * 2 for mask in range(1, chips)):
            if bin(mask).count("1") != hops:
                continue
            for color, bits in enumerate(here.colors()):
                self.incoming[(mask, color)].wait_recv()
                last = max(i for i, bit in enumerate(bits) if mask & bit)
                for bit in bits[last + 1 :]:
                    self._send(mask, color, bit)
                self._send(mask, color, 1)

    def hops(self, first=1):
        for hops in range(first, len(self.here.chip_bits) + 1):
            self.hop(hops)

    def finish(self):
        for mask in range(1, self.here.parts, 2):
            for color in (0, 1):
                self.incoming[(mask, color)].wait_recv()


class PlaneScatter:
    def __init__(self, wire, here, product, give, take, current, landing, model):
        self.wire, self.here, self.product = wire, here, product
        self.give, self.take, self.current, self.landing = give, take, current, landing
        self.model = model

    def start(self):
        here = self.here
        chips = here.parts // 2
        self.swaps = {}
        tokens = self.give.shape[1]
        seats = [2 * flip(here.chip, mask, [b // 2 for b in here.chip_bits]) for mask in range(chips)]
        for part in range(self.model // 512):
            columns = slice(part * 512, (part + 1) * 512)
            rows = self.product([seat + 1 - here.core for seat in seats], columns)
            for mask in range(chips):
                self.give[mask, :, columns] = rows[mask * tokens : (mask + 1) * tokens].astype(
                    self.give.dtype
                )
        for mask in range(chips)[::-1]:
            self.swaps[mask] = self.wire.send(
                self.give.at[mask], self.take.at[mask], {"seq": here.at(1)}
            )
        half = self.model // 2
        for part in range(self.model // 512):
            columns = slice(part * 512, (part + 1) * 512)
            rows = self.product([seat + here.core for seat in seats], columns)
            color, inside = divmod(part * 512, half)
            for mask in range(chips):
                self.current[color, mask, :, inside : inside + 512] = rows[
                    mask * tokens : (mask + 1) * tokens
                ].astype(self.current.dtype)

    def join(self):
        half = self.model // 2
        chips = self.here.parts // 2
        for mask in range(chips)[::-1]:
            self.swaps[mask].wait_recv()
            for color in (0, 1):
                mine = self.current.at[color, mask]
                add_rows(mine, mine, self.take.at[mask, :, pl.ds(color * half, half)])

    def stage(self, position):
        here = self.here
        self.moved = getattr(self, "moved", {})
        for onward in (True, False):
            for color, bits in enumerate(here.colors()):
                bit = bits[position]
                done = sum(bits[:position])
                for mask in range(here.parts // 2):
                    low = mask ^ (bit // 2)
                    if not mask * 2 & bit or mask * 2 & done:
                        continue
                    if self._onward(position, color, low) != onward:
                        continue
                    self.moved[(position, color, low)] = self.wire.send(
                        self.current.at[color, mask],
                        self.landing.at[position, color, low],
                        {"seq": here.at(bit)},
                    )

    def _onward(self, position, color, low):
        bits = self.here.colors()[color]
        return position + 1 < len(bits) and bool(low * 2 & bits[position + 1])

    def settle(self, position, out, onward):
        half = self.model // 2
        last = position == len(self.here.chip_bits) - 1
        for (stage, color, low), copy in self.moved.items():
            if stage != position or self._onward(position, color, low) != onward:
                continue
            copy.wait_recv()
            mine = self.current.at[color, low]
            target = out.at[:, pl.ds(color * half, half)] if last else mine
            add_rows(target, mine, self.landing.at[position, color, low])


def pick_lanes(low, high, width):
    lane = lax.broadcasted_iota(jnp.int32, low.shape, low.ndim - 1)
    return jnp.where(lane % (2 * width) < width, low, high)


def group_mean(values, group, width):
    high = values.astype(jnp.bfloat16)
    low = (values - high.astype(jnp.float32)).astype(jnp.bfloat16)
    total = jnp.dot(high, group, preferred_element_type=jnp.float32) + jnp.dot(
        low, group, preferred_element_type=jnp.float32
    )
    return total * (1.0 / width)


def turn(values, width):
    lanes = values.shape[1]
    half = width // 2
    return pick_lanes(
        pltpu.roll(values, lanes - half, 1), pltpu.roll(values, half, 1), half
    )


def attend_block(index, block, width, heads, queries, pair, twin, left, right, out_rows, logs):
    rows = pl.ds(index * block, block)
    before = index * block
    columns = 2 * width
    row = lax.broadcasted_iota(jnp.int32, (block, block), 0)
    column = lax.broadcasted_iota(jnp.int32, (block, block), 1)
    allowed = row >= column
    contract = (((1,), (1,)), ((), ()))
    lane = lax.broadcasted_iota(jnp.int32, (block, 128), 1)

    def two_heads(number, table):
        at = pl.ds(pl.multiple_of(number * columns, columns), columns)
        both = queries[rows, at]
        both = (both.astype(jnp.float32) * width**-0.5).astype(both.dtype)
        zero = jnp.zeros_like(both)
        result = None
        for side, values in ((0, left), (1, right)):
            mine = pick_lanes(both, zero, width) if side == 0 else pick_lanes(zero, both, width)
            scores = lax.dot_general(
                mine, twin[rows, :], contract, preferred_element_type=jnp.float32
            )
            weights = jnp.where(allowed, jnp.exp(scores), 0.0)
            total = jnp.sum(weights, axis=1, keepdims=True)
            summed = jnp.dot(
                weights.astype(jnp.bfloat16), values[rows, :], preferred_element_type=jnp.float32
            )
            if before:
                scores = lax.dot_general(
                    mine, twin[0:before, :], contract, preferred_element_type=jnp.float32
                )
                weights = jnp.exp(scores)
                total = total + jnp.sum(weights, axis=1, keepdims=True)
                summed = summed + jnp.dot(
                    weights.astype(jnp.bfloat16),
                    values[0:before, :],
                    preferred_element_type=jnp.float32,
                )
            table = jnp.where(lane == 2 * number + side, total, table)
            part = summed / total
            result = part if result is None else result + part
        out_rows[rows, at] = result.astype(out_rows.dtype)
        return table

    table = lax.fori_loop(0, heads // 2, two_heads, jnp.ones((block, 128), jnp.float32))
    logs[rows, :] = jnp.log(table)


def back_block(
    index, block, width, heads, queries, grads, outs, logs, keys, values, query_back, key_back, value_back
):
    rows = pl.ds(index * block, block)
    before = index * block
    scale = width**-0.5
    row = lax.broadcasted_iota(jnp.int32, (block, block), 0)
    column = lax.broadcasted_iota(jnp.int32, (block, block), 1)
    allowed = row >= column
    lane = lax.broadcasted_iota(jnp.int32, (block, 2 * width), 1)
    across = (((1,), (1,)), ((), ()))
    down = (((0,), (0,)), ((), ()))
    f32 = jnp.float32
    spans = [(rows, True)] + ([(slice(0, before), False)] if before else [])

    def one_head(head, carry):
        number, side = head // 2, head % 2
        at = pl.ds(pl.multiple_of(number * 2 * width, 2 * width), 2 * width)
        mine = lane // width == side
        query = jnp.where(mine, queries[rows, at], 0)
        grad = jnp.where(mine, grads[rows, at], 0)
        scaled = (query.astype(f32) * scale).astype(query.dtype)
        shift = jnp.sum(grad.astype(f32) * outs[rows, at].astype(f32), axis=1, keepdims=True)
        log = jnp.sum(jnp.where(lane == head, logs[rows, :], 0.0), axis=1, keepdims=True)
        total = query_back[rows, at]
        for span, masked in spans:
            scores = lax.dot_general(
                scaled, keys[0, span, :], across, preferred_element_type=f32
            )
            weights = jnp.exp(scores - log)
            if masked:
                weights = jnp.where(allowed, weights, 0.0)
            prob_grad = lax.dot_general(
                grad, values[span, :], across, preferred_element_type=f32
            )
            score_grad = (weights * (prob_grad - shift) * scale).astype(query.dtype)
            total = total + jnp.dot(
                score_grad, keys[1 + side, span, :], preferred_element_type=f32
            )
            key_back[span, :] += lax.dot_general(
                score_grad, query, down, preferred_element_type=f32
            )
            value_back[span, :] += lax.dot_general(
                weights.astype(query.dtype), grad, down, preferred_element_type=f32
            )
        query_back[rows, at] = total
        return carry

    lax.fori_loop(0, heads, one_head, 0)


def back_kernel(
    width,
    normed,
    middle,
    out_slice,
    outs,
    logs,
    queries,
    pair,
    proj,
    gain,
    cosine,
    sine,
    group,
    halves,
    head_part,
    out_part,
    slopes,
    grads,
    query_back,
    key_back,
    value_back,
    keys,
    values,
):
    length = normed.shape[0]
    block = min(256, length)
    blocks = length // block
    query_cols = queries.shape[1]
    heads = query_cols // width
    f32 = jnp.float32
    query_back[...] = jnp.zeros_like(query_back)
    key_back[...] = jnp.zeros_like(key_back)
    value_back[...] = jnp.zeros_like(value_back)

    def ready(index, carry):
        at = pl.ds(pl.multiple_of(index * block, block), block)
        grads[at, :] = lax.dot_general(
            middle[at, :], out_slice[...], (((1,), (1,)), ((), ())), preferred_element_type=f32
        ).astype(grads.dtype)
        both = pair[at, :].astype(f32)
        swapped = pltpu.roll(both, width, 1)
        zero = jnp.zeros_like(both)
        keys[0, at, :] = pick_lanes(both, swapped, width).astype(keys.dtype)
        keys[1, at, :] = pick_lanes(both, zero, width).astype(keys.dtype)
        keys[2, at, :] = pick_lanes(zero, swapped, width).astype(keys.dtype)
        values[at, :] = pick_lanes(swapped, both, width).astype(values.dtype)
        return carry

    lax.fori_loop(0, blocks, ready, 0)
    for index in range(blocks):
        back_block(
            index,
            block,
            width,
            heads,
            queries,
            grads,
            outs,
            logs,
            keys,
            values,
            query_back,
            key_back,
            value_back,
        )

    def norms(index, slope):
        at = pl.ds(pl.multiple_of(index * block, block), block)
        key_sum, value_sum = key_back[at, :], value_back[at, :]
        key_sum = key_sum + pltpu.roll(key_sum, width, 1)
        value_sum = value_sum + pltpu.roll(value_sum, width, 1)
        back = jnp.concatenate(
            [query_back[at, :], pick_lanes(key_sum, value_sum, width)], axis=1
        )
        value = proj[at, :]
        factor = lax.rsqrt(group_mean(value * value, group[...], width) + EPS)
        repeat = value.shape[1] // cosine.shape[1]
        cosines = jnp.concatenate([cosine[at, :]] * repeat, axis=1)
        sines = jnp.concatenate([sine[at, :]] * repeat, axis=1)
        turned = back * cosines + turn(back * sines, width)
        slope = slope + jnp.sum(turned * value * factor, axis=0, keepdims=True)
        scaled = turned * gain[...]
        result = factor * (
            scaled - value * factor * factor * group_mean(scaled * value, group[...], width)
        )
        lane = lax.broadcasted_iota(jnp.int32, back.shape, 1)
        result = jnp.where(lane >= query_cols + width, back, result)
        halves[at, :] = result.astype(halves.dtype)
        return slope

    slope = lax.fori_loop(0, blocks, norms, jnp.zeros((1, proj.shape[1]), f32))
    slopes[...] = jnp.broadcast_to(slope, slopes.shape)

    def terms(number, carry):
        at = pl.ds(pl.multiple_of(number * 256, 256), 256)
        down = (((0,), (0,)), ((), ()))
        head_part[at, :] = lax.dot_general(
            normed[:, at], halves[...], down, preferred_element_type=f32
        ).astype(head_part.dtype)
        out_part[:, at] = lax.dot_general(
            outs[...], middle[:, at], down, preferred_element_type=f32
        ).astype(out_part.dtype)
        return carry

    lax.fori_loop(0, normed.shape[1] // 256, terms, 0)


def row_blocks(rows, step, work):
    def body(index, carry):
        work(pl.ds(pl.multiple_of(index * step, step), step))
        return carry

    lax.fori_loop(0, rows // step, body, 0)


def front_kernel(
    width,
    copies,
    parts,
    planes,
    x,
    c,
    query_weight,
    key_weight,
    value_weight,
    output_weight,
    in_gain,
    mid_gain,
    gain,
    rates,
    x_store,
    w_store,
    o_store,
    proj_store,
    query_store,
    pair_store,
    out_store,
    log_store,
    cosine_store,
    sine_store,
    group_store,
    middle,
    mid,
    c_store,
    x_all,
    w_all,
    o_slice,
    proj,
    queries,
    pair,
    out_rows,
    logs,
    cosine,
    sine,
    group,
    c_all,
    o_all,
    twin,
    left,
    right,
    key_block,
    value_block,
    give,
    take,
    current,
    landing,
    *sems,
):
    here = Place(parts, planes)
    wire = Wire(*sems)
    tokens, model = x.shape
    shard = query_weight.shape[0]
    query_cols = queries.shape[1]
    rows = o_all.shape[1]
    half = tokens // 2
    chips = parts // 2
    f32 = jnp.float32
    chip_masks = [mask * 2 for mask in range(1, chips)]
    pair_head = here.seat // copies
    own_shard = pl.ds(pl.multiple_of(here.plane * shard, shard), shard)
    head_block = pl.ds(pl.multiple_of(pair_head // 2 * 2 * width, 2 * width), 2 * width)
    loads = [
        wire.local(key_weight.at[:, head_block], key_block),
        wire.local(value_weight.at[:, head_block], value_block),
        wire.local(
            query_weight.at[:, pl.ds(pl.multiple_of(here.seat * query_cols, query_cols), query_cols)],
            w_all.at[own_shard, pl.ds(0, query_cols)],
        ),
    ]
    piece = (here.core * chips + here.chip) * rows
    o = output_weight.at[pl.ds(pl.multiple_of(piece, rows), rows)]
    here.enter(chip_masks + [1], line=True)
    o_own = wire.local(o, o_all.at[here.plane])
    for load in loads[:2]:
        load.wait()
    upper = (pair_head % 2) * jnp.ones((1, 1), jnp.int32)
    keys, values = key_block[...].astype(f32), value_block[...].astype(f32)
    keys = jnp.where(upper == 1, pltpu.roll(keys, width, 1), keys)
    values = jnp.where(upper == 1, values, pltpu.roll(values, width, 1))
    w_all[own_shard, query_cols:] = pick_lanes(keys, values, width).astype(w_all.dtype)
    loads[2].wait()
    weights = gather_lines(
        wire,
        here,
        w_all.at[own_shard],
        lambda index: w_all.at[pl.ds(pl.multiple_of(index * shard, shard), shard)],
    )
    weights.start(1)

    def norm_rows(at):
        value = x[at, :].astype(f32)
        factor = lax.rsqrt(jnp.mean(value * value, axis=-1, keepdims=True) + EPS)
        own_at = pl.ds(pl.multiple_of(here.seat * tokens + at.start, 32), 32)
        x_all[own_at, :] = (value * factor * in_gain[...]).astype(x_all.dtype)

    row_blocks(tokens, 32, norm_rows)

    def seat_rows(seat, color):
        return x_all.at[pl.ds(pl.multiple_of(seat * tokens + color * half, half), half)]

    plane_rows = PlaneGather(
        wire, here, lambda color: seat_rows(here.seat, color), seat_rows
    )
    plane_rows.start()
    outer = gather_lines(wire, here, o, lambda index: o_all.at[index])

    def c_spot(index):
        return c_all.at[index, here.core]

    cots = gather_lines(wire, here, c, c_spot, c_spot)
    c_own = wire.local(c, c_spot(here.plane))

    lane = lax.broadcasted_iota(jnp.int32, (32, 2 * width), 1)
    row = lax.broadcasted_iota(jnp.int32, (32, 2 * width), 0)
    sign = jnp.where(lane % width < width // 2, -1.0, 1.0)

    def table_rows(at):
        angle = (row + at.start).astype(f32) * rates[...]
        cosine[at, :] = jnp.cos(angle)
        sine[at, :] = jnp.sin(angle) * sign

    columns = group.shape[0]
    group[...] = jnp.where(
        lax.broadcasted_iota(jnp.int32, (columns, columns), 0) // width
        == lax.broadcasted_iota(jnp.int32, (columns, columns), 1) // width,
        1.0,
        0.0,
    ).astype(group.dtype)
    length = x_all.shape[0]
    row_blocks(length, 32, table_rows)
    weights.members[0].arrive(1)
    if planes > 2:
        weights.members[0].start(2)
    plane_rows.hop(1)
    weights.members[1].arrive(1)
    if planes > 2:
        weights.members[1].start(2)
    outer.start(1)
    plane_rows.hops(2)
    spot = o_slice.at[pl.ds(pl.multiple_of(here.chip * rows, rows), rows)]
    deals = []
    for mask in chip_masks:
        chip = here.at(mask) // 2
        deals.append((chip, wire.remote(o_all.at[chip], spot, {"seq": here.at(mask)})))
    keep_own = wire.quiet(o_all.at[here.chip], spot)

    def deal(step):
        for chip, copy in deals + [(here.chip, keep_own)]:

            @pl.when((chip == here.plane + step) | (chip + step == here.plane))
            def _(copy=copy):
                copy.start()

    o_own.wait()
    deal(0)
    plane_rows.finish()
    block = min(256, length)
    blocks = length // block

    for step in range(2, planes):
        weights.pass_on(step)
    stores = [
        wire.local(x_all, x_store),
        wire.local(w_all, w_store),
        wire.local(cosine, cosine_store),
        wire.local(sine, sine_store),
        wire.local(group, group_store),
    ]
    heads = query_cols // width

    def project(index, carry):
        at = pl.ds(pl.multiple_of(index * block, block), block)
        value = jnp.dot(x_all[at, :], w_all[...], preferred_element_type=f32)
        proj[at, :] = value
        factor = lax.rsqrt(group_mean(value * value, group[...], width) + EPS)
        normed = value * factor * gain[...]
        repeat = value.shape[1] // cosine.shape[1]
        cosines = jnp.concatenate([cosine[at, :]] * repeat, axis=1)
        sines = jnp.concatenate([sine[at, :]] * repeat, axis=1)
        turned = normed * cosines + turn(normed, width) * sines
        queries[at, :] = turned[:, :query_cols].astype(queries.dtype)
        keys, values = turned[:, query_cols:], value[:, query_cols:]
        both = pick_lanes(keys, values, width)
        pair[at, :] = both.astype(pair.dtype)
        swapped = pltpu.roll(both, width, 1)
        twin[at, :] = pick_lanes(both, swapped, width).astype(twin.dtype)
        zero = jnp.zeros_like(both)
        left[at, :] = pick_lanes(swapped, zero, width).astype(left.dtype)
        right[at, :] = pick_lanes(zero, both, width).astype(right.dtype)
        return carry

    def outer_step(step):
        outer.pass_on(step)
        deal(step)
        if step == min(2, planes - 1):
            cots.start(1)

    outer_step(1)
    lax.fori_loop(0, blocks, project, 0)
    across = wire.send(c, c_spot(here.plane), {"seq": here.at(1)})
    waits = list(range(2, planes))
    cot_waits = list(range(1, planes))
    for index in range(blocks):
        while waits and (waits[0] - 1) * blocks <= (index + 1) * planes:
            outer_step(waits.pop(0))
        attend_block(
            index, block, width, heads, queries, pair, twin, left, right, out_rows, logs
        )
    for step in waits:
        outer_step(step)
    cots.pass_on(cot_waits.pop(0))
    keep_own.wait()
    for _, copy in deals:
        copy.wait()

    def product(seats, at):
        chosen = [
            out_rows[pl.ds(pl.multiple_of(seat * tokens, tokens), tokens), :] for seat in seats
        ]
        return jnp.dot(
            jnp.concatenate(chosen, axis=0), o_slice[:, at], preferred_element_type=f32
        )

    stores += [
        wire.local(o_slice, o_store),
        wire.local(proj, proj_store),
        wire.local(queries, query_store),
        wire.local(pair, pair_store),
        wire.local(out_rows, out_store),
        wire.local(logs, log_store),
    ]
    sums = PlaneScatter(wire, here, product, give, take, current, landing, model)
    sums.start()
    sums.join()
    sums.stage(0)
    stages = len(here.chip_bits)
    for stage in range(stages):
        sums.settle(stage, middle, True)
        if stage + 1 < stages:
            sums.stage(stage + 1)
        if cot_waits:
            cots.pass_on(cot_waits.pop(0))
        sums.settle(stage, middle, False)

    def mid_rows(at):
        value = x[at, :].astype(f32) + middle[at, :]
        middle[at, :] = value
        factor = lax.rsqrt(jnp.mean(value * value, axis=-1, keepdims=True) + EPS)
        mid[at, :] = (value * factor * mid_gain[...]).astype(mid.dtype)

    for step in cot_waits:
        cots.pass_on(step)
    cots.close()
    c_own.wait()
    across.wait_recv()
    stores.append(wire.local(c_all, c_store))
    row_blocks(tokens, 32, mid_rows)
    for copy in stores:
        copy.wait()
    wire.close()
    weights.close()
    outer.close()


def feed_kernel(
    parts,
    planes,
    m,
    mid_gain,
    cots_whole,
    middle_whole,
    gate_weight,
    up_weight,
    down_weight,
    mid_half,
    mid_slope,
    mid_store,
    s_down,
    s_early_a,
    s_early_b,
    s_late_a,
    s_late_b,
    down_give,
    down_keep,
    gate_half,
    up_half,
    down_half,
    cots,
    middle,
    mid,
    mids,
    hidden,
    unit_grads,
    away,
    sums,
    *rest,
):
    here = Place(parts, planes)
    stages = len(here.chip_bits) - 1
    landings, rest = rest[:stages], rest[stages:]
    give, take, current, line_landing, *sems = rest
    wire = Wire(*sems)
    tokens, model = m.shape
    units = gate_half.shape[1]
    own_units = pl.ds(pl.multiple_of(here.core * units, units), units)
    here.enter(here.seat_bits, line=True)

    def spot(index):
        return mids.at[index, here.core]

    lines = gather_lines(wire, here, m, spot, spot)
    lines.start(1)
    across = wire.send(m, spot(here.plane), {"seq": here.at(1)})
    own = wire.local(m, spot(here.plane))
    loads = [
        wire.local(whole.at[:, own_units], part)
        for whole, part in (
            (gate_weight, gate_half),
            (up_weight, up_half),
            (down_weight, down_half),
        )
    ]
    loads += [wire.local(cots_whole, cots), wire.local(middle_whole, middle)]

    def block(index):
        rows = pl.ds(pl.multiple_of(index * 2 * tokens, 2 * tokens), 2 * tokens)
        mid_rows = mids[index].reshape(2 * tokens, model)
        cot_rows = cots[rows, :]

        def part(number, carry):
            at = pl.ds(pl.multiple_of(number * 256, 256), 256)
            gate = jnp.dot(mid_rows, gate_half[:, at], preferred_element_type=jnp.float32)
            lifted = jnp.dot(mid_rows, up_half[:, at], preferred_element_type=jnp.float32)
            hidden_grad = jnp.dot(cot_rows, down_half[:, at], preferred_element_type=jnp.float32)
            sigma = 1.0 / (1.0 + jnp.exp(-gate))
            active = gate * sigma
            hidden[rows, at] = (active * lifted).astype(hidden.dtype)
            unit_grads[1, rows, at] = (hidden_grad * active).astype(hidden.dtype)
            unit_grads[0, rows, at] = (
                hidden_grad * lifted * sigma * (1.0 + gate * (1.0 - sigma))
            ).astype(hidden.dtype)
            return carry

        lax.fori_loop(0, units // 256, part, 0)

    for load in loads:
        load.wait()
    own.wait()
    across.wait_recv()
    plane = here.plane

    above, below = plane, planes - 1 - plane
    shared_steps = jnp.where(above < below, above, below)

    def arrivals(step, carry):
        for number in range(1, planes):

            @pl.when(step == number)
            def _(number=number):
                lines.pass_on(number)

        entry = step - 1
        paired = entry < 2 * shared_steps
        stage_of = jnp.where(paired, entry // 2 + 1, entry - shared_steps + 1)
        from_up = jnp.where(paired, entry % 2 == 0, above > below)
        for stage in range(1, planes):
            for way, chosen in ((0, from_up), (1, jnp.logical_not(from_up))):

                @pl.when((step > 0) & (stage_of == stage) & chosen)
                def _(stage=stage, way=way):
                    for line in lines.members:
                        line.shared[(stage, way)].wait_recv()

        index = jnp.where(from_up, plane + planes - stage_of, plane + stage_of) % planes
        block(jnp.where(step == 0, plane, index))
        return carry

    lax.fori_loop(0, planes, arrivals, 0)

    flat_mids = mids.reshape(2 * planes * tokens, model)
    quarter = model // 4
    moved = {}

    def gradients(left, right, target, start, count):
        parts_of = quarter // 256

        def part(number, carry):
            k, inside = number // parts_of, number % parts_of * 256
            at = pl.ds(pl.multiple_of(start(k) + inside, 256), 256)
            target(k)[pl.ds(pl.multiple_of(inside, 256), 256), :] = lax.dot_general(
                left[:, at],
                right(k)[...],
                (((0,), (0,)), ((), ())),
                preferred_element_type=jnp.float32,
            ).astype(away.dtype)
            return carry

        lax.fori_loop(0, count * parts_of, part, 0)

    def first_half(color, mine):
        sides = [here.side(bits[0]) if mine else 1 - here.side(bits[0]) for bits in here.colors()]
        if isinstance(color, int):
            side = sides[color]
        else:
            side = sides[0] * (1 - color) + sides[1] * color
        return pl.multiple_of(color * (model // 2) + side * quarter, quarter)

    def send_away(number):
        for color, bits in enumerate(here.colors()):
            moved[(number, color)] = wire.send(
                away.at[number, color], landings[0].at[number, color], {"seq": here.at(bits[0])}
            )

    def mid_term(target, core):
        rows = [pl.ds(pl.multiple_of((2 * p + core) * tokens, tokens), tokens) for p in range(planes)]
        gates = jnp.concatenate([unit_grads[0, at, :] for at in rows], axis=0)
        lifts = jnp.concatenate([unit_grads[1, at, :] for at in rows], axis=0)

        def part(number, carry):
            at = pl.ds(pl.multiple_of(number * 256, 256), 256)
            term = lax.dot_general(
                gates, gate_half[at, :], (((1,), (1,)), ((), ())), preferred_element_type=jnp.float32
            ) + lax.dot_general(
                lifts, up_half[at, :], (((1,), (1,)), ((), ())), preferred_element_type=jnp.float32
            )
            target[:, :, at] = term.reshape(planes, tokens, 256).astype(target.dtype)
            return carry

        lax.fori_loop(0, model // 256, part, 0)

    def down_term(target, core):
        rows = [pl.ds(pl.multiple_of((2 * p + core) * tokens, tokens), tokens) for p in range(planes)]
        hiddens = jnp.concatenate([hidden[at, :] for at in rows], axis=0)

        def part(number, carry):
            at = pl.ds(pl.multiple_of(number * 256, 256), 256)
            term = lax.dot_general(
                hiddens, down_half[at, :], (((1,), (1,)), ((), ())), preferred_element_type=jnp.float32
            )
            target[:, :, at] = term.reshape(planes, tokens, 256).astype(target.dtype)
            return carry

        lax.fori_loop(0, model // 256, part, 0)

    gradients(
        cots,
        lambda k: hidden,
        lambda k: away.at[0, k],
        lambda k: first_half(k, False),
        2,
    )
    send_away(0)
    swaps = TokenSum(wire, here, current, take, line_landing)
    mid_term(give, 1 - here.core)
    swaps.start(give)
    mid_term(current, here.core)
    swaps.join()
    swaps.step(1)
    gradients(
        flat_mids,
        lambda k: unit_grads.at[k // 2],
        lambda k: away.at[1 + k // 2, k % 2],
        lambda k: first_half(k % 2, False),
        4,
    )
    send_away(1)
    send_away(2)
    for step in range(2, planes):
        swaps.step(step)

    early = s_early_a.shape[0]

    def store(number, color):
        done = sums.at[number, color]
        if number == 0:
            return [wire.local(done, s_down.at[color])]
        late = (s_late_a, s_late_b)[color]
        size = done.shape[0]
        if number == 1:
            return [
                wire.local(done.at[pl.ds(0, early)], (s_early_a, s_early_b)[color]),
                wire.local(done.at[pl.ds(early, size - early)], late.at[pl.ds(0, size - early)]),
            ]
        return [wire.local(done, late.at[pl.ds(size - early, size)])]

    wire.sent(swaps.across)
    down_term(give, 1 - here.core)
    down_term(take, here.core)
    handed = [wire.local(give, down_give), wire.local(take, down_keep)]
    rows = quarter
    keeps = {}
    if stages > 1:
        for copy in moved.values():
            wire.sent(copy)
    keep_in = sums if stages == 1 else away
    gradients(
        cots,
        lambda k: hidden,
        lambda k: keep_in.at[0, k],
        lambda k: first_half(k, True),
        2,
    )
    gradients(
        flat_mids,
        lambda k: unit_grads.at[k // 2],
        lambda k: keep_in.at[1 + k // 2, k % 2],
        lambda k: first_half(k % 2, True),
        4,
    )
    for number in range(3):
        for color in (0, 1):
            keeps[(number, color)] = (keep_in.at[number, color], 0)
    swaps.finish(mid)
    f32 = jnp.float32

    def norm_back_rows(index, slope):
        at = pl.ds(pl.multiple_of(index * 32, 32), 32)
        own_cots = (here.plane * 2 + here.core) * tokens + index * 32
        grad, value = mid[at, :], middle[at, :]
        factor = lax.rsqrt(jnp.mean(value * value, axis=-1, keepdims=True) + EPS)
        scaled = grad * mid_gain[...]
        back = factor * (
            scaled
            - value * factor * factor * jnp.mean(scaled * value, axis=-1, keepdims=True)
        )
        result = cots[pl.ds(pl.multiple_of(own_cots, 32), 32), :].astype(f32) + back
        mid[at, :] = result
        mid_half[at, :] = result.astype(mid_half.dtype)
        return slope + jnp.sum(grad * value * factor, axis=0, keepdims=True)

    mid_slope[...] = lax.fori_loop(
        0, tokens // 32, norm_back_rows, jnp.zeros((1, model), f32)
    )
    handed.append(wire.local(mid, mid_store))
    for stage in range(stages):
        last = stage == stages - 1
        for number in range(3):
            for color, bits in enumerate(here.colors()):
                keep, begin = keeps[(number, color)]
                moved[(number, color)].wait_recv()
                mine = keep.at[pl.ds(begin, rows)]
                if last:
                    add_rows(
                        sums.at[number, color], mine, landings[stage].at[number, color]
                    )
                    handed.extend(store(number, color))
                else:
                    add_rows(mine, mine, landings[stage].at[number, color])
                    bit = bits[stage + 1]
                    half = rows // 2
                    gone = pl.multiple_of(begin + (1 - here.side(bit)) * half, half)
                    moved[(number, color)] = wire.send(
                        keep.at[pl.ds(gone, half)],
                        landings[stage + 1].at[number, color],
                        {"seq": here.at(bit)},
                    )
                    keeps[(number, color)] = (
                        keep,
                        pl.multiple_of(begin + here.side(bit) * half, half),
                    )
        rows //= 2
    for copy in handed:
        copy.wait()
    wire.close()
    lines.close(True)
    swaps.close()


class TokenSum:
    def __init__(self, wire, here, current, take, landing):
        self.wire, self.here = wire, here
        self.current, self.take = current, take
        self.cuts = 2
        rows = current.shape[1] // self.cuts
        self.lines = []
        for cut in range(self.cuts):
            at = pl.ds(cut * rows, rows)
            self.lines.append(
                LineScatter(
                    wire,
                    here,
                    lambda index, at=at: current.at[index, at],
                    lambda way, step, at=at: landing.at[way, step, at],
                )
            )

    def start(self, give):
        self.across = self.wire.send(give, self.take, {"seq": self.here.at(1)})

    def join(self):
        self.across.wait_recv()

        def body(index, carry):
            row = self.current.at[index]
            add_rows(row, row, self.take.at[index])
            return carry

        lax.fori_loop(0, self.here.planes, body, 0)

    def step(self, step):
        for line in self.lines:
            line.step(step)

    def finish(self, out):
        rows = out.shape[0] // self.cuts
        for cut, line in enumerate(self.lines):
            line.finish(out.at[pl.ds(cut * rows, rows)])

    def close(self):
        for line in self.lines:
            line.close()


def spread_kernel(
    parts,
    planes,
    h,
    s,
    early_a,
    early_b,
    give,
    keep,
    h_store,
    t,
    came_a,
    came_b,
    block,
    h_all,
    current,
    take,
    line_landing,
    *sems,
):
    here = Place(parts, planes)
    wire = Wire(*sems)
    here.enter(here.seat_bits, line=True)
    tokens = h.shape[0]
    half = tokens // 2
    rows = PlaneGather(
        wire,
        here,
        lambda color: h.at[pl.ds(color * half, half)],
        lambda seat, color: h_all.at[pl.ds(pl.multiple_of(seat * tokens + color * half, half), half)],
    )
    swaps = TokenSum(wire, here, current, take, line_landing)
    swaps.start(give)
    kept = wire.local(keep, current)
    rows.start()
    own = wire.local(h, h_all.at[pl.ds(pl.multiple_of(here.seat * tokens, tokens), tokens)])
    moved = [
        wire.send(s.at[color], t.at[color], {"seq": here.at(bits[-1])})
        for color, bits in enumerate(here.colors())
    ]
    kept.wait()
    swaps.join()
    swaps.step(1)
    rows.hop(1)
    moved += [
        wire.send(source, target, {"seq": here.at(bits[-1])})
        for source, target, bits in zip((early_a, early_b), (came_a, came_b), here.colors())
    ]
    for step in range(2, planes):
        if step == 3:
            rows.hops(2)
        swaps.step(step)
    if planes <= 3:
        rows.hops(2)
    rows.finish()
    own.wait()
    store = wire.local(h_all, h_store)
    for color in (0, 1):
        moved[color].wait_recv()
        add_rows(t.at[color], t.at[color], s.at[color])
    swaps.finish(block)
    for copy in moved[2:]:
        copy.wait_recv()
    store.wait()
    wire.close()
    swaps.close()


def final_kernel(
    parts,
    planes,
    a,
    w,
    head_part,
    out_part,
    t_down,
    source,
    slope,
    *rest,
):
    sent, came, rest = rest[:4], rest[4:8], rest[8:]
    out, near, far, query_all, pair_all, outer_all, slope_out, *rest = rest
    joined, rest = rest[:4], rest[4:]
    (
        give,
        take,
        current,
        landing,
        head_current,
        head_landing,
        dealt,
        out_landing,
        head_sum,
        out_sum,
        left,
        right,
        slope_sums,
        slope_landing,
        *sems,
    ) = rest
    here = Place(parts, planes)
    wire = Wire(*sems)
    tokens, model = out.shape
    shard = head_sum.shape[0]
    columns = query_all.shape[1] // parts
    rows_out = out_sum.shape[0]
    chips = parts // 2
    chip_masks = [mask * 2 for mask in range(1, chips)]
    here.enter(chip_masks + [1], line=True, plane_masks=here.plane_bits)
    weights = [
        WeightGather(wire, here, (t_down.at[0], t_down.at[1]), near, far, cut, 2)
        for cut in range(2)
    ]
    head_own = wire.local(head_part, head_current)
    deals = []
    for mask in chip_masks:
        chip = here.at(mask) // 2
        deals.append(
            wire.send(
                out_part.at[pl.ds(pl.multiple_of(chip * rows_out, rows_out), rows_out)],
                dealt.at[here.chip],
                {"seq": here.at(mask)},
            )
        )
    deal_own = wire.local(
        out_part.at[pl.ds(pl.multiple_of(here.chip * rows_out, rows_out), rows_out)],
        dealt.at[here.chip],
    )

    def product(seats, columns):
        rows = [a[pl.ds(pl.multiple_of(seat * tokens, tokens), tokens), :] for seat in seats]
        return lax.dot_general(
            jnp.concatenate(rows, axis=0),
            w[columns, :],
            (((1,), (1,)), ((), ())),
            preferred_element_type=jnp.float32,
        )

    heads = LineScatter(
        wire, here, lambda index: head_current.at[index], lambda way, step: head_landing.at[way, step]
    )
    outer = LineScatter(
        wire, here, lambda index: dealt.at[index], lambda way, step: out_landing.at[way, step]
    )
    head_own.wait()
    heads.step(1)
    rows = PlaneScatter(wire, here, product, give, take, current, landing, model)
    rows.start()
    loads = []
    size, early = left.shape[1], sent[0].shape[0]
    for number in range(4):
        color = number % 2
        copies = []
        for pieces, working in ((sent, left), (came, right)):
            first, late = pieces[color], pieces[2 + color]
            if number < 2:
                copies.append(wire.local(first, working.at[number, pl.ds(0, early)]))
                copies.append(
                    wire.local(
                        late.at[pl.ds(0, size - early)],
                        working.at[number, pl.ds(early, size - early)],
                    )
                )
            else:
                copies.append(wire.local(late.at[pl.ds(size - early, size)], working.at[number]))
        loads.append(copies)
    heads.step(2)
    rows.join()
    rows.stage(0)
    weights[0].start()
    weights[0].own()
    deal_own.wait()
    for copy in deals:
        copy.wait_recv()
    outer.step(1)

    stores = []

    def join(number):
        for load in loads[number]:
            load.wait()
        add_rows(left.at[number], left.at[number], right.at[number])
        stores.append(wire.local(left.at[number], joined[number]))

    stages = len(here.chip_bits)
    for step in range(3, planes):
        heads.step(step)
    for stage in range(1, stages):
        rows.settle(stage - 1, out, True)
        rows.stage(stage)
        if stage == 1:
            weights[1].start()
            weights[1].own()
        rows.settle(stage - 1, out, False)
        if stage + 1 < planes:
            outer.step(stage + 1)
        if stage == 1:
            heads.finish(head_sum)
    half, half_out = shard // 2, rows_out // 2

    def seat_columns(seat):
        return pl.ds(pl.multiple_of(seat * columns, columns), columns)

    gathers = [
        PlaneGather(
            wire,
            here,
            lambda color: head_sum.at[pl.ds(color * half, half), pl.ds(0, columns)],
            lambda seat, color: query_all.at[pl.ds(color * half, half), seat_columns(seat)],
        ),
        PlaneGather(
            wire,
            here,
            lambda color: head_sum.at[
                pl.ds(color * half, half), pl.ds(columns, pair_all.shape[2])
            ],
            lambda seat, color: pair_all.at[seat, pl.ds(color * half, half)],
        ),
        PlaneGather(
            wire,
            here,
            lambda color: out_sum.at[pl.ds(color * half_out, half_out)],
            lambda seat, color: outer_all.at[
                pl.ds(
                    pl.multiple_of(
                        ((seat % 2) * chips + seat // 2) * rows_out + color * half_out, half_out
                    ),
                    half_out,
                )
            ],
        ),
    ]
    own = []
    for gather in gathers[:2]:
        gather.start()
    own.append(
        wire.local(head_sum.at[:, pl.ds(0, columns)], query_all.at[:, seat_columns(here.seat)])
    )
    own.append(
        wire.local(
            head_sum.at[:, pl.ds(columns, pair_all.shape[2])], pair_all.at[here.seat]
        )
    )

    rows.settle(stages - 1, out, False)
    slope_sums[0] = slope[...]
    value = source[...].astype(jnp.float32)
    factor = lax.rsqrt(jnp.mean(value * value, axis=-1, keepdims=True) + EPS)
    slope_sums[0, 0:1, :] = jnp.sum(out[...] * value * factor, axis=0, keepdims=True)
    bits = [("seq", bit) for bit in here.seat_bits] + [("fsdp", bit) for bit in here.plane_bits]
    slope_copies = []

    def slope_send(number):
        axis, bit = bits[number]
        index = here.at(bit) if axis == "seq" else flip(here.plane, bit, here.plane_bits)
        slope_copies.append(
            wire.send(slope_sums.at[number], slope_landing.at[number], {axis: index})
        )

    def slope_add(number):
        slope_copies[number].wait_recv()
        target = slope_out if number == len(bits) - 1 else slope_sums.at[number + 1]
        target[...] = slope_sums[number] + slope_landing[number]

    slope_send(0)
    for step in range(stages + 1, planes):
        outer.step(step)
    join(0)
    gathers[0].hop(1)
    gathers[1].hop(1)
    slope_add(0)
    slope_send(1)
    outer.finish(out_sum)
    gathers[2].start()
    weights[0].forward()
    own_start = (here.core * chips + here.chip) * rows_out
    own.append(
        wire.local(out_sum, outer_all.at[pl.ds(pl.multiple_of(own_start, rows_out), rows_out)])
    )
    join(1)
    for number in range(1, len(bits)):
        slope_add(number)
        if number + 1 < len(bits):
            slope_send(number + 1)
        if number < 3:
            join(number + 1)
        if number == 2:
            gathers[0].hops(2)
            gathers[1].hops(2)
        if number == 3:
            gathers[2].hop(1)
    gathers[2].hops(2)
    weights[1].forward()
    for gather in gathers:
        gather.finish()
    for weight in weights:
        weight.finish()
    for copy in own + stores:
        copy.wait()
    wire.close()
    heads.close()
    outer.close()


class WeightGather:
    def __init__(self, wire, here, finals, near, far, cut=0, cuts=1):
        self.wire, self.here, self.near, self.far = wire, here, near, far
        self.size = finals[0].shape[0]
        self.rows = self.size // cuts
        self.shift = cut * self.rows
        model = near.shape[0]
        self.finals = [final.at[pl.ds(self.shift, self.rows)] for final in finals]
        self.starts = []
        for color, order in enumerate(here.colors()):
            start = color * (model // 2)
            rows = model // 2
            for bit in order[:-1]:
                rows //= 2
                start = start + here.side(bit) * rows
            self.starts.append(start)
        self.swaps, self.kept = [], []

    def _rows(self, start):
        return pl.ds(pl.multiple_of(start + self.shift, self.rows), self.rows)

    def _pass(self, start, source, bit, rows):
        copy = self.wire.send(
            source, self.near.at[self._rows(start)], {"seq": self.here.at(bit)}
        )
        start = start + rows - 2 * rows * self.here.side(bit)
        return (start, self.near.at[self._rows(start)], copy)

    def _swap(self, start, source):
        self.swaps.append(
            self.wire.send(source, self.far.at[self._rows(start)], {"seq": self.here.at(1)})
        )

    def start(self):
        self.held = []
        for color, order in enumerate(self.here.colors()):
            source, start = self.finals[color], self.starts[color]
            pieces = [(start, source, None)]
            if order[:-1]:
                pieces.append(self._pass(start, source, order[-2], self.size))
            self.held.append(pieces)

    def own(self):
        for color in (0, 1):
            source, start = self.finals[color], self.starts[color]
            self._swap(start, source)
            self.kept.append(self.wire.local(source, self.near.at[self._rows(start)]))

    def forward(self):
        for color, order in enumerate(self.here.colors()):
            rest = order[:-1]
            pieces = self.held[color]
            rows = self.size
            for position in range(len(rest) - 1, -1, -1):
                for start, source, copy in pieces:
                    if copy is not None:
                        copy.wait_recv()
                        self._swap(start, source)
                pieces = [(start, source, None) for start, source, _ in pieces]
                rows *= 2
                if position > 0:
                    pieces = pieces + [
                        self._pass(start, source, rest[position - 1], rows)
                        for start, source, _ in pieces
                    ]

    def finish(self):
        for copy in self.swaps:
            copy.wait_recv()
        for copy in self.kept:
            copy.wait()


def widen_kernel(near, far, out):
    core = lax.axis_index("seq") % 2
    units = near.shape[1]
    out[:, pl.ds(pl.multiple_of(core * units, units), units)] = near[...].astype(out.dtype)
    out[:, pl.ds(pl.multiple_of((1 - core) * units, units), units)] = far[...].astype(out.dtype)


def widen_pieces_kernel(count, steps, starts, *refs):
    nears, fars, out = refs[:count], refs[count : 2 * count], refs[-1]
    core = lax.axis_index("seq") % 2
    units = nears[0].shape[1]
    index = pl.program_id(0)
    for number in range(count):

        @pl.when(index // steps == number)
        def _(near=nears[number], far=fars[number]):
            own = pl.ds(pl.multiple_of(core * units, units), units)
            other = pl.ds(pl.multiple_of((1 - core) * units, units), units)
            out[:, own] = near[...].astype(out.dtype)
            out[:, other] = far[...].astype(out.dtype)


def results_kernel(
    copies, width, query, pair, outer, slope, grad_query, grad_key, grad_value, grad_output, *gains
):
    f32 = jnp.float32
    grad_query[...] = query[...].astype(f32)
    grad_output[...] = outer[...].astype(f32)
    columns = 2 * width
    for number in range(pair.shape[0] // (2 * copies)):
        low, high = (
            sum(
                pair[(2 * number + side) * copies + copy].astype(f32) for copy in range(copies)
            )
            for side in (0, 1)
        )
        at = pl.ds(number * columns, columns)
        grad_key[:, at] = pick_lanes(low, pltpu.roll(high, width, 1), width)
        grad_value[:, at] = pick_lanes(pltpu.roll(low, width, 1), high, width)
    in_slope, mid_slope, query_slope, key_slope = gains
    in_slope[...] = slope[0:1, :]
    mid_slope[...] = slope[1:2, :]
    query_slope[...] = slope[2:3, 0:width]
    key_slope[...] = slope[3:4, 0:width]


SENDS, LOCALS = 192, 48


def call(kernel, mesh_sizes, number, inputs, in_vmem, outputs, scratch, out_vmem=None):
    vmem = pl.BlockSpec(memory_space=pltpu.VMEM)
    anywhere = pl.BlockSpec(memory_space=pl.ANY)
    out_vmem = out_vmem or [True] * len(outputs)
    semaphores = [
        pltpu.SemaphoreType.DMA((SENDS,)),
        pltpu.SemaphoreType.DMA((SENDS,)),
        pltpu.SemaphoreType.DMA((LOCALS,)),
    ]
    return pl.pallas_call(
        functools.partial(kernel, *mesh_sizes),
        out_shape=[jax.ShapeDtypeStruct(shape, kind) for shape, kind in outputs],
        in_specs=[vmem if inside else anywhere for inside in in_vmem],
        out_specs=[vmem if inside else anywhere for inside in out_vmem],
        scratch_shapes=[pltpu.VMEM(shape, kind) for shape, kind in scratch] + semaphores,
        compiler_params=pltpu.CompilerParams(
            collective_id=number, has_side_effects=True, vmem_limit_bytes=VMEM_BYTES
        ),
    )(*inputs)


def widen(near, far):
    rows, units = near.shape
    step = min(512, rows)
    return pl.pallas_call(
        widen_kernel,
        grid=(rows // step,),
        out_shape=jax.ShapeDtypeStruct((rows, 2 * units), jnp.float32),
        in_specs=[pl.BlockSpec((step, units), lambda index: (index, 0))] * 2,
        out_specs=pl.BlockSpec((step, 2 * units), lambda index: (index, 0)),
        compiler_params=pltpu.CompilerParams(vmem_limit_bytes=VMEM_BYTES),
        cost_estimate=pl.CostEstimate(
            flops=0, transcendentals=0, bytes_accessed=12 * rows * units
        ),
    )(near, far)


def widen_pieces(pieces, fars, whole=None, into=None):
    rows, units = fars[0].shape
    count = len(fars)
    step = min(512, rows)
    steps = rows // step
    starts = jnp.stack([jnp.asarray(start, jnp.int32) >> (step.bit_length() - 1) for start, _ in pieces])

    def block(number):
        return pl.BlockSpec(
            (step, units),
            lambda index, starts: (jnp.clip(index - number * steps, 0, steps - 1), 0),
        )

    more = () if into is None else (into,)
    return pl.pallas_call(
        functools.partial(widen_pieces_kernel, count, steps),
        out_shape=jax.ShapeDtypeStruct((whole or count * rows, 2 * units), jnp.float32),
        grid_spec=pltpu.PrefetchScalarGridSpec(
            num_scalar_prefetch=1,
            grid=(count * steps,),
            in_specs=[block(number) for number in range(count)] * 2
            + [pl.BlockSpec(memory_space=pl.ANY) for _ in more],
            out_specs=pl.BlockSpec(
                (step, 2 * units), lambda index, starts: (starts[index // steps] + index % steps, 0)
            ),
        ),
        input_output_aliases={2 * count + 1: 0} if more else {},
        compiler_params=pltpu.CompilerParams(vmem_limit_bytes=VMEM_BYTES),
        cost_estimate=pl.CostEstimate(
            flops=0, transcendentals=0, bytes_accessed=12 * count * rows * units
        ),
    )(starts, *[value for _, value in pieces], *fars, *more)


def results(copies, width, query, pair, outer, slope):
    shard, model = query.shape
    seats = pair.shape[0]
    step = min(128, shard)
    f32 = jnp.float32
    pair_cols = seats // copies * width
    row = pl.BlockSpec((step, model), lambda index: (index, 0))
    row_pair = pl.BlockSpec((step, pair_cols), lambda index: (index, 0))
    fixed = lambda *shape: pl.BlockSpec(shape, lambda index: (0, 0))
    return pl.pallas_call(
        functools.partial(results_kernel, copies, width),
        grid=(shard // step,),
        out_shape=[
            jax.ShapeDtypeStruct((shard, model), f32),
            jax.ShapeDtypeStruct((shard, pair_cols), f32),
            jax.ShapeDtypeStruct((shard, pair_cols), f32),
            jax.ShapeDtypeStruct((shard, model), f32),
            jax.ShapeDtypeStruct((1, model), f32),
            jax.ShapeDtypeStruct((1, model), f32),
            jax.ShapeDtypeStruct((1, width), f32),
            jax.ShapeDtypeStruct((1, width), f32),
        ],
        in_specs=[
            row,
            pl.BlockSpec((seats, step, 2 * width), lambda index: (0, index, 0)),
            row,
            fixed(8, model),
        ],
        out_specs=[row, row_pair, row_pair, row]
        + [fixed(1, model), fixed(1, model), fixed(1, width), fixed(1, width)],
        cost_estimate=pl.CostEstimate(
            flops=0, transcendentals=0, bytes_accessed=16 * shard * model
        ),
    )(query, pair, outer, slope)


VMEM_BYTES = 67_000_000


def per_device(
    inputs,
    cotangent,
    attention_gain,
    query_weight,
    key_weight,
    value_weight,
    output_weight,
    query_gain,
    key_gain,
    feedforward_gain,
    gate_weight,
    up_weight,
    down_weight,
):
    tokens = inputs.shape[1]
    model = inputs.shape[2]
    width = query_gain.shape[0]
    pair_heads = key_weight.shape[1] // width
    parts = lax.axis_size("seq")
    planes = lax.axis_size("fsdp")
    sizes = (parts, planes)
    chips = parts // 2
    copies = max(1, parts // pair_heads)
    place = lax.axis_index("seq")
    plane = lax.axis_index("fsdp")
    core = place % 2
    query_cols = model // parts
    head_cols = query_cols + 2 * width
    local_groups = query_cols // width
    shard = query_weight.shape[0]
    piece_rows = shard // parts
    length = parts * tokens
    units = gate_weight.shape[1] // 2
    f32, bf16 = jnp.float32, jnp.bfloat16
    halvings = chips.bit_length() - 2
    last_rows = model // 2 >> halvings
    rows_in = inputs.reshape(tokens, model)
    cot_rows = cotangent.reshape(tokens, model)

    exponents = jnp.arange(width // 2).astype(f32) * 2.0 / width
    rates = jnp.power(jnp.float32(THETA), -exponents)
    rates = jnp.concatenate([rates] * 4)[None, :]
    gain_row = jnp.concatenate([query_gain] * local_groups + [key_gain] * 2)[None, :]
    half = model // 2
    scatter_scratch = [
        ((chips, tokens, model), bf16),
        ((chips, tokens, model), bf16),
        ((2, chips, tokens, half), bf16),
        ((halvings + 1, 2, chips, tokens, half), bf16),
    ]
    mid_gain = feedforward_gain[None, :]
    kept = [
        ((length, model), bf16),
        ((model, head_cols), bf16),
        ((query_cols, model), bf16),
        ((length, head_cols), f32),
        ((length, query_cols), bf16),
        ((length, 2 * width), bf16),
        ((length, query_cols), bf16),
        ((length, 128), f32),
        ((length, 2 * width), f32),
        ((length, 2 * width), f32),
        ((head_cols, head_cols), bf16),
        ((planes, 2, tokens, model), bf16),
    ]
    (
        normed_all,
        head_full,
        out_slice,
        proj,
        queries,
        pair_rows,
        out_rows,
        log_rows,
        cosine,
        sine,
        group,
        middle,
        normed_mid,
        cot_all,
    ) = call(
        functools.partial(front_kernel, width, copies),
        sizes,
        0,
        (
            rows_in,
            cot_rows,
            query_weight,
            key_weight,
            value_weight,
            output_weight,
            attention_gain[None, :],
            mid_gain,
            gain_row,
            rates,
        ),
        (True, True, False, False, False, False, True, True, True, True),
        kept[:11] + [((tokens, model), f32), ((tokens, model), bf16)] + kept[11:],
        kept
        + [((planes, piece_rows, model), bf16)]
        + [((length, 2 * width), bf16)] * 3
        + [((shard, 2 * width), bf16)] * 2
        + scatter_scratch,
        [False] * 11 + [True] * 2 + [False],
    )
    tables = (gain_row, cosine, sine, group)

    quarter = model // 4
    rows_shape = (planes, tokens, model)
    line_scratch = [
        (rows_shape, bf16),
        (rows_shape, bf16),
        ((2, planes - 1, tokens, model), bf16),
    ]
    acts = (2 * planes * tokens, units)
    early = last_rows // 2
    early_piece, late_piece = ((early, units), bf16), ((2 * last_rows - early, units), bf16)
    (
        middle_half,
        mid_slope,
        middle_grad,
        s_down,
        early_a,
        early_b,
        late_a,
        late_b,
        down_give,
        down_keep,
    ) = call(
        feed_kernel,
        sizes,
        2,
        (
            normed_mid,
            mid_gain,
            cot_all.reshape(-1, model),
            middle,
            gate_weight,
            up_weight,
            down_weight,
        ),
        (True, True, False, False, False, False, False),
        [
            ((tokens, model), bf16),
            ((1, model), f32),
            ((tokens, model), f32),
            ((2, last_rows, units), bf16),
            early_piece,
            early_piece,
            late_piece,
            late_piece,
            (rows_shape, bf16),
            (rows_shape, bf16),
        ],
        [((model, units), bf16)] * 3
        + [
            ((2 * planes * tokens, model), bf16),
            ((tokens, model), f32),
            ((tokens, model), f32),
            ((planes, 2, tokens, model), bf16),
            (acts, bf16),
            ((2,) + acts, bf16),
            ((3, 2, quarter, units), bf16),
            ((3, 2, last_rows, units), bf16),
        ]
        + [((3, 2, quarter >> stage, units), bf16) for stage in range(halvings)]
        + [(rows_shape, bf16)]
        + line_scratch,
        [True] * 2 + [False] * 8,
    )

    middle_all, t_down, came_a, came_b, down_sum = call(
        spread_kernel,
        sizes,
        4,
        (middle_half, s_down, early_a, early_b, down_give, down_keep),
        (True, True, False, False, False, False),
        [
            ((length, model), bf16),
            ((2, last_rows, units), bf16),
            early_piece,
            early_piece,
            ((tokens, model), f32),
        ],
        [((length, model), bf16)] + line_scratch,
        [False, True, False, False, True],
    )

    def swap(value, bit):
        return lax.ppermute(value, "seq", [(i, i ^ bit) for i in range(parts)])

    late_a, late_b, middle_all = lax.optimization_barrier((late_a, late_b, middle_all))
    bit_orders = ([2 << i for i in range(halvings + 1)], [chips >> i for i in range(halvings + 1)])
    sent = [early_a, early_b, late_a, late_b]
    came = [came_a, came_b, swap(late_a, bit_orders[0][-1]), swap(late_b, bit_orders[1][-1])]

    vmem = pl.BlockSpec(memory_space=pltpu.VMEM)
    halves, head_part, out_part, head_slopes = pl.pallas_call(
        functools.partial(back_kernel, width),
        out_shape=[
            jax.ShapeDtypeStruct((length, head_cols), bf16),
            jax.ShapeDtypeStruct((model, head_cols), bf16),
            jax.ShapeDtypeStruct((query_cols, model), bf16),
            jax.ShapeDtypeStruct((8, head_cols), f32),
        ],
        in_specs=[vmem] * 12,
        out_specs=[vmem] * 4,
        scratch_shapes=[
            pltpu.VMEM((length, query_cols), bf16),
            pltpu.VMEM((length, query_cols), f32),
            pltpu.VMEM((length, 2 * width), f32),
            pltpu.VMEM((length, 2 * width), f32),
        ]
        + [pltpu.VMEM((3, length, 2 * width), bf16), pltpu.VMEM((length, 2 * width), bf16)],
        compiler_params=pltpu.CompilerParams(vmem_limit_bytes=VMEM_BYTES),
        cost_estimate=pl.CostEstimate(
            flops=10 * length * model * head_cols,
            transcendentals=length * length * local_groups,
            bytes_accessed=16 * length * model,
        ),
    )(
        normed_all,
        middle_all,
        out_slice,
        out_rows,
        log_rows,
        queries,
        pair_rows,
        proj,
        *tables,
    )
    head_part = head_part.reshape(planes, shard, head_cols)
    query_slope = head_slopes[:1, :query_cols].reshape(local_groups, width).sum(axis=0)
    key_slope = head_slopes[0, query_cols : query_cols + width]
    gains = jnp.pad(jnp.stack([query_slope, key_slope]), ((0, 0), (0, model - width)))
    slopes = jnp.concatenate(
        [jnp.zeros_like(mid_slope), mid_slope, gains, jnp.zeros((4, model), f32)], axis=0
    )
    rounds = (parts * planes).bit_length() - 1
    side = ((model, units), bf16)
    piece = ((last_rows, units), bf16)
    in_grad, near_down, far_down, query_all, pair_all, outer_all, slopes, *pieces = call(
        final_kernel,
        sizes,
        5,
        (halves, head_full, head_part, out_part, t_down, rows_in, slopes, *sent, *came),
        (True, True, False, False, True, True, True) + (False,) * 8,
        [
            ((tokens, model), f32),
            side,
            side,
            ((shard, model), bf16),
            ((parts, shard, 2 * width), bf16),
            ((shard, model), bf16),
            ((8, model), f32),
        ]
        + [piece] * 4,
        scatter_scratch
        + [
            ((planes, shard, head_cols), bf16),
            ((2, planes - 1, shard, head_cols), bf16),
            ((planes, piece_rows, model), bf16),
            ((2, planes - 1, piece_rows, model), bf16),
            ((shard, head_cols), bf16),
            ((piece_rows, model), bf16),
            ((4, last_rows, units), bf16),
            ((4, last_rows, units), bf16),
            ((rounds, 8, model), f32),
            ((rounds, 8, model), f32),
        ],
        [True, False, False] + [True] * 4 + [False] * 4,
    )
    pieces, near_down, far_down, in_grad = lax.optimization_barrier(
        (pieces, near_down, far_down, in_grad)
    )
    source = rows_in.astype(f32)
    first = rms_factor(source)
    input_rows = (middle_grad + norm_back(in_grad, source, first, attention_gain)).astype(bf16)

    def plane_pieces(values):
        whole = []
        for color, order in enumerate(bit_orders):
            start, rows = color * (model // 2), model // 2
            for bit in order[:-1]:
                rows //= 2
                start = start + (place // bit) % 2 * rows
            held = [(start, values[color])]
            rows = last_rows
            for bit in order[-2::-1]:
                held = held + [
                    (start + rows - 2 * rows * ((place // bit) % 2), swap(value, bit))
                    for start, value in held
                ]
                rows *= 2
            whole = whole + held
        return whole

    gate_pieces = plane_pieces(pieces[:2])
    grad_down = widen(near_down, far_down)
    (
        grad_query,
        grad_key,
        grad_value,
        grad_output,
        attention_slope,
        feedforward_slope,
        query_slope,
        key_slope,
    ) = results(copies, width, query_all, pair_all, outer_all, slopes)
    block_out = (middle + down_sum).astype(bf16).reshape(1, tokens, model)
    pieces[2:], grad_down = lax.optimization_barrier((pieces[2:], grad_down))
    up_pieces = plane_pieces(pieces[2:])
    written = (grad_down, grad_query, grad_key, grad_value, grad_output, input_rows, block_out)
    gate_pieces, written = lax.optimization_barrier((gate_pieces, written))
    grad_down, grad_query, grad_key, grad_value, grad_output, input_rows, block_out = written
    grad_gate = widen_pieces(gate_pieces, [swap(value, 1) for _, value in gate_pieces])
    own = [up_pieces[0], up_pieces[len(up_pieces) // 2]]
    others = [piece for piece in up_pieces if all(piece is not mine for mine in own)]
    grad_up = widen_pieces(own, [swap(value, 1) for _, value in own], model)
    others, grad_gate, grad_up = lax.optimization_barrier((others, grad_gate, grad_up))
    grad_up = widen_pieces(others, [swap(value, 1) for _, value in others], model, grad_up)
    attention_slope, feedforward_slope = attention_slope[0], feedforward_slope[0]
    query_slope, key_slope = query_slope[0], key_slope[0]
    input_grad = input_rows.reshape(1, tokens, model)
    return (
        block_out,
        input_grad,
        attention_slope,
        grad_query,
        grad_key,
        grad_value,
        grad_output,
        query_slope,
        key_slope,
        feedforward_slope,
        grad_gate,
        grad_up,
        grad_down,
    )


def solution(mesh):
    in_specs = (
        P("fsdp", "seq", None),
        P("fsdp", "seq", None),
        P(),
        P("fsdp", None),
        P("fsdp", None),
        P("fsdp", None),
        P("fsdp", None),
        P(),
        P(),
        P(),
        P(None, "fsdp"),
        P(None, "fsdp"),
        P(None, "fsdp"),
    )
    out_specs = (
        P("fsdp", "seq", None),
        P("fsdp", "seq", None),
        P(),
        P("fsdp", None),
        P("fsdp", None),
        P("fsdp", None),
        P("fsdp", None),
        P(),
        P(),
        P(),
        P(None, "fsdp"),
        P(None, "fsdp"),
        P(None, "fsdp"),
    )
    return jax.shard_map(
        per_device, mesh=mesh, in_specs=in_specs, out_specs=out_specs, check_vma=False
    )
```
